16 devices in a mesh: rep: 4 (over y, z, core), dp: 4 (over x).
Axes of the slice: x: 4, y: 2, z: 1, core: 2. Of those that a mesh axis runs over, the one named last changes fastest.
The devices are a block of a 4x4x8 slice.
Arguments:
- x: bfloat16 [16, 2048, 512], P(('rep', 'dp')), parts along dimension 0
- dy: bfloat16 [16, 2048, 512], P(('rep', 'dp')), parts along dimension 0
- wq: bfloat16 [2, 512, 512], replicated
- wk: bfloat16 [2, 512, 512], replicated
- wv: bfloat16 [2, 512, 512], replicated
- wo: bfloat16 [2, 512, 512], replicated
- w_gate: bfloat16 [2, 512, 2048], replicated
- w_up: bfloat16 [2, 512, 2048], replicated
- w_down: bfloat16 [2, 2048, 512], replicated
- m_wq: float32 [2, 512, 512], P(None, 'dp')
- m_wk: float32 [2, 512, 512], P(None, 'dp')
- m_wv: float32 [2, 512, 512], P(None, 'dp')
- m_wo: float32 [2, 512, 512], P(None, 'dp')
- m_w_gate: float32 [2, 512, 2048], P(None, 'dp')
- m_w_up: float32 [2, 512, 2048], P(None, 'dp')
- m_w_down: float32 [2, 2048, 512], P(None, 'dp')
- v_wq: float32 [2, 512, 512], P(None, 'dp')
- v_wk: float32 [2, 512, 512], P(None, 'dp')
- v_wv: float32 [2, 512, 512], P(None, 'dp')
- v_wo: float32 [2, 512, 512], P(None, 'dp')
- v_w_gate: float32 [2, 512, 2048], P(None, 'dp')
- v_w_up: float32 [2, 512, 2048], P(None, 'dp')
- v_w_down: float32 [2, 2048, 512], P(None, 'dp')
Outputs:
- output 1: bfloat16 [8, 512, 512], P('rep'), parts along dimension 0
- output 2: bfloat16 [8, 512, 512], P('rep'), parts along dimension 0
- output 3: bfloat16 [8, 512, 512], P('rep'), parts along dimension 0
- output 4: bfloat16 [8, 512, 512], P('rep'), parts along dimension 0
- output 5: bfloat16 [8, 512, 2048], P('rep'), parts along dimension 0
- output 6: bfloat16 [8, 512, 2048], P('rep'), parts along dimension 0
- output 7: bfloat16 [8, 2048, 512], P('rep'), parts along dimension 0
- output 8: float32 [8, 512, 512], P('rep', 'dp'), parts along dimension 0
- output 9: float32 [8, 512, 512], P('rep', 'dp'), parts along dimension 0
- output 10: float32 [8, 512, 512], P('rep', 'dp'), parts along dimension 0
- output 11: float32 [8, 512, 512], P('rep', 'dp'), parts along dimension 0
- output 12: float32 [8, 512, 2048], P('rep', 'dp'), parts along dimension 0
- output 13: float32 [8, 512, 2048], P('rep', 'dp'), parts along dimension 0
- output 14: float32 [8, 2048, 512], P('rep', 'dp'), parts along dimension 0
- output 15: float32 [8, 512, 512], P('rep', 'dp'), parts along dimension 0
- output 16: float32 [8, 512, 512], P('rep', 'dp'), parts along dimension 0
- output 17: float32 [8, 512, 512], P('rep', 'dp'), parts along dimension 0
- output 18: float32 [8, 512, 512], P('rep', 'dp'), parts along dimension 0
- output 19: float32 [8, 512, 2048], P('rep', 'dp'), parts along dimension 0
- output 20: float32 [8, 512, 2048], P('rep', 'dp'), parts along dimension 0
- output 21: float32 [8, 2048, 512], P('rep', 'dp'), parts along dimension 0
There are 4 independent parts. The reference program is written for one: setup_inputs(seed, part) draws one part's arguments, and reference() takes and returns one part's arrays. A program takes and returns all parts, laid end to end along the dimension named above; an argument that names none is the same for every part.
All inputs are finite; a program needn't handle non-finite values.
Results may differ from the reference program's by a relative error of at most 0.024.
Values are sent between devices in bfloat16 or wider.
A program may use at most 768 MiB of HBM per device.

```python
import jax
import jax.numpy as jnp
from jax import lax

SEQUENCES = 4
TOKENS = 2048
D = 512
HEADS = 4
KV_HEADS = 4
HEAD = 128
FF = 2048
LAYERS = 2
THETA = 10000
NAMES = ("wq", "wk", "wv", "wo", "w_gate", "w_up", "w_down")
SHAPES = {
    "wq": (LAYERS, D, HEADS * HEAD),
    "wk": (LAYERS, D, KV_HEADS * HEAD),
    "wv": (LAYERS, D, KV_HEADS * HEAD),
    "wo": (LAYERS, HEADS * HEAD, D),
    "w_gate": (LAYERS, D, FF),
    "w_up": (LAYERS, D, FF),
    "w_down": (LAYERS, FF, D),
}


def bump(key, n, height):
    away = (jnp.arange(n, dtype=jnp.int32) - jax.random.randint(key, (), 0, n, jnp.int32)) % n
    return jnp.where(away < n // 8, height, 1.0)


def together(key, own, strength):
    shared = jax.random.normal(key, own.shape[1:], jnp.float32)
    return (own + strength * shared) * lax.rsqrt(1 + strength * strength)


def setup_inputs(seed: int = 0, part: int = 0) -> dict:
    kx, kdy, ka, kb, kz, kf, kh, kl, *keys = jax.random.split(jax.random.key(seed), 8 + 3 * len(NAMES))
    kx, kdy, ka, kb = (jax.random.fold_in(k, part) for k in (kx, kdy, ka, kb))
    kw, km, kv = (keys[i::3] for i in range(3))
    shape = (SEQUENCES, TOKENS, D)
    much_x, much_dy = jax.random.uniform(kz, (2,), jnp.float32, 0.0, 1.0)
    loud = 2.0 ** jax.random.uniform(jax.random.fold_in(kz, 1), (), jnp.float32, -1.0, 2.0)
    layers = 2.0 ** jax.random.uniform(kl, (LAYERS, 1, 1), jnp.float32, -1.0, 1.0)
    times = {"wq": 1.0, "wk": 1.0, "wv": 2.0, "wo": layers, "w_gate": 1.0, "w_up": bump(kh, FF, 4.0), "w_down": layers}
    x = together(ka, jax.random.normal(kx, shape, jnp.float32), much_x) * bump(kf, D, 4.0)
    dy = together(kb, jax.random.normal(kdy, shape, jnp.float32), much_dy)
    drawn = {"x": x.astype(jnp.bfloat16), "dy": (loud * dy * (SEQUENCES * TOKENS) ** -0.5).astype(jnp.bfloat16)}
    for key, name in zip(kw, NAMES, strict=True):
        drawn[name] = (jax.random.normal(key, SHAPES[name], jnp.float32) * SHAPES[name][1] ** -0.5 * times[name]).astype(jnp.bfloat16)
    for key, name in zip(km, NAMES, strict=True):
        drawn[f"m_{name}"] = 0.1 * jax.random.normal(key, SHAPES[name], jnp.float32)
    for key, name in zip(kv, NAMES, strict=True):
        drawn[f"v_{name}"] = jax.random.uniform(key, SHAPES[name], jnp.float32, 0.02, 0.06)
    return drawn


def matmul(a, w):
    return jnp.dot(a, w, preferred_element_type=jnp.float32).astype(jnp.bfloat16)


def normed(h):
    wide = h.astype(jnp.float32)
    scale = lax.rsqrt(jnp.mean(wide**2, -1, keepdims=True) + 1e-6)
    return (wide * scale).astype(jnp.bfloat16)


def turned(t, theta):
    half = t.shape[-1] // 2
    angle = jnp.arange(t.shape[0], dtype=jnp.float32)[:, None] * theta ** (-jnp.arange(half, dtype=jnp.float32) / half)
    cos, sin = jnp.cos(angle)[:, None], jnp.sin(angle)[:, None]
    a, b = t[..., :half].astype(jnp.float32), t[..., half:].astype(jnp.float32)
    return jnp.concatenate([a * cos - b * sin, b * cos + a * sin], -1).astype(jnp.bfloat16)


def seen_by(q, k, v):
    tokens, kv = q.shape[0], k.shape[1]
    q = q.reshape(tokens, kv, -1, q.shape[-1])
    scores = jnp.einsum("tgsd,ugd->gstu", q.astype(jnp.float32), k.astype(jnp.float32)) * q.shape[-1] ** -0.5
    place = jnp.arange(tokens)
    weights = jax.nn.softmax(jnp.where(place[:, None] >= place, scores, -jnp.inf), -1).astype(jnp.bfloat16)
    return jnp.einsum("gstu,ugd->tgsd", weights.astype(jnp.float32), v.astype(jnp.float32)).astype(jnp.bfloat16).reshape(tokens, -1)


def layer(h, w):
    a = normed(h)
    q, k = (turned(matmul(a, w[name]).reshape(h.shape[0], -1, HEAD), THETA) for name in ("wq", "wk"))
    h = h + matmul(seen_by(q, k, matmul(a, w["wv"]).reshape(h.shape[0], -1, HEAD)), w["wo"])
    b = normed(h)
    gate = jnp.dot(b, w["w_gate"], preferred_element_type=jnp.float32)
    up = jnp.dot(b, w["w_up"], preferred_element_type=jnp.float32)
    return h + matmul((jax.nn.silu(gate) * up).astype(jnp.bfloat16), w["w_down"])


def adamw(w, m, v, g):
    m = 0.9 * m + 0.1 * g
    v = 0.95 * v + 0.05 * g * g
    step = m * lax.rsqrt(v + 1e-8) + 0.1 * w
    return (w - 0.02 * step).astype(jnp.bfloat16), m, v


def clipped(gradients, sum_of_squares, count):
    factor = jnp.minimum(1.0, 0.5 * lax.rsqrt(sum_of_squares / count + 1e-30))
    return [g * factor for g in gradients]


def stack(weights, h):
    return lax.scan(lambda h, w: (layer(h, w), None), h, weights)[0]


def reference(x, dy, wq, wk, wv, wo, w_gate, w_up, w_down, m_wq, m_wk, m_wv, m_wo, m_w_gate, m_w_up, m_w_down, v_wq, v_wk, v_wv, v_wo, v_w_gate, v_w_up, v_w_down):
    weights = dict(zip(NAMES, (wq, wk, wv, wo, w_gate, w_up, w_down), strict=True))

    def take(so_far, sequence):
        h, by_y = sequence
        _, back = jax.vjp(stack, weights, h)
        by_weights, by_h = back(by_y)
        return jax.tree.map(lambda total, term: total + term.astype(jnp.float32), so_far, by_weights), by_h

    none_yet = {name: jnp.zeros(w.shape, jnp.float32) for name, w in weights.items()}
    by_weights, by_x = lax.scan(take, none_yet, (x, dy))
    gradients = [by_weights[name].astype(jnp.bfloat16).astype(jnp.float32) for name in NAMES]
    gradients = clipped(gradients, sum(jnp.sum(g * g) for g in gradients), sum(g.size for g in gradients))
    first = (m_wq, m_wk, m_wv, m_wo, m_w_gate, m_w_up, m_w_down)
    second = (v_wq, v_wk, v_wv, v_wo, v_w_gate, v_w_up, v_w_down)
    new = [adamw(weights[name].astype(jnp.float32), m, v, g) for name, m, v, g in zip(NAMES, first, second, gradients, strict=True)]
    return tuple(one[which] for which in range(3) for one in new)
```

```python
import functools

import jax
import jax.numpy as jnp
import numpy as np
from jax import lax
from jax.experimental import pallas as pl
from jax.experimental.pallas import tpu as pltpu
from jax.sharding import PartitionSpec as P

F32, BF16 = jnp.float32, jnp.bfloat16
HEAD = 128
THETA = 10000
NEG = -1e30
HIDDEN = 2 * NEG
LOG2E = 1.4426950408889634
SCALE = HEAD**-0.5
VMEM = 60 * 2**20


def _dot(a, b, ca=1, cb=0):
    return lax.dot_general(a, b, (((ca,), (cb,)), ((), ())), preferred_element_type=F32)


def _tile(size, most=512):
    return max(n for n in range(128, most + 1, 128) if size % n == 0)


def _call(kernel, grid, ins, outs, scratch, args, flops, moved, vmem=VMEM, **more):
    return pl.pallas_call(
        kernel,
        grid=grid,
        in_specs=[spec for spec in ins],
        out_specs=[spec for spec, _ in outs],
        out_shape=[shape for _, shape in outs],
        scratch_shapes=scratch,
        compiler_params=pltpu.CompilerParams(dimension_semantics=("arbitrary",) * len(grid), vmem_limit_bytes=vmem),
        cost_estimate=pl.CostEstimate(flops=int(flops), transcendentals=0, bytes_accessed=int(moved)),
        **more,
    )(*args)


def _norm_scale(x):
    return lax.rsqrt(jnp.mean(x * x, -1, keepdims=True) + 1e-6)


def _norm_back(x, d_out):
    s = _norm_scale(x)
    inner = jnp.mean(x * d_out, -1, keepdims=True)
    return s * d_out - x * (s * s * s * inner)


def _turn(x, cos, sin):
    parts = [x[:, n : n + HEAD] for n in range(0, x.shape[1], HEAD)]
    return jnp.concatenate([p * cos + pltpu.roll(p, HEAD // 2, 1) * sin for p in parts], 1)


def _qkv(h, wq, wk, wv, cos, sin, q_ref, k_ref, v_ref):
    a = (h * _norm_scale(h)).astype(BF16)
    q_ref[...] = _turn(_dot(a, wq).astype(BF16).astype(F32), cos, sin).astype(BF16)
    k_ref[...] = _turn(_dot(a, wk).astype(BF16).astype(F32), cos, sin).astype(BF16)
    v_ref[...] = _dot(a, wv).astype(BF16)


def _first(h_ref, wq, wk, wv, cos, sin, q_ref, k_ref, v_ref):
    _qkv(h_ref[...].astype(F32), wq[0], wk[0], wv[0], cos[...], sin[...], q_ref, k_ref, v_ref)


def _after_attention(h_ref, att_ref, wo):
    return (h_ref[...].astype(F32) + _dot(att_ref[...], wo).astype(BF16).astype(F32)).astype(BF16)


def _between(h_ref, att_ref, wo, wg, wu, wd, wq, wk, wv, cos, sin, h1_ref, y_ref, gate_ref, up_ref, q_ref, k_ref, v_ref):
    h1 = _after_attention(h_ref, att_ref, wo[0])
    h1_ref[...] = h1
    h1 = h1.astype(F32)
    b = (h1 * _norm_scale(h1)).astype(BF16)
    ff = wg.shape[2]
    part = _tile(ff)
    total = jnp.zeros(h1.shape, F32)
    for at in range(0, ff, part):
        gate, up = _dot(b, wg[0, :, at : at + part]), _dot(b, wu[0, :, at : at + part])
        gate_ref[:, at : at + part] = gate
        up_ref[:, at : at + part] = up
        total += _dot((gate * jax.nn.sigmoid(gate) * up).astype(BF16), wd[0, at : at + part, :])
    y = (h1 + total.astype(BF16).astype(F32)).astype(BF16)
    y_ref[...] = y
    _qkv(y.astype(F32), wq[0], wk[0], wv[0], cos[...], sin[...], q_ref, k_ref, v_ref)


def _attend(q_ref, k_ref, v_ref, o_ref, lse_ref, top_s, mix_s, *, bk):
    iq = pl.program_id(0)
    bq = q_ref.shape[0]
    heads = q_ref.shape[1] // HEAD
    e = SCALE * LOG2E
    ones = jnp.ones((8, bk), BF16)
    top_s[...] = jnp.full(top_s.shape, NEG, F32)
    mix_s[...] = jnp.zeros(mix_s.shape, F32)

    def block(j, first_query):
        here = pl.ds(pl.multiple_of(j * bk, bk), bk)
        cols = [slice(n * HEAD, (n + 1) * HEAD) for n in range(heads)]
        scores = [_dot(k_ref[here, c], q_ref[:, c], 1, 1) for c in cols]
        weights, keeps = [], []
        if first_query is not None:
            seen = lax.broadcasted_iota(jnp.int32, (bk, bq), 1) + first_query >= lax.broadcasted_iota(jnp.int32, (bk, bq), 0)
        for n, s in enumerate(scores):
            if first_query is not None:
                s = jnp.where(seen, s, HIDDEN)
            old = top_s[n : n + 1, :]
            top = jnp.maximum(old, s.max(axis=0, keepdims=True))
            top_s[n : n + 1, :] = top
            weights.append(jnp.exp2((s - top) * e).astype(BF16))
            keeps.append(jnp.exp2((old - top) * e))
        for n, (c, p, keep) in enumerate(zip(cols, weights, keeps)):
            values = jnp.concatenate([v_ref[here, c].T, ones], axis=0)
            mix_s[n] = mix_s[n] * keep + _dot(values, p, 1, 0)

    lax.fori_loop(0, iq * (bq // bk), lambda j, _: block(j, None), None)
    for i in range(bq // bk):
        block(iq * (bq // bk) + i, -i * bk)
    for n in range(heads):
        total = mix_s[n, HEAD : HEAD + 1, :]
        o_ref[:, n * HEAD : (n + 1) * HEAD] = (mix_s[n, :HEAD, :] * (1 / total)).T.astype(BF16)
        lse_ref[n : n + 1, :] = top_s[n : n + 1, :] * e + jnp.log2(total)


def attend(q, k, v):
    t, width = q.shape
    heads = width // HEAD
    bq = bk = _tile(t)
    rows, whole = pl.BlockSpec((bq, width), lambda i: (i, 0)), pl.BlockSpec((t, width), lambda i: (0, 0))
    return _call(
        functools.partial(_attend, bk=bk),
        (t // bq,),
        [rows, whole, whole],
        [(rows, jax.ShapeDtypeStruct((t, width), BF16)), (pl.BlockSpec((heads, bq), lambda i: (0, i)), jax.ShapeDtypeStruct((heads, t), F32))],
        [pltpu.VMEM((heads, bq), F32), pltpu.VMEM((heads, HEAD + 8, bq), F32)],
        (q, k, v),
        2 * t * t * width,
        8 * t * width,
    )


def _attend_back(q_ref, k_ref, v_ref, do_ref, lse_ref, delta_ref, dq_ref, dk_ref, dv_ref, dq_s, dk_s, dv_s, *, bk):
    iq = pl.program_id(0)
    bq = q_ref.shape[0]
    heads = q_ref.shape[1] // HEAD
    e = SCALE * LOG2E

    @pl.when(iq == 0)
    def _():
        dk_s[...] = jnp.zeros_like(dk_s)
        dv_s[...] = jnp.zeros_like(dv_s)

    dq_s[...] = jnp.zeros_like(dq_s)

    def block(j, first_query):
        here = pl.ds(pl.multiple_of(j * bk, bk), bk)
        cols = [slice(n * HEAD, (n + 1) * HEAD) for n in range(heads)]
        scores = [_dot(k_ref[here, c], q_ref[:, c], 1, 1) for c in cols]
        dps = [_dot(v_ref[here, c], do_ref[:, c], 1, 1) for c in cols]
        if first_query is not None:
            seen = lax.broadcasted_iota(jnp.int32, (bk, bq), 1) + first_query >= lax.broadcasted_iota(jnp.int32, (bk, bq), 0)
        for n, c in enumerate(cols):
            p = jnp.exp2(scores[n] * e - lse_ref[n : n + 1, :])
            if first_query is not None:
                p = jnp.where(seen, p, 0.0)
            ds = (p * (dps[n] - delta_ref[n : n + 1, :])).astype(BF16)
            dv_s[here, c] += _dot(p.astype(BF16), do_ref[:, c], 1, 0)
            dk_s[here, c] += _dot(ds, q_ref[:, c], 1, 0)
            dq_s[n] += _dot(k_ref[here, c].T, ds, 1, 0)

    lax.fori_loop(0, iq * (bq // bk), lambda j, _: block(j, None), None)
    for i in range(bq // bk):
        block(iq * (bq // bk) + i, -i * bk)
    for n in range(heads):
        dq_ref[:, n * HEAD : (n + 1) * HEAD] = (dq_s[n] * SCALE).T.astype(BF16)

    @pl.when(iq == pl.num_programs(0) - 1)
    def _():
        dk_ref[...] = (dk_s[...] * SCALE).astype(BF16)
        dv_ref[...] = dv_s[...].astype(BF16)


def attend_back(q, k, v, d_out, lse, delta):
    t, width = q.shape
    heads = width // HEAD
    bq = bk = _tile(t)
    rows, whole = pl.BlockSpec((bq, width), lambda i: (i, 0)), pl.BlockSpec((t, width), lambda i: (0, 0))
    stats = pl.BlockSpec((heads, bq), lambda i: (0, i))
    one = jax.ShapeDtypeStruct((t, width), BF16)
    return _call(
        functools.partial(_attend_back, bk=bk),
        (t // bq,),
        [rows, whole, whole, rows, stats, stats],
        [(rows, one), (whole, one), (whole, one)],
        [pltpu.VMEM((heads, HEAD, bq), F32), pltpu.VMEM((t, width), F32), pltpu.VMEM((t, width), F32)],
        (q, k, v, d_out, lse, delta),
        5 * t * t * width,
        14 * t * width,
    )


def _qkv_back(h, dq, dk, dv, wq, wk, wv, cos, sin, first, sums):
    a = (h * _norm_scale(h)).astype(BF16)
    dq, dk = (_turn(d.astype(F32), cos, -sin).astype(BF16) for d in (dq, dk))
    for s, d in zip(sums, (dq, dk, dv), strict=True):
        term = _dot(a, d, 0, 0)

        @pl.when(first)
        def _():
            s[...] = term

        @pl.when(jnp.logical_not(first))
        def _():
            s[...] += term

    if wq is None:
        return None
    return sum(_dot(d, w, 1, 1).astype(BF16).astype(F32) for d, w in ((dq, wq), (dk, wk), (dv, wv)))


def _scatter_rows(ref, value):
    n = ref.shape[0]
    each = value.shape[0] // n
    for d in range(n):
        ref[d, 0] = value[d * each : (d + 1) * each].astype(BF16)


def _mlp_back(*refs, tiles, blocks, last):
    if last:
        h_ref, att_ref, dy_ref, wo, wg, wu, wd = refs[:7]
        outs, scratch = refs[7:14], refs[14:]
    else:
        (h_ref, att_ref, hn_ref, dq_ref, dk_ref, dv_ref, dh_ref, wq, wk, wv, cos, sin, gate_ref, up_ref, wo, wg, wu, wd) = refs[:18]
        outs, scratch = refs[18:28], refs[28:]
    g_down, g_gate, g_up, g_o, dh1_ref, datt_ref, delta_ref = outs[:7]
    b_s, h1_s, dy_s, p_s, dg_s, du_s, sum_g, sum_u, sum_o = scratch[:9]
    step = pl.program_id(0)
    bt = h_ref.shape[0]
    middle = tiles * blocks
    r = jnp.where(step < tiles, step, lax.rem(step - tiles, tiles))
    rows = pl.ds(pl.multiple_of(r * bt, bt), bt)

    @pl.when(step < tiles)
    def _():
        if last:
            h1 = _after_attention(h_ref, att_ref, wo[0])
            dy_s[rows, :] = dy_ref[...]
        else:
            h1 = h_ref[...]
            hn = hn_ref[...].astype(F32)
            da = _qkv_back(hn, dq_ref[...], dk_ref[...], dv_ref[...], wq[0], wk[0], wv[0], cos[...], sin[...], step == 0, scratch[9:12])
            dy_s[rows, :] = (dh_ref[...].astype(F32) + _norm_back(hn, da.astype(BF16).astype(F32)).astype(BF16).astype(F32)).astype(BF16)

            @pl.when(step == tiles - 1)
            def _():
                for ref, s in zip(outs[7:10], scratch[9:12], strict=True):
                    _scatter_rows(ref, s[...])

        h1_s[rows, :] = h1
        h1 = h1.astype(F32)
        b_s[rows, :] = (h1 * _norm_scale(h1)).astype(BF16)

    @pl.when((step >= tiles) & (step < tiles + middle))
    def _():
        b, dy = b_s[rows, :], dy_s[rows, :]
        if last:
            gate, up = _dot(b, wg[0]), _dot(b, wu[0])
        else:
            gate, up = gate_ref[...], up_ref[...]
        dp = _dot(dy, wd[0], 1, 1).astype(BF16).astype(F32)
        sg = jax.nn.sigmoid(gate)
        silu = gate * sg
        p_s[rows, :] = (silu * up).astype(BF16)
        du = (dp * silu).astype(BF16)
        dg = (dp * up * (sg + silu * (1 - sg))).astype(BF16)
        du_s[rows, :] = du
        dg_s[rows, :] = dg
        by_gate, by_up = _dot(dg, wg[0], 1, 1), _dot(du, wu[0], 1, 1)

        @pl.when(step < 2 * tiles)
        def _():
            sum_g[rows, :] = by_gate
            sum_u[rows, :] = by_up

        @pl.when(step >= 2 * tiles)
        def _():
            sum_g[rows, :] += by_gate
            sum_u[rows, :] += by_up

        @pl.when(r == tiles - 1)
        def _():
            down = _dot(p_s[...], dy_s[...], 0, 0)
            n = g_down.shape[1]
            each = down.shape[0] // n
            for i in range(n):
                g_down[0, i] = down[i * each : (i + 1) * each].astype(BF16)
            _scatter_rows(g_gate, _dot(b_s[...], dg_s[...], 0, 0))
            _scatter_rows(g_up, _dot(b_s[...], du_s[...], 0, 0))

    @pl.when(step >= tiles + middle)
    def _():
        db = sum_g[rows, :].astype(BF16).astype(F32) + sum_u[rows, :].astype(BF16).astype(F32)
        dh1 = dy_s[rows, :].astype(F32) + _norm_back(h1_s[rows, :].astype(F32), db.astype(BF16).astype(F32)).astype(BF16).astype(F32)
        dh1 = dh1.astype(BF16)
        dh1_ref[...] = dh1
        datt = _dot(dh1, wo[0], 1, 1).astype(BF16)
        datt_ref[...] = datt
        att = att_ref[...]
        both = att.astype(F32) * datt.astype(F32)
        for n in range(both.shape[1] // HEAD):
            delta_ref[n : n + 1, :] = both[:, n * HEAD : (n + 1) * HEAD].T.sum(axis=0, keepdims=True)
        term = _dot(att, dh1, 0, 0)

        @pl.when(step == tiles + middle)
        def _():
            sum_o[...] = term

        @pl.when(step > tiles + middle)
        def _():
            sum_o[...] += term

        @pl.when(step == 2 * tiles + middle - 1)
        def _():
            _scatter_rows(g_o, sum_o[...])


def mlp_back(n, layer, h, att, by, weights, rope, upper=None, hidden=None):
    t, d = h.shape
    ff = weights["w_gate"].shape[2]
    bt = _tile(t)
    tiles, blocks = t // bt, n
    fb = ff // blocks
    heads = att.shape[1] // HEAD
    middle = tiles * blocks
    r = lambda s: jnp.where(s < tiles, s, lax.rem(s - tiles, tiles))
    j = lambda s: jnp.clip(lax.div(s - tiles, tiles), 0, blocks - 1)
    edge = lambda s: jnp.where(s < tiles, s, jnp.maximum(s - middle, tiles) - tiles)
    edge = lambda s: jnp.where(s < tiles, s, jnp.where(s < tiles + middle, tiles - 1, s - tiles - middle))
    before = lambda s: jnp.minimum(s, tiles - 1)
    after = lambda s: jnp.maximum(s - tiles - middle, 0)
    tile = lambda f, w=d: pl.BlockSpec((bt, w), lambda s: (f(s), 0))
    square = pl.BlockSpec((1, d, d), lambda s: (layer, 0, 0))
    up_square = pl.BlockSpec((1, d, d), lambda s: (layer + 1, 0, 0))
    mlp = [square, pl.BlockSpec((1, d, fb), lambda s: (layer, 0, j(s))), pl.BlockSpec((1, d, fb), lambda s: (layer, 0, j(s))),
           pl.BlockSpec((1, fb, d), lambda s: (layer, j(s), 0))]
    w4 = [weights[name] for name in ("wo", "w_gate", "w_up", "w_down")]
    last = upper is None
    if last:
        ins = [tile(before), tile(edge), tile(before), *mlp]
        args = [h, att, by, *w4]
    else:
        hn, dq, dk, dv = upper
        table = pl.BlockSpec((bt, HEAD), lambda s: (before(s), 0))
        block = pl.BlockSpec((bt, fb), lambda s: (r(jnp.clip(s, tiles, tiles + middle - 1)), j(s)))
        ins = [tile(before), tile(after), *[tile(before)] * 5, up_square, up_square, up_square, table, table, block, block, *mlp]
        args = [h, att, hn, dq, dk, dv, by, weights["wq"], weights["wk"], weights["wv"], *rope, *hidden, *w4]
    small = pl.BlockSpec((n, 1, d // n, d), lambda s: (0, 0, 0, 0))
    small_shape = jax.ShapeDtypeStruct((n, 1, d // n, d), BF16)
    each = d // n
    wide = jax.ShapeDtypeStruct((n, blocks, each, fb), BF16)
    outs = [
        (pl.BlockSpec((1, fb // each, each, d), lambda s: (j(s), 0, 0, 0)), jax.ShapeDtypeStruct((n, fb // each, each, d), BF16)),
        (pl.BlockSpec((n, 1, each, fb), lambda s: (0, j(s), 0, 0)), wide),
        (pl.BlockSpec((n, 1, each, fb), lambda s: (0, j(s), 0, 0)), wide),
        (small, small_shape),
        (tile(after), jax.ShapeDtypeStruct((t, d), BF16)),
        (tile(after), jax.ShapeDtypeStruct((t, d), BF16)),
        (pl.BlockSpec((heads, bt), lambda s: (0, after(s))), jax.ShapeDtypeStruct((heads, t), F32)),
    ]
    scratch = [pltpu.VMEM((t, d), BF16)] * 3 + [pltpu.VMEM((t, fb), BF16)] * 3 + [pltpu.VMEM((t, d), F32)] * 2 + [pltpu.VMEM((d, d), F32)]
    if not last:
        outs += [(small, small_shape)] * 3
        scratch += [pltpu.VMEM((d, d), F32)] * 3
    return _call(
        functools.partial(_mlp_back, tiles=tiles, blocks=blocks, last=last),
        (2 * tiles + middle,),
        ins,
        outs,
        scratch,
        args,
        2 * t * d * (ff * 8 + d * 4),
        sum(a.size * a.dtype.itemsize for a in args),
    )


def _last_back(h_ref, dq_ref, dk_ref, dv_ref, cos, sin, g_q, g_k, g_v, *sums):
    step = pl.program_id(0)
    _qkv_back(h_ref[...].astype(F32), dq_ref[...], dk_ref[...], dv_ref[...], None, None, None, cos[...], sin[...], step == 0, sums)

    @pl.when(step == pl.num_programs(0) - 1)
    def _():
        for ref, s in zip((g_q, g_k, g_v), sums, strict=True):
            _scatter_rows(ref, s[...])


def last_back(n, h, dq, dk, dv, rope):
    t, d = h.shape
    bt = _tile(t)
    tile, table = pl.BlockSpec((bt, d), lambda s: (s, 0)), pl.BlockSpec((bt, HEAD), lambda s: (s, 0))
    small = (pl.BlockSpec((n, 1, d // n, d), lambda s: (0, 0, 0, 0)), jax.ShapeDtypeStruct((n, 1, d // n, d), BF16))
    return _call(_last_back, (t // bt,), [tile] * 4 + [table] * 2, [small] * 3, [pltpu.VMEM((d, d), F32)] * 3, (h, dq, dk, dv, *rope),
                 6 * t * d * d, 8 * t * d)


NAMES = ("wq", "wk", "wv", "wo", "w_gate", "w_up", "w_down")


def rope_tables(t):
    half = HEAD // 2
    angle = np.arange(t, dtype=np.float32)[:, None] * (np.float32(THETA) ** (-np.arange(half, dtype=np.float32) / half)).astype(np.float32)
    cos, sin = np.cos(angle.astype(np.float64)).astype(np.float32), np.sin(angle.astype(np.float64)).astype(np.float32)
    return jnp.asarray(np.concatenate([cos, cos], 1)), jnp.asarray(np.concatenate([-sin, sin], 1))


def first(h, weights, rope):
    t, d = h.shape
    bt = _tile(t)
    tile, table = pl.BlockSpec((bt, d), lambda s: (s, 0)), pl.BlockSpec((bt, HEAD), lambda s: (s, 0))
    square = pl.BlockSpec((1, d, d), lambda s: (0, 0, 0))
    one = (tile, jax.ShapeDtypeStruct((t, d), BF16))
    return _call(_first, (t // bt,), [tile, square, square, square, table, table], [one] * 3, [],
                 (h, weights["wq"], weights["wk"], weights["wv"], *rope), 6 * t * d * d, 8 * t * d)


def between(layer, h, att, weights, rope):
    t, d = h.shape
    ff = weights["w_gate"].shape[2]
    bt = _tile(t)
    at = lambda k, *shape: pl.BlockSpec((1, *shape), lambda s: (k, 0, 0))
    tile, table, wide = (pl.BlockSpec((bt, w), lambda s: (s, 0)) for w in (d, HEAD, ff))
    one, two = (tile, jax.ShapeDtypeStruct((t, d), BF16)), (wide, jax.ShapeDtypeStruct((t, ff), F32))
    return _call(
        _between,
        (t // bt,),
        [tile, tile, at(layer, d, d), at(layer, d, ff), at(layer, d, ff), at(layer, ff, d), *[at(layer + 1, d, d)] * 3, table, table],
        [one, one, two, two, one, one, one],
        [],
        (h, att, *(weights[name] for name in ("wo", "w_gate", "w_up", "w_down", "wq", "wk", "wv")), *rope),
        2 * t * d * (4 * d + 3 * ff),
        14 * t * d + 8 * t * ff,
    )


def adamw(w, m, v, g):
    m = 0.9 * m + 0.1 * g
    v = 0.95 * v + 0.05 * g * g
    step = m * lax.rsqrt(v + 1e-8) + 0.1 * w
    return (w - 0.02 * step).astype(BF16), m, v


def solution(mesh):
    n = mesh.shape["dp"]

    def step(x, dy, *arrays):
        weights = dict(zip(NAMES, arrays[:7], strict=True))
        m, v = arrays[7:14], arrays[14:]
        layers = weights["wq"].shape[0]
        h = x[0]
        rope = rope_tables(h.shape[0])
        hs, atts, qkvs, lses, mids, hidden = [h], [], [], [], [], []
        q, k, v_ = first(h, weights, rope)
        for number in range(layers):
            qkvs.append((q, k, v_))
            att, lse = attend(q, k, v_)
            atts.append(att)
            lses.append(lse)
            if number < layers - 1:
                h1, h, gate, up, q, k, v_ = between(number, h, att, weights, rope)
                hs.append(h)
                mids.append(h1)
                hidden.append((gate, up))
        scatter = lambda parts: lax.psum_scatter(jnp.concatenate(parts, 1), "dp", scatter_dimension=0, tiled=True)[0]
        own = {}
        by, upper, behind = dy[0], None, []
        for number in reversed(range(layers)):
            if upper is None:
                got = mlp_back(n, number, hs[number], atts[number], by, weights, rope)
            else:
                got = mlp_back(n, number, mids[number], atts[number], by, weights, rope, upper, hidden[number])
            parts = [*got[:4], *got[7:]]
            mine = scatter(parts)
            at = 0
            for name, part in zip(["w_down", "w_gate", "w_up", "wo", *(["wq", "wk", "wv"] if got[7:] else [])], parts):
                own[name, number + (name in ("wq", "wk", "wv"))] = mine[at : at + part.shape[1]]
                at += part.shape[1]
            by, datt, delta = got[4:7]
            upper = (hs[number], *attend_back(*qkvs[number], datt, lses[number], delta))
        mine = scatter(last_back(n, *upper, rope))
        for i, name in enumerate(("wq", "wk", "wv")):
            own[name, 0] = mine[i : i + 1]
        gradients = []
        for name, one in zip(NAMES, m, strict=True):
            blocks = jnp.stack([own[name, number] for number in range(layers)]).astype(F32)
            if one.shape[2] != blocks.shape[3]:
                blocks = blocks.transpose(0, 2, 1, 3)
            gradients.append(blocks.reshape(one.shape))
        squares = lax.psum(sum(jnp.sum(g * g) for g in gradients), "dp")
        count = lax.psum(1, "dp") * sum(g.size for g in gradients)
        factor = jnp.minimum(1.0, 0.5 * lax.rsqrt(squares / count + 1e-30))
        me = lax.axis_index("dp")
        mine = [lax.dynamic_slice_in_dim(w, me * one.shape[1], one.shape[1], 1).astype(F32) for w, one in zip(arrays[:7], m, strict=True)]
        new = [adamw(w, m, v, g * factor) for w, m, v, g in zip(mine, m, v, gradients, strict=True)]
        whole = [lax.all_gather(one[0], "dp", axis=1, tiled=True) for one in new]
        return (*whole, *(one[1] for one in new), *(one[2] for one in new))

    states, all_of, cut = P(("rep", "dp"), None, None), P(None, None, None), P(None, "dp", None)
    return jax.shard_map(
        step,
        mesh=mesh,
        in_specs=(states, states) + (all_of,) * 7 + (cut,) * 14,
        out_specs=(P("rep", None, None),) * 7 + (P("rep", "dp", None),) * 14,
        check_vma=False,
    )
```

```python
import functools

import jax
import jax.numpy as jnp
import numpy as np
from jax import lax
from jax.experimental import pallas as pl
from jax.experimental.pallas import tpu as pltpu
from jax.sharding import PartitionSpec as P

F32, BF16 = jnp.float32, jnp.bfloat16
HEAD = 128
THETA = 10000
NEG = -1e30
HIDDEN = 2 * NEG
LOG2E = 1.4426950408889634
SCALE = HEAD**-0.5
VMEM = 67043328


def _dot(a, b, ca=1, cb=0):
    return lax.dot_general(a, b, (((ca,), (cb,)), ((), ())), preferred_element_type=F32)


def _tile(size, most=512):
    return max(n for n in range(128, most + 1, 128) if size % n == 0)


def _call(kernel, grid, ins, outs, scratch, args, flops, moved, collective=None):
    return pl.pallas_call(
        kernel,
        grid=grid,
        in_specs=[spec for spec in ins],
        out_specs=[spec for spec, _ in outs],
        out_shape=[shape for _, shape in outs],
        scratch_shapes=scratch,
        compiler_params=pltpu.CompilerParams(dimension_semantics=("arbitrary",) * len(grid), vmem_limit_bytes=VMEM, collective_id=collective,
                                             has_side_effects=collective is not None),
        cost_estimate=pl.CostEstimate(flops=int(flops), transcendentals=0, bytes_accessed=int(moved)),
    )(*args)


def _norm_scale(x):
    return lax.rsqrt(jnp.mean(x * x, -1, keepdims=True) + 1e-6)


def _norm_back(x, d_out):
    s = _norm_scale(x)
    inner = jnp.mean(x * d_out, -1, keepdims=True)
    return s * d_out - x * (s * s * s * inner)


def _turn(x, cos, sin):
    parts = [x[:, n : n + HEAD] for n in range(0, x.shape[1], HEAD)]
    return jnp.concatenate([p * cos + pltpu.roll(p, HEAD // 2, 1) * sin for p in parts], 1)


def _qkv(h, wq, wk, wv, cos, sin, q_ref, k_ref, v_ref):
    a = (h * _norm_scale(h)).astype(BF16)
    q_ref[...] = _turn(_dot(a, wq).astype(BF16).astype(F32), cos, sin).astype(BF16)
    k_ref[...] = _turn(_dot(a, wk).astype(BF16).astype(F32), cos, sin).astype(BF16)
    v_ref[...] = _dot(a, wv).astype(BF16)


def _first(h_ref, wq, wk, wv, cos, sin, q_ref, k_ref, v_ref):
    _qkv(h_ref[...].astype(F32), wq[0], wk[0], wv[0], cos[...], sin[...], q_ref, k_ref, v_ref)


def _after_attention(h_ref, att_ref, wo):
    return (h_ref[...].astype(F32) + _dot(att_ref[...], wo).astype(BF16).astype(F32)).astype(BF16)


def _between(h_ref, att_ref, wo, wg, wu, wd, wq, wk, wv, cos, sin, h1_ref, y_ref, gate_ref, up_ref, q_ref, k_ref, v_ref, *, n):
    h1 = _after_attention(h_ref, att_ref, wo[0])
    h1_ref[...] = h1
    h1 = h1.astype(F32)
    b = (h1 * _norm_scale(h1)).astype(BF16)
    total = jnp.zeros(h1.shape, F32)
    for j in range(n):
        gate, up = _dot(b, _strips(wg, j, n, n, 2)), _dot(b, _strips(wu, j, n, n, 2))
        gate_ref[j] = gate
        up_ref[j] = up
        total += _dot((gate * jax.nn.sigmoid(gate) * up).astype(BF16), _strips(wd, j, n, n, 1))
    y = (h1 + total.astype(BF16).astype(F32)).astype(BF16)
    y_ref[...] = y
    _qkv(y.astype(F32), wq[0], wk[0], wv[0], cos[...], sin[...], q_ref, k_ref, v_ref)


def _attend(q_ref, k_ref, v_ref, o_ref, lse_ref, top_s, mix_s, *, bk):
    iq = pl.program_id(0)
    bq = q_ref.shape[0]
    heads = q_ref.shape[1] // HEAD
    e = SCALE * LOG2E
    ones = jnp.ones((8, bk), BF16)
    top_s[...] = jnp.full(top_s.shape, NEG, F32)
    mix_s[...] = jnp.zeros(mix_s.shape, F32)

    def block(j, first_query):
        here = pl.ds(pl.multiple_of(j * bk, bk), bk)
        cols = [slice(n * HEAD, (n + 1) * HEAD) for n in range(heads)]
        scores = [_dot(k_ref[here, c], q_ref[:, c], 1, 1) for c in cols]
        weights, keeps = [], []
        if first_query is not None:
            seen = lax.broadcasted_iota(jnp.int32, (bk, bq), 1) + first_query >= lax.broadcasted_iota(jnp.int32, (bk, bq), 0)
        for n, s in enumerate(scores):
            if first_query is not None:
                s = jnp.where(seen, s, HIDDEN)
            old = top_s[n : n + 1, :]
            top = jnp.maximum(old, s.max(axis=0, keepdims=True))
            top_s[n : n + 1, :] = top
            weights.append(jnp.exp2((s - top) * e).astype(BF16))
            keeps.append(jnp.exp2((old - top) * e))
        for n, (c, p, keep) in enumerate(zip(cols, weights, keeps)):
            values = jnp.concatenate([v_ref[here, c].T, ones], axis=0)
            mix_s[n] = mix_s[n] * keep + _dot(values, p, 1, 0)

    lax.fori_loop(0, iq * (bq // bk), lambda j, _: block(j, None), None)
    for i in range(bq // bk):
        block(iq * (bq // bk) + i, -i * bk)
    for n in range(heads):
        total = mix_s[n, HEAD : HEAD + 1, :]
        o_ref[:, n * HEAD : (n + 1) * HEAD] = (mix_s[n, :HEAD, :] * (1 / total)).T.astype(BF16)
        lse_ref[n : n + 1, :] = top_s[n : n + 1, :] * e + jnp.log2(total)


def attend(q, k, v):
    t, width = q.shape
    heads = width // HEAD
    bq = bk = _tile(t)
    rows, whole = pl.BlockSpec((bq, width), lambda i: (i, 0)), pl.BlockSpec((t, width), lambda i: (0, 0))
    return _call(
        functools.partial(_attend, bk=bk),
        (t // bq,),
        [rows, whole, whole],
        [(rows, jax.ShapeDtypeStruct((t, width), BF16)), (pl.BlockSpec((heads, bq), lambda i: (0, i)), jax.ShapeDtypeStruct((heads, t), F32))],
        [pltpu.VMEM((heads, bq), F32), pltpu.VMEM((heads, HEAD + 8, bq), F32)],
        (q, k, v),
        2 * t * t * width,
        8 * t * width,
    )


def _ring(n):
    me = lax.axis_index("dp")
    return me, lax.rem(me + 1, n), lax.rem(me + 2, n), lax.rem(me + n - 1, n)


def _greet(n):
    _, right, _, left = _ring(n)
    barrier = pltpu.get_barrier_semaphore()
    for other in (right, left):
        pl.semaphore_signal(barrier, inc=1, device_id={"dp": other}, device_id_type=pl.DeviceIdType.MESH)


def _met():
    pl.semaphore_wait(pltpu.get_barrier_semaphore(), 2)


def _rows_loop(rows, body, most=32):
    each = max(c for c in range(16, most + 1, 16) if rows % c == 0)
    lax.fori_loop(0, rows // each, lambda i, _: body(pl.ds(pl.multiple_of(i * each, each), each)), None)


class RingSum:
    def __init__(self, n, block, passing, arrived, sent, got):
        self.block, self.passing, self.arrived = block, passing, arrived
        self.me, right, far, left = _ring(n)
        self.near = right, left
        half = block.shape[1] // 2
        self.half = half
        a, b = pl.ds(0, half), pl.ds(half, half)
        moves = [
            (block.at[far, a], passing.at[0], right),
            (block.at[far, b], passing.at[1], left),
            (block.at[right, b], arrived.at[0, b], right),
            (block.at[left, a], arrived.at[1, a], left),
            (passing.at[0], arrived.at[0, a], right),
            (passing.at[1], arrived.at[1, b], left),
        ]
        self.copies = [
            pltpu.make_async_remote_copy(src_ref=s, dst_ref=d, send_sem=sent.at[i], recv_sem=got.at[i], device_id={"dp": to},
                                         device_id_type=pl.DeviceIdType.MESH)
            for i, (s, d, to) in enumerate(moves)
        ]

    @staticmethod
    def scratch(n, rows, columns):
        half = pltpu.VMEM((2, rows // 2, columns), BF16)
        return [half, pltpu.VMEM((2, rows, columns), BF16), pltpu.SemaphoreType.DMA((6,)), pltpu.SemaphoreType.DMA((6,))]

    def start(self):
        for c in self.copies[:4]:
            c.start()

    def add(self):
        for c in self.copies[:2]:
            c.wait_recv()
        for i, other in enumerate(self.near):

            def one(rows, i=i, other=other):
                mine = self.block[other, pl.ds(rows.start + i * self.half, rows.size), :]
                self.passing[i, rows, :] = (self.passing[i, rows, :].astype(F32) + mine.astype(F32)).astype(BF16)

            _rows_loop(self.half, one)

    def forward(self):
        for c in self.copies[4:]:
            c.start()

    def finish(self, out, squares=None):
        for c in self.copies[2:]:
            c.wait_recv()

        def one(rows):
            total = self.block[self.me, rows, :].astype(F32) + self.arrived[0, rows, :].astype(F32) + self.arrived[1, rows, :].astype(F32)
            total = total.astype(BF16)
            out[rows, :] = total
            if squares is not None:
                _add_squares(squares, total)

        _rows_loop(self.half * 2, one)
        for c in self.copies:
            c.wait_send()


def _add_squares(squares, value):
    value = value.astype(F32)
    value = value * value
    squares[...] += sum(value[i : i + 8] for i in range(0, value.shape[0], 8))


def _attend_back(q_ref, k_ref, v_ref, do_ref, lse_ref, delta_ref, ff_ref, o_ref, dq_ref, dk_ref, dv_ref, own_ref, dq_s, dk_s, dv_s, block_s, load_sem,
                 *ring, bk, n):
    iq = pl.program_id(0)
    bq = q_ref.shape[0]
    heads = q_ref.shape[1] // HEAD
    e = SCALE * LOG2E
    steps = pl.num_programs(0)
    split = ff_ref.shape[1]
    loads = [
        pltpu.make_async_copy(ff_ref, block_s.at[:, pl.ds(0, split)], load_sem.at[0]),
        pltpu.make_async_copy(o_ref, block_s.at[:, pl.ds(split, o_ref.shape[1])], load_sem.at[1]),
    ]
    job = RingSum(n, block_s, *ring)

    @pl.when(iq == 0)
    def _():
        _greet(n)
        for load in loads:
            load.start()
        dk_s[...] = jnp.zeros_like(dk_s)
        dv_s[...] = jnp.zeros_like(dv_s)
        for load in loads:
            load.wait()
        _met()
        job.start()

    @pl.when(iq == steps - 2)
    def _():
        job.add()

    dq_s[...] = jnp.zeros_like(dq_s)

    def block(j, first_query):
        here = pl.ds(pl.multiple_of(j * bk, bk), bk)
        cols = [slice(i * HEAD, (i + 1) * HEAD) for i in range(heads)]
        scores = [_dot(k_ref[here, c], q_ref[:, c], 1, 1) for c in cols]
        dps = [_dot(v_ref[here, c], do_ref[:, c], 1, 1) for c in cols]
        if first_query is not None:
            seen = lax.broadcasted_iota(jnp.int32, (bk, bq), 1) + first_query >= lax.broadcasted_iota(jnp.int32, (bk, bq), 0)
        for i, c in enumerate(cols):
            p = jnp.exp2(scores[i] * e - lse_ref[i : i + 1, :])
            if first_query is not None:
                p = jnp.where(seen, p, 0.0)
            ds = (p * (dps[i] - delta_ref[i : i + 1, :])).astype(BF16)
            dv_s[here, c] += _dot(p.astype(BF16), do_ref[:, c], 1, 0)
            dk_s[here, c] += _dot(ds, q_ref[:, c], 1, 0)
            dq_s[i] += _dot(k_ref[here, c].T, ds, 1, 0)

    lax.fori_loop(0, iq * (bq // bk), lambda j, _: block(j, None), None)

    @pl.when(iq == steps - 2)
    def _():
        job.forward()

    for i in range(bq // bk):
        block(iq * (bq // bk) + i, -i * bk)
    for i in range(heads):
        dq_ref[:, i * HEAD : (i + 1) * HEAD] = (dq_s[i] * SCALE).T.astype(BF16)

    @pl.when(iq == steps - 1)
    def _():
        dk_ref[...] = (dk_s[...] * SCALE).astype(BF16)
        dv_ref[...] = dv_s[...].astype(BF16)
        job.finish(own_ref)


def attend_back(n, number, q, k, v, d_out, lse, delta, ff, o):
    t, width = q.shape
    heads = width // HEAD
    bq = bk = _tile(t)
    rows, whole = pl.BlockSpec((bq, width), lambda i: (i, 0)), pl.BlockSpec((t, width), lambda i: (0, 0))
    stats = pl.BlockSpec((heads, bq), lambda i: (0, i))
    one = jax.ShapeDtypeStruct((t, width), BF16)
    height, columns = ff.shape[1] + o.shape[1], ff.shape[2]
    return _call(
        functools.partial(_attend_back, bk=bk, n=n),
        (t // bq,),
        [rows, whole, whole, rows, stats, stats, pl.BlockSpec(memory_space=pl.ANY), pl.BlockSpec(memory_space=pl.ANY)],
        [(rows, one), (whole, one), (whole, one),
         (pl.BlockSpec((height, columns), lambda i: (0, 0)), jax.ShapeDtypeStruct((height, columns), BF16))],
        [pltpu.VMEM((heads, HEAD, bq), F32), pltpu.VMEM((t, width), F32), pltpu.VMEM((t, width), F32),
         pltpu.VMEM((n, height, columns), BF16), pltpu.SemaphoreType.DMA((2,)), *RingSum.scratch(n, height, columns)],
        (q, k, v, d_out, lse, delta, ff, o),
        5 * t * t * width,
        14 * t * width,
        collective=number,
    )


def _strips(ref, block, n, blocks, axis):
    width = ref.shape[axis] // (n * blocks)
    at = [pl.ds(pl.multiple_of((d * blocks + block) * width, width), width) for d in range(n)]
    return jnp.concatenate([ref[0, :, a] if axis == 2 else ref[0, a, :] for a in at], axis - 1)


def _qkv_back(h, dq, dk, dv, wq, wk, wv, cos, sin, first, sums):
    a = (h * _norm_scale(h)).astype(BF16)
    dq, dk = (_turn(d.astype(F32), cos, -sin).astype(BF16) for d in (dq, dk))
    for s, d in zip(sums, (dq, dk, dv), strict=True):
        term = _dot(a, d, 0, 0)

        @pl.when(first)
        def _():
            s[...] = term

        @pl.when(jnp.logical_not(first))
        def _():
            s[...] += term

    return sum(_dot(d, w, 1, 1).astype(BF16).astype(F32) for d, w in ((dq, wq), (dk, wk), (dv, wv)))


def _cut(ref, at, value):
    n = ref.shape[0]
    each = value.shape[0] // n
    for d in range(n):
        ref[d, at : at + each] = value[d * each : (d + 1) * each].astype(BF16)


def _mlp_back(*refs, n, tiles, blocks, last):
    take = iter(range(len(refs)))
    some = lambda count: [refs[next(take)] for _ in range(count)]
    h_ref, att_ref = some(2)
    if last:
        (dy_ref,) = some(1)
    else:
        hn_ref, dq_ref, dk_ref, dv_ref, dh_ref, wq, wk, wv, cos, sin, gate_ref, up_ref = some(12)
    wo, wg, wu, wd = some(4)
    dh1_ref, datt_ref, delta_ref, left_ff, left_o = some(5)
    own = some(blocks - 1 + (not last))
    h1_s = some(1)[0] if last else None
    b_s, dy_s, p_s, dg_s, du_s, sum_g, sum_u, g_s, go_s, out_sem = some(10)
    sums3 = some(1 if last else 3)
    sum_o = sums3[0]
    jobs = []
    for i in range(len(own)):
        if i < blocks - 1:
            block = g_s.at[i]
        else:
            block = gqkv_s = g_s.at[blocks - 1]
        jobs.append(RingSum(n, block, *some(4)))
    step = pl.program_id(0)
    bt = h_ref.shape[0]
    middle = tiles * blocks
    r = jnp.where(step < tiles, step, lax.rem(step - tiles, tiles))
    j = lax.div(step - tiles, tiles)
    rows = pl.ds(pl.multiple_of(r * bt, bt), bt)
    wait = max(1, tiles - 1)

    @pl.when(step == 0)
    def _():
        _greet(n)

    begin = [tiles * (2 + i) for i in range(blocks - 1)] + [tiles] * (not last)

    @pl.when(step == min(begin))
    def _():
        _met()

    for job, at, out in zip(jobs, begin, own, strict=True):

        @pl.when(step == at + 2 * wait)
        def _(job=job, out=out):
            job.finish(out)

    for job, at in zip(jobs, begin, strict=True):

        @pl.when(step == at + wait)
        def _(job=job):
            job.add()

        @pl.when(step == at)
        def _(job=job):
            job.start()

    @pl.when(step < tiles)
    def _():
        if last:
            h1 = _after_attention(h_ref, att_ref, wo[0])
            h1_s[rows, :] = h1
            dy_s[rows, :] = dy_ref[...]
        else:
            h1 = h_ref[...]
            hn = hn_ref[...].astype(F32)
            da = _qkv_back(hn, dq_ref[...], dk_ref[...], dv_ref[...], wq[0], wk[0], wv[0], cos[...], sin[...], step == 0, sums3)
            dy_s[rows, :] = (dh_ref[...].astype(F32) + _norm_back(hn, da.astype(BF16).astype(F32)).astype(BF16).astype(F32)).astype(BF16)

            @pl.when(step == tiles - 1)
            def _():
                for i, s in enumerate(sums3):
                    _cut(gqkv_s, i * (s.shape[0] // n), s[...])

        h1 = h1.astype(F32)
        b_s[rows, :] = (h1 * _norm_scale(h1)).astype(BF16)

    @pl.when((step >= tiles) & (step < tiles + middle))
    def _():
        b, dy = b_s[rows, :], dy_s[rows, :]
        gate_w, up_w = _strips(wg, j, n, blocks, 2), _strips(wu, j, n, blocks, 2)
        if last:
            gate, up = _dot(b, gate_w), _dot(b, up_w)
        else:
            gate, up = gate_ref[0], up_ref[0]
        dp = _dot(dy, _strips(wd, j, n, blocks, 1), 1, 1).astype(BF16).astype(F32)
        sg = jax.nn.sigmoid(gate)
        silu = gate * sg
        p_s[rows, :] = (silu * up).astype(BF16)
        du = (dp * silu).astype(BF16)
        dg = (dp * up * (sg + silu * (1 - sg))).astype(BF16)
        du_s[rows, :] = du
        dg_s[rows, :] = dg
        by_gate, by_up = _dot(dg, gate_w, 1, 1), _dot(du, up_w, 1, 1)

        @pl.when(step < 2 * tiles)
        def _():
            sum_g[rows, :] = by_gate
            sum_u[rows, :] = by_up

        @pl.when(step >= 2 * tiles)
        def _():
            sum_g[rows, :] += by_gate
            sum_u[rows, :] += by_up

        @pl.when(r == tiles - 1)
        def _():
            each = b.shape[1] // n
            mine = g_s.at[j]
            _cut(mine, 0, _dot(p_s[...], dy_s[...], 0, 0))
            _cut(mine, mine.shape[1] - 2 * each, _dot(b_s[...], dg_s[...], 0, 0))
            _cut(mine, mine.shape[1] - each, _dot(b_s[...], du_s[...], 0, 0))

    out_copies = [pltpu.make_async_copy(g_s.at[blocks - 1], left_ff, out_sem.at[0]), pltpu.make_async_copy(go_s, left_o, out_sem.at[1])]

    @pl.when(step >= tiles + middle)
    def _():
        db = sum_g[rows, :].astype(BF16).astype(F32) + sum_u[rows, :].astype(BF16).astype(F32)
        h1 = h1_s[rows, :] if last else h_ref[...]
        dh1 = dy_s[rows, :].astype(F32) + _norm_back(h1.astype(F32), db.astype(BF16).astype(F32)).astype(BF16).astype(F32)
        dh1 = dh1.astype(BF16)
        dh1_ref[...] = dh1
        datt = _dot(dh1, wo[0], 1, 1).astype(BF16)
        datt_ref[...] = datt
        att = att_ref[...]
        both = att.astype(F32) * datt.astype(F32)
        for i in range(both.shape[1] // HEAD):
            delta_ref[i : i + 1, :] = both[:, i * HEAD : (i + 1) * HEAD].T.sum(axis=0, keepdims=True)
        term = _dot(att, dh1, 0, 0)

        @pl.when(step == tiles + middle)
        def _():
            out_copies[0].start()
            sum_o[...] = term

        @pl.when(step > tiles + middle)
        def _():
            sum_o[...] += term

        @pl.when(step == 2 * tiles + middle - 1)
        def _():
            _cut(go_s, 0, sum_o[...])
            out_copies[1].start()
            for c in out_copies:
                c.wait()

    for job, at in zip(jobs, begin, strict=True):

        @pl.when(step == at + wait)
        def _(job=job):
            job.forward()


def mlp_back(n, number, layer, h, att, by, weights, rope, upper=None, hidden=None):
    t, d = h.shape
    ff = weights["w_gate"].shape[2]
    bt = _tile(t)
    tiles, blocks = t // bt, n
    fb, each = ff // blocks, d // n
    down = fb // n
    height = down + 2 * each
    assert n == 4 and fb == d and height == 3 * each
    heads = att.shape[1] // HEAD
    middle = tiles * blocks
    r = lambda s: jnp.where(s < tiles, s, lax.rem(s - tiles, tiles))
    j = lambda s: jnp.clip(lax.div(s - tiles, tiles), 0, blocks - 1)
    edge = lambda s: jnp.where(s < tiles, s, jnp.where(s < tiles + middle, tiles - 1, s - tiles - middle))
    before = lambda s: jnp.minimum(s, tiles - 1)
    after = lambda s: jnp.maximum(s - tiles - middle, 0)
    tile = lambda f, w=d: pl.BlockSpec((bt, w), lambda s: (f(s), 0))
    fixed = lambda which, *shape: pl.BlockSpec((1, *shape), lambda s: (which, 0, 0), pipeline_mode=pl.Buffered(1))
    square, up_square, wide, tall = fixed(layer, d, d), fixed(layer + 1, d, d), fixed(layer, d, ff), fixed(layer, ff, d)
    mlp = [square, wide, wide, tall]
    w4 = [weights[name] for name in ("wo", "w_gate", "w_up", "w_down")]
    last = upper is None
    if last:
        ins = [tile(before), tile(edge), tile(before), *mlp]
        args = [h, att, by, *w4]
    else:
        hn, dq, dk, dv = upper
        table = pl.BlockSpec((bt, HEAD), lambda s: (before(s), 0))
        block = pl.BlockSpec((1, bt, fb), lambda s: (j(s), r(jnp.clip(s, tiles, tiles + middle - 1)), 0))
        ins = [tile(edge), tile(after), *[tile(before)] * 5, up_square, up_square, up_square, table, table, block, block, *mlp]
        args = [h, att, hn, dq, dk, dv, by, weights["wq"], weights["wk"], weights["wv"], *rope, *hidden, *w4]
    anywhere = pl.BlockSpec(memory_space=pl.ANY)
    outs = [
        (tile(after), jax.ShapeDtypeStruct((t, d), BF16)),
        (tile(after), jax.ShapeDtypeStruct((t, d), BF16)),
        (pl.BlockSpec((heads, bt), lambda s: (0, after(s))), jax.ShapeDtypeStruct((heads, t), F32)),
        (anywhere, jax.ShapeDtypeStruct((n, height, d), BF16)),
        (anywhere, jax.ShapeDtypeStruct((n, each, d), BF16)),
        *[(pl.BlockSpec((height, d), lambda s: (0, 0)), jax.ShapeDtypeStruct((height, d), BF16))] * (blocks - 1),
    ]
    scratch = [pltpu.VMEM((t, d), BF16)] * (2 + last) + [pltpu.VMEM((t, fb), BF16)] * 3 + [pltpu.VMEM((t, d), F32)] * 2
    scratch += [pltpu.VMEM((blocks, n, height, d), BF16), pltpu.VMEM((n, each, d), BF16), pltpu.SemaphoreType.DMA((2,))]
    scratch += [pltpu.VMEM((d, d), F32)] * (1 if last else 3)
    for _ in range(blocks - 1):
        scratch += RingSum.scratch(n, height, d)
    if not last:
        outs += [(pl.BlockSpec((3 * each, d), lambda s: (0, 0)), jax.ShapeDtypeStruct((3 * each, d), BF16))]
        scratch += RingSum.scratch(n, 3 * each, d)
    return _call(
        functools.partial(_mlp_back, n=n, tiles=tiles, blocks=blocks, last=last),
        (2 * tiles + middle,),
        ins,
        outs,
        scratch,
        args,
        2 * t * d * (ff * 8 + d * 4),
        sum(a.size * a.dtype.itemsize for a in args),
        collective=number,
    )


def _last_back(h_ref, dq_ref, dk_ref, dv_ref, cos, sin, *refs, n, pieces, count):
    own_in, (own_ref, factor_ref) = refs[:pieces], refs[pieces : pieces + 2]
    h_s, dq_s, dk_s, dv_s, cos_s, sin_s, a_s, g_s, squares, total_s, others_s, load_sem, out_sem, swap_out, swap_in = refs[pieces + 2 : pieces + 17]
    rest = refs[pieces + 17 :]
    pieces_s, rest = rest[:pieces], rest[pieces:]
    jobs = [RingSum(n, g_s.at[i], *rest[4 * i : 4 * i + 4]) for i in range(3)]
    me, right, far, left = _ring(n)
    barrier = pltpu.get_barrier_semaphore()
    for other in (right, far, left):
        pl.semaphore_signal(barrier, inc=1, device_id={"dp": other}, device_id_type=pl.DeviceIdType.MESH)
    pairs = [(h_ref, h_s), (dv_ref, dv_s), (dk_ref, dk_s), (cos, cos_s), (sin, sin_s), (dq_ref, dq_s), *zip(own_in, pieces_s, strict=True)]
    loads = [pltpu.make_async_copy(s, d, load_sem.at[i]) for i, (s, d) in enumerate(pairs)]
    for load in loads:
        load.start()
    t = h_s.shape[0]
    squares[...] = jnp.zeros_like(squares)
    loads[0].wait()

    def norm(rows):
        h = h_s[rows, :].astype(F32)
        a_s[rows, :] = (h * _norm_scale(h)).astype(BF16)

    _rows_loop(t, norm, 256)

    def turn(ref):
        def one(rows):
            ref[rows, :] = _turn(ref[rows, :].astype(F32), cos_s[rows, :], -sin_s[rows, :]).astype(BF16)

        _rows_loop(t, one, 256)

    loads[1].wait()
    _cut(g_s.at[2], 0, _dot(a_s[...], dv_s[...], 0, 0))
    pl.semaphore_wait(barrier, 3)
    for i in (2, 3, 4):
        loads[i].wait()
    turn(dk_s)
    jobs[2].start()
    _cut(g_s.at[1], 0, _dot(a_s[...], dk_s[...], 0, 0))
    loads[5].wait()
    turn(dq_s)
    jobs[1].start()
    jobs[2].add()
    _cut(g_s.at[0], 0, _dot(a_s[...], dq_s[...], 0, 0))
    jobs[2].forward()
    jobs[1].add()
    jobs[0].start()
    for i, piece in enumerate(pieces_s):
        loads[6 + i].wait()
        if i == pieces // 2:
            jobs[1].forward()
        _rows_loop(piece.shape[0], lambda rows, piece=piece: _add_squares(squares, piece[rows, :]))
    jobs[0].add()
    each = g_s.shape[2]
    jobs[2].finish(own_ref.at[pl.ds(2 * each, each)], squares)
    jobs[0].forward()
    jobs[1].finish(own_ref.at[pl.ds(each, each)], squares)
    jobs[0].finish(own_ref.at[pl.ds(0, each)], squares)
    total_s[...] = sum(squares[:, i : i + 128] for i in range(0, squares.shape[1], 128))
    swaps = [
        pltpu.make_async_remote_copy(src_ref=total_s, dst_ref=others_s.at[i], send_sem=swap_out.at[i], recv_sem=swap_in.at[i], device_id={"dp": other},
                                     device_id_type=pl.DeviceIdType.MESH)
        for i, other in enumerate((right, far, left))
    ]
    for s in swaps:
        s.start()
    for s in swaps:
        s.wait()
    everything = jnp.sum(total_s[...] + others_s[0] + others_s[1] + others_s[2], keepdims=True)
    factor_ref[...] = jnp.broadcast_to(jnp.minimum(1.0, 0.5 * lax.rsqrt(everything / count + 1e-30)), factor_ref.shape)


def last_back(n, number, h, dq, dk, dv, rope, own, count):
    t, d = h.shape
    each = d // n
    anywhere, here = pl.BlockSpec(memory_space=pl.ANY), pl.BlockSpec(memory_space=pltpu.VMEM)
    scratch = [pltpu.VMEM((t, d), BF16)] * 4 + [pltpu.VMEM((t, HEAD), F32)] * 2
    scratch += [pltpu.VMEM((t, d), BF16), pltpu.VMEM((3, n, each, d), BF16), pltpu.VMEM((8, d), F32), pltpu.VMEM((8, 128), F32),
                pltpu.VMEM((3, 8, 128), F32), pltpu.SemaphoreType.DMA((6 + len(own),)), pltpu.SemaphoreType.DMA((2,)),
                pltpu.SemaphoreType.DMA((3,)), pltpu.SemaphoreType.DMA((3,))]
    scratch += [pltpu.VMEM(o.shape, BF16) for o in own]
    for _ in range(3):
        scratch += RingSum.scratch(n, each, d)
    return _call(
        functools.partial(_last_back, n=n, pieces=len(own), count=count),
        (),
        [anywhere] * (6 + len(own)),
        [(here, jax.ShapeDtypeStruct((3 * each, d), BF16)), (here, jax.ShapeDtypeStruct((8, 128), F32))],
        scratch,
        (h, dq, dk, dv, *rope, *own),
        6 * t * d * d,
        8 * t * d,
        collective=number,
    )


def _update(w, m, v, g):
    m = 0.9 * m + 0.1 * g
    v = 0.95 * v + 0.05 * g * g
    return (w - 0.02 * (m * lax.rsqrt(v + 1e-8) + 0.1 * w)).astype(BF16), m, v


def _adamw(_, factor_ref, *refs, n, blocks, layers):
    per = blocks + 1
    own, rest = refs[: layers * per], refs[layers * per :]
    w, m, v, new, m_out, v_out = (rest[7 * i : 7 * i + 7] for i in range(6))
    factor = factor_ref[0:1, 0:1]

    def one(i, g, at, at_w, at_new):
        new[i][at_new], m_out[i][at], v_out[i][at] = _update(w[i][at_w].astype(F32), m[i][at], v[i][at], g.astype(F32) * factor)

    for layer in range(layers):
        *ff, qkv = own[layer * per : layer * per + per]
        for i in range(3):
            one(i, qkv[i], (layer,), (layer, 0), (layer,))
        one(3, ff[-1][3], (layer,), (layer, 0), (layer,))
        for i in (4, 5):
            width = ff[0].shape[2] // n
            for d in range(n):
                for b in range(blocks):
                    at = slice((d * blocks + b) * width, (d * blocks + b + 1) * width)
                    one(i, ff[b][i - 3, :, d * width : (d + 1) * width], (layer, slice(None), at), (layer, 0, slice(None), at), (layer, slice(None), at))
        for b in range(blocks):
            one(6, ff[b][0], (layer, b), (layer, 0, b), (layer, b))


def adamw(n, factor, own, weights, m, v):
    layers = weights[0].shape[0]
    d, ff = weights[4].shape[1:]
    each, blocks = d // n, n
    deep = 16
    steps = each // deep
    cube = lambda a: a.reshape(a.shape[0] // each, each, d)
    flat = [cube(a) for one in own for a in one]
    five = lambda w: w.reshape(layers, n, blocks, each, d)
    me = lax.axis_index("dp").astype(jnp.int32)[None]
    w_in = [*(w.reshape(layers, n, each, w.shape[2]) for w in weights[:6]), five(weights[6])]
    four = lambda a: a.reshape(layers, blocks, each, d)
    thin, thick, down = (pl.BlockSpec(s, f) for s, f in (
        ((layers, deep, d), lambda s, me: (0, s, 0)),
        ((layers, deep, ff), lambda s, me: (0, s, 0)),
        ((layers, blocks, deep, d), lambda s, me: (0, 0, s, 0)),
    ))
    state = [thin] * 4 + [thick] * 2 + [down]
    w_specs = [pl.BlockSpec((layers, 1, deep, w), lambda s, me: (0, me[0], s, 0)) for w in (d, d, d, d, ff, ff)]
    w_specs += [pl.BlockSpec((layers, 1, blocks, deep, d), lambda s, me: (0, me[0], 0, s, 0))]
    pieces = [pl.BlockSpec((a.shape[0], deep, d), lambda s, me: (0, s, 0)) for a in flat]
    m_in, v_in = [*m[:6], four(m[6])], [*v[:6], four(v[6])]
    shapes = [jax.ShapeDtypeStruct(a.shape, F32) for a in m_in]
    out = pl.pallas_call(
        functools.partial(_adamw, n=n, blocks=blocks, layers=layers),
        grid_spec=pltpu.PrefetchScalarGridSpec(
            num_scalar_prefetch=1,
            grid=(steps,),
            in_specs=[pl.BlockSpec((8, 128), lambda s, me: (0, 0)), *pieces, *w_specs, *state, *state],
            out_specs=state * 3,
        ),
        out_shape=[*(jax.ShapeDtypeStruct(s.shape, BF16) for s in shapes), *shapes, *shapes],
        compiler_params=pltpu.CompilerParams(dimension_semantics=("arbitrary",), vmem_limit_bytes=VMEM),
        cost_estimate=pl.CostEstimate(flops=20 * sum(a.size for a in m), transcendentals=0, bytes_accessed=20 * sum(a.size for a in m)),
    )(me, factor, *flat, *w_in, *m_in, *v_in)
    new, m_new, v_new = out[:7], out[7:14], out[14:]
    return new, [*m_new[:6], m_new[6].reshape(m[6].shape)], [*v_new[:6], v_new[6].reshape(v[6].shape)]


def _gather(*refs, n, units):
    parts, outs, lands = refs[:7], refs[7:14], refs[14:21]
    load_sem, store_sem, out_r, out_l, in_l, in_r, pass_r, pass_l, far_l, far_r = refs[21:]
    me, right, far, left = _ring(n)
    remote = lambda src, to, sent, got: pltpu.make_async_remote_copy(
        src_ref=src, dst_ref=src, send_sem=sent, recv_sem=got, device_id={"dp": to}, device_id_type=pl.DeviceIdType.MESH)
    _greet(n)

    def view(which, unit):
        i, layer, at, rows = unit
        return lands[i].at[layer, which, pl.ds(at, rows)]

    loads = [pltpu.make_async_copy(parts[i].at[layer, pl.ds(at, rows)], view(me, (i, layer, at, rows)), load_sem.at[u])
             for u, (i, layer, at, rows) in enumerate(units)]
    for load in loads:
        load.start()

    def store(which, kind, u):
        i, layer, at, rows = units[u]
        return pltpu.make_async_copy(view(which, units[u]), outs[i].at[layer, which, pl.ds(at, rows)], store_sem.at[kind, u])

    _met()
    sends = []
    for u, unit in enumerate(units):
        loads[u].wait()
        mine = view(me, unit)
        sends.append((remote(mine, right, out_r.at[u], in_l.at[u]), remote(mine, left, out_l.at[u], in_r.at[u])))
        for s in sends[-1]:
            s.start()
        store(me, 0, u).start()
    passes = []
    for u, (i, layer, at, rows) in enumerate(units):
        half = rows // 2
        sends[u][0].wait_recv()
        first = remote(lands[i].at[layer, left, pl.ds(at, half)], right, pass_r.at[u], far_l.at[u])
        first.start()
        store(left, 1, u).start()
        sends[u][1].wait_recv()
        second = remote(lands[i].at[layer, right, pl.ds(at + half, half)], left, pass_l.at[u], far_r.at[u])
        second.start()
        store(right, 2, u).start()
        passes.append((first, second))
    for u in range(len(units)):
        for p in passes[u]:
            p.wait_recv()
        store(far, 3, u).start()
    for u in range(len(units)):
        for c in (*sends[u], *passes[u]):
            c.wait_send()
        for kind, which in enumerate((me, left, right, far)):
            store(which, kind, u).wait()


def gather(n, number, parts):
    layers = parts[0].shape[0]
    parts = [p.reshape(layers, -1, p.shape[-1]) for p in parts]
    shapes = [(layers, n, *p.shape[1:]) for p in parts]
    units = []
    for i in (6, 4, 5, 0, 1, 2, 3):
        rows = parts[i].shape[1]
        units += [(i, layer, 0, rows) for layer in range(layers)]
    count = len(units)
    anywhere = pl.BlockSpec(memory_space=pl.ANY)
    out = _call(
        functools.partial(_gather, n=n, units=units),
        (),
        [anywhere] * 7,
        [(anywhere, jax.ShapeDtypeStruct(s, BF16)) for s in shapes],
        [*(pltpu.VMEM(s, BF16) for s in shapes), pltpu.SemaphoreType.DMA((count,)), pltpu.SemaphoreType.DMA((4, count)),
         *[pltpu.SemaphoreType.DMA((count,))] * 8],
        parts,
        0,
        2 * sum(p.size for p in parts) * n,
        collective=number,
    )
    return [o.reshape(layers, -1, o.shape[-1]) for o in out]


NAMES = ("wq", "wk", "wv", "wo", "w_gate", "w_up", "w_down")


def rope_tables(t):
    half = HEAD // 2
    angle = np.arange(t, dtype=np.float32)[:, None] * (np.float32(THETA) ** (-np.arange(half, dtype=np.float32) / half)).astype(np.float32)
    cos, sin = np.cos(angle.astype(np.float64)).astype(np.float32), np.sin(angle.astype(np.float64)).astype(np.float32)
    return jnp.asarray(np.concatenate([cos, cos], 1)), jnp.asarray(np.concatenate([-sin, sin], 1))


def first(h, weights, rope):
    t, d = h.shape
    bt = _tile(t)
    tile, table = pl.BlockSpec((bt, d), lambda s: (s, 0)), pl.BlockSpec((bt, HEAD), lambda s: (s, 0))
    square = pl.BlockSpec((1, d, d), lambda s: (0, 0, 0))
    one = (tile, jax.ShapeDtypeStruct((t, d), BF16))
    return _call(_first, (t // bt,), [tile, square, square, square, table, table], [one] * 3, [],
                 (h, weights["wq"], weights["wk"], weights["wv"], *rope), 6 * t * d * d, 8 * t * d)


def between(n, layer, h, att, weights, rope):
    t, d = h.shape
    ff = weights["w_gate"].shape[2]
    bt = _tile(t)
    at = lambda k, *shape: pl.BlockSpec((1, *shape), lambda s: (k, 0, 0))
    tile, table = (pl.BlockSpec((bt, w), lambda s: (s, 0)) for w in (d, HEAD))
    one = (tile, jax.ShapeDtypeStruct((t, d), BF16))
    two = (pl.BlockSpec((n, bt, ff // n), lambda s: (0, s, 0)), jax.ShapeDtypeStruct((n, t, ff // n), F32))
    return _call(
        functools.partial(_between, n=n),
        (t // bt,),
        [tile, tile, at(layer, d, d), at(layer, d, ff), at(layer, d, ff), at(layer, ff, d), *[at(layer + 1, d, d)] * 3, table, table],
        [one, one, two, two, one, one, one],
        [],
        (h, att, *(weights[name] for name in ("wo", "w_gate", "w_up", "w_down", "wq", "wk", "wv")), *rope),
        2 * t * d * (4 * d + 3 * ff),
        14 * t * d + 8 * t * ff,
    )


def solution(mesh):
    n = mesh.shape["dp"]

    def step(x, dy, *arrays):
        weights = dict(zip(NAMES, arrays[:7], strict=True))
        m, v = arrays[7:14], arrays[14:]
        layers = weights["wq"].shape[0]
        h = x[0]
        rope = rope_tables(h.shape[0])
        hs, atts, qkvs, lses, mids, hidden = [h], [], [], [], [], []
        q, k, v_ = first(h, weights, rope)
        for layer in range(layers):
            qkvs.append((q, k, v_))
            att, lse = attend(q, k, v_)
            atts.append(att)
            lses.append(lse)
            if layer < layers - 1:
                h1, h, gate, up, q, k, v_ = between(n, layer, h, att, weights, rope)
                hs.append(h)
                mids.append(h1)
                hidden.append((gate, up))
        blocks = n
        ff_own, qkv_own = {}, {}
        by, upper, number = dy[0], None, 0
        for layer in reversed(range(layers)):
            if upper is None:
                got = mlp_back(n, number, layer, hs[layer], atts[layer], by, weights, rope)
            else:
                got = mlp_back(n, number, layer, mids[layer], atts[layer], by, weights, rope, upper, hidden[layer])
                qkv_own[layer + 1] = got[5 + blocks - 1]
            by, datt, delta, left_ff, left_o = got[:5]
            dq, dk, dv, rest = attend_back(n, number + 1, *qkvs[layer], datt, lses[layer], delta, left_ff, left_o)
            ff_own[layer] = [*got[5 : 5 + blocks - 1], rest]
            upper = hs[layer], dq, dk, dv
            number += 2
        pieces = [p for layer in range(layers) for p in (*ff_own[layer], *([qkv_own[layer]] if layer else []))]
        qkv_own[0], factor = last_back(n, number, *upper, rope, pieces, n * sum(one.size for one in m))
        new, m, v = adamw(n, factor, [[*ff_own[layer], qkv_own[layer]] for layer in range(layers)], arrays[:7], m, v)
        return (*gather(n, number + 1, new), *m, *v)

    states, all_of, cut = P(("rep", "dp"), None, None), P(None, None, None), P(None, "dp", None)
    return jax.shard_map(
        step,
        mesh=mesh,
        in_specs=(states, states) + (all_of,) * 7 + (cut,) * 14,
        out_specs=(P("rep", None, None),) * 7 + (P("rep", "dp", None),) * 14,
        check_vma=False,
    )
```

```python
import functools

import jax
import jax.numpy as jnp
import numpy as np
from jax import lax
from jax.experimental import pallas as pl
from jax.experimental.pallas import tpu as pltpu
from jax.sharding import PartitionSpec as P

F32, BF16 = jnp.float32, jnp.bfloat16
HEAD = 128
THETA = 10000
NEG = -1e30
HIDDEN = 2 * NEG
LOG2E = 1.4426950408889634
SCALE = HEAD**-0.5
VMEM = 67043328


def _dot(a, b, ca=1, cb=0):
    return lax.dot_general(a, b, (((ca,), (cb,)), ((), ())), preferred_element_type=F32)


def _tile(size, most=512):
    return max(n for n in range(128, most + 1, 128) if size % n == 0)


def _call(kernel, grid, ins, outs, scratch, args, flops, moved, collective=None):
    return pl.pallas_call(
        kernel,
        grid=grid,
        in_specs=[spec for spec in ins],
        out_specs=[spec for spec, _ in outs],
        out_shape=[shape for _, shape in outs],
        scratch_shapes=scratch,
        compiler_params=pltpu.CompilerParams(dimension_semantics=("arbitrary",) * len(grid), vmem_limit_bytes=VMEM, collective_id=collective,
                                             has_side_effects=collective is not None),
        cost_estimate=pl.CostEstimate(flops=int(flops), transcendentals=0, bytes_accessed=int(moved)),
    )(*args)


def _norm_scale(x):
    return lax.rsqrt(jnp.mean(x * x, -1, keepdims=True) + 1e-6)


def _norm_back(x, d_out):
    s = _norm_scale(x)
    inner = jnp.mean(x * d_out, -1, keepdims=True)
    return s * d_out - x * (s * s * s * inner)


def _turn(x, cos, sin):
    parts = [x[:, n : n + HEAD] for n in range(0, x.shape[1], HEAD)]
    return jnp.concatenate([p * cos + pltpu.roll(p, HEAD // 2, 1) * sin for p in parts], 1)


def _qkv(h, wq, wk, wv, cos, sin, q_ref, k_ref, v_ref):
    a = (h * _norm_scale(h)).astype(BF16)
    q_ref[...] = _turn(_dot(a, wq).astype(BF16).astype(F32), cos, sin).astype(BF16)
    k_ref[...] = _turn(_dot(a, wk).astype(BF16).astype(F32), cos, sin).astype(BF16)
    v_ref[...] = _dot(a, wv).astype(BF16)


def _first(h_ref, wq, wk, wv, cos, sin, q_ref, k_ref, v_ref):
    _qkv(h_ref[...].astype(F32), wq[0], wk[0], wv[0], cos[...], sin[...], q_ref, k_ref, v_ref)


def _after_attention(h_ref, att_ref, wo):
    return (h_ref[...].astype(F32) + _dot(att_ref[...], wo).astype(BF16).astype(F32)).astype(BF16)


def _between(h_ref, att_ref, wo, wg, wu, wd, wq, wk, wv, cos, sin, h1_ref, y_ref, gate_ref, up_ref, q_ref, k_ref, v_ref, *, n):
    h1 = _after_attention(h_ref, att_ref, wo[0])
    h1_ref[...] = h1
    h1 = h1.astype(F32)
    b = (h1 * _norm_scale(h1)).astype(BF16)
    total = jnp.zeros(h1.shape, F32)
    for j in range(n):
        gate, up = _dot(b, _strips(wg, j, n, n, 2)), _dot(b, _strips(wu, j, n, n, 2))
        gate_ref[j] = gate
        up_ref[j] = up
        total += _dot((gate * jax.nn.sigmoid(gate) * up).astype(BF16), _strips(wd, j, n, n, 1))
    y = (h1 + total.astype(BF16).astype(F32)).astype(BF16)
    y_ref[...] = y
    _qkv(y.astype(F32), wq[0], wk[0], wv[0], cos[...], sin[...], q_ref, k_ref, v_ref)


def _seen(keys, queries):
    return lax.broadcasted_iota(jnp.int32, (keys, queries), 1) >= lax.broadcasted_iota(jnp.int32, (keys, queries), 0)


def diagonal(block, first, size, part=256):
    part = min(part, size)
    for at in range(0, size, part):
        block(first + at, part, at, True)


def _attend(q_ref, k_ref, v_ref, o_ref, lse_ref, top_s, mix_s, *, bk):
    iq = pl.program_id(0)
    bq = q_ref.shape[0]
    heads = q_ref.shape[1] // HEAD
    e = SCALE * LOG2E
    top_s[...] = jnp.full(top_s.shape, NEG, F32)
    mix_s[...] = jnp.zeros(mix_s.shape, F32)

    def block(first, keys, at, masked):
        here, ask = pl.ds(pl.multiple_of(first, keys), keys), slice(at, bq)
        cols = [slice(n * HEAD, (n + 1) * HEAD) for n in range(heads)]
        scores = [_dot(k_ref[here, c], q_ref[ask, c], 1, 1) for c in cols]
        weights, keeps = [], []
        seen = _seen(keys, bq - at) if masked else None
        for n, s in enumerate(scores):
            if masked:
                s = jnp.where(seen, s, HIDDEN)
            old = top_s[n : n + 1, ask]
            top = jnp.maximum(old, s.max(axis=0, keepdims=True))
            top_s[n : n + 1, ask] = top
            weights.append(jnp.exp2((s - top) * e).astype(BF16))
            keeps.append(jnp.exp2((old - top) * e))
        ones = jnp.ones((8, keys), BF16)
        for n, (c, p, keep) in enumerate(zip(cols, weights, keeps)):
            values = jnp.concatenate([v_ref[here, c].T, ones], axis=0)
            mix_s[n, :, ask] = mix_s[n, :, ask] * keep + _dot(values, p, 1, 0)

    lax.fori_loop(0, iq * (bq // bk), lambda j, _: block(j * bk, bk, 0, False), None)
    diagonal(block, iq * bq, bq)
    for n in range(heads):
        total = mix_s[n, HEAD : HEAD + 1, :]
        o_ref[:, n * HEAD : (n + 1) * HEAD] = (mix_s[n, :HEAD, :] * (1 / total)).T.astype(BF16)
        lse_ref[n : n + 1, :] = top_s[n : n + 1, :] * e + jnp.log2(total)


def attend(q, k, v):
    t, width = q.shape
    heads = width // HEAD
    bq = bk = _tile(t)
    rows, whole = pl.BlockSpec((bq, width), lambda i: (i, 0)), pl.BlockSpec((t, width), lambda i: (0, 0))
    return _call(
        functools.partial(_attend, bk=bk),
        (t // bq,),
        [rows, whole, whole],
        [(rows, jax.ShapeDtypeStruct((t, width), BF16)), (pl.BlockSpec((heads, bq), lambda i: (0, i)), jax.ShapeDtypeStruct((heads, t), F32))],
        [pltpu.VMEM((heads, bq), F32), pltpu.VMEM((heads, HEAD + 8, bq), F32)],
        (q, k, v),
        2 * t * t * width,
        8 * t * width,
    )


def _ring(n):
    me = lax.axis_index("dp")
    return me, lax.rem(me + 1, n), lax.rem(me + 2, n), lax.rem(me + n - 1, n)


def _greet(n):
    _, right, _, left = _ring(n)
    barrier = pltpu.get_barrier_semaphore()
    for other in (right, left):
        pl.semaphore_signal(barrier, inc=1, device_id={"dp": other}, device_id_type=pl.DeviceIdType.MESH)


def _met():
    pl.semaphore_wait(pltpu.get_barrier_semaphore(), 2)


def _rows_loop(rows, body, most=32):
    each = max(c for c in range(16, most + 1, 16) if rows % c == 0)
    lax.fori_loop(0, rows // each, lambda i, _: body(pl.ds(pl.multiple_of(i * each, each), each)), None)


class RingSum:
    def __init__(self, n, block, passing, arrived, sent, got):
        self.block, self.passing, self.arrived = block, passing, arrived
        self.me, right, far, left = _ring(n)
        self.near = right, left
        half = block.shape[1] // 2
        self.half = half
        a, b = pl.ds(0, half), pl.ds(half, half)
        moves = [
            (block.at[far, a], passing.at[0], right),
            (block.at[far, b], passing.at[1], left),
            (block.at[right, b], arrived.at[0, b], right),
            (block.at[left, a], arrived.at[1, a], left),
            (passing.at[0], arrived.at[0, a], right),
            (passing.at[1], arrived.at[1, b], left),
        ]
        self.copies = [
            pltpu.make_async_remote_copy(src_ref=s, dst_ref=d, send_sem=sent.at[i], recv_sem=got.at[i], device_id={"dp": to},
                                         device_id_type=pl.DeviceIdType.MESH)
            for i, (s, d, to) in enumerate(moves)
        ]

    @staticmethod
    def scratch(n, rows, columns):
        half = pltpu.VMEM((2, rows // 2, columns), BF16)
        return [half, pltpu.VMEM((2, rows, columns), BF16), pltpu.SemaphoreType.DMA((6,)), pltpu.SemaphoreType.DMA((6,))]

    def start(self):
        for c in self.copies[:4]:
            c.start()

    def add(self):
        for c in self.copies[:2]:
            c.wait_recv()
        for i, other in enumerate(self.near):

            def one(rows, i=i, other=other):
                mine = self.block[other, pl.ds(rows.start + i * self.half, rows.size), :]
                self.passing[i, rows, :] = (self.passing[i, rows, :].astype(F32) + mine.astype(F32)).astype(BF16)

            _rows_loop(self.half, one)

    def forward(self):
        for c in self.copies[4:]:
            c.start()

    def finish(self, out, squares=None):
        for c in self.copies[2:]:
            c.wait_recv()

        def one(rows):
            total = self.block[self.me, rows, :].astype(F32) + self.arrived[0, rows, :].astype(F32) + self.arrived[1, rows, :].astype(F32)
            total = total.astype(BF16)
            out[rows, :] = total
            if squares is not None:
                _add_squares(squares, total)

        _rows_loop(self.half * 2, one)
        for c in self.copies:
            c.wait_send()


def _add_squares(squares, value):
    value = value.astype(F32)
    value = value * value
    squares[...] += sum(value[i : i + 8] for i in range(0, value.shape[0], 8))


def _attend_back(q_ref, k_ref, v_ref, do_ref, lse_ref, delta_ref, ff_ref, o_ref, dq_ref, dk_ref, dv_ref, own_ref, dq_s, dk_s, dv_s, block_s, load_sem,
                 *ring, bk, n):
    iq = pl.program_id(0)
    bq = q_ref.shape[0]
    heads = q_ref.shape[1] // HEAD
    e = SCALE * LOG2E
    steps = pl.num_programs(0)
    split = ff_ref.shape[1]
    loads = [
        pltpu.make_async_copy(ff_ref, block_s.at[:, pl.ds(0, split)], load_sem.at[0]),
        pltpu.make_async_copy(o_ref, block_s.at[:, pl.ds(split, o_ref.shape[1])], load_sem.at[1]),
    ]
    job = RingSum(n, block_s, *ring)

    @pl.when(iq == 0)
    def _():
        _greet(n)
        for load in loads:
            load.start()
        dk_s[...] = jnp.zeros_like(dk_s)
        dv_s[...] = jnp.zeros_like(dv_s)
        for load in loads:
            load.wait()
        _met()
        job.start()

    @pl.when(iq == steps - 2)
    def _():
        job.forward()

    dq_s[...] = jnp.zeros_like(dq_s)

    def block(first, keys, at, masked):
        here, ask = pl.ds(pl.multiple_of(first, keys), keys), slice(at, bq)
        cols = [slice(i * HEAD, (i + 1) * HEAD) for i in range(heads)]
        scores = [_dot(k_ref[here, c], q_ref[ask, c], 1, 1) for c in cols]
        dps = [_dot(v_ref[here, c], do_ref[ask, c], 1, 1) for c in cols]
        seen = _seen(keys, bq - at) if masked else None
        for i, c in enumerate(cols):
            p = jnp.exp2(scores[i] * e - lse_ref[i : i + 1, ask])
            if masked:
                p = jnp.where(seen, p, 0.0)
            ds = (p * (dps[i] - delta_ref[i : i + 1, ask])).astype(BF16)
            dv_s[here, c] += _dot(p.astype(BF16), do_ref[ask, c], 1, 0)
            dk_s[here, c] += _dot(ds, q_ref[ask, c], 1, 0)
            dq_s[i, :, ask] += _dot(k_ref[here, c].T, ds, 1, 0)

    lax.fori_loop(0, iq * (bq // bk), lambda j, _: block(j * bk, bk, 0, False), None)
    diagonal(block, iq * bq, bq)

    @pl.when(iq == steps - 3)
    def _():
        job.add()

    for i in range(heads):
        dq_ref[:, i * HEAD : (i + 1) * HEAD] = (dq_s[i] * SCALE).T.astype(BF16)

    @pl.when(iq == steps - 1)
    def _():
        dk_ref[...] = (dk_s[...] * SCALE).astype(BF16)
        dv_ref[...] = dv_s[...].astype(BF16)
        job.finish(own_ref)


def attend_back(n, number, q, k, v, d_out, lse, delta, ff, o):
    t, width = q.shape
    heads = width // HEAD
    bq = bk = _tile(t)
    rows, whole = pl.BlockSpec((bq, width), lambda i: (i, 0)), pl.BlockSpec((t, width), lambda i: (0, 0))
    stats = pl.BlockSpec((heads, bq), lambda i: (0, i))
    one = jax.ShapeDtypeStruct((t, width), BF16)
    height, columns = ff.shape[1] + o.shape[1], ff.shape[2]
    return _call(
        functools.partial(_attend_back, bk=bk, n=n),
        (t // bq,),
        [rows, whole, whole, rows, stats, stats, pl.BlockSpec(memory_space=pl.ANY), pl.BlockSpec(memory_space=pl.ANY)],
        [(rows, one), (whole, one), (whole, one),
         (pl.BlockSpec((height, columns), lambda i: (0, 0)), jax.ShapeDtypeStruct((height, columns), BF16))],
        [pltpu.VMEM((heads, HEAD, bq), F32), pltpu.VMEM((t, width), F32), pltpu.VMEM((t, width), F32),
         pltpu.VMEM((n, height, columns), BF16), pltpu.SemaphoreType.DMA((2,)), *RingSum.scratch(n, height, columns)],
        (q, k, v, d_out, lse, delta, ff, o),
        5 * t * t * width,
        14 * t * width,
        collective=number,
    )


def _strips(ref, block, n, blocks, axis):
    width = ref.shape[axis] // (n * blocks)
    at = [pl.ds(pl.multiple_of((d * blocks + block) * width, width), width) for d in range(n)]
    return jnp.concatenate([ref[0, :, a] if axis == 2 else ref[0, a, :] for a in at], axis - 1)


def _qkv_back(h, dq, dk, dv, wq, wk, wv, cos, sin, sums):
    a = (h * _norm_scale(h)).astype(BF16)
    dq, dk = (_turn(d.astype(F32), cos, -sin).astype(BF16) for d in (dq, dk))
    for s, d in zip(sums, (dq, dk, dv), strict=True):
        s[...] += _dot(a, d, 0, 0)
    return sum(_dot(d, w, 1, 1).astype(BF16).astype(F32) for d, w in ((dq, wq), (dk, wk), (dv, wv)))


def _cut(ref, at, value):
    n = ref.shape[0]
    each = value.shape[0] // n
    for d in range(n):
        ref[d, at : at + each] = value[d * each : (d + 1) * each].astype(BF16)


def _mlp_back(*refs, n, tiles, blocks, last):
    take = iter(range(len(refs)))
    some = lambda count: [refs[next(take)] for _ in range(count)]
    h_ref, att_ref = some(2)
    if last:
        (dy_ref,) = some(1)
    else:
        hn_ref, dq_ref, dk_ref, dv_ref, dh_ref, wq, wk, wv, cos, sin, gate_ref, up_ref = some(12)
    wo, wg, wu, wd = some(4)
    dh1_ref, datt_ref, delta_ref, left_ff, left_o = some(5)
    own = some(blocks - 1 + (not last))
    h1_s = some(1)[0] if last else None
    b_s, dy_s, p_s, dg_s, du_s, sum_g, sum_u, g_s, go_s, out_sem = some(10)
    sums3 = some(1 if last else 3)
    sum_o = sums3[0]
    jobs = []
    for i in range(len(own)):
        if i < blocks - 1:
            block = g_s.at[i]
        else:
            block = gqkv_s = g_s.at[blocks - 1]
        jobs.append(RingSum(n, block, *some(4)))
    step = pl.program_id(0)
    bt = h_ref.shape[0]
    middle = tiles * blocks
    r = jnp.where(step < tiles, step, lax.rem(step - tiles, tiles))
    j = lax.div(step - tiles, tiles)
    rows = pl.ds(pl.multiple_of(r * bt, bt), bt)
    wait, final = tiles, 2 * tiles + middle - 1

    @pl.when(step == 0)
    def _():
        _greet(n)
        for s in sums3:
            s[...] = jnp.zeros_like(s)

    begin = [tiles * (2 + i) for i in range(blocks - 1)] + [tiles] * (not last)

    @pl.when(step == min(begin))
    def _():
        _met()

    for job, at in zip(jobs, begin, strict=True):

        @pl.when(step == at + wait)
        def _(job=job):
            job.forward()

    for job, at in zip(jobs, begin, strict=True):

        @pl.when(step == at)
        def _(job=job):
            job.start()

    @pl.when(step < tiles)
    def _():
        if last:
            h1 = _after_attention(h_ref, att_ref, wo[0])
            h1_s[rows, :] = h1
            dy_s[rows, :] = dy_ref[...]
        else:
            h1 = h_ref[...]
            hn = hn_ref[...].astype(F32)
            da = _qkv_back(hn, dq_ref[...], dk_ref[...], dv_ref[...], wq[0], wk[0], wv[0], cos[...], sin[...], sums3)
            dy_s[rows, :] = (dh_ref[...].astype(F32) + _norm_back(hn, da.astype(BF16).astype(F32)).astype(BF16).astype(F32)).astype(BF16)

            @pl.when(step == tiles - 1)
            def _():
                for i, s in enumerate(sums3):
                    _cut(gqkv_s, i * (s.shape[0] // n), s[...])
                sum_o[...] = jnp.zeros_like(sum_o)

        h1 = h1.astype(F32)
        b_s[rows, :] = (h1 * _norm_scale(h1)).astype(BF16)
        sum_g[rows, :] = jnp.zeros((bt, sum_g.shape[1]), F32)
        sum_u[rows, :] = jnp.zeros((bt, sum_u.shape[1]), F32)

    @pl.when((step >= tiles) & (step < tiles + middle))
    def _():
        b, dy = b_s[rows, :], dy_s[rows, :]
        gate_w, up_w = _strips(wg, j, n, blocks, 2), _strips(wu, j, n, blocks, 2)
        if last:
            gate, up = _dot(b, gate_w), _dot(b, up_w)
        else:
            gate, up = gate_ref[0], up_ref[0]
        dp = _dot(dy, _strips(wd, j, n, blocks, 1), 1, 1).astype(BF16).astype(F32)
        sg = jax.nn.sigmoid(gate)
        silu = gate * sg
        p_s[rows, :] = (silu * up).astype(BF16)
        du = (dp * silu).astype(BF16)
        dg = (dp * up * (sg + silu * (1 - sg))).astype(BF16)
        du_s[rows, :] = du
        dg_s[rows, :] = dg
        sum_g[rows, :] += _dot(dg, gate_w, 1, 1)
        sum_u[rows, :] += _dot(du, up_w, 1, 1)

        @pl.when(r == tiles - 1)
        def _():
            each = b.shape[1] // n
            mine = g_s.at[j]
            _cut(mine, 0, _dot(p_s[...], dy_s[...], 0, 0))
            _cut(mine, mine.shape[1] - 2 * each, _dot(b_s[...], dg_s[...], 0, 0))
            _cut(mine, mine.shape[1] - each, _dot(b_s[...], du_s[...], 0, 0))

    out_copies = [pltpu.make_async_copy(g_s.at[blocks - 1], left_ff, out_sem.at[0]), pltpu.make_async_copy(go_s, left_o, out_sem.at[1])]

    @pl.when(step >= tiles + middle)
    def _():
        db = sum_g[rows, :].astype(BF16).astype(F32) + sum_u[rows, :].astype(BF16).astype(F32)
        h1 = h1_s[rows, :] if last else h_ref[...]
        dh1 = dy_s[rows, :].astype(F32) + _norm_back(h1.astype(F32), db.astype(BF16).astype(F32)).astype(BF16).astype(F32)
        dh1 = dh1.astype(BF16)
        dh1_ref[...] = dh1
        datt = _dot(dh1, wo[0], 1, 1).astype(BF16)
        datt_ref[...] = datt
        att = att_ref[...]
        both = att.astype(F32) * datt.astype(F32)
        for i in range(both.shape[1] // HEAD):
            delta_ref[i : i + 1, :] = both[:, i * HEAD : (i + 1) * HEAD].T.sum(axis=0, keepdims=True)
        sum_o[...] += _dot(att, dh1, 0, 0)

        @pl.when(step == tiles + middle)
        def _():
            out_copies[0].start()

        @pl.when(step == 2 * tiles + middle - 1)
        def _():
            _cut(go_s, 0, sum_o[...])
            out_copies[1].start()
            for c in out_copies:
                c.wait()

    for job, at in zip(jobs, begin, strict=True):

        @pl.when(step == at + wait - 1)
        def _(job=job):
            job.add()

    for job, at, out in zip(jobs, begin, own, strict=True):

        @pl.when(step == min(at + 2 * wait - 1, final))
        def _(job=job, out=out):
            job.finish(out)


def mlp_back(n, number, layer, h, att, by, weights, rope, upper=None, hidden=None):
    t, d = h.shape
    ff = weights["w_gate"].shape[2]
    bt = _tile(t)
    tiles, blocks = t // bt, n
    fb, each = ff // blocks, d // n
    down = fb // n
    height = down + 2 * each
    assert n == 4 and fb == d and height == 3 * each
    heads = att.shape[1] // HEAD
    middle = tiles * blocks
    r = lambda s: jnp.where(s < tiles, s, lax.rem(s - tiles, tiles))
    j = lambda s: jnp.clip(lax.div(s - tiles, tiles), 0, blocks - 1)
    edge = lambda s: jnp.where(s < tiles, s, jnp.where(s < tiles + middle, tiles - 1, s - tiles - middle))
    before = lambda s: jnp.minimum(s, tiles - 1)
    after = lambda s: jnp.maximum(s - tiles - middle, 0)
    tile = lambda f, w=d: pl.BlockSpec((bt, w), lambda s: (f(s), 0))
    fixed = lambda which, *shape: pl.BlockSpec((1, *shape), lambda s: (which, 0, 0), pipeline_mode=pl.Buffered(1))
    square, up_square, wide, tall = fixed(layer, d, d), fixed(layer + 1, d, d), fixed(layer, d, ff), fixed(layer, ff, d)
    mlp = [square, wide, wide, tall]
    w4 = [weights[name] for name in ("wo", "w_gate", "w_up", "w_down")]
    last = upper is None
    if last:
        ins = [tile(before), tile(edge), tile(before), *mlp]
        args = [h, att, by, *w4]
    else:
        hn, dq, dk, dv = upper
        table = pl.BlockSpec((bt, HEAD), lambda s: (before(s), 0))
        block = pl.BlockSpec((1, bt, fb), lambda s: (j(s), r(jnp.clip(s, tiles, tiles + middle - 1)), 0))
        ins = [tile(edge), tile(after), *[tile(before)] * 5, up_square, up_square, up_square, table, table, block, block, *mlp]
        args = [h, att, hn, dq, dk, dv, by, weights["wq"], weights["wk"], weights["wv"], *rope, *hidden, *w4]
    anywhere = pl.BlockSpec(memory_space=pl.ANY)
    outs = [
        (tile(after), jax.ShapeDtypeStruct((t, d), BF16)),
        (tile(after), jax.ShapeDtypeStruct((t, d), BF16)),
        (pl.BlockSpec((heads, bt), lambda s: (0, after(s))), jax.ShapeDtypeStruct((heads, t), F32)),
        (anywhere, jax.ShapeDtypeStruct((n, height, d), BF16)),
        (anywhere, jax.ShapeDtypeStruct((n, each, d), BF16)),
        *[(pl.BlockSpec((height, d), lambda s: (0, 0)), jax.ShapeDtypeStruct((height, d), BF16))] * (blocks - 1),
    ]
    scratch = [pltpu.VMEM((t, d), BF16)] * (2 + last) + [pltpu.VMEM((t, fb), BF16)] * 3 + [pltpu.VMEM((t, d), F32)] * 2
    scratch += [pltpu.VMEM((blocks, n, height, d), BF16), pltpu.VMEM((n, each, d), BF16), pltpu.SemaphoreType.DMA((2,))]
    scratch += [pltpu.VMEM((d, d), F32)] * (1 if last else 3)
    for _ in range(blocks - 1):
        scratch += RingSum.scratch(n, height, d)
    if not last:
        outs += [(pl.BlockSpec((3 * each, d), lambda s: (0, 0)), jax.ShapeDtypeStruct((3 * each, d), BF16))]
        scratch += RingSum.scratch(n, 3 * each, d)
    return _call(
        functools.partial(_mlp_back, n=n, tiles=tiles, blocks=blocks, last=last),
        (2 * tiles + middle,),
        ins,
        outs,
        scratch,
        args,
        2 * t * d * (ff * 8 + d * 4),
        sum(a.size * a.dtype.itemsize for a in args),
        collective=number,
    )


def _last_back(h_ref, dq_ref, dk_ref, dv_ref, cos, sin, *refs, n, pieces, count):
    own_in, (own_ref, factor_ref) = refs[:pieces], refs[pieces : pieces + 2]
    h_s, dq_s, dk_s, dv_s, cos_s, sin_s, a_s, g_s, squares, total_s, others_s, load_sem, out_sem, swap_out, swap_in = refs[pieces + 2 : pieces + 17]
    rest = refs[pieces + 17 :]
    pieces_s, rest = rest[:pieces], rest[pieces:]
    jobs = [RingSum(n, g_s.at[i], *rest[4 * i : 4 * i + 4]) for i in range(3)]
    me, right, far, left = _ring(n)
    barrier = pltpu.get_barrier_semaphore()
    for other in (right, far, left):
        pl.semaphore_signal(barrier, inc=1, device_id={"dp": other}, device_id_type=pl.DeviceIdType.MESH)
    pairs = [(h_ref, h_s), (dv_ref, dv_s), (dk_ref, dk_s), (cos, cos_s), (sin, sin_s), (dq_ref, dq_s), *zip(own_in, pieces_s, strict=True)]
    loads = [pltpu.make_async_copy(s, d, load_sem.at[i]) for i, (s, d) in enumerate(pairs)]
    for load in loads:
        load.start()
    t = h_s.shape[0]
    squares[...] = jnp.zeros_like(squares)
    loads[0].wait()

    def norm(rows):
        h = h_s[rows, :].astype(F32)
        a_s[rows, :] = (h * _norm_scale(h)).astype(BF16)

    _rows_loop(t, norm, 256)

    def turn(ref):
        def one(rows):
            ref[rows, :] = _turn(ref[rows, :].astype(F32), cos_s[rows, :], -sin_s[rows, :]).astype(BF16)

        _rows_loop(t, one, 256)

    loads[1].wait()
    _cut(g_s.at[2], 0, _dot(a_s[...], dv_s[...], 0, 0))
    pl.semaphore_wait(barrier, 3)
    for i in (2, 3, 4):
        loads[i].wait()
    turn(dk_s)
    jobs[2].start()
    _cut(g_s.at[1], 0, _dot(a_s[...], dk_s[...], 0, 0))
    loads[5].wait()
    turn(dq_s)
    jobs[1].start()
    jobs[2].add()
    _cut(g_s.at[0], 0, _dot(a_s[...], dq_s[...], 0, 0))
    jobs[2].forward()
    jobs[1].add()
    jobs[0].start()
    for i, piece in enumerate(pieces_s):
        loads[6 + i].wait()
        if i == pieces // 2:
            jobs[1].forward()
        _rows_loop(piece.shape[0], lambda rows, piece=piece: _add_squares(squares, piece[rows, :]))
    jobs[0].add()
    each = g_s.shape[2]
    jobs[2].finish(own_ref.at[pl.ds(2 * each, each)], squares)
    jobs[0].forward()
    jobs[1].finish(own_ref.at[pl.ds(each, each)], squares)
    jobs[0].finish(own_ref.at[pl.ds(0, each)], squares)
    total_s[...] = sum(squares[:, i : i + 128] for i in range(0, squares.shape[1], 128))
    swaps = [
        pltpu.make_async_remote_copy(src_ref=total_s, dst_ref=others_s.at[i], send_sem=swap_out.at[i], recv_sem=swap_in.at[i], device_id={"dp": other},
                                     device_id_type=pl.DeviceIdType.MESH)
        for i, other in enumerate((right, far, left))
    ]
    for s in swaps:
        s.start()
    for s in swaps:
        s.wait()
    everything = jnp.sum(total_s[...] + others_s[0] + others_s[1] + others_s[2], keepdims=True)
    factor_ref[...] = jnp.broadcast_to(jnp.minimum(1.0, 0.5 * lax.rsqrt(everything / count + 1e-30)), factor_ref.shape)


def last_back(n, number, h, dq, dk, dv, rope, own, count):
    t, d = h.shape
    each = d // n
    anywhere, here = pl.BlockSpec(memory_space=pl.ANY), pl.BlockSpec(memory_space=pltpu.VMEM)
    scratch = [pltpu.VMEM((t, d), BF16)] * 4 + [pltpu.VMEM((t, HEAD), F32)] * 2
    scratch += [pltpu.VMEM((t, d), BF16), pltpu.VMEM((3, n, each, d), BF16), pltpu.VMEM((8, d), F32), pltpu.VMEM((8, 128), F32),
                pltpu.VMEM((3, 8, 128), F32), pltpu.SemaphoreType.DMA((6 + len(own),)), pltpu.SemaphoreType.DMA((2,)),
                pltpu.SemaphoreType.DMA((3,)), pltpu.SemaphoreType.DMA((3,))]
    scratch += [pltpu.VMEM(o.shape, BF16) for o in own]
    for _ in range(3):
        scratch += RingSum.scratch(n, each, d)
    return _call(
        functools.partial(_last_back, n=n, pieces=len(own), count=count),
        (),
        [anywhere] * (6 + len(own)),
        [(here, jax.ShapeDtypeStruct((3 * each, d), BF16)), (here, jax.ShapeDtypeStruct((8, 128), F32))],
        scratch,
        (h, dq, dk, dv, *rope, *own),
        6 * t * d * d,
        8 * t * d,
        collective=number,
    )


def _update(w, m, v, g):
    m = 0.9 * m + 0.1 * g
    v = 0.95 * v + 0.05 * g * g
    return (w - 0.02 * (m * lax.rsqrt(v + 1e-8) + 0.1 * w)).astype(BF16), m, v


def _adamw(_, factor_ref, *refs, n, blocks, layers):
    per = blocks + 1
    own, rest = refs[: layers * per], refs[layers * per :]
    w, m, v, new, m_out, v_out = (rest[7 * i : 7 * i + 7] for i in range(6))
    factor = factor_ref[0:1, 0:1]

    def one(i, g, at, at_w, at_new):
        new[i][at_new], m_out[i][at], v_out[i][at] = _update(w[i][at_w].astype(F32), m[i][at], v[i][at], g.astype(F32) * factor)

    for layer in range(layers):
        *ff, qkv = own[layer * per : layer * per + per]
        for i in range(3):
            one(i, qkv[i], (layer,), (layer, 0), (layer,))
        one(3, ff[-1][3], (layer,), (layer, 0), (layer,))
        for i in (4, 5):
            width = ff[0].shape[2] // n
            for d in range(n):
                for b in range(blocks):
                    at = slice((d * blocks + b) * width, (d * blocks + b + 1) * width)
                    one(i, ff[b][i - 3, :, d * width : (d + 1) * width], (layer, slice(None), at), (layer, 0, slice(None), at), (layer, slice(None), at))
        for b in range(blocks):
            one(6, ff[b][0], (layer, b), (layer, 0, b), (layer, b))


def adamw(n, factor, own, weights, m, v):
    layers = weights[0].shape[0]
    d, ff = weights[4].shape[1:]
    each, blocks = d // n, n
    deep = 16
    steps = each // deep
    cube = lambda a: a.reshape(a.shape[0] // each, each, d)
    flat = [cube(a) for one in own for a in one]
    five = lambda w: w.reshape(layers, n, blocks, each, d)
    me = lax.axis_index("dp").astype(jnp.int32)[None]
    w_in = [*(w.reshape(layers, n, each, w.shape[2]) for w in weights[:6]), five(weights[6])]
    four = lambda a: a.reshape(layers, blocks, each, d)
    thin, thick, down = (pl.BlockSpec(s, f) for s, f in (
        ((layers, deep, d), lambda s, me: (0, s, 0)),
        ((layers, deep, ff), lambda s, me: (0, s, 0)),
        ((layers, blocks, deep, d), lambda s, me: (0, 0, s, 0)),
    ))
    state = [thin] * 4 + [thick] * 2 + [down]
    w_specs = [pl.BlockSpec((layers, 1, deep, w), lambda s, me: (0, me[0], s, 0)) for w in (d, d, d, d, ff, ff)]
    w_specs += [pl.BlockSpec((layers, 1, blocks, deep, d), lambda s, me: (0, me[0], 0, s, 0))]
    pieces = [pl.BlockSpec((a.shape[0], deep, d), lambda s, me: (0, s, 0)) for a in flat]
    m_in, v_in = [*m[:6], four(m[6])], [*v[:6], four(v[6])]
    shapes = [jax.ShapeDtypeStruct(a.shape, F32) for a in m_in]
    out = pl.pallas_call(
        functools.partial(_adamw, n=n, blocks=blocks, layers=layers),
        grid_spec=pltpu.PrefetchScalarGridSpec(
            num_scalar_prefetch=1,
            grid=(steps,),
            in_specs=[pl.BlockSpec((8, 128), lambda s, me: (0, 0)), *pieces, *w_specs, *state, *state],
            out_specs=state * 3,
        ),
        out_shape=[*(jax.ShapeDtypeStruct(s.shape, BF16) for s in shapes), *shapes, *shapes],
        compiler_params=pltpu.CompilerParams(dimension_semantics=("arbitrary",), vmem_limit_bytes=VMEM),
        cost_estimate=pl.CostEstimate(flops=20 * sum(a.size for a in m), transcendentals=0, bytes_accessed=20 * sum(a.size for a in m)),
    )(me, factor, *flat, *w_in, *m_in, *v_in)
    new, m_new, v_new = out[:7], out[7:14], out[14:]
    return new, [*m_new[:6], m_new[6].reshape(m[6].shape)], [*v_new[:6], v_new[6].reshape(v[6].shape)]


def _gather(*refs, n, units):
    parts, outs, lands = refs[:7], refs[7:14], refs[14:21]
    load_sem, store_sem, out_r, out_l, in_l, in_r, pass_r, pass_l, far_l, far_r = refs[21:]
    me, right, far, left = _ring(n)
    remote = lambda src, to, sent, got: pltpu.make_async_remote_copy(
        src_ref=src, dst_ref=src, send_sem=sent, recv_sem=got, device_id={"dp": to}, device_id_type=pl.DeviceIdType.MESH)
    _greet(n)

    def view(which, unit):
        i, layer, at, rows = unit
        return lands[i].at[layer, which, pl.ds(at, rows)]

    loads = [pltpu.make_async_copy(parts[i].at[layer, pl.ds(at, rows)], view(me, (i, layer, at, rows)), load_sem.at[u])
             for u, (i, layer, at, rows) in enumerate(units)]
    for load in loads:
        load.start()

    def store(which, kind, u):
        i, layer, at, rows = units[u]
        return pltpu.make_async_copy(view(which, units[u]), outs[i].at[layer, which, pl.ds(at, rows)], store_sem.at[kind, u])

    _met()
    sends = []
    for u, unit in enumerate(units):
        loads[u].wait()
        mine = view(me, unit)
        sends.append((remote(mine, right, out_r.at[u], in_l.at[u]), remote(mine, left, out_l.at[u], in_r.at[u])))
        for s in sends[-1]:
            s.start()
        store(me, 0, u).start()
    passes = []
    for u, (i, layer, at, rows) in enumerate(units):
        half = rows // 2
        sends[u][0].wait_recv()
        first = remote(lands[i].at[layer, left, pl.ds(at, half)], right, pass_r.at[u], far_l.at[u])
        first.start()
        store(left, 1, u).start()
        sends[u][1].wait_recv()
        second = remote(lands[i].at[layer, right, pl.ds(at + half, half)], left, pass_l.at[u], far_r.at[u])
        second.start()
        store(right, 2, u).start()
        passes.append((first, second))
    for u in range(len(units)):
        for p in passes[u]:
            p.wait_recv()
        store(far, 3, u).start()
    for u in range(len(units)):
        for c in (*sends[u], *passes[u]):
            c.wait_send()
        for kind, which in enumerate((me, left, right, far)):
            store(which, kind, u).wait()


def gather(n, number, parts):
    layers = parts[0].shape[0]
    parts = [p.reshape(layers, -1, p.shape[-1]) for p in parts]
    shapes = [(layers, n, *p.shape[1:]) for p in parts]
    units = []
    for i in (6, 4, 5, 0, 1, 2, 3):
        rows = parts[i].shape[1]
        units += [(i, layer, 0, rows) for layer in range(layers)]
    count = len(units)
    anywhere = pl.BlockSpec(memory_space=pl.ANY)
    out = _call(
        functools.partial(_gather, n=n, units=units),
        (),
        [anywhere] * 7,
        [(anywhere, jax.ShapeDtypeStruct(s, BF16)) for s in shapes],
        [*(pltpu.VMEM(s, BF16) for s in shapes), pltpu.SemaphoreType.DMA((count,)), pltpu.SemaphoreType.DMA((4, count)),
         *[pltpu.SemaphoreType.DMA((count,))] * 8],
        parts,
        0,
        2 * sum(p.size for p in parts) * n,
        collective=number,
    )
    return [o.reshape(layers, -1, o.shape[-1]) for o in out]


NAMES = ("wq", "wk", "wv", "wo", "w_gate", "w_up", "w_down")


def rope_tables(t):
    half = HEAD // 2
    angle = np.arange(t, dtype=np.float32)[:, None] * (np.float32(THETA) ** (-np.arange(half, dtype=np.float32) / half)).astype(np.float32)
    cos, sin = np.cos(angle.astype(np.float64)).astype(np.float32), np.sin(angle.astype(np.float64)).astype(np.float32)
    return jnp.asarray(np.concatenate([cos, cos], 1)), jnp.asarray(np.concatenate([-sin, sin], 1))


def first(h, weights, rope):
    t, d = h.shape
    bt = _tile(t)
    tile, table = pl.BlockSpec((bt, d), lambda s: (s, 0)), pl.BlockSpec((bt, HEAD), lambda s: (s, 0))
    square = pl.BlockSpec((1, d, d), lambda s: (0, 0, 0))
    one = (tile, jax.ShapeDtypeStruct((t, d), BF16))
    return _call(_first, (t // bt,), [tile, square, square, square, table, table], [one] * 3, [],
                 (h, weights["wq"], weights["wk"], weights["wv"], *rope), 6 * t * d * d, 8 * t * d)


def between(n, layer, h, att, weights, rope):
    t, d = h.shape
    ff = weights["w_gate"].shape[2]
    bt = _tile(t, 256)
    at = lambda k, *shape: pl.BlockSpec((1, *shape), lambda s: (k, 0, 0))
    tile, table = (pl.BlockSpec((bt, w), lambda s: (s, 0)) for w in (d, HEAD))
    one = (tile, jax.ShapeDtypeStruct((t, d), BF16))
    two = (pl.BlockSpec((n, bt, ff // n), lambda s: (0, s, 0)), jax.ShapeDtypeStruct((n, t, ff // n), F32))
    return _call(
        functools.partial(_between, n=n),
        (t // bt,),
        [tile, tile, at(layer, d, d), at(layer, d, ff), at(layer, d, ff), at(layer, ff, d), *[at(layer + 1, d, d)] * 3, table, table],
        [one, one, two, two, one, one, one],
        [],
        (h, att, *(weights[name] for name in ("wo", "w_gate", "w_up", "w_down", "wq", "wk", "wv")), *rope),
        2 * t * d * (4 * d + 3 * ff),
        14 * t * d + 8 * t * ff,
    )


def solution(mesh):
    n = mesh.shape["dp"]

    def step(x, dy, *arrays):
        weights = dict(zip(NAMES, arrays[:7], strict=True))
        m, v = arrays[7:14], arrays[14:]
        layers = weights["wq"].shape[0]
        h = x[0]
        rope = rope_tables(h.shape[0])
        hs, atts, qkvs, lses, mids, hidden = [h], [], [], [], [], []
        q, k, v_ = first(h, weights, rope)
        for layer in range(layers):
            qkvs.append((q, k, v_))
            att, lse = attend(q, k, v_)
            atts.append(att)
            lses.append(lse)
            if layer < layers - 1:
                h1, h, gate, up, q, k, v_ = between(n, layer, h, att, weights, rope)
                hs.append(h)
                mids.append(h1)
                hidden.append((gate, up))
        blocks = n
        ff_own, qkv_own = {}, {}
        by, upper, number = dy[0], None, 0
        for layer in reversed(range(layers)):
            if upper is None:
                got = mlp_back(n, number, layer, hs[layer], atts[layer], by, weights, rope)
            else:
                got = mlp_back(n, number, layer, mids[layer], atts[layer], by, weights, rope, upper, hidden[layer])
                qkv_own[layer + 1] = got[5 + blocks - 1]
            by, datt, delta, left_ff, left_o = got[:5]
            dq, dk, dv, rest = attend_back(n, number + 1, *qkvs[layer], datt, lses[layer], delta, left_ff, left_o)
            ff_own[layer] = [*got[5 : 5 + blocks - 1], rest]
            upper = hs[layer], dq, dk, dv
            number += 2
        pieces = [p for layer in range(layers) for p in (*ff_own[layer], *([qkv_own[layer]] if layer else []))]
        qkv_own[0], factor = last_back(n, number, *upper, rope, pieces, n * sum(one.size for one in m))
        new, m, v = adamw(n, factor, [[*ff_own[layer], qkv_own[layer]] for layer in range(layers)], arrays[:7], m, v)
        return (*gather(n, number + 1, new), *m, *v)

    states, all_of, cut = P(("rep", "dp"), None, None), P(None, None, None), P(None, "dp", None)
    return jax.shard_map(
        step,
        mesh=mesh,
        in_specs=(states, states) + (all_of,) * 7 + (cut,) * 14,
        out_specs=(P("rep", None, None),) * 7 + (P("rep", "dp", None),) * 14,
        check_vma=False,
    )
```

```python
import functools

import jax
import jax.numpy as jnp
import numpy as np
from jax import lax
from jax.experimental import pallas as pl
from jax.experimental.pallas import tpu as pltpu
from jax.sharding import PartitionSpec as P

F32, BF16 = jnp.float32, jnp.bfloat16
HEAD = 128
THETA = 10000
NEG = -1e30
HIDDEN = 2 * NEG
LOG2E = 1.4426950408889634
SCALE = HEAD**-0.5
MIB = 2**20
VMEM = 67043328
BEHIND = 2


def _dot(a, b, ca=1, cb=0):
    return lax.dot_general(a, b, (((ca,), (cb,)), ((), ())), preferred_element_type=F32)


def _tile(size, most=512):
    return max(n for n in range(128, most + 1, 128) if size % n == 0)


def _call(kernel, grid, ins, outs, scratch, args, flops, moved, collective=None, vmem=VMEM):
    return pl.pallas_call(
        kernel,
        grid=grid,
        in_specs=[spec for spec in ins],
        out_specs=[spec for spec, _ in outs],
        out_shape=[shape for _, shape in outs],
        scratch_shapes=scratch,
        compiler_params=pltpu.CompilerParams(dimension_semantics=("arbitrary",) * len(grid), vmem_limit_bytes=vmem, collective_id=collective,
                                             has_side_effects=collective is not None),
        cost_estimate=pl.CostEstimate(flops=int(flops), transcendentals=0, bytes_accessed=int(moved)),
    )(*args)


def _norm_scale(x):
    return lax.rsqrt(jnp.mean(x * x, -1, keepdims=True) + 1e-6)


def _norm_back(x, d_out):
    s = _norm_scale(x)
    inner = jnp.mean(x * d_out, -1, keepdims=True)
    return s * d_out - x * (s * s * s * inner)


def _turn(x, cos, sin):
    parts = [x[:, n : n + HEAD] for n in range(0, x.shape[1], HEAD)]
    return jnp.concatenate([p * cos + pltpu.roll(p, HEAD // 2, 1) * sin for p in parts], 1)


def _qkv(h, wq, wk, wv, cos, sin, q_ref, k_ref, v_ref):
    a = (h * _norm_scale(h)).astype(BF16)
    q_ref[...] = _turn(_dot(a, wq).astype(BF16).astype(F32), cos, sin).astype(BF16)
    k_ref[...] = _turn(_dot(a, wk).astype(BF16).astype(F32), cos, sin).astype(BF16)
    v_ref[...] = _dot(a, wv).astype(BF16)


def _first(h_ref, wq, wk, wv, cos, sin, q_ref, k_ref, v_ref):
    _qkv(h_ref[...].astype(F32), wq[0], wk[0], wv[0], cos[...], sin[...], q_ref, k_ref, v_ref)


def _after_attention(h_ref, att_ref, wo):
    return (h_ref[...].astype(F32) + _dot(att_ref[...], wo).astype(BF16).astype(F32)).astype(BF16)


def _between(h_ref, att_ref, wo, wg, wu, wd, wq, wk, wv, cos, sin, h1_ref, y_ref, gate_ref, up_ref, q_ref, k_ref, v_ref, *, n):
    h1 = _after_attention(h_ref, att_ref, wo[0])
    h1_ref[...] = h1
    h1 = h1.astype(F32)
    b = (h1 * _norm_scale(h1)).astype(BF16)
    total = jnp.zeros(h1.shape, F32)
    for j in range(n):
        gate, up = _dot(b, _strips(wg, j, n, n, 2)), _dot(b, _strips(wu, j, n, n, 2))
        gate_ref[j] = gate
        up_ref[j] = up
        total += _dot((gate * jax.nn.sigmoid(gate) * up).astype(BF16), _strips(wd, j, n, n, 1))
    y = (h1 + total.astype(BF16).astype(F32)).astype(BF16)
    y_ref[...] = y
    _qkv(y.astype(F32), wq[0], wk[0], wv[0], cos[...], sin[...], q_ref, k_ref, v_ref)


def _seen(keys, queries):
    return lax.broadcasted_iota(jnp.int32, (keys, queries), 1) >= lax.broadcasted_iota(jnp.int32, (keys, queries), 0)


def diagonal(block, first, size, part=256):
    part = min(part, size)
    for at in range(0, size, part):
        block(first + at, part, at, True)


def _attend(q_ref, k_ref, v_ref, o_ref, lse_ref, top_s, mix_s, *, bk):
    iq = pl.program_id(0)
    bq = q_ref.shape[0]
    heads = q_ref.shape[1] // HEAD
    e = SCALE * LOG2E
    top_s[...] = jnp.full(top_s.shape, NEG, F32)
    mix_s[...] = jnp.zeros(mix_s.shape, F32)

    def block(first, keys, at, masked):
        here, ask = pl.ds(pl.multiple_of(first, keys), keys), slice(at, bq)
        cols = [slice(n * HEAD, (n + 1) * HEAD) for n in range(heads)]
        scores = [_dot(k_ref[here, c], q_ref[ask, c], 1, 1) for c in cols]
        weights, keeps = [], []
        seen = _seen(keys, bq - at) if masked else None
        for n, s in enumerate(scores):
            if masked:
                s = jnp.where(seen, s, HIDDEN)
            old = top_s[n : n + 1, ask]
            top = jnp.maximum(old, s.max(axis=0, keepdims=True))
            top_s[n : n + 1, ask] = top
            weights.append(jnp.exp2((s - top) * e).astype(BF16))
            keeps.append(jnp.exp2((old - top) * e))
        ones = jnp.ones((8, keys), BF16)
        for n, (c, p, keep) in enumerate(zip(cols, weights, keeps)):
            values = jnp.concatenate([v_ref[here, c].T, ones], axis=0)
            mix_s[n, :, ask] = mix_s[n, :, ask] * keep + _dot(values, p, 1, 0)

    lax.fori_loop(0, iq * (bq // bk), lambda j, _: block(j * bk, bk, 0, False), None)
    diagonal(block, iq * bq, bq)
    for n in range(heads):
        total = mix_s[n, HEAD : HEAD + 1, :]
        o_ref[:, n * HEAD : (n + 1) * HEAD] = (mix_s[n, :HEAD, :] * (1 / total)).T.astype(BF16)
        lse_ref[n : n + 1, :] = top_s[n : n + 1, :] * e + jnp.log2(total)


def attend(q, k, v):
    t, width = q.shape
    heads = width // HEAD
    bq = bk = _tile(t)
    rows, whole = pl.BlockSpec((bq, width), lambda i: (i, 0)), pl.BlockSpec((t, width), lambda i: (0, 0))
    return _call(
        functools.partial(_attend, bk=bk),
        (t // bq,),
        [rows, whole, whole],
        [(rows, jax.ShapeDtypeStruct((t, width), BF16)), (pl.BlockSpec((heads, bq), lambda i: (0, i)), jax.ShapeDtypeStruct((heads, t), F32))],
        [pltpu.VMEM((heads, bq), F32), pltpu.VMEM((heads, HEAD + 8, bq), F32)],
        (q, k, v),
        2 * t * t * width,
        8 * t * width,
        vmem=14 * MIB,
    )


def _ring(n):
    me = lax.axis_index("dp")
    return me, lax.rem(me + 1, n), lax.rem(me + 2, n), lax.rem(me + n - 1, n)


def _greet(n):
    _, right, _, left = _ring(n)
    barrier = pltpu.get_barrier_semaphore()
    for other in (right, left):
        pl.semaphore_signal(barrier, inc=1, device_id={"dp": other}, device_id_type=pl.DeviceIdType.MESH)


def _met():
    pl.semaphore_wait(pltpu.get_barrier_semaphore(), 2)


def _rows_loop(rows, body, most=32):
    each = max(c for c in range(16, most + 1, 16) if rows % c == 0)
    lax.fori_loop(0, rows // each, lambda i, _: body(pl.ds(pl.multiple_of(i * each, each), each)), None)


class RingSum:
    def __init__(self, n, block, passing, arrived, sent, got):
        self.block, self.passing, self.arrived = block, passing, arrived
        self.me, right, far, left = _ring(n)
        self.near = right, left
        half = block.shape[1] // 2
        self.half = half
        a, b = pl.ds(0, half), pl.ds(half, half)
        moves = [
            (block.at[far, a], passing.at[0], right),
            (block.at[far, b], passing.at[1], left),
            (block.at[right, b], arrived.at[0, b], right),
            (block.at[left, a], arrived.at[1, a], left),
            (passing.at[0], arrived.at[0, a], right),
            (passing.at[1], arrived.at[1, b], left),
        ]
        self.copies = [
            pltpu.make_async_remote_copy(src_ref=s, dst_ref=d, send_sem=sent.at[i], recv_sem=got.at[i], device_id={"dp": to},
                                         device_id_type=pl.DeviceIdType.MESH)
            for i, (s, d, to) in enumerate(moves)
        ]

    @staticmethod
    def scratch(n, rows, columns):
        half = pltpu.VMEM((2, rows // 2, columns), BF16)
        return [half, pltpu.VMEM((2, rows, columns), BF16), pltpu.SemaphoreType.DMA((6,)), pltpu.SemaphoreType.DMA((6,))]

    def start(self):
        for c in self.copies[:4]:
            c.start()

    def add(self):
        for c in self.copies[:2]:
            c.wait_recv()
        for i, other in enumerate(self.near):

            def one(rows, i=i, other=other):
                mine = self.block[other, pl.ds(rows.start + i * self.half, rows.size), :]
                self.passing[i, rows, :] = (self.passing[i, rows, :].astype(F32) + mine.astype(F32)).astype(BF16)

            _rows_loop(self.half, one)

    def forward(self):
        for c in self.copies[4:]:
            c.start()

    def finish(self, out, squares=None):
        for c in self.copies[2:]:
            c.wait_recv()

        def one(rows):
            total = self.block[self.me, rows, :].astype(F32) + self.arrived[0, rows, :].astype(F32) + self.arrived[1, rows, :].astype(F32)
            total = total.astype(BF16)
            out[rows, :] = total
            if squares is not None:
                _add_squares(squares, total)

        _rows_loop(self.half * 2, one)
        for c in self.copies:
            c.wait_send()


def _add_squares(squares, value):
    value = value.astype(F32)
    value = value * value
    squares[...] += sum(value[i : i + 8] for i in range(0, value.shape[0], 8))


def _attend_back(q_ref, k_ref, v_ref, do_ref, lse_ref, delta_ref, ff_ref, o_ref, dq_ref, dk_ref, dv_ref, own_ref, dq_s, dk_s, dv_s, block_s, load_sem,
                 *ring, bk, n):
    iq = pl.program_id(0)
    bq = q_ref.shape[0]
    heads = q_ref.shape[1] // HEAD
    e = SCALE * LOG2E
    steps = pl.num_programs(0)
    behind, _, each, _ = ff_ref.shape
    loads = [pltpu.make_async_copy(ff_ref.at[i], block_s.at[:, pl.ds(i * each, each)], load_sem.at[i]) for i in range(behind)]
    loads.append(pltpu.make_async_copy(o_ref, block_s.at[:, pl.ds(behind * each, o_ref.shape[1])], load_sem.at[behind]))
    job = RingSum(n, block_s, *ring)

    @pl.when(iq == 0)
    def _():
        _greet(n)
        for load in loads:
            load.start()
        dk_s[...] = jnp.zeros_like(dk_s)
        dv_s[...] = jnp.zeros_like(dv_s)
        for load in loads:
            load.wait()
        _met()
        job.start()

    @pl.when(iq == steps - 1)
    def _():
        job.forward()

    dq_s[...] = jnp.zeros_like(dq_s)

    def block(first, keys, at, masked):
        here, ask = pl.ds(pl.multiple_of(first, keys), keys), slice(at, bq)
        cols = [slice(i * HEAD, (i + 1) * HEAD) for i in range(heads)]
        scores = [_dot(k_ref[here, c], q_ref[ask, c], 1, 1) for c in cols]
        dps = [_dot(v_ref[here, c], do_ref[ask, c], 1, 1) for c in cols]
        seen = _seen(keys, bq - at) if masked else None
        for i, c in enumerate(cols):
            p = jnp.exp2(scores[i] * e - lse_ref[i : i + 1, ask])
            if masked:
                p = jnp.where(seen, p, 0.0)
            ds = (p * (dps[i] - delta_ref[i : i + 1, ask])).astype(BF16)
            dv_s[here, c] += _dot(p.astype(BF16), do_ref[ask, c], 1, 0)
            dk_s[here, c] += _dot(ds, q_ref[ask, c], 1, 0)
            dq_s[i, :, ask] += _dot(k_ref[here, c].T, ds, 1, 0)

    lax.fori_loop(0, iq * (bq // bk), lambda j, _: block(j * bk, bk, 0, False), None)
    diagonal(block, iq * bq, bq)

    @pl.when(iq == steps - 2)
    def _():
        job.add()

    for i in range(heads):
        dq_ref[:, i * HEAD : (i + 1) * HEAD] = (dq_s[i] * SCALE).T.astype(BF16)

    @pl.when(iq == steps - 1)
    def _():
        dk_ref[...] = (dk_s[...] * SCALE).astype(BF16)
        dv_ref[...] = dv_s[...].astype(BF16)
        job.finish(own_ref)


def attend_back(n, number, q, k, v, d_out, lse, delta, ff, o):
    t, width = q.shape
    heads = width // HEAD
    bq = bk = _tile(t)
    rows, whole = pl.BlockSpec((bq, width), lambda i: (i, 0)), pl.BlockSpec((t, width), lambda i: (0, 0))
    stats = pl.BlockSpec((heads, bq), lambda i: (0, i))
    one = jax.ShapeDtypeStruct((t, width), BF16)
    height, columns = ff.shape[0] * ff.shape[2] + o.shape[1], ff.shape[3]
    return _call(
        functools.partial(_attend_back, bk=bk, n=n),
        (t // bq,),
        [rows, whole, whole, rows, stats, stats, pl.BlockSpec(memory_space=pltpu.HBM), pl.BlockSpec(memory_space=pltpu.HBM)],
        [(rows, one), (whole, one), (whole, one),
         (pl.BlockSpec((height, columns), lambda i: (0, 0)), jax.ShapeDtypeStruct((height, columns), BF16))],
        [pltpu.VMEM((heads, HEAD, bq), F32), pltpu.VMEM((t, width), F32), pltpu.VMEM((t, width), F32),
         pltpu.VMEM((n, height, columns), BF16), pltpu.SemaphoreType.DMA((ff.shape[0] + 1,)), *RingSum.scratch(n, height, columns)],
        (q, k, v, d_out, lse, delta, ff, o),
        5 * t * t * width,
        14 * t * width,
        collective=number,
    )


def _strips(ref, block, n, blocks, axis):
    width = ref.shape[axis] // (n * blocks)
    at = [pl.ds(pl.multiple_of((d * blocks + block) * width, width), width) for d in range(n)]
    return jnp.concatenate([ref[0, :, a] if axis == 2 else ref[0, a, :] for a in at], axis - 1)


def _qkv_back(h, dq, dk, dv, wq, wk, wv, cos, sin, sums):
    a = (h * _norm_scale(h)).astype(BF16)
    dq, dk = (_turn(d.astype(F32), cos, -sin).astype(BF16) for d in (dq, dk))
    for s, d in zip(sums, (dq, dk, dv), strict=True):
        s[...] += _dot(a, d, 0, 0)
    return sum(_dot(d, w, 1, 1).astype(BF16).astype(F32) for d, w in ((dq, wq), (dk, wk), (dv, wv)))


def _cut(ref, at, value):
    n = ref.shape[0]
    each = value.shape[0] // n
    for d in range(n):
        ref[d, at : at + each] = value[d * each : (d + 1) * each].astype(BF16)


def _mlp_back(*refs, n, tiles, blocks, behind, last):
    take = iter(range(len(refs)))
    some = lambda count: [refs[next(take)] for _ in range(count)]
    h_ref, att_ref = some(2)
    if last:
        (dy_ref,) = some(1)
    else:
        hn_ref, dq_ref, dk_ref, dv_ref, dh_ref, wq, wk, wv, cos, sin, gate_ref, up_ref = some(12)
    wo, wg, wu, wd = some(4)
    dh1_ref, datt_ref, delta_ref, left_ff, left_o = some(5)
    hosted = blocks - behind
    own = some(hosted + (not last))
    h1_s = some(1)[0] if last else None
    b_s, dy_s, p_s, dg_s, du_s, sum_g, sum_u, g_s, go_s, out_sem = some(10)
    sums3 = some(1 if last else 3)
    sum_o = sums3[0]
    jobs = []
    for i in range(len(own)):
        if i < hosted:
            block = g_s.at[i]
        else:
            block = gqkv_s = g_s.at[blocks - 1]
        jobs.append(RingSum(n, block, *some(4)))
    step = pl.program_id(0)
    bt = h_ref.shape[0]
    middle = tiles * blocks
    r = jnp.where(step < tiles, step, lax.rem(step - tiles, tiles))
    j = lax.div(step - tiles, tiles)
    rows = pl.ds(pl.multiple_of(r * bt, bt), bt)
    wait, final = tiles, 2 * tiles + middle - 1

    @pl.when(step == 0)
    def _():
        _greet(n)
        for s in sums3:
            s[...] = jnp.zeros_like(s)

    begin = [tiles * (2 + i) for i in range(hosted)] + [tiles] * (not last)

    @pl.when(step == min(begin))
    def _():
        _met()

    for job, at in zip(jobs, begin, strict=True):

        @pl.when(step == at + wait)
        def _(job=job):
            job.forward()

    for job, at in zip(jobs, begin, strict=True):

        @pl.when(step == at)
        def _(job=job):
            job.start()

    @pl.when(step < tiles)
    def _():
        if last:
            h1 = _after_attention(h_ref, att_ref, wo[0])
            h1_s[rows, :] = h1
            dy_s[rows, :] = dy_ref[...]
        else:
            h1 = h_ref[...]
            hn = hn_ref[...].astype(F32)
            da = _qkv_back(hn, dq_ref[...], dk_ref[...], dv_ref[...], wq[0], wk[0], wv[0], cos[...], sin[...], sums3)
            dy_s[rows, :] = (dh_ref[...].astype(F32) + _norm_back(hn, da.astype(BF16).astype(F32)).astype(BF16).astype(F32)).astype(BF16)

            @pl.when(step == tiles - 1)
            def _():
                for i, s in enumerate(sums3):
                    _cut(gqkv_s, i * (s.shape[0] // n), s[...])
                sum_o[...] = jnp.zeros_like(sum_o)

        h1 = h1.astype(F32)
        b_s[rows, :] = (h1 * _norm_scale(h1)).astype(BF16)
        sum_g[rows, :] = jnp.zeros((bt, sum_g.shape[1]), F32)
        sum_u[rows, :] = jnp.zeros((bt, sum_u.shape[1]), F32)

    @pl.when((step >= tiles) & (step < tiles + middle))
    def _():
        b, dy = b_s[rows, :], dy_s[rows, :]
        gate_w, up_w = _strips(wg, j, n, blocks, 2), _strips(wu, j, n, blocks, 2)
        if last:
            gate, up = _dot(b, gate_w), _dot(b, up_w)
        else:
            gate, up = gate_ref[0], up_ref[0]
        dp = _dot(dy, _strips(wd, j, n, blocks, 1), 1, 1).astype(BF16).astype(F32)
        sg = jax.nn.sigmoid(gate)
        silu = gate * sg
        p_s[rows, :] = (silu * up).astype(BF16)
        du = (dp * silu).astype(BF16)
        dg = (dp * up * (sg + silu * (1 - sg))).astype(BF16)
        du_s[rows, :] = du
        dg_s[rows, :] = dg
        sum_g[rows, :] += _dot(dg, gate_w, 1, 1)
        sum_u[rows, :] += _dot(du, up_w, 1, 1)

        @pl.when(r == tiles - 1)
        def _():
            each = b.shape[1] // n
            mine = g_s.at[j]
            _cut(mine, 0, _dot(p_s[...], dy_s[...], 0, 0))
            _cut(mine, mine.shape[1] - 2 * each, _dot(b_s[...], dg_s[...], 0, 0))
            _cut(mine, mine.shape[1] - each, _dot(b_s[...], du_s[...], 0, 0))

    out_copies = [pltpu.make_async_copy(g_s.at[hosted + i], left_ff.at[i], out_sem.at[i]) for i in range(behind)]
    out_copies.append(pltpu.make_async_copy(go_s, left_o, out_sem.at[behind]))

    @pl.when(step >= tiles + middle)
    def _():
        db = sum_g[rows, :].astype(BF16).astype(F32) + sum_u[rows, :].astype(BF16).astype(F32)
        h1 = h1_s[rows, :] if last else h_ref[...]
        dh1 = dy_s[rows, :].astype(F32) + _norm_back(h1.astype(F32), db.astype(BF16).astype(F32)).astype(BF16).astype(F32)
        dh1 = dh1.astype(BF16)
        dh1_ref[...] = dh1
        datt = _dot(dh1, wo[0], 1, 1).astype(BF16)
        datt_ref[...] = datt
        att = att_ref[...]
        both = att.astype(F32) * datt.astype(F32)
        for i in range(both.shape[1] // HEAD):
            delta_ref[i : i + 1, :] = both[:, i * HEAD : (i + 1) * HEAD].T.sum(axis=0, keepdims=True)
        sum_o[...] += _dot(att, dh1, 0, 0)

        @pl.when(step == tiles + middle)
        def _():
            for c in out_copies[:-1]:
                c.start()

        @pl.when(step == 2 * tiles + middle - 1)
        def _():
            _cut(go_s, 0, sum_o[...])
            out_copies[-1].start()
            for c in out_copies:
                c.wait()

    for job, at in zip(jobs, begin, strict=True):

        @pl.when(step == at + wait - 1)
        def _(job=job):
            job.add()

    for job, at, out in zip(jobs, begin, own, strict=True):

        @pl.when(step == min(at + 2 * wait - 1, final))
        def _(job=job, out=out):
            job.finish(out)


def mlp_back(n, number, layer, h, att, by, weights, rope, upper=None, hidden=None):
    t, d = h.shape
    ff = weights["w_gate"].shape[2]
    bt = _tile(t)
    tiles, blocks = t // bt, n
    fb, each = ff // blocks, d // n
    down = fb // n
    height = down + 2 * each
    assert n == 4 and fb == d and height == 3 * each
    heads = att.shape[1] // HEAD
    middle = tiles * blocks
    r = lambda s: jnp.where(s < tiles, s, lax.rem(s - tiles, tiles))
    j = lambda s: jnp.clip(lax.div(s - tiles, tiles), 0, blocks - 1)
    edge = lambda s: jnp.where(s < tiles, s, jnp.where(s < tiles + middle, tiles - 1, s - tiles - middle))
    before = lambda s: jnp.minimum(s, tiles - 1)
    after = lambda s: jnp.maximum(s - tiles - middle, 0)
    tile = lambda f, w=d: pl.BlockSpec((bt, w), lambda s: (f(s), 0))
    fixed = lambda which, *shape: pl.BlockSpec((1, *shape), lambda s: (which, 0, 0), pipeline_mode=pl.Buffered(1))
    square, up_square, wide, tall = fixed(layer, d, d), fixed(layer + 1, d, d), fixed(layer, d, ff), fixed(layer, ff, d)
    mlp = [square, wide, wide, tall]
    w4 = [weights[name] for name in ("wo", "w_gate", "w_up", "w_down")]
    last = upper is None
    if last:
        ins = [tile(before), tile(edge), tile(before), *mlp]
        args = [h, att, by, *w4]
    else:
        hn, dq, dk, dv = upper
        table = pl.BlockSpec((bt, HEAD), lambda s: (before(s), 0))
        block = pl.BlockSpec((1, bt, fb), lambda s: (j(s), r(jnp.clip(s, tiles, tiles + middle - 1)), 0))
        ins = [tile(edge), tile(after), *[tile(before)] * 5, up_square, up_square, up_square, table, table, block, block, *mlp]
        args = [h, att, hn, dq, dk, dv, by, weights["wq"], weights["wk"], weights["wv"], *rope, *hidden, *w4]
    anywhere = pl.BlockSpec(memory_space=pltpu.HBM)
    outs = [
        (tile(after), jax.ShapeDtypeStruct((t, d), BF16)),
        (tile(after), jax.ShapeDtypeStruct((t, d), BF16)),
        (pl.BlockSpec((heads, bt), lambda s: (0, after(s))), jax.ShapeDtypeStruct((heads, t), F32)),
        (anywhere, jax.ShapeDtypeStruct((BEHIND, n, height, d), BF16)),
        (anywhere, jax.ShapeDtypeStruct((n, each, d), BF16)),
        *[(pl.BlockSpec((height, d), lambda s: (0, 0)), jax.ShapeDtypeStruct((height, d), BF16))] * (blocks - BEHIND),
    ]
    scratch = [pltpu.VMEM((t, d), BF16)] * (2 + last) + [pltpu.VMEM((t, fb), BF16)] * 3 + [pltpu.VMEM((t, d), F32)] * 2
    scratch += [pltpu.VMEM((blocks, n, height, d), BF16), pltpu.VMEM((n, each, d), BF16), pltpu.SemaphoreType.DMA((BEHIND + 1,))]
    scratch += [pltpu.VMEM((d, d), F32)] * (1 if last else 3)
    for _ in range(blocks - BEHIND):
        scratch += RingSum.scratch(n, height, d)
    if not last:
        outs += [(pl.BlockSpec((3 * each, d), lambda s: (0, 0)), jax.ShapeDtypeStruct((3 * each, d), BF16))]
        scratch += RingSum.scratch(n, 3 * each, d)
    return _call(
        functools.partial(_mlp_back, n=n, tiles=tiles, blocks=blocks, behind=BEHIND, last=last),
        (2 * tiles + middle,),
        ins,
        outs,
        scratch,
        args,
        2 * t * d * (ff * 8 + d * 4),
        sum(a.size * a.dtype.itemsize for a in args),
        collective=number,
    )


class Parts:
    def __init__(self, n, layers, each):
        self.hosted, self.per, self.each = n - BEHIND, n - BEHIND + 2, each

    def ff(self, layer, block, which):
        if block < self.hosted:
            return layer * self.per + block, which * self.each
        return layer * self.per + self.hosted, ((block - self.hosted) * 3 + which) * self.each

    def square(self, layer, which):
        if which == 3:
            return layer * self.per + self.hosted, BEHIND * 3 * self.each
        return layer * self.per + self.hosted + 1, which * self.each


def _moments(m, v, g):
    return 0.9 * m + 0.1 * g, 0.95 * v + 0.05 * g * g


def _stepped(w, m, v):
    return (w - 0.02 * (m * lax.rsqrt(v + 1e-8) + 0.1 * w)).astype(BF16)


def _finish(*refs, n, layers, own_count, count):
    take = iter(range(len(refs)))
    some = lambda k: [refs[next(take)] for _ in range(k)]
    h_ref, dq_ref, dk_ref, dv_ref, cos, sin = some(6)
    own_in, w_ref, m_ref, v_ref = some(own_count), some(7), some(7), some(7)
    own_ref, factor_ref = some(2)
    outs = some(7)
    h_s, dq_s, dk_s, dv_s, cos_s, sin_s, a_s, g_s, squares, total_s, others_s = some(11)
    pieces_s, lands, m_s, v_s = some(own_count), some(7), some(7), some(7)
    load_sem, w_sem, m_sem, v_sem, swap_out, swap_in, store_sem, out_r, out_l, in_l, in_r, pass_r, pass_l, far_l, far_r = some(15)
    jobs = [RingSum(n, g_s.at[i], *some(4)) for i in range(3)]
    me, right, far, left = _ring(n)
    mesh = pl.DeviceIdType.MESH
    barrier = pltpu.get_barrier_semaphore()
    for other in (right, far, left):
        pl.semaphore_signal(barrier, inc=1, device_id={"dp": other}, device_id_type=mesh)
    pairs = [(h_ref, h_s), (dv_ref, dv_s), (dk_ref, dk_s), (cos, cos_s), (sin, sin_s), (dq_ref, dq_s), *zip(own_in, pieces_s, strict=True)]
    loads = [pltpu.make_async_copy(s, d, load_sem.at[i]) for i, (s, d) in enumerate(pairs)]
    for load in loads:
        load.start()
    state = []
    for i in range(7):
        state.append(pltpu.make_async_copy(w_ref[i].at[:, me], lands[i].at[:, me], w_sem.at[i]))
        state.append(pltpu.make_async_copy(m_ref[i], m_s[i], m_sem.at[i]))
        state.append(pltpu.make_async_copy(v_ref[i], v_s[i], v_sem.at[i]))
    t = h_s.shape[0]
    each = g_s.shape[2]
    squares[...] = jnp.zeros_like(squares)
    loads[0].wait()

    def norm(rows):
        h = h_s[rows, :].astype(F32)
        a_s[rows, :] = (h * _norm_scale(h)).astype(BF16)

    _rows_loop(t, norm, 256)

    def turn(ref):
        def one(rows):
            ref[rows, :] = _turn(ref[rows, :].astype(F32), cos_s[rows, :], -sin_s[rows, :]).astype(BF16)

        _rows_loop(t, one, 256)

    loads[1].wait()
    _cut(g_s.at[2], 0, _dot(a_s[...], dv_s[...], 0, 0))
    pl.semaphore_wait(barrier, 3)
    for i in (2, 3, 4):
        loads[i].wait()
    turn(dk_s)
    jobs[2].start()
    for c in state:
        c.start()
    _cut(g_s.at[1], 0, _dot(a_s[...], dk_s[...], 0, 0))
    loads[5].wait()
    turn(dq_s)
    jobs[1].start()
    jobs[2].add()
    _cut(g_s.at[0], 0, _dot(a_s[...], dq_s[...], 0, 0))
    jobs[2].forward()
    jobs[1].add()
    jobs[0].start()
    for i, piece in enumerate(pieces_s):
        loads[6 + i].wait()
        if i == 1:
            jobs[1].forward()
        _rows_loop(piece.shape[0], lambda rows, piece=piece: _add_squares(squares, piece[rows, :]))
    jobs[0].add()
    jobs[2].finish(own_ref.at[pl.ds(2 * each, each)], squares)
    jobs[0].forward()
    jobs[1].finish(own_ref.at[pl.ds(each, each)], squares)
    jobs[0].finish(own_ref.at[pl.ds(0, each)], squares)
    total_s[...] = sum(squares[:, i : i + 128] for i in range(0, squares.shape[1], 128))
    swaps = [
        pltpu.make_async_remote_copy(src_ref=total_s, dst_ref=others_s.at[i], send_sem=swap_out.at[i], recv_sem=swap_in.at[i], device_id={"dp": other},
                                     device_id_type=mesh)
        for i, other in enumerate((right, far, left))
    ]
    for s in swaps:
        s.start()
    for c in state:
        c.wait()
    for s in swaps:
        s.wait()
    everything = jnp.sum(total_s[...] + others_s[0] + others_s[1] + others_s[2], keepdims=True)
    factor = jnp.minimum(1.0, 0.5 * lax.rsqrt(everything / count + 1e-30))
    factor_ref[...] = jnp.broadcast_to(factor, factor_ref.shape)

    parts = Parts(n, layers, each)
    grads = [*pieces_s[: parts.per - 1], own_ref, *pieces_s[parts.per - 1 :]]
    blocks = n

    def new_weights(i, layer):
        land, m_i, v_i = lands[i], m_s[i], v_s[i]

        def one(at, piece, row, rows, column, g_column, width):
            def body(some):
                here = pl.ds(at + some.start, some.size)
                g = grads[piece][pl.ds(row + some.start, some.size), g_column : g_column + width].astype(F32) * factor
                m, v = _moments(m_i[layer, here, column : column + width], v_i[layer, here, column : column + width], g)
                w = land[layer, me, here, column : column + width].astype(F32)
                land[layer, me, here, column : column + width] = _stepped(w, m, v)

            return body

        if i < 4:
            bodies, rows = [one(0, *parts.square(layer, i), each, 0, 0, land.shape[3])], each
        elif i == 6:
            rows = each
            bodies = [one(b * each, *parts.ff(layer, b, 0), each, 0, 0, land.shape[3]) for b in range(blocks)]
        else:
            width, rows = g_s.shape[3] // n, each
            bodies = [
                one(0, *parts.ff(layer, b, i - 3), each, (d * blocks + b) * width, d * width, width) for d in range(n) for b in range(blocks)
            ]

        def run(some):
            for body in bodies:
                body(some)

        _rows_loop(rows, run, 16)

    remote = lambda ref, to, sent, got: pltpu.make_async_remote_copy(
        src_ref=ref, dst_ref=ref, send_sem=sent, recv_sem=got, device_id={"dp": to}, device_id_type=mesh)
    units = [(i, layer) for i in (3, 0, 1, 2, 6, 4, 5) for layer in range(layers)]
    store = lambda which, kind, u: pltpu.make_async_copy(
        lands[units[u][0]].at[units[u][1], which], outs[units[u][0]].at[units[u][1], which], store_sem.at[kind, u])
    sends, passes = [], []
    for u, (i, layer) in enumerate(units):
        new_weights(i, layer)
        mine = lands[i].at[layer, me]
        sends.append((remote(mine, right, out_r.at[u], in_l.at[u]), remote(mine, left, out_l.at[u], in_r.at[u])))
        for c in sends[-1]:
            c.start()
        store(me, 0, u).start()
    for u, (i, layer) in enumerate(units):
        half = lands[i].shape[2] // 2
        sends[u][0].wait_recv()
        one = remote(lands[i].at[layer, left, pl.ds(0, half)], right, pass_r.at[u], far_l.at[u])
        one.start()
        store(left, 1, u).start()
        sends[u][1].wait_recv()
        two = remote(lands[i].at[layer, right, pl.ds(half, half)], left, pass_l.at[u], far_r.at[u])
        two.start()
        store(right, 2, u).start()
        passes.append((one, two))
    for u in range(len(units)):
        for c in passes[u]:
            c.wait_recv()
        store(far, 3, u).start()
    for u in range(len(units)):
        for c in (*sends[u], *passes[u]):
            c.wait_send()
        for kind, which in enumerate((me, left, right, far)):
            store(which, kind, u).wait()


def finish(n, number, h, dq, dk, dv, rope, own, w, m, v):
    t, d = h.shape
    each, layers = d // n, w[0].shape[0]
    anywhere, here = pl.BlockSpec(memory_space=pltpu.HBM), pl.BlockSpec(memory_space=pltpu.VMEM)
    w = [a.reshape(layers, n, a.shape[1] // n, a.shape[2]) for a in w]
    shapes = [a.shape for a in w]
    scratch = [pltpu.VMEM((t, d), BF16)] * 4 + [pltpu.VMEM((t, HEAD), F32)] * 2
    scratch += [pltpu.VMEM((t, d), BF16), pltpu.VMEM((3, n, each, d), BF16), pltpu.VMEM((8, d), F32), pltpu.VMEM((8, 128), F32),
                pltpu.VMEM((3, 8, 128), F32)]
    scratch += [pltpu.VMEM(o.shape, BF16) for o in own] + [pltpu.VMEM(s, BF16) for s in shapes] + [pltpu.VMEM(a.shape, F32) for a in (*m, *v)]
    units = 7 * layers
    sem = lambda *k: pltpu.SemaphoreType.DMA(k)
    scratch += [sem(6 + len(own)), sem(7), sem(7), sem(7), sem(3), sem(3), sem(4, units), *[sem(units)] * 8]
    for _ in range(3):
        scratch += RingSum.scratch(n, each, d)
    return _call(
        functools.partial(_finish, n=n, layers=layers, own_count=len(own), count=n * sum(a.size for a in m)),
        (),
        [anywhere] * (6 + len(own) + 21),
        [(here, jax.ShapeDtypeStruct((3 * each, d), BF16)), (here, jax.ShapeDtypeStruct((8, 128), F32)),
         *((anywhere, jax.ShapeDtypeStruct(s, BF16)) for s in shapes)],
        scratch,
        (h, dq, dk, dv, *rope, *own, *w, *m, *v),
        6 * t * d * d,
        8 * t * d,
        collective=number,
    )


def _settle(factor_ref, *refs, n, layers, own_count):
    own, rest = refs[:own_count], refs[own_count:]
    m, v, w, w_out, m_out, v_out = (rest[7 * i : 7 * i + 7] for i in range(6))
    factor = factor_ref[0:1, 0:1]
    parts = Parts(n, layers, 1)
    for i in range(7):
        w_out[i][...] = w[i][...]

    def one(i, at, piece, row, columns=slice(None)):
        g = own[piece][row][:, columns].astype(F32) * factor
        m_out[i][at], v_out[i][at] = _moments(m[i][at], v[i][at], g)

    for layer in range(layers):
        for i in range(4):
            one(i, (layer,), *parts.square(layer, i))
        for b in range(n):
            one(6, (layer, b), *parts.ff(layer, b, 0))
            width = own[0].shape[2] // n
            for d in range(n):
                for i in (4, 5):
                    at = slice((d * n + b) * width, (d * n + b + 1) * width)
                    one(i, (layer, slice(None), at), *parts.ff(layer, b, i - 3), slice(d * width, (d + 1) * width))


def settle(n, factor, own, w, m, v):
    layers, _, each, d = w[0].shape
    ff = w[4].shape[3]
    deep = 16
    steps = each // deep
    own = [a.reshape(a.shape[0] // each, each, d) for a in own]
    cut = lambda a: a.reshape(layers, -1, each, d)
    m_in, v_in, w_in = [*m[:6], cut(m[6])], [*v[:6], cut(v[6])], [*w[:6], cut(w[6])]
    thin, thick = (pl.BlockSpec((layers, deep, c), lambda s: (0, s, 0)) for c in (d, ff))
    deeper = lambda a: pl.BlockSpec((layers, a.shape[1], deep, a.shape[3]), lambda s: (0, 0, s, 0))
    state = [thin] * 4 + [thick] * 2 + [deeper(m_in[6])]
    whole = [deeper(a) for a in w_in]
    out = _call(
        functools.partial(_settle, n=n, layers=layers, own_count=len(own)),
        (steps,),
        [pl.BlockSpec((8, 128), lambda s: (0, 0)), *(pl.BlockSpec((a.shape[0], deep, d), lambda s: (0, s, 0)) for a in own), *state, *state, *whole],
        [*((spec, jax.ShapeDtypeStruct(a.shape, a.dtype)) for spec, a in zip((*whole, *state, *state), (*w_in, *m_in, *v_in), strict=True))],
        [],
        (factor, *own, *m_in, *v_in, *w_in),
        8 * sum(a.size for a in m),
        32 * sum(a.size for a in m),
    )
    flat = lambda a: a.reshape(layers, -1, a.shape[-1])
    return tuple(flat(a) for a in out)


NAMES = ("wq", "wk", "wv", "wo", "w_gate", "w_up", "w_down")


def rope_tables(t):
    half = HEAD // 2
    angle = np.arange(t, dtype=np.float32)[:, None] * (np.float32(THETA) ** (-np.arange(half, dtype=np.float32) / half)).astype(np.float32)
    cos, sin = np.cos(angle.astype(np.float64)).astype(np.float32), np.sin(angle.astype(np.float64)).astype(np.float32)
    return jnp.asarray(np.concatenate([cos, cos], 1)), jnp.asarray(np.concatenate([-sin, sin], 1))


def first(h, weights, rope):
    t, d = h.shape
    bt = _tile(t)
    tile, table = pl.BlockSpec((bt, d), lambda s: (s, 0)), pl.BlockSpec((bt, HEAD), lambda s: (s, 0))
    square = pl.BlockSpec((1, d, d), lambda s: (0, 0, 0))
    one = (tile, jax.ShapeDtypeStruct((t, d), BF16))
    return _call(_first, (t // bt,), [tile, square, square, square, table, table], [one] * 3, [],
                 (h, weights["wq"], weights["wk"], weights["wv"], *rope), 6 * t * d * d, 8 * t * d, vmem=12 * MIB)


def between(n, layer, h, att, weights, rope):
    t, d = h.shape
    ff = weights["w_gate"].shape[2]
    bt = _tile(t)
    at = lambda k, *shape: pl.BlockSpec((1, *shape), lambda s: (k, 0, 0))
    tile, table = (pl.BlockSpec((bt, w), lambda s: (s, 0)) for w in (d, HEAD))
    one = (tile, jax.ShapeDtypeStruct((t, d), BF16))
    two = (pl.BlockSpec((n, bt, ff // n), lambda s: (0, s, 0)), jax.ShapeDtypeStruct((n, t, ff // n), F32))
    return _call(
        functools.partial(_between, n=n),
        (t // bt,),
        [tile, tile, at(layer, d, d), at(layer, d, ff), at(layer, d, ff), at(layer, ff, d), *[at(layer + 1, d, d)] * 3, table, table],
        [one, one, two, two, one, one, one],
        [],
        (h, att, *(weights[name] for name in ("wo", "w_gate", "w_up", "w_down", "wq", "wk", "wv")), *rope),
        2 * t * d * (4 * d + 3 * ff),
        14 * t * d + 8 * t * ff,
        vmem=44 * MIB,
    )


def solution(mesh):
    n = mesh.shape["dp"]

    def step(x, dy, *arrays):
        weights = dict(zip(NAMES, arrays[:7], strict=True))
        m, v = arrays[7:14], arrays[14:]
        layers = weights["wq"].shape[0]
        h = x[0]
        rope = rope_tables(h.shape[0])
        hs, atts, qkvs, lses, mids, hidden = [h], [], [], [], [], []
        q, k, v_ = first(h, weights, rope)
        for layer in range(layers):
            qkvs.append((q, k, v_))
            att, lse = attend(q, k, v_)
            atts.append(att)
            lses.append(lse)
            if layer < layers - 1:
                h1, h, gate, up, q, k, v_ = between(n, layer, h, att, weights, rope)
                hs.append(h)
                mids.append(h1)
                hidden.append((gate, up))
        own = {}
        by, upper, number = dy[0], None, 0
        for layer in reversed(range(layers)):
            if upper is None:
                got = mlp_back(n, number, layer, hs[layer], atts[layer], by, weights, rope)
            else:
                got = mlp_back(n, number, layer, mids[layer], atts[layer], by, weights, rope, upper, hidden[layer])
                own[layer + 1].append(got[5 + n - BEHIND])
            by, datt, delta, left_ff, left_o = got[:5]
            dq, dk, dv, rest = attend_back(n, number + 1, *qkvs[layer], datt, lses[layer], delta, left_ff, left_o)
            own[layer] = [*got[5 : 5 + n - BEHIND], rest]
            upper = hs[layer], dq, dk, dv
            number += 2
        pieces = [p for layer in range(layers) for p in own[layer]]
        last, factor, *whole = finish(n, number, *upper, rope, pieces, arrays[:7], m, v)
        own[0].append(last)
        return settle(n, factor, [p for layer in range(layers) for p in own[layer]], whole, m, v)

    states, all_of, cut = P(("rep", "dp"), None, None), P(None, None, None), P(None, "dp", None)
    return jax.shard_map(
        step,
        mesh=mesh,
        in_specs=(states, states) + (all_of,) * 7 + (cut,) * 14,
        out_specs=(P("rep", None, None),) * 7 + (P("rep", "dp", None),) * 14,
        check_vma=False,
    )
```

```python
import functools

import jax
import jax.numpy as jnp
import numpy as np
from jax import lax
from jax.experimental import pallas as pl
from jax.experimental.pallas import tpu as pltpu
from jax.sharding import PartitionSpec as P

F32, BF16 = jnp.float32, jnp.bfloat16
HEAD = 128
THETA = 10000
NEG = -1e30
HIDDEN = 2 * NEG
LOG2E = 1.4426950408889634
SCALE = HEAD**-0.5
VMEM = 67043328
BEHIND = 2


def _dot(a, b, ca=1, cb=0):
    return lax.dot_general(a, b, (((ca,), (cb,)), ((), ())), preferred_element_type=F32)


def _tile(size, most=512):
    return max(n for n in range(128, most + 1, 128) if size % n == 0)


def _call(kernel, grid, ins, outs, scratch, args, flops, moved, collective=None):
    return pl.pallas_call(
        kernel,
        grid=grid,
        in_specs=[spec for spec in ins],
        out_specs=[spec for spec, _ in outs],
        out_shape=[shape for _, shape in outs],
        scratch_shapes=scratch,
        compiler_params=pltpu.CompilerParams(dimension_semantics=("arbitrary",) * len(grid), vmem_limit_bytes=VMEM, collective_id=collective,
                                             has_side_effects=collective is not None),
        cost_estimate=pl.CostEstimate(flops=int(flops), transcendentals=0, bytes_accessed=int(moved)),
    )(*args)


def _norm_scale(x):
    return lax.rsqrt(jnp.mean(x * x, -1, keepdims=True) + 1e-6)


def _norm_back(x, d_out):
    s = _norm_scale(x)
    inner = jnp.mean(x * d_out, -1, keepdims=True)
    return s * d_out - x * (s * s * s * inner)


def _turn(x, cos, sin):
    parts = [x[:, n : n + HEAD] for n in range(0, x.shape[1], HEAD)]
    return jnp.concatenate([p * cos + pltpu.roll(p, HEAD // 2, 1) * sin for p in parts], 1)


def _qkv(h, wq, wk, wv, cos, sin):
    a = (h * _norm_scale(h)).astype(BF16)
    q, k = (_turn(_dot(a, w).astype(BF16).astype(F32), cos, sin).astype(BF16) for w in (wq, wk))
    return q, k, _dot(a, wv).astype(BF16)


def _after_attention(h_ref, att_ref, wo):
    return (h_ref[...].astype(F32) + _dot(att_ref[...], wo).astype(BF16).astype(F32)).astype(BF16)


def _seen(keys, queries):
    return lax.broadcasted_iota(jnp.int32, (keys, queries), 1) >= lax.broadcasted_iota(jnp.int32, (keys, queries), 0)


def diagonal(block, first, size, part=256):
    part = min(part, size)
    for at in range(0, size, part):
        block(first + at, part, at, True)


def _attend(iq, q_ref, k_ref, v_ref, o_ref, lse_ref, top_s, mix_s, bk):
    bq = q_ref.shape[0]
    heads = q_ref.shape[1] // HEAD
    e = SCALE * LOG2E
    top_s[...] = jnp.full(top_s.shape, NEG, F32)
    mix_s[...] = jnp.zeros(mix_s.shape, F32)

    def block(first, keys, at, masked):
        here, ask = pl.ds(pl.multiple_of(first, keys), keys), slice(at, bq)
        cols = [slice(n * HEAD, (n + 1) * HEAD) for n in range(heads)]
        scores = [_dot(k_ref[here, c], q_ref[ask, c], 1, 1) for c in cols]
        weights, keeps = [], []
        seen = _seen(keys, bq - at) if masked else None
        for n, s in enumerate(scores):
            if masked:
                s = jnp.where(seen, s, HIDDEN)
            old = top_s[n : n + 1, ask]
            top = jnp.maximum(old, s.max(axis=0, keepdims=True))
            top_s[n : n + 1, ask] = top
            weights.append(jnp.exp2((s - top) * e).astype(BF16))
            keeps.append(jnp.exp2((old - top) * e))
        ones = jnp.ones((8, keys), BF16)
        for n, (c, p, keep) in enumerate(zip(cols, weights, keeps)):
            values = jnp.concatenate([v_ref[here, c].T, ones], axis=0)
            mix_s[n, :, ask] = mix_s[n, :, ask] * keep + _dot(values, p, 1, 0)

    lax.fori_loop(0, iq * (bq // bk), lambda j, _: block(j * bk, bk, 0, False), None)
    diagonal(block, iq * bq, bq)
    for n in range(heads):
        total = mix_s[n, HEAD : HEAD + 1, :]
        o_ref[:, n * HEAD : (n + 1) * HEAD] = (mix_s[n, :HEAD, :] * (1 / total)).T.astype(BF16)
        lse_ref[n : n + 1, :] = top_s[n : n + 1, :] * e + jnp.log2(total)


def _forward(h_ref, wq, wk, wv, wo, wg_ref, wu_ref, wd_ref, cos, sin, *refs, n, layers):
    outs, scratch = refs[: 9 * layers - 4], refs[9 * layers - 4 :]
    k_s, v_s, wg, wu, wd, gate_s, up_s, top_s, mix_s, w_sem, out_sem = scratch
    step = pl.program_id(0)
    bt = h_ref.shape[0]
    rows = pl.ds(pl.multiple_of(step * bt, bt), bt)
    loads = [pltpu.make_async_copy(a.at[0], b.at[0], w_sem.at[i]) for i, (a, b) in enumerate(((wg_ref, wg), (wu_ref, wu), (wd_ref, wd)))]

    @pl.when(step == 0)
    def _():
        for load in loads:
            load.start()

    for layer in range(layers):
        q_ref, k_ref, v_ref, att_ref, lse_ref = outs[9 * layer : 9 * layer + 5]
        q_ref[...], k, v = _qkv(h_ref[...].astype(F32), wq[layer], wk[layer], wv[layer], cos[...], sin[...])
        k_ref[...] = k_s[layer, rows, :] = k
        v_ref[...] = v_s[layer, rows, :] = v
        _attend(step, q_ref, k_s.at[layer], v_s.at[layer], att_ref, lse_ref, top_s, mix_s, bt)
        if layer == layers - 1:
            break
        h1_ref, y_ref, gate_ref, up_ref = outs[9 * layer + 5 : 9 * layer + 9]
        stores = [
            pltpu.make_async_copy(a.at[j], b.at[j, rows], out_sem.at[layer, i, j])
            for i, (a, b) in enumerate(((gate_s, gate_ref), (up_s, up_ref)))
            for j in range(n)
        ]

        @pl.when(step == 0)
        def _(layer=layer):
            for load in loads:
                load.wait()

        @pl.when(step > 0)
        def _(stores=stores):
            for c in stores:
                c.wait()

        h1 = _after_attention(h_ref, att_ref, wo[layer])
        h1_ref[...] = h1
        h1 = h1.astype(F32)
        b = (h1 * _norm_scale(h1)).astype(BF16)
        total = jnp.zeros(h1.shape, F32)
        for j in range(n):
            gate, up = _dot(b, _strips(wg, j, n, n, 2)), _dot(b, _strips(wu, j, n, n, 2))
            gate_s[j] = gate
            up_s[j] = up
            total += _dot((gate * jax.nn.sigmoid(gate) * up).astype(BF16), _strips(wd, j, n, n, 1))
        for c in stores:
            c.start()
        y_ref[...] = (h1 + total.astype(BF16).astype(F32)).astype(BF16)
        h_ref = y_ref

        @pl.when(step == pl.num_programs(0) - 1)
        def _(stores=stores):
            for c in stores:
                c.wait()


def forward(n, h, weights, rope):
    t, d = h.shape
    layers, _, ff = weights["w_gate"].shape
    assert layers == 2
    heads = weights["wq"].shape[2] // HEAD
    bt = _tile(t)
    tile, table = (pl.BlockSpec((bt, w), lambda s: (s, 0)) for w in (d, HEAD))
    square = pl.BlockSpec((layers, d, d), lambda s: (0, 0, 0), pipeline_mode=pl.Buffered(1))
    anywhere = pl.BlockSpec(memory_space=pltpu.HBM)
    one = (tile, jax.ShapeDtypeStruct((t, d), BF16))
    two = (anywhere, jax.ShapeDtypeStruct((n, t, ff // n), F32))
    stats = (pl.BlockSpec((heads, bt), lambda s: (0, s)), jax.ShapeDtypeStruct((heads, t), F32))
    upper = [*[one] * 4, stats]
    got = _call(
        functools.partial(_forward, n=n, layers=layers),
        (t // bt,),
        [tile, *[square] * 4, *[anywhere] * 3, table, table],
        [*[*upper, one, one, two, two] * (layers - 1), *upper],
        [pltpu.VMEM((layers, t, d), BF16)] * 2
        + [pltpu.VMEM((1, d, ff), BF16)] * 2
        + [pltpu.VMEM((1, ff, d), BF16)]
        + [pltpu.VMEM((n, bt, ff // n), F32)] * 2
        + [pltpu.VMEM((heads, bt), F32), pltpu.VMEM((heads, HEAD + 8, bt), F32), pltpu.SemaphoreType.DMA((3,)),
           pltpu.SemaphoreType.DMA((layers, 2, n))],
        (h, *(weights[name] for name in ("wq", "wk", "wv", "wo")), *(weights[name] for name in ("w_gate", "w_up", "w_down")), *rope),
        2 * t * d * (8 * d + 3 * ff) + 4 * t * t * d,
        30 * t * d + 8 * t * ff,
    )
    return [got[9 * layer : 9 * layer + 9] for layer in range(layers)]


def _ring(n):
    me = lax.axis_index("dp")
    return me, lax.rem(me + 1, n), lax.rem(me + 2, n), lax.rem(me + n - 1, n)


def _greet(n):
    _, right, _, left = _ring(n)
    barrier = pltpu.get_barrier_semaphore()
    for other in (right, left):
        pl.semaphore_signal(barrier, inc=1, device_id={"dp": other}, device_id_type=pl.DeviceIdType.MESH)


def _met():
    pl.semaphore_wait(pltpu.get_barrier_semaphore(), 2)


def _rows_loop(rows, body, most=32):
    each = max(c for c in range(16, most + 1, 16) if rows % c == 0)
    lax.fori_loop(0, rows // each, lambda i, _: body(pl.ds(pl.multiple_of(i * each, each), each)), None)


class RingSum:
    def __init__(self, n, block, passing, arrived, sent, got):
        self.block, self.passing, self.arrived = block, passing, arrived
        self.me, right, far, left = _ring(n)
        self.near = right, left
        half = block.shape[1] // 2
        self.half = half
        a, b = pl.ds(0, half), pl.ds(half, half)
        moves = [
            (block.at[far, a], passing.at[0], right),
            (block.at[far, b], passing.at[1], left),
            (block.at[right, b], arrived.at[0, b], right),
            (block.at[left, a], arrived.at[1, a], left),
            (passing.at[0], arrived.at[0, a], right),
            (passing.at[1], arrived.at[1, b], left),
        ]
        self.copies = [
            pltpu.make_async_remote_copy(src_ref=s, dst_ref=d, send_sem=sent.at[i], recv_sem=got.at[i], device_id={"dp": to},
                                         device_id_type=pl.DeviceIdType.MESH)
            for i, (s, d, to) in enumerate(moves)
        ]

    @staticmethod
    def scratch(n, rows, columns):
        half = pltpu.VMEM((2, rows // 2, columns), BF16)
        return [half, pltpu.VMEM((2, rows, columns), BF16), pltpu.SemaphoreType.DMA((6,)), pltpu.SemaphoreType.DMA((6,))]

    def start(self):
        for c in self.copies[:4]:
            c.start()

    def add(self):
        for c in self.copies[:2]:
            c.wait_recv()
        for i, other in enumerate(self.near):

            def one(rows, i=i, other=other):
                mine = self.block[other, pl.ds(rows.start + i * self.half, rows.size), :]
                self.passing[i, rows, :] = (self.passing[i, rows, :].astype(F32) + mine.astype(F32)).astype(BF16)

            _rows_loop(self.half, one)

    def forward(self):
        for c in self.copies[4:]:
            c.start()

    def finish(self, out, squares=None):
        for c in self.copies[2:]:
            c.wait_recv()

        def one(rows):
            total = self.block[self.me, rows, :].astype(F32) + self.arrived[0, rows, :].astype(F32) + self.arrived[1, rows, :].astype(F32)
            total = total.astype(BF16)
            out[rows, :] = total
            if squares is not None:
                _add_squares(squares, total)

        _rows_loop(self.half * 2, one)
        for c in self.copies:
            c.wait_send()


def _add_squares(squares, value):
    value = value.astype(F32)
    value = value * value
    squares[...] += sum(value[i : i + 8] for i in range(0, value.shape[0], 8))


def _attend_back(q_ref, k_ref, v_ref, do_ref, lse_ref, delta_ref, ff_ref, o_ref, dq_ref, dk_ref, dv_ref, own_ref, dq_s, dk_s, dv_s, block_s, load_sem,
                 *ring, bk, n):
    iq = pl.program_id(0)
    bq = q_ref.shape[0]
    heads = q_ref.shape[1] // HEAD
    e = SCALE * LOG2E
    steps = pl.num_programs(0)
    behind, _, each, _ = ff_ref.shape
    loads = [pltpu.make_async_copy(ff_ref.at[i], block_s.at[:, pl.ds(i * each, each)], load_sem.at[i]) for i in range(behind)]
    loads.append(pltpu.make_async_copy(o_ref, block_s.at[:, pl.ds(behind * each, o_ref.shape[1])], load_sem.at[behind]))
    early = (behind - 1) * each
    jobs = [RingSum(n, block_s.at[:, pl.ds(0, early)], *ring[:4]), RingSum(n, block_s.at[:, pl.ds(early, block_s.shape[1] - early)], *ring[4:])]

    @pl.when(iq == 0)
    def _():
        _greet(n)
        for load in loads:
            load.start()
        dk_s[...] = jnp.zeros_like(dk_s)
        dv_s[...] = jnp.zeros_like(dv_s)
        for load in loads:
            load.wait()
        _met()
        for job in jobs:
            job.start()

    for i, job in enumerate(jobs):

        @pl.when(iq == steps - 2 + i)
        def _(job=job):
            job.forward()

    dq_s[...] = jnp.zeros_like(dq_s)

    def block(first, keys, at, masked):
        here, ask = pl.ds(pl.multiple_of(first, keys), keys), slice(at, bq)
        cols = [slice(i * HEAD, (i + 1) * HEAD) for i in range(heads)]
        scores = [_dot(k_ref[here, c], q_ref[ask, c], 1, 1) for c in cols]
        dps = [_dot(v_ref[here, c], do_ref[ask, c], 1, 1) for c in cols]
        seen = _seen(keys, bq - at) if masked else None
        for i, c in enumerate(cols):
            p = jnp.exp2(scores[i] * e - lse_ref[i : i + 1, ask])
            if masked:
                p = jnp.where(seen, p, 0.0)
            ds = (p * (dps[i] - delta_ref[i : i + 1, ask])).astype(BF16)
            dv_s[here, c] += _dot(p.astype(BF16), do_ref[ask, c], 1, 0)
            dk_s[here, c] += _dot(ds, q_ref[ask, c], 1, 0)
            dq_s[i, :, ask] += _dot(k_ref[here, c].T, ds, 1, 0)

    lax.fori_loop(0, iq * (bq // bk), lambda j, _: block(j * bk, bk, 0, False), None)
    diagonal(block, iq * bq, bq)

    for i, job in enumerate(jobs):

        @pl.when(iq == steps - 3 + i)
        def _(job=job):
            job.add()

    for i in range(heads):
        dq_ref[:, i * HEAD : (i + 1) * HEAD] = (dq_s[i] * SCALE).T.astype(BF16)

    @pl.when(iq == steps - 1)
    def _():
        dk_ref[...] = (dk_s[...] * SCALE).astype(BF16)
        dv_ref[...] = dv_s[...].astype(BF16)
        jobs[0].finish(own_ref.at[pl.ds(0, early)])
        jobs[1].finish(own_ref.at[pl.ds(early, own_ref.shape[0] - early)])


def attend_back(n, number, q, k, v, d_out, lse, delta, ff, o):
    t, width = q.shape
    heads = width // HEAD
    bq = bk = _tile(t)
    rows, whole = pl.BlockSpec((bq, width), lambda i: (i, 0)), pl.BlockSpec((t, width), lambda i: (0, 0))
    stats = pl.BlockSpec((heads, bq), lambda i: (0, i))
    one = jax.ShapeDtypeStruct((t, width), BF16)
    early = (ff.shape[0] - 1) * ff.shape[2]
    height, columns = ff.shape[0] * ff.shape[2] + o.shape[1], ff.shape[3]
    return _call(
        functools.partial(_attend_back, bk=bk, n=n),
        (t // bq,),
        [rows, whole, whole, rows, stats, stats, pl.BlockSpec(memory_space=pltpu.HBM), pl.BlockSpec(memory_space=pltpu.HBM)],
        [(rows, one), (whole, one), (whole, one),
         (pl.BlockSpec((height, columns), lambda i: (0, 0)), jax.ShapeDtypeStruct((height, columns), BF16))],
        [pltpu.VMEM((heads, HEAD, bq), F32), pltpu.VMEM((t, width), F32), pltpu.VMEM((t, width), F32),
         pltpu.VMEM((n, height, columns), BF16), pltpu.SemaphoreType.DMA((ff.shape[0] + 1,)),
         *RingSum.scratch(n, early, columns), *RingSum.scratch(n, height - early, columns)],
        (q, k, v, d_out, lse, delta, ff, o),
        5 * t * t * width,
        14 * t * width,
        collective=number,
    )


def _strips(ref, block, n, blocks, axis):
    width = ref.shape[axis] // (n * blocks)
    at = [pl.ds(pl.multiple_of((d * blocks + block) * width, width), width) for d in range(n)]
    return jnp.concatenate([ref[0, :, a] if axis == 2 else ref[0, a, :] for a in at], axis - 1)


def _qkv_back(h, dq, dk, dv, wq, wk, wv, cos, sin, sums):
    a = (h * _norm_scale(h)).astype(BF16)
    dq, dk = (_turn(d.astype(F32), cos, -sin).astype(BF16) for d in (dq, dk))
    for s, d in zip(sums, (dq, dk, dv), strict=True):
        s[...] += _dot(a, d, 0, 0)
    return sum(_dot(d, w, 1, 1).astype(BF16).astype(F32) for d, w in ((dq, wq), (dk, wk), (dv, wv)))


def _cut(ref, at, value):
    n = ref.shape[0]
    each = value.shape[0] // n
    for d in range(n):
        ref[d, at : at + each] = value[d * each : (d + 1) * each].astype(BF16)


def _mlp_back(*refs, n, layer, tiles, blocks, behind, last):
    take = iter(range(len(refs)))
    some = lambda count: [refs[next(take)] for _ in range(count)]
    h_ref, att_ref = some(2)
    if last:
        (dy_ref,) = some(1)
    else:
        hn_ref, dq_ref, dk_ref, dv_ref, dh_ref, wq, wk, wv, cos, sin, gate_ref, up_ref = some(12)
    wo, wg_ref, wu_ref, wd_ref = some(4)
    dh1_ref, datt_ref, delta_ref, left_ff, left_o = some(5)
    hosted = blocks - behind
    own = some(hosted + (not last))
    h1_s = some(1)[0] if last else None
    b_s, dy_s, p_s, dg_s, du_s, sum_g, sum_u, g_s, go_s, out_sem = some(10)
    wg, wu, wd, w_sem = some(4)
    sums3 = some(1 if last else 3)
    sum_o = sums3[0]
    jobs = []
    for i in range(len(own)):
        if i < hosted:
            block = g_s.at[i]
        else:
            block = gqkv_s = g_s.at[blocks - 1]
        jobs.append(RingSum(n, block, *some(4)))
    step = pl.program_id(0)
    bt = h_ref.shape[0]
    middle = tiles * blocks
    r = jnp.where(step < tiles, step, lax.rem(step - tiles, tiles))
    j = lax.div(step - tiles, tiles)
    rows = pl.ds(pl.multiple_of(r * bt, bt), bt)
    @pl.when(step == 0)
    def _():
        _greet(n)
        for s in sums3:
            s[...] = jnp.zeros_like(s)

    loads = [pltpu.make_async_copy(a.at[layer], b.at[0], w_sem.at[i]) for i, (a, b) in enumerate(((wg_ref, wg), (wu_ref, wu), (wd_ref, wd)))]

    @pl.when(step == 0)
    def _():
        for load in loads:
            load.start()

    @pl.when(step == tiles)
    def _():
        for load in loads:
            load.wait()

    final = 2 * tiles + middle - 1
    times = [(tiles * (2 + i), tiles * (2 + i) + tiles * 3 // 2) for i in range(hosted)] + [(tiles, 2 * tiles)] * (not last)
    times = [(start, forward - 1, forward, min(forward + tiles * 3 // 2, final)) for start, forward in times]

    @pl.when(step == min(t[0] for t in times))
    def _():
        _met()

    for job, (_, _, at, _) in zip(jobs, times, strict=True):

        @pl.when(step == at)
        def _(job=job):
            job.forward()

    for job, (at, _, _, _) in zip(jobs, times, strict=True):

        @pl.when(step == at)
        def _(job=job):
            job.start()

    @pl.when(step < tiles)
    def _():
        if last:
            h1 = _after_attention(h_ref, att_ref, wo[0])
            h1_s[rows, :] = h1
            dy_s[rows, :] = dy_ref[...]
        else:
            h1 = h_ref[...]
            hn = hn_ref[...].astype(F32)
            da = _qkv_back(hn, dq_ref[...], dk_ref[...], dv_ref[...], wq[0], wk[0], wv[0], cos[...], sin[...], sums3)
            dy_s[rows, :] = (dh_ref[...].astype(F32) + _norm_back(hn, da.astype(BF16).astype(F32)).astype(BF16).astype(F32)).astype(BF16)

            @pl.when(step == tiles - 1)
            def _():
                for i, s in enumerate(sums3):
                    _cut(gqkv_s, i * (s.shape[0] // n), s[...])
                sum_o[...] = jnp.zeros_like(sum_o)

        h1 = h1.astype(F32)
        b_s[rows, :] = (h1 * _norm_scale(h1)).astype(BF16)
        sum_g[rows, :] = jnp.zeros((bt, sum_g.shape[1]), F32)
        sum_u[rows, :] = jnp.zeros((bt, sum_u.shape[1]), F32)

    @pl.when((step >= tiles) & (step < tiles + middle))
    def _():
        b, dy = b_s[rows, :], dy_s[rows, :]
        gate_w, up_w = _strips(wg, j, n, blocks, 2), _strips(wu, j, n, blocks, 2)
        if last:
            gate, up = _dot(b, gate_w), _dot(b, up_w)
        else:
            gate, up = gate_ref[0], up_ref[0]
        dp = _dot(dy, _strips(wd, j, n, blocks, 1), 1, 1).astype(BF16).astype(F32)
        sg = jax.nn.sigmoid(gate)
        silu = gate * sg
        p_s[rows, :] = (silu * up).astype(BF16)
        du = (dp * silu).astype(BF16)
        dg = (dp * up * (sg + silu * (1 - sg))).astype(BF16)
        du_s[rows, :] = du
        dg_s[rows, :] = dg
        sum_g[rows, :] += _dot(dg, gate_w, 1, 1)
        sum_u[rows, :] += _dot(du, up_w, 1, 1)

        @pl.when(r == tiles - 1)
        def _():
            each = b.shape[1] // n
            mine = g_s.at[j]
            _cut(mine, 0, _dot(p_s[...], dy_s[...], 0, 0))
            _cut(mine, mine.shape[1] - 2 * each, _dot(b_s[...], dg_s[...], 0, 0))
            _cut(mine, mine.shape[1] - each, _dot(b_s[...], du_s[...], 0, 0))

    out_copies = [pltpu.make_async_copy(g_s.at[hosted + i], left_ff.at[i], out_sem.at[i]) for i in range(behind)]
    out_copies.append(pltpu.make_async_copy(go_s, left_o, out_sem.at[behind]))

    @pl.when(step >= tiles + middle)
    def _():
        db = sum_g[rows, :].astype(BF16).astype(F32) + sum_u[rows, :].astype(BF16).astype(F32)
        h1 = h1_s[rows, :] if last else h_ref[...]
        dh1 = dy_s[rows, :].astype(F32) + _norm_back(h1.astype(F32), db.astype(BF16).astype(F32)).astype(BF16).astype(F32)
        dh1 = dh1.astype(BF16)
        dh1_ref[...] = dh1
        datt = _dot(dh1, wo[0], 1, 1).astype(BF16)
        datt_ref[...] = datt
        att = att_ref[...]
        both = att.astype(F32) * datt.astype(F32)
        for i in range(both.shape[1] // HEAD):
            delta_ref[i : i + 1, :] = both[:, i * HEAD : (i + 1) * HEAD].T.sum(axis=0, keepdims=True)
        sum_o[...] += _dot(att, dh1, 0, 0)

        @pl.when(step == tiles + middle)
        def _():
            for c in out_copies[:-1]:
                c.start()

        @pl.when(step == 2 * tiles + middle - 1)
        def _():
            _cut(go_s, 0, sum_o[...])
            out_copies[-1].start()
            for c in out_copies:
                c.wait()

    for job, (_, at, _, _) in zip(jobs, times, strict=True):

        @pl.when(step == at)
        def _(job=job):
            job.add()

    for job, (_, _, _, at), out in zip(jobs, times, own, strict=True):

        @pl.when(step == at)
        def _(job=job, out=out):
            job.finish(out)


def mlp_back(n, number, layer, h, att, by, weights, rope, upper=None, hidden=None):
    t, d = h.shape
    ff = weights["w_gate"].shape[2]
    bt = _tile(t)
    tiles, blocks = t // bt, n
    fb, each = ff // blocks, d // n
    down = fb // n
    height = down + 2 * each
    assert n == 4 and fb == d and height == 3 * each
    heads = att.shape[1] // HEAD
    middle = tiles * blocks
    r = lambda s: jnp.where(s < tiles, s, lax.rem(s - tiles, tiles))
    j = lambda s: jnp.clip(lax.div(s - tiles, tiles), 0, blocks - 1)
    edge = lambda s: jnp.where(s < tiles, s, jnp.where(s < tiles + middle, tiles - 1, s - tiles - middle))
    before = lambda s: jnp.minimum(s, tiles - 1)
    after = lambda s: jnp.maximum(s - tiles - middle, 0)
    tile = lambda f, w=d: pl.BlockSpec((bt, w), lambda s: (f(s), 0))
    fixed = lambda which, *shape: pl.BlockSpec((1, *shape), lambda s: (which, 0, 0), pipeline_mode=pl.Buffered(1))
    square, up_square = fixed(layer, d, d), fixed(layer + 1, d, d)
    anywhere = pl.BlockSpec(memory_space=pltpu.HBM)
    mlp = [square, anywhere, anywhere, anywhere]
    w4 = [weights[name] for name in ("wo", "w_gate", "w_up", "w_down")]
    last = upper is None
    if last:
        ins = [tile(before), tile(edge), tile(before), *mlp]
        args = [h, att, by, *w4]
    else:
        hn, dq, dk, dv = upper
        table = pl.BlockSpec((bt, HEAD), lambda s: (before(s), 0))
        block = pl.BlockSpec((1, bt, fb), lambda s: (j(s), r(jnp.clip(s, tiles, tiles + middle - 1)), 0))
        ins = [tile(edge), tile(after), *[tile(before)] * 5, up_square, up_square, up_square, table, table, block, block, *mlp]
        args = [h, att, hn, dq, dk, dv, by, weights["wq"], weights["wk"], weights["wv"], *rope, *hidden, *w4]
    anywhere = pl.BlockSpec(memory_space=pltpu.HBM)
    outs = [
        (tile(after), jax.ShapeDtypeStruct((t, d), BF16)),
        (tile(after), jax.ShapeDtypeStruct((t, d), BF16)),
        (pl.BlockSpec((heads, bt), lambda s: (0, after(s))), jax.ShapeDtypeStruct((heads, t), F32)),
        (anywhere, jax.ShapeDtypeStruct((BEHIND, n, height, d), BF16)),
        (anywhere, jax.ShapeDtypeStruct((n, each, d), BF16)),
        *[(pl.BlockSpec((height, d), lambda s: (0, 0)), jax.ShapeDtypeStruct((height, d), BF16))] * (blocks - BEHIND),
    ]
    scratch = [pltpu.VMEM((t, d), BF16)] * (2 + last) + [pltpu.VMEM((t, fb), BF16)] * 3 + [pltpu.VMEM((t, d), F32)] * 2
    scratch += [pltpu.VMEM((blocks, n, height, d), BF16), pltpu.VMEM((n, each, d), BF16), pltpu.SemaphoreType.DMA((BEHIND + 1,))]
    scratch += [pltpu.VMEM((1, d, ff), BF16)] * 2 + [pltpu.VMEM((1, ff, d), BF16), pltpu.SemaphoreType.DMA((3,))]
    scratch += [pltpu.VMEM((d, d), F32)] * (1 if last else 3)
    for _ in range(blocks - BEHIND):
        scratch += RingSum.scratch(n, height, d)
    if not last:
        outs += [(pl.BlockSpec((3 * each, d), lambda s: (0, 0)), jax.ShapeDtypeStruct((3 * each, d), BF16))]
        scratch += RingSum.scratch(n, 3 * each, d)
    return _call(
        functools.partial(_mlp_back, n=n, layer=layer, tiles=tiles, blocks=blocks, behind=BEHIND, last=last),
        (2 * tiles + middle,),
        ins,
        outs,
        scratch,
        args,
        2 * t * d * (ff * 8 + d * 4),
        sum(a.size * a.dtype.itemsize for a in args),
        collective=number,
    )


class Parts:
    def __init__(self, n, layers, each):
        self.hosted, self.per, self.each = n - BEHIND, n - BEHIND + 2, each

    def ff(self, layer, block, which):
        if block < self.hosted:
            return layer * self.per + block, which * self.each
        return layer * self.per + self.hosted, ((block - self.hosted) * 3 + which) * self.each

    def square(self, layer, which):
        if which == 3:
            return layer * self.per + self.hosted, BEHIND * 3 * self.each
        return layer * self.per + self.hosted + 1, which * self.each


def _moments(m, v, g):
    return 0.9 * m + 0.1 * g, 0.95 * v + 0.05 * g * g


def _stepped(w, m, v):
    return (w - 0.02 * (m * lax.rsqrt(v + 1e-8) + 0.1 * w)).astype(BF16)


def _finish(*refs, n, layers, own_count, count):
    take = iter(range(len(refs)))
    some = lambda k: [refs[next(take)] for _ in range(k)]
    h_ref, dq_ref, dk_ref, dv_ref, cos, sin = some(6)
    own_in, w_ref, m_ref, v_ref = some(own_count), some(7), some(7), some(7)
    own_ref, factor_ref = some(2)
    outs = some(7)
    h_s, dq_s, dk_s, dv_s, cos_s, sin_s, a_s, g_s, squares, total_s, others_s = some(11)
    pieces_s, lands, m_s, v_s = some(own_count), some(7), some(7), some(7)
    load_sem, w_sem, m_sem, v_sem, swap_out, swap_in, store_sem, out_r, out_l, in_l, in_r, pass_r, pass_l, far_l, far_r = some(15)
    jobs = [RingSum(n, g_s.at[i], *some(4)) for i in range(3)]
    me, right, far, left = _ring(n)
    mesh = pl.DeviceIdType.MESH
    barrier = pltpu.get_barrier_semaphore()
    for other in (right, far, left):
        pl.semaphore_signal(barrier, inc=1, device_id={"dp": other}, device_id_type=mesh)
    pairs = [(h_ref, h_s), (dv_ref, dv_s), (dk_ref, dk_s), (cos, cos_s), (sin, sin_s), (dq_ref, dq_s), *zip(own_in, pieces_s, strict=True)]
    loads = [pltpu.make_async_copy(s, d, load_sem.at[i]) for i, (s, d) in enumerate(pairs)]
    for load in loads:
        load.start()
    state = []
    for i in range(7):
        state.append(pltpu.make_async_copy(w_ref[i].at[:, me], lands[i].at[:, me], w_sem.at[i]))
        state.append(pltpu.make_async_copy(m_ref[i], m_s[i], m_sem.at[i]))
        state.append(pltpu.make_async_copy(v_ref[i], v_s[i], v_sem.at[i]))
    t = h_s.shape[0]
    each = g_s.shape[2]
    squares[...] = jnp.zeros_like(squares)
    loads[0].wait()

    def norm(rows):
        h = h_s[rows, :].astype(F32)
        a_s[rows, :] = (h * _norm_scale(h)).astype(BF16)

    _rows_loop(t, norm, 256)

    def turn(ref):
        def one(rows):
            ref[rows, :] = _turn(ref[rows, :].astype(F32), cos_s[rows, :], -sin_s[rows, :]).astype(BF16)

        _rows_loop(t, one, 256)

    loads[1].wait()
    _cut(g_s.at[2], 0, _dot(a_s[...], dv_s[...], 0, 0))
    pl.semaphore_wait(barrier, 3)
    for i in (2, 3, 4):
        loads[i].wait()
    turn(dk_s)
    jobs[2].start()
    for c in state:
        c.start()
    _cut(g_s.at[1], 0, _dot(a_s[...], dk_s[...], 0, 0))
    loads[5].wait()
    turn(dq_s)
    jobs[1].start()
    jobs[2].add()
    _cut(g_s.at[0], 0, _dot(a_s[...], dq_s[...], 0, 0))
    jobs[2].forward()
    jobs[1].add()
    jobs[0].start()
    for i, piece in enumerate(pieces_s):
        loads[6 + i].wait()
        if i == 1:
            jobs[1].forward()
        _rows_loop(piece.shape[0], lambda rows, piece=piece: _add_squares(squares, piece[rows, :]))
    jobs[0].add()
    jobs[2].finish(own_ref.at[pl.ds(2 * each, each)], squares)
    jobs[0].forward()
    jobs[1].finish(own_ref.at[pl.ds(each, each)], squares)
    jobs[0].finish(own_ref.at[pl.ds(0, each)], squares)
    total_s[...] = sum(squares[:, i : i + 128] for i in range(0, squares.shape[1], 128))
    swaps = [
        pltpu.make_async_remote_copy(src_ref=total_s, dst_ref=others_s.at[i], send_sem=swap_out.at[i], recv_sem=swap_in.at[i], device_id={"dp": other},
                                     device_id_type=mesh)
        for i, other in enumerate((right, far, left))
    ]
    for s in swaps:
        s.start()
    for c in state:
        c.wait()
    for s in swaps:
        s.wait()
    everything = jnp.sum(total_s[...] + others_s[0] + others_s[1] + others_s[2], keepdims=True)
    factor = jnp.minimum(1.0, 0.5 * lax.rsqrt(everything / count + 1e-30))
    factor_ref[...] = jnp.broadcast_to(factor, factor_ref.shape)

    parts = Parts(n, layers, each)
    grads = [*pieces_s[: parts.per - 1], own_ref, *pieces_s[parts.per - 1 :]]
    blocks = n

    def new_weights(i, layer):
        land, m_i, v_i = lands[i], m_s[i], v_s[i]

        def one(at, piece, row, rows, column, g_column, width):
            def body(some):
                here = pl.ds(at + some.start, some.size)
                g = grads[piece][pl.ds(row + some.start, some.size), g_column : g_column + width].astype(F32) * factor
                m, v = _moments(m_i[layer, here, column : column + width], v_i[layer, here, column : column + width], g)
                w = land[layer, me, here, column : column + width].astype(F32)
                land[layer, me, here, column : column + width] = _stepped(w, m, v)

            return body

        if i < 4:
            bodies, rows = [one(0, *parts.square(layer, i), each, 0, 0, land.shape[3])], each
        elif i == 6:
            rows = each
            bodies = [one(b * each, *parts.ff(layer, b, 0), each, 0, 0, land.shape[3]) for b in range(blocks)]
        else:
            width, rows = g_s.shape[3] // n, each
            bodies = [
                one(0, *parts.ff(layer, b, i - 3), each, (d * blocks + b) * width, d * width, width) for d in range(n) for b in range(blocks)
            ]

        def run(some):
            for body in bodies:
                body(some)

        _rows_loop(rows, run, 16)

    remote = lambda ref, to, sent, got: pltpu.make_async_remote_copy(
        src_ref=ref, dst_ref=ref, send_sem=sent, recv_sem=got, device_id={"dp": to}, device_id_type=mesh)
    units = [(i, layer) for i in (3, 0, 1, 2, 6, 4, 5) for layer in range(layers)]
    store = lambda which, kind, u: pltpu.make_async_copy(
        lands[units[u][0]].at[units[u][1], which], outs[units[u][0]].at[units[u][1], which], store_sem.at[kind, u])
    sends, passes = [], []
    for u, (i, layer) in enumerate(units):
        new_weights(i, layer)
        mine = lands[i].at[layer, me]
        sends.append((remote(mine, right, out_r.at[u], in_l.at[u]), remote(mine, left, out_l.at[u], in_r.at[u])))
        for c in sends[-1]:
            c.start()
        store(me, 0, u).start()
    for u, (i, layer) in enumerate(units):
        half = lands[i].shape[2] // 2
        sends[u][0].wait_recv()
        one = remote(lands[i].at[layer, left, pl.ds(0, half)], right, pass_r.at[u], far_l.at[u])
        one.start()
        store(left, 1, u).start()
        sends[u][1].wait_recv()
        two = remote(lands[i].at[layer, right, pl.ds(half, half)], left, pass_l.at[u], far_r.at[u])
        two.start()
        store(right, 2, u).start()
        passes.append((one, two))
    for u in range(len(units)):
        for c in passes[u]:
            c.wait_recv()
        store(far, 3, u).start()
    for u in range(len(units)):
        for c in (*sends[u], *passes[u]):
            c.wait_send()
        for kind, which in enumerate((me, left, right, far)):
            store(which, kind, u).wait()


def finish(n, number, h, dq, dk, dv, rope, own, w, m, v):
    t, d = h.shape
    each, layers = d // n, w[0].shape[0]
    anywhere, here = pl.BlockSpec(memory_space=pltpu.HBM), pl.BlockSpec(memory_space=pltpu.VMEM)
    w = [a.reshape(layers, n, a.shape[1] // n, a.shape[2]) for a in w]
    shapes = [a.shape for a in w]
    scratch = [pltpu.VMEM((t, d), BF16)] * 4 + [pltpu.VMEM((t, HEAD), F32)] * 2
    scratch += [pltpu.VMEM((t, d), BF16), pltpu.VMEM((3, n, each, d), BF16), pltpu.VMEM((8, d), F32), pltpu.VMEM((8, 128), F32),
                pltpu.VMEM((3, 8, 128), F32)]
    scratch += [pltpu.VMEM(o.shape, BF16) for o in own] + [pltpu.VMEM(s, BF16) for s in shapes] + [pltpu.VMEM(a.shape, F32) for a in (*m, *v)]
    units = 7 * layers
    sem = lambda *k: pltpu.SemaphoreType.DMA(k)
    scratch += [sem(6 + len(own)), sem(7), sem(7), sem(7), sem(3), sem(3), sem(4, units), *[sem(units)] * 8]
    for _ in range(3):
        scratch += RingSum.scratch(n, each, d)
    return _call(
        functools.partial(_finish, n=n, layers=layers, own_count=len(own), count=n * sum(a.size for a in m)),
        (),
        [anywhere] * (6 + len(own) + 21),
        [(here, jax.ShapeDtypeStruct((3 * each, d), BF16)), (here, jax.ShapeDtypeStruct((8, 128), F32)),
         *((anywhere, jax.ShapeDtypeStruct(s, BF16)) for s in shapes)],
        scratch,
        (h, dq, dk, dv, *rope, *own, *w, *m, *v),
        6 * t * d * d,
        8 * t * d,
        collective=number,
    )


def _settle(factor_ref, *refs, n, layers, own_count):
    own, rest = refs[:own_count], refs[own_count:]
    m, v, w, w_out, m_out, v_out = (rest[7 * i : 7 * i + 7] for i in range(6))
    factor = factor_ref[0:1, 0:1]
    parts = Parts(n, layers, 1)
    for i in range(7):
        w_out[i][...] = w[i][...]

    def one(i, at, piece, row, columns=slice(None)):
        g = own[piece][row][:, columns].astype(F32) * factor
        m_out[i][at], v_out[i][at] = _moments(m[i][at], v[i][at], g)

    for layer in range(layers):
        for i in range(4):
            one(i, (layer,), *parts.square(layer, i))
        for b in range(n):
            one(6, (layer, b), *parts.ff(layer, b, 0))
            width = own[0].shape[2] // n
            for d in range(n):
                for i in (4, 5):
                    at = slice((d * n + b) * width, (d * n + b + 1) * width)
                    one(i, (layer, slice(None), at), *parts.ff(layer, b, i - 3), slice(d * width, (d + 1) * width))


def settle(n, factor, own, w, m, v):
    layers, _, each, d = w[0].shape
    ff = w[4].shape[3]
    deep = 16
    steps = each // deep
    own = [a.reshape(a.shape[0] // each, each, d) for a in own]
    cut = lambda a: a.reshape(layers, -1, each, d)
    m_in, v_in, w_in = [*m[:6], cut(m[6])], [*v[:6], cut(v[6])], [*w[:6], cut(w[6])]
    thin, thick = (pl.BlockSpec((layers, deep, c), lambda s: (0, s, 0)) for c in (d, ff))
    deeper = lambda a: pl.BlockSpec((layers, a.shape[1], deep, a.shape[3]), lambda s: (0, 0, s, 0))
    state = [thin] * 4 + [thick] * 2 + [deeper(m_in[6])]
    whole = [deeper(a) for a in w_in]
    out = _call(
        functools.partial(_settle, n=n, layers=layers, own_count=len(own)),
        (steps,),
        [pl.BlockSpec((8, 128), lambda s: (0, 0)), *(pl.BlockSpec((a.shape[0], deep, d), lambda s: (0, s, 0)) for a in own), *state, *state, *whole],
        [*((spec, jax.ShapeDtypeStruct(a.shape, a.dtype)) for spec, a in zip((*whole, *state, *state), (*w_in, *m_in, *v_in), strict=True))],
        [],
        (factor, *own, *m_in, *v_in, *w_in),
        8 * sum(a.size for a in m),
        32 * sum(a.size for a in m),
    )
    flat = lambda a: a.reshape(layers, -1, a.shape[-1])
    return tuple(flat(a) for a in out)


NAMES = ("wq", "wk", "wv", "wo", "w_gate", "w_up", "w_down")


def rope_tables(t):
    half = HEAD // 2
    angle = np.arange(t, dtype=np.float32)[:, None] * (np.float32(THETA) ** (-np.arange(half, dtype=np.float32) / half)).astype(np.float32)
    cos, sin = np.cos(angle.astype(np.float64)).astype(np.float32), np.sin(angle.astype(np.float64)).astype(np.float32)
    return jnp.asarray(np.concatenate([cos, cos], 1)), jnp.asarray(np.concatenate([-sin, sin], 1))


def solution(mesh):
    n = mesh.shape["dp"]

    def step(x, dy, *arrays):
        weights = dict(zip(NAMES, arrays[:7], strict=True))
        m, v = arrays[7:14], arrays[14:]
        layers = weights["wq"].shape[0]
        h = x[0]
        rope = rope_tables(h.shape[0])
        made = forward(n, h, weights, rope)
        hs = [h, *(one[6] for one in made[:-1])]
        own = {}
        by, upper, number = dy[0], None, 0
        for layer in reversed(range(layers)):
            if upper is None:
                got = mlp_back(n, number, layer, hs[layer], made[layer][3], by, weights, rope)
            else:
                got = mlp_back(n, number, layer, made[layer][5], made[layer][3], by, weights, rope, upper, made[layer][7:9])
                own[layer + 1].append(got[5 + n - BEHIND])
            by, datt, delta, left_ff, left_o = got[:5]
            dq, dk, dv, rest = attend_back(n, number + 1, *made[layer][:3], datt, made[layer][4], delta, left_ff, left_o)
            own[layer] = [*got[5 : 5 + n - BEHIND], rest]
            upper = hs[layer], dq, dk, dv
            number += 2
        pieces = [p for layer in range(layers) for p in own[layer]]
        last, factor, *whole = finish(n, number, *upper, rope, pieces, arrays[:7], m, v)
        own[0].append(last)
        return settle(n, factor, [p for layer in range(layers) for p in own[layer]], whole, m, v)

    states, all_of, cut = P(("rep", "dp"), None, None), P(None, None, None), P(None, "dp", None)
    return jax.shard_map(
        step,
        mesh=mesh,
        in_specs=(states, states) + (all_of,) * 7 + (cut,) * 14,
        out_specs=(P("rep", None, None),) * 7 + (P("rep", "dp", None),) * 14,
        check_vma=False,
    )
```

```python
import functools

import jax
import jax.numpy as jnp
import numpy as np
from jax import lax
from jax.experimental import pallas as pl
from jax.experimental.pallas import tpu as pltpu
from jax.sharding import PartitionSpec as P

F32, BF16 = jnp.float32, jnp.bfloat16
HEAD = 128
THETA = 10000
NEG = -1e30
HIDDEN = 2 * NEG
LOG2E = 1.4426950408889634
SCALE = HEAD**-0.5
VMEM = 67043328
REST = 46 * 2**20
BEHIND = 1


def _dot(a, b, ca=1, cb=0):
    return lax.dot_general(a, b, (((ca,), (cb,)), ((), ())), preferred_element_type=F32)


def _tile(size, most=512):
    return max(n for n in range(128, most + 1, 128) if size % n == 0)


def _call(kernel, grid, ins, outs, scratch, args, flops, moved, collective=None, vmem=VMEM):
    return pl.pallas_call(
        kernel,
        grid=grid,
        in_specs=[spec for spec in ins],
        out_specs=[spec for spec, _ in outs],
        out_shape=[shape for _, shape in outs],
        scratch_shapes=scratch,
        compiler_params=pltpu.CompilerParams(dimension_semantics=("arbitrary",) * len(grid), vmem_limit_bytes=vmem, collective_id=collective,
                                             has_side_effects=collective is not None),
        cost_estimate=pl.CostEstimate(flops=int(flops), transcendentals=0, bytes_accessed=int(moved)),
    )(*args)


def _norm_scale(x):
    return lax.rsqrt(jnp.mean(x * x, -1, keepdims=True) + 1e-6)


def _norm_back(x, d_out):
    s = _norm_scale(x)
    inner = jnp.mean(x * d_out, -1, keepdims=True)
    return s * d_out - x * (s * s * s * inner)


def _turn(x, cos, sin):
    parts = [x[:, n : n + HEAD] for n in range(0, x.shape[1], HEAD)]
    return jnp.concatenate([p * cos + pltpu.roll(p, HEAD // 2, 1) * sin for p in parts], 1)


def _qkv(h, wq, wk, wv, cos, sin):
    a = (h * _norm_scale(h)).astype(BF16)
    q, k = (_turn(_dot(a, w).astype(BF16).astype(F32), cos, sin).astype(BF16) for w in (wq, wk))
    return q, k, _dot(a, wv).astype(BF16)


def _after_attention(h_ref, att_ref, wo):
    return (h_ref[...].astype(F32) + _dot(att_ref[...], wo).astype(BF16).astype(F32)).astype(BF16)


def _seen(keys, queries):
    return lax.broadcasted_iota(jnp.int32, (keys, queries), 1) >= lax.broadcasted_iota(jnp.int32, (keys, queries), 0)


def diagonal(block, first, size, part=256):
    part = min(part, size)
    for at in range(0, size, part):
        block(first + at, part, at, True)


def _attend(iq, q_ref, k_ref, v_ref, o_ref, lse_ref, top_s, mix_s, bk):
    bq = q_ref.shape[0]
    heads = q_ref.shape[1] // HEAD
    e = SCALE * LOG2E
    top_s[...] = jnp.full(top_s.shape, NEG, F32)
    mix_s[...] = jnp.zeros(mix_s.shape, F32)

    def block(first, keys, at, masked):
        here, ask = pl.ds(pl.multiple_of(first, keys), keys), slice(at, bq)
        cols = [slice(n * HEAD, (n + 1) * HEAD) for n in range(heads)]
        scores = [_dot(k_ref[here, c], q_ref[ask, c], 1, 1) for c in cols]
        weights, keeps = [], []
        seen = _seen(keys, bq - at) if masked else None
        for n, s in enumerate(scores):
            if masked:
                s = jnp.where(seen, s, HIDDEN)
            old = top_s[n : n + 1, ask]
            top = jnp.maximum(old, s.max(axis=0, keepdims=True))
            top_s[n : n + 1, ask] = top
            weights.append(jnp.exp2((s - top) * e).astype(BF16))
            keeps.append(jnp.exp2((old - top) * e))
        ones = jnp.ones((8, keys), BF16)
        for n, (c, p, keep) in enumerate(zip(cols, weights, keeps)):
            values = jnp.concatenate([v_ref[here, c].T, ones], axis=0)
            mix_s[n, :, ask] = mix_s[n, :, ask] * keep + _dot(values, p, 1, 0)

    lax.fori_loop(0, iq * (bq // bk), lambda j, _: block(j * bk, bk, 0, False), None)
    diagonal(block, iq * bq, bq)
    for n in range(heads):
        total = mix_s[n, HEAD : HEAD + 1, :]
        o_ref[:, n * HEAD : (n + 1) * HEAD] = (mix_s[n, :HEAD, :] * (1 / total)).T.astype(BF16)
        lse_ref[n : n + 1, :] = top_s[n : n + 1, :] * e + jnp.log2(total)


def _forward(h_ref, wq, wk, wv, wo, wg_ref, wu_ref, wd_ref, cos, sin, *refs, n, layers):
    outs, scratch = refs[: 9 * layers - 4], refs[9 * layers - 4 :]
    k_s, v_s, wg, wu, wd, gate_s, up_s, top_s, mix_s, w_sem, out_sem = scratch
    step = pl.program_id(0)
    bt = h_ref.shape[0]
    rows = pl.ds(pl.multiple_of(step * bt, bt), bt)
    loads = [pltpu.make_async_copy(a.at[0], b.at[0], w_sem.at[i]) for i, (a, b) in enumerate(((wg_ref, wg), (wu_ref, wu), (wd_ref, wd)))]

    @pl.when(step == 0)
    def _():
        for load in loads:
            load.start()

    for layer in range(layers):
        q_ref, k_ref, v_ref, att_ref, lse_ref = outs[9 * layer : 9 * layer + 5]
        q_ref[...], k, v = _qkv(h_ref[...].astype(F32), wq[layer], wk[layer], wv[layer], cos[...], sin[...])
        k_ref[...] = k_s[layer, rows, :] = k
        v_ref[...] = v_s[layer, rows, :] = v
        _attend(step, q_ref, k_s.at[layer], v_s.at[layer], att_ref, lse_ref, top_s, mix_s, bt)
        if layer == layers - 1:
            break
        h1_ref, y_ref, gate_ref, up_ref = outs[9 * layer + 5 : 9 * layer + 9]
        stores = [
            pltpu.make_async_copy(a.at[j], b.at[j, rows], out_sem.at[layer, i, j])
            for i, (a, b) in enumerate(((gate_s, gate_ref), (up_s, up_ref)))
            for j in range(n)
        ]

        @pl.when(step == 0)
        def _(layer=layer):
            for load in loads:
                load.wait()

        @pl.when(step > 0)
        def _(stores=stores):
            for c in stores:
                c.wait()

        h1 = _after_attention(h_ref, att_ref, wo[layer])
        h1_ref[...] = h1
        h1 = h1.astype(F32)
        b = (h1 * _norm_scale(h1)).astype(BF16)
        total = jnp.zeros(h1.shape, F32)
        for j in range(n):
            gate, up = _dot(b, _strips(wg, j, n, n, 2)), _dot(b, _strips(wu, j, n, n, 2))
            gate_s[j] = gate
            up_s[j] = up
            total += _dot((gate * jax.nn.sigmoid(gate) * up).astype(BF16), _strips(wd, j, n, n, 1))
        for c in stores:
            c.start()
        y_ref[...] = (h1 + total.astype(BF16).astype(F32)).astype(BF16)
        h_ref = y_ref

        @pl.when(step == pl.num_programs(0) - 1)
        def _(stores=stores):
            for c in stores:
                c.wait()


def forward(n, h, weights, rope):
    t, d = h.shape
    layers, _, ff = weights["w_gate"].shape
    assert layers == 2
    heads = weights["wq"].shape[2] // HEAD
    bt = _tile(t)
    tile, table = (pl.BlockSpec((bt, w), lambda s: (s, 0)) for w in (d, HEAD))
    square = pl.BlockSpec((layers, d, d), lambda s: (0, 0, 0), pipeline_mode=pl.Buffered(1))
    anywhere = pl.BlockSpec(memory_space=pltpu.HBM)
    one = (tile, jax.ShapeDtypeStruct((t, d), BF16))
    two = (anywhere, jax.ShapeDtypeStruct((n, t, ff // n), F32))
    stats = (pl.BlockSpec((heads, bt), lambda s: (0, s)), jax.ShapeDtypeStruct((heads, t), F32))
    upper = [*[one] * 4, stats]
    got = _call(
        functools.partial(_forward, n=n, layers=layers),
        (t // bt,),
        [tile, *[square] * 4, *[anywhere] * 3, table, table],
        [*[*upper, one, one, two, two] * (layers - 1), *upper],
        [pltpu.VMEM((layers, t, d), BF16)] * 2
        + [pltpu.VMEM((1, d, ff), BF16)] * 2
        + [pltpu.VMEM((1, ff, d), BF16)]
        + [pltpu.VMEM((n, bt, ff // n), F32)] * 2
        + [pltpu.VMEM((heads, bt), F32), pltpu.VMEM((heads, HEAD + 8, bt), F32), pltpu.SemaphoreType.DMA((3,)),
           pltpu.SemaphoreType.DMA((layers, 2, n))],
        (h, *(weights[name] for name in ("wq", "wk", "wv", "wo")), *(weights[name] for name in ("w_gate", "w_up", "w_down")), *rope),
        2 * t * d * (8 * d + 3 * ff) + 4 * t * t * d,
        30 * t * d + 8 * t * ff,
    )
    return [got[9 * layer : 9 * layer + 9] for layer in range(layers)]


def _ring(n):
    me = lax.axis_index("dp")
    return me, lax.rem(me + 1, n), lax.rem(me + 2, n), lax.rem(me + n - 1, n)


def _greet(n):
    _, right, _, left = _ring(n)
    barrier = pltpu.get_barrier_semaphore()
    for other in (right, left):
        pl.semaphore_signal(barrier, inc=1, device_id={"dp": other}, device_id_type=pl.DeviceIdType.MESH)


def _met():
    pl.semaphore_wait(pltpu.get_barrier_semaphore(), 2)


def _rows_loop(rows, body, most=32):
    each = max(c for c in range(16, most + 1, 16) if rows % c == 0)
    lax.fori_loop(0, rows // each, lambda i, _: body(pl.ds(pl.multiple_of(i * each, each), each)), None)


class RingSum:
    def __init__(self, n, block, passing, arrived, sent, got):
        self.block, self.passing, self.arrived = block, passing, arrived
        self.me, right, far, left = _ring(n)
        self.near = right, left
        half = block.shape[1] // 2
        self.half = half
        a, b = pl.ds(0, half), pl.ds(half, half)
        moves = [
            (block.at[far, a], passing.at[0], right),
            (block.at[far, b], passing.at[1], left),
            (block.at[right, b], arrived.at[0, b], right),
            (block.at[left, a], arrived.at[1, a], left),
            (passing.at[0], arrived.at[0, a], right),
            (passing.at[1], arrived.at[1, b], left),
        ]
        self.copies = [
            pltpu.make_async_remote_copy(src_ref=s, dst_ref=d, send_sem=sent.at[i], recv_sem=got.at[i], device_id={"dp": to},
                                         device_id_type=pl.DeviceIdType.MESH)
            for i, (s, d, to) in enumerate(moves)
        ]

    @staticmethod
    def scratch(n, rows, columns):
        half = pltpu.VMEM((2, rows // 2, columns), BF16)
        return [half, pltpu.VMEM((2, rows, columns), BF16), pltpu.SemaphoreType.DMA((6,)), pltpu.SemaphoreType.DMA((6,))]

    def start(self):
        for c in self.copies[:4]:
            c.start()

    def add(self):
        for c in self.copies[:2]:
            c.wait_recv()
        for i, other in enumerate(self.near):

            def one(rows, i=i, other=other):
                mine = self.block[other, pl.ds(rows.start + i * self.half, rows.size), :]
                self.passing[i, rows, :] = (self.passing[i, rows, :].astype(F32) + mine.astype(F32)).astype(BF16)

            _rows_loop(self.half, one)

    def forward(self):
        for c in self.copies[4:]:
            c.start()

    def finish(self, out, squares=None):
        for c in self.copies[2:]:
            c.wait_recv()

        def one(rows):
            total = self.block[self.me, rows, :].astype(F32) + self.arrived[0, rows, :].astype(F32) + self.arrived[1, rows, :].astype(F32)
            total = total.astype(BF16)
            out[rows, :] = total
            if squares is not None:
                _add_squares(squares, total)

        _rows_loop(self.half * 2, one)
        for c in self.copies:
            c.wait_send()


def _add_squares(squares, value):
    value = value.astype(F32)
    value = value * value
    squares[...] += sum(value[i : i + 8] for i in range(0, value.shape[0], 8))


def _attend_back(q_ref, k_ref, v_ref, do_ref, lse_ref, delta_ref, ff_ref, o_ref, dq_ref, dk_ref, dv_ref, own_ref, dq_s, dk_s, dv_s, block_s, load_sem,
                 *ring, bk, n):
    iq = pl.program_id(0)
    bq = q_ref.shape[0]
    heads = q_ref.shape[1] // HEAD
    e = SCALE * LOG2E
    steps = pl.num_programs(0)
    behind, _, each, _ = ff_ref.shape
    loads = [pltpu.make_async_copy(ff_ref.at[i], block_s.at[:, pl.ds(i * each, each)], load_sem.at[i]) for i in range(behind)]
    loads.append(pltpu.make_async_copy(o_ref, block_s.at[:, pl.ds(behind * each, o_ref.shape[1])], load_sem.at[behind]))
    job = RingSum(n, block_s, *ring)

    @pl.when(iq == 0)
    def _():
        _greet(n)
        for load in loads:
            load.start()
        dk_s[...] = jnp.zeros_like(dk_s)
        dv_s[...] = jnp.zeros_like(dv_s)

    @pl.when(iq == 1)
    def _():
        for load in loads:
            load.wait()
        _met()
        job.start()

    @pl.when(iq == steps - 1)
    def _():
        job.forward()

    dq_s[...] = jnp.zeros_like(dq_s)

    def block(first, keys, at, masked):
        here, ask = pl.ds(pl.multiple_of(first, keys), keys), slice(at, bq)
        cols = [slice(i * HEAD, (i + 1) * HEAD) for i in range(heads)]
        scores = [_dot(k_ref[here, c], q_ref[ask, c], 1, 1) for c in cols]
        dps = [_dot(v_ref[here, c], do_ref[ask, c], 1, 1) for c in cols]
        seen = _seen(keys, bq - at) if masked else None
        for i, c in enumerate(cols):
            p = jnp.exp2(scores[i] * e - lse_ref[i : i + 1, ask])
            if masked:
                p = jnp.where(seen, p, 0.0)
            ds = (p * (dps[i] - delta_ref[i : i + 1, ask])).astype(BF16)
            dv_s[here, c] += _dot(p.astype(BF16), do_ref[ask, c], 1, 0)
            dk_s[here, c] += _dot(ds, q_ref[ask, c], 1, 0)
            dq_s[i, :, ask] += _dot(k_ref[here, c].T, ds, 1, 0)

    lax.fori_loop(0, iq * (bq // bk), lambda j, _: block(j * bk, bk, 0, False), None)
    diagonal(block, iq * bq, bq)

    @pl.when(iq == steps - 2)
    def _():
        job.add()

    for i in range(heads):
        dq_ref[:, i * HEAD : (i + 1) * HEAD] = (dq_s[i] * SCALE).T.astype(BF16)

    @pl.when(iq == steps - 1)
    def _():
        dk_ref[...] = (dk_s[...] * SCALE).astype(BF16)
        dv_ref[...] = dv_s[...].astype(BF16)
        job.finish(own_ref)


def attend_back(n, number, q, k, v, d_out, lse, delta, ff, o):
    t, width = q.shape
    heads = width // HEAD
    bq = bk = _tile(t)
    rows, whole = pl.BlockSpec((bq, width), lambda i: (i, 0)), pl.BlockSpec((t, width), lambda i: (0, 0))
    stats = pl.BlockSpec((heads, bq), lambda i: (0, i))
    one = jax.ShapeDtypeStruct((t, width), BF16)
    height, columns = ff.shape[0] * ff.shape[2] + o.shape[1], ff.shape[3]
    return _call(
        functools.partial(_attend_back, bk=bk, n=n),
        (t // bq,),
        [rows, whole, whole, rows, stats, stats, pl.BlockSpec(memory_space=pltpu.HBM), pl.BlockSpec(memory_space=pltpu.HBM)],
        [(rows, one), (whole, one), (whole, one),
         (pl.BlockSpec((height, columns), lambda i: (0, 0)), jax.ShapeDtypeStruct((height, columns), BF16))],
        [pltpu.VMEM((heads, HEAD, bq), F32), pltpu.VMEM((t, width), F32), pltpu.VMEM((t, width), F32),
         pltpu.VMEM((n, height, columns), BF16), pltpu.SemaphoreType.DMA((ff.shape[0] + 1,)),
         *RingSum.scratch(n, height, columns)],
        (q, k, v, d_out, lse, delta, ff, o),
        5 * t * t * width,
        14 * t * width,
        collective=number,
    )


def _strips(ref, block, n, blocks, axis):
    width = ref.shape[axis] // (n * blocks)
    at = [pl.ds(pl.multiple_of((d * blocks + block) * width, width), width) for d in range(n)]
    return jnp.concatenate([ref[0, :, a] if axis == 2 else ref[0, a, :] for a in at], axis - 1)


def _qkv_back(h, dq, dk, dv, wq, wk, wv, cos, sin, sums):
    a = (h * _norm_scale(h)).astype(BF16)
    dq, dk = (_turn(d.astype(F32), cos, -sin).astype(BF16) for d in (dq, dk))
    for s, d in zip(sums, (dq, dk, dv), strict=True):
        s[...] += _dot(a, d, 0, 0)
    return _dot(jnp.concatenate([dq, dk, dv], 1), jnp.concatenate([wq, wk, wv], 1), 1, 1)


def _cut(ref, at, value):
    n = ref.shape[0]
    each = value.shape[0] // n
    for d in range(n):
        ref[d, at : at + each] = value[d * each : (d + 1) * each].astype(BF16)


def _mlp_back(*refs, n, layer, tiles, blocks, behind, last):
    take = iter(range(len(refs)))
    some = lambda count: [refs[next(take)] for _ in range(count)]
    h_ref, att_ref = some(2)
    if last:
        (dy_ref,) = some(1)
    else:
        hn_ref, dq_ref, dk_ref, dv_ref, dh_ref, wq, wk, wv, cos, sin, gate_ref, up_ref = some(12)
    wo, wg_ref, wu_ref, wd_ref = some(4)
    dh1_ref, datt_ref, delta_ref, left_ff, left_o = some(5)
    hosted = blocks - behind
    own = some(hosted + (not last))
    h1_s = some(1)[0] if last else None
    b_s, dy_s, p_s, dg_s, du_s, sum_b, g_s, go_s, out_sem = some(9)
    wg, wu, wd, w_sem = some(4)
    sums3 = some(1 if last else 3)
    sum_o = sums3[0]
    jobs = []
    for i in range(len(own)):
        if i < hosted:
            block = g_s.at[i]
        else:
            block = gqkv_s = g_s.at[blocks - 1]
        jobs.append(RingSum(n, block, *some(4)))
    step = pl.program_id(0)
    bt = h_ref.shape[0]
    middle = tiles * blocks
    r = jnp.where(step < tiles, step, lax.rem(step - tiles, tiles))
    j = lax.div(step - tiles, tiles)
    rows = pl.ds(pl.multiple_of(r * bt, bt), bt)
    @pl.when(step == 0)
    def _():
        _greet(n)
        for s in sums3:
            s[...] = jnp.zeros_like(s)

    loads = [pltpu.make_async_copy(a.at[layer], b.at[0], w_sem.at[i]) for i, (a, b) in enumerate(((wg_ref, wg), (wu_ref, wu), (wd_ref, wd)))]

    @pl.when(step == 0)
    def _():
        for load in loads:
            load.start()

    @pl.when(step == tiles)
    def _():
        for load in loads:
            load.wait()

    final = 2 * tiles + middle - 1
    times = [(at, min(at + tiles * 3 // 2, tiles + middle)) for at in (tiles * (2 + i) for i in range(hosted))] + [(tiles, 2 * tiles)] * (not last)
    times = [(start, forward - 1, forward, min(forward + tiles * 3 // 2, final)) for start, forward in times]

    @pl.when(step == min(t[0] for t in times))
    def _():
        _met()

    for job, (_, _, at, _) in zip(jobs, times, strict=True):

        @pl.when(step == at)
        def _(job=job):
            job.forward()

    for job, (at, _, _, _) in zip(jobs, times, strict=True):

        @pl.when(step == at)
        def _(job=job):
            job.start()

    @pl.when(step < tiles)
    def _():
        if last:
            h1 = _after_attention(h_ref, att_ref, wo[0])
            h1_s[rows, :] = h1
            dy_s[rows, :] = dy_ref[...]
        else:
            h1 = h_ref[...]
            hn = hn_ref[...].astype(F32)
            da = _qkv_back(hn, dq_ref[...], dk_ref[...], dv_ref[...], wq[0], wk[0], wv[0], cos[...], sin[...], sums3)
            dy_s[rows, :] = (dh_ref[...].astype(F32) + _norm_back(hn, da.astype(BF16).astype(F32)).astype(BF16).astype(F32)).astype(BF16)

            @pl.when(step == tiles - 1)
            def _():
                for i, s in enumerate(sums3):
                    _cut(gqkv_s, i * (s.shape[0] // n), s[...])
                sum_o[...] = jnp.zeros_like(sum_o)

        h1 = h1.astype(F32)
        b_s[rows, :] = (h1 * _norm_scale(h1)).astype(BF16)
        sum_b[rows, :] = jnp.zeros((bt, sum_b.shape[1]), F32)

    @pl.when((step >= tiles) & (step < tiles + middle))
    def _():
        b, dy = b_s[rows, :], dy_s[rows, :]
        gate_w, up_w, down_w = _strips(wg, j, n, blocks, 2), _strips(wu, j, n, blocks, 2), _strips(wd, j, n, blocks, 1)
        terms = []
        for at in range(0, gate_w.shape[1], 256):
            c = slice(at, at + 256)
            gate, up = (_dot(b, gate_w[:, c]), _dot(b, up_w[:, c])) if last else (gate_ref[0, :, c], up_ref[0, :, c])
            dp = _dot(dy, down_w[c], 1, 1).astype(BF16).astype(F32)
            sg = jax.nn.sigmoid(gate)
            silu = gate * sg
            p_s[rows, c] = (silu * up).astype(BF16)
            du = (dp * silu).astype(BF16)
            dg = (dp * up * (sg + silu * (1 - sg))).astype(BF16)
            du_s[rows, c] = du
            dg_s[rows, c] = dg
            terms.append((dg, du))
        sum_b[rows, :] += _dot(jnp.concatenate([g for g, _ in terms] + [u for _, u in terms], 1), jnp.concatenate([gate_w, up_w], 1), 1, 1)

        @pl.when(r == tiles - 1)
        def _():
            each = b.shape[1] // n
            mine = g_s.at[j]
            _cut(mine, 0, _dot(p_s[...], dy_s[...], 0, 0))
            _cut(mine, mine.shape[1] - 2 * each, _dot(b_s[...], dg_s[...], 0, 0))
            _cut(mine, mine.shape[1] - each, _dot(b_s[...], du_s[...], 0, 0))

    out_copies = [pltpu.make_async_copy(g_s.at[hosted + i], left_ff.at[i], out_sem.at[i]) for i in range(behind)]
    out_copies.append(pltpu.make_async_copy(go_s, left_o, out_sem.at[behind]))

    @pl.when(step >= tiles + middle)
    def _():
        db = sum_b[rows, :]
        h1 = h1_s[rows, :] if last else h_ref[...]
        dh1 = dy_s[rows, :].astype(F32) + _norm_back(h1.astype(F32), db.astype(BF16).astype(F32)).astype(BF16).astype(F32)
        dh1 = dh1.astype(BF16)
        dh1_ref[...] = dh1
        datt = _dot(dh1, wo[0], 1, 1).astype(BF16)
        datt_ref[...] = datt
        att = att_ref[...]
        both = att.astype(F32) * datt.astype(F32)
        for i in range(both.shape[1] // HEAD):
            delta_ref[i : i + 1, :] = both[:, i * HEAD : (i + 1) * HEAD].T.sum(axis=0, keepdims=True)
        sum_o[...] += _dot(att, dh1, 0, 0)

        @pl.when(step == tiles + middle)
        def _():
            for c in out_copies[:-1]:
                c.start()

        @pl.when(step == 2 * tiles + middle - 1)
        def _():
            _cut(go_s, 0, sum_o[...])
            out_copies[-1].start()
            for c in out_copies:
                c.wait()

    for job, (_, at, _, _) in zip(jobs, times, strict=True):

        @pl.when(step == at)
        def _(job=job):
            job.add()

    for job, (_, _, _, at), out in zip(jobs, times, own, strict=True):

        @pl.when(step == at)
        def _(job=job, out=out):
            job.finish(out)


def mlp_back(n, number, layer, h, att, by, weights, rope, upper=None, hidden=None):
    t, d = h.shape
    ff = weights["w_gate"].shape[2]
    bt = _tile(t)
    tiles, blocks = t // bt, n
    fb, each = ff // blocks, d // n
    down = fb // n
    height = down + 2 * each
    assert n == 4 and fb == d and height == 3 * each
    heads = att.shape[1] // HEAD
    middle = tiles * blocks
    r = lambda s: jnp.where(s < tiles, s, lax.rem(s - tiles, tiles))
    j = lambda s: jnp.clip(lax.div(s - tiles, tiles), 0, blocks - 1)
    edge = lambda s: jnp.where(s < tiles, s, jnp.where(s < tiles + middle, tiles - 1, s - tiles - middle))
    before = lambda s: jnp.minimum(s, tiles - 1)
    after = lambda s: jnp.maximum(s - tiles - middle, 0)
    tile = lambda f, w=d: pl.BlockSpec((bt, w), lambda s: (f(s), 0))
    fixed = lambda which, *shape: pl.BlockSpec((1, *shape), lambda s: (which, 0, 0), pipeline_mode=pl.Buffered(1))
    square, up_square = fixed(layer, d, d), fixed(layer + 1, d, d)
    anywhere = pl.BlockSpec(memory_space=pltpu.HBM)
    mlp = [square, anywhere, anywhere, anywhere]
    w4 = [weights[name] for name in ("wo", "w_gate", "w_up", "w_down")]
    last = upper is None
    if last:
        ins = [tile(before), tile(edge), tile(before), *mlp]
        args = [h, att, by, *w4]
    else:
        hn, dq, dk, dv = upper
        table = pl.BlockSpec((bt, HEAD), lambda s: (before(s), 0))
        block = pl.BlockSpec((1, bt, fb), lambda s: (j(s), r(jnp.clip(s, tiles, tiles + middle - 1)), 0))
        ins = [tile(edge), tile(after), *[tile(before)] * 5, up_square, up_square, up_square, table, table, block, block, *mlp]
        args = [h, att, hn, dq, dk, dv, by, weights["wq"], weights["wk"], weights["wv"], *rope, *hidden, *w4]
    anywhere = pl.BlockSpec(memory_space=pltpu.HBM)
    outs = [
        (tile(after), jax.ShapeDtypeStruct((t, d), BF16)),
        (tile(after), jax.ShapeDtypeStruct((t, d), BF16)),
        (pl.BlockSpec((heads, bt), lambda s: (0, after(s))), jax.ShapeDtypeStruct((heads, t), F32)),
        (anywhere, jax.ShapeDtypeStruct((BEHIND, n, height, d), BF16)),
        (anywhere, jax.ShapeDtypeStruct((n, each, d), BF16)),
        *[(pl.BlockSpec((height, d), lambda s: (0, 0)), jax.ShapeDtypeStruct((height, d), BF16))] * (blocks - BEHIND),
    ]
    scratch = [pltpu.VMEM((t, d), BF16)] * (2 + last) + [pltpu.VMEM((t, fb), BF16)] * 3 + [pltpu.VMEM((t, d), F32)]
    scratch += [pltpu.VMEM((blocks, n, height, d), BF16), pltpu.VMEM((n, each, d), BF16), pltpu.SemaphoreType.DMA((BEHIND + 1,))]
    scratch += [pltpu.VMEM((1, d, ff), BF16)] * 2 + [pltpu.VMEM((1, ff, d), BF16), pltpu.SemaphoreType.DMA((3,))]
    scratch += [pltpu.VMEM((d, d), F32)] * (1 if last else 3)
    for _ in range(blocks - BEHIND):
        scratch += RingSum.scratch(n, height, d)
    if not last:
        outs += [(pl.BlockSpec((3 * each, d), lambda s: (0, 0)), jax.ShapeDtypeStruct((3 * each, d), BF16))]
        scratch += RingSum.scratch(n, 3 * each, d)
    return _call(
        functools.partial(_mlp_back, n=n, layer=layer, tiles=tiles, blocks=blocks, behind=BEHIND, last=last),
        (2 * tiles + middle,),
        ins,
        outs,
        scratch,
        args,
        2 * t * d * (ff * 8 + d * 4),
        sum(a.size * a.dtype.itemsize for a in args),
        collective=number,
    )


class Parts:
    def __init__(self, n, layers, each):
        self.hosted, self.per, self.each = n - BEHIND, n - BEHIND + 2, each

    def ff(self, layer, block, which):
        if block < self.hosted:
            return layer * self.per + block, which * self.each
        return layer * self.per + self.hosted, ((block - self.hosted) * 3 + which) * self.each

    def square(self, layer, which):
        if which == 3:
            return layer * self.per + self.hosted, BEHIND * 3 * self.each
        return layer * self.per + self.hosted + 1, which * self.each


def _moments(m, v, g):
    return 0.9 * m + 0.1 * g, 0.95 * v + 0.05 * g * g


def _stepped(w, m, v):
    return (w - 0.02 * (m * lax.rsqrt(v + 1e-8) + 0.1 * w)).astype(BF16)


def _finish(*refs, n, layers, own_count, count):
    take = iter(range(len(refs)))
    some = lambda k: [refs[next(take)] for _ in range(k)]
    h_ref, dq_ref, dk_ref, dv_ref, cos, sin = some(6)
    own_in, w_ref, m_ref, v_ref = some(own_count), some(7), some(7), some(7)
    own_ref, factor_ref = some(2)
    lands = some(7)
    h_s, dq_s, dk_s, dv_s, cos_s, sin_s, a_s, g_s, squares, total_s, others_s = some(11)
    pieces_s, m_s, v_s = some(own_count), some(7), some(7)
    load_sem, w_sem, m_sem, v_sem, swap_out, swap_in, out_r, out_l, in_l, in_r, pass_r, pass_l, far_l, far_r = some(14)
    jobs = [RingSum(n, g_s.at[i], *some(4)) for i in range(3)]
    me, right, far, left = _ring(n)
    mesh = pl.DeviceIdType.MESH
    barrier = pltpu.get_barrier_semaphore()
    for other in (right, far, left):
        pl.semaphore_signal(barrier, inc=1, device_id={"dp": other}, device_id_type=mesh)
    pairs = [(h_ref, h_s), (dv_ref, dv_s), (dk_ref, dk_s), (cos, cos_s), (sin, sin_s), (dq_ref, dq_s), *zip(own_in, pieces_s, strict=True)]
    loads = [pltpu.make_async_copy(s, d, load_sem.at[i]) for i, (s, d) in enumerate(pairs)]
    for load in loads:
        load.start()
    state = []
    for i in range(7):
        state.append(pltpu.make_async_copy(w_ref[i].at[:, me], lands[i].at[:, me], w_sem.at[i]))
        state.append(pltpu.make_async_copy(m_ref[i], m_s[i], m_sem.at[i]))
        state.append(pltpu.make_async_copy(v_ref[i], v_s[i], v_sem.at[i]))
    t = h_s.shape[0]
    each = g_s.shape[2]
    squares[...] = jnp.zeros_like(squares)
    loads[0].wait()

    def norm(rows):
        h = h_s[rows, :].astype(F32)
        a_s[rows, :] = (h * _norm_scale(h)).astype(BF16)

    _rows_loop(t, norm, 256)

    def turn(ref):
        def one(rows):
            ref[rows, :] = _turn(ref[rows, :].astype(F32), cos_s[rows, :], -sin_s[rows, :]).astype(BF16)

        _rows_loop(t, one, 256)

    loads[1].wait()
    _cut(g_s.at[2], 0, _dot(a_s[...], dv_s[...], 0, 0))
    pl.semaphore_wait(barrier, 3)
    for i in (2, 3, 4):
        loads[i].wait()
    turn(dk_s)
    jobs[2].start()
    for c in state:
        c.start()
    _cut(g_s.at[1], 0, _dot(a_s[...], dk_s[...], 0, 0))
    loads[5].wait()
    turn(dq_s)
    jobs[1].start()
    jobs[2].add()
    _cut(g_s.at[0], 0, _dot(a_s[...], dq_s[...], 0, 0))
    jobs[2].forward()
    jobs[1].add()
    jobs[0].start()
    jobs[1].forward()
    for i, piece in enumerate(pieces_s):
        if i == len(pieces_s) // 2:
            jobs[0].add()
        loads[6 + i].wait()
        _rows_loop(piece.shape[0], lambda rows, piece=piece: _add_squares(squares, piece[rows, :]))
        if i == len(pieces_s) // 2:
            jobs[0].forward()
    jobs[2].finish(own_ref.at[pl.ds(2 * each, each)], squares)
    jobs[1].finish(own_ref.at[pl.ds(each, each)], squares)
    jobs[0].finish(own_ref.at[pl.ds(0, each)], squares)
    total_s[...] = sum(squares[:, i : i + 128] for i in range(0, squares.shape[1], 128))
    swaps = [
        pltpu.make_async_remote_copy(src_ref=total_s, dst_ref=others_s.at[i], send_sem=swap_out.at[i], recv_sem=swap_in.at[i], device_id={"dp": other},
                                     device_id_type=mesh)
        for i, other in enumerate((right, far, left))
    ]
    for c in state:
        c.wait()
    for s in swaps:
        s.start()
    for s in swaps:
        s.wait()
    everything = jnp.sum(total_s[...] + others_s[0] + others_s[1] + others_s[2], keepdims=True)
    factor = jnp.minimum(1.0, 0.5 * lax.rsqrt(everything / count + 1e-30))
    factor_ref[...] = jnp.broadcast_to(factor, factor_ref.shape)

    parts = Parts(n, layers, each)
    grads = [*pieces_s[: parts.per - 1], own_ref, *pieces_s[parts.per - 1 :]]
    blocks = n

    def new_weights(i, layer):
        land, m_i, v_i = lands[i], m_s[i], v_s[i]

        def one(at, piece, row, rows, column, g_column, width):
            def body(some):
                here = pl.ds(at + some.start, some.size)
                g = grads[piece][pl.ds(row + some.start, some.size), g_column : g_column + width].astype(F32) * factor
                m, v = _moments(m_i[layer, here, column : column + width], v_i[layer, here, column : column + width], g)
                w = land[layer, me, here, column : column + width].astype(F32)
                land[layer, me, here, column : column + width] = _stepped(w, m, v)

            return body

        if i < 4:
            bodies, rows = [one(0, *parts.square(layer, i), each, 0, 0, land.shape[3])], each
        elif i == 6:
            rows = each
            bodies = [one(b * each, *parts.ff(layer, b, 0), each, 0, 0, land.shape[3]) for b in range(blocks)]
        else:
            width, rows = g_s.shape[3] // n, each
            bodies = [
                one(0, *parts.ff(layer, b, i - 3), each, (d * blocks + b) * width, d * width, width) for d in range(n) for b in range(blocks)
            ]

        def run(some):
            for body in bodies:
                body(some)

        _rows_loop(rows, run, 16)

    remote = lambda ref, to, sent, got: pltpu.make_async_remote_copy(
        src_ref=ref, dst_ref=ref, send_sem=sent, recv_sem=got, device_id={"dp": to}, device_id_type=mesh)
    units = [(i, layer) for i in (3, 0, 1, 2, 6, 4, 5) for layer in range(layers)]
    sends, passes = [], []
    for u, (i, layer) in enumerate(units):
        mine = lands[i].at[layer, me]
        sends.append((remote(mine, right, out_r.at[u], in_l.at[u]), remote(mine, left, out_l.at[u], in_r.at[u])))
    for u in range(len(units) + 1):
        if u < len(units):
            new_weights(*units[u])
        if u > 0:
            for c in sends[u - 1]:
                c.start()
    for u, (i, layer) in enumerate(units):
        half = lands[i].shape[2] // 2
        sends[u][0].wait_recv()
        one = remote(lands[i].at[layer, left, pl.ds(0, half)], right, pass_r.at[u], far_l.at[u])
        one.start()
        sends[u][1].wait_recv()
        two = remote(lands[i].at[layer, right, pl.ds(half, half)], left, pass_l.at[u], far_r.at[u])
        two.start()
        passes.append((one, two))
    for u in range(len(units)):
        for c in passes[u]:
            c.wait_recv()
        for c in (*sends[u], *passes[u]):
            c.wait_send()


def finish(n, number, h, dq, dk, dv, rope, own, w, m, v):
    t, d = h.shape
    each, layers = d // n, w[0].shape[0]
    anywhere, here = pl.BlockSpec(memory_space=pltpu.HBM), pl.BlockSpec(memory_space=pltpu.VMEM)
    w = [a.reshape(layers, n, a.shape[1] // n, a.shape[2]) for a in w]
    shapes = [a.shape for a in w]
    scratch = [pltpu.VMEM((t, d), BF16)] * 4 + [pltpu.VMEM((t, HEAD), F32)] * 2
    scratch += [pltpu.VMEM((t, d), BF16), pltpu.VMEM((3, n, each, d), BF16), pltpu.VMEM((8, d), F32), pltpu.VMEM((8, 128), F32),
                pltpu.VMEM((3, 8, 128), F32)]
    scratch += [pltpu.VMEM(o.shape, BF16) for o in own] + [pltpu.VMEM(a.shape, F32) for a in (*m, *v)]
    units = 7 * layers
    sem = lambda *k: pltpu.SemaphoreType.DMA(k)
    scratch += [sem(6 + len(own)), sem(7), sem(7), sem(7), sem(3), sem(3), *[sem(units)] * 8]
    for _ in range(3):
        scratch += RingSum.scratch(n, each, d)
    return _call(
        functools.partial(_finish, n=n, layers=layers, own_count=len(own), count=n * sum(a.size for a in m)),
        (),
        [anywhere] * (6 + len(own) + 21),
        [(here, jax.ShapeDtypeStruct((3 * each, d), BF16)), (here, jax.ShapeDtypeStruct((8, 128), F32)),
         *((here, pltpu.VMEM(s, BF16)) for s in shapes)],
        scratch,
        (h, dq, dk, dv, *rope, *own, *w, *m, *v),
        6 * t * d * d,
        8 * t * d,
        collective=number,
        vmem=REST,
    )


def _settle(factor_ref, *refs, n, layers, own_count):
    own, rest = refs[:own_count], refs[own_count:]
    m, v, w, w_out, m_out, v_out = (rest[7 * i : 7 * i + 7] for i in range(6))
    sem = rest[42]
    copies = [pltpu.make_async_copy(w[i], w_out[i], sem.at[i]) for i in range(7)]

    @pl.when(pl.program_id(0) == 0)
    def _():
        for c in copies:
            c.start()

    factor = factor_ref[0:1, 0:1]
    parts = Parts(n, layers, 1)
    def one(i, at, piece, row, columns=slice(None)):
        g = own[piece][row][:, columns].astype(F32) * factor
        m_out[i][at], v_out[i][at] = _moments(m[i][at], v[i][at], g)

    for layer in range(layers):
        for i in range(4):
            one(i, (layer,), *parts.square(layer, i))
        for b in range(n):
            one(6, (layer, b), *parts.ff(layer, b, 0))
            width = own[0].shape[2] // n
            for d in range(n):
                for i in (4, 5):
                    at = slice((d * n + b) * width, (d * n + b + 1) * width)
                    one(i, (layer, slice(None), at), *parts.ff(layer, b, i - 3), slice(d * width, (d + 1) * width))

    @pl.when(pl.program_id(0) == pl.num_programs(0) - 1)
    def _():
        for c in copies:
            c.wait()


def settle(n, factor, own, w, m, v):
    layers, _, each, d = w[0].shape
    ff = w[4].shape[3]
    deep = 16
    steps = each // deep
    own = [a.reshape(a.shape[0] // each, each, d) for a in own]
    cut = lambda a: a.reshape(layers, -1, each, d)
    m_in, v_in = [*m[:6], cut(m[6])], [*v[:6], cut(v[6])]
    w = [pltpu.with_memory_space_constraint(a, pltpu.VMEM) for a in w]
    thin, thick = (pl.BlockSpec((layers, deep, c), lambda s: (0, s, 0)) for c in (d, ff))
    deeper = lambda a: pl.BlockSpec((layers, a.shape[1], deep, a.shape[3]), lambda s: (0, 0, s, 0))
    state = [thin] * 4 + [thick] * 2 + [deeper(m_in[6])]
    here, there = pl.BlockSpec(memory_space=pltpu.VMEM), pl.BlockSpec(memory_space=pltpu.HBM)
    out = _call(
        functools.partial(_settle, n=n, layers=layers, own_count=len(own)),
        (steps,),
        [pl.BlockSpec((8, 128), lambda s: (0, 0)), *(pl.BlockSpec((a.shape[0], deep, d), lambda s: (0, s, 0)) for a in own), *state, *state, *[here] * 7],
        [*((spec, jax.ShapeDtypeStruct(a.shape, a.dtype)) for spec, a in zip((*[there] * 7, *state, *state), (*w, *m_in, *v_in), strict=True))],
        [pltpu.SemaphoreType.DMA((7,))],
        (factor, *own, *m_in, *v_in, *w),
        8 * sum(a.size for a in m),
        32 * sum(a.size for a in m),
        vmem=REST,
    )
    flat = lambda a: a.reshape(layers, -1, a.shape[-1])
    return tuple(flat(a) for a in out)


NAMES = ("wq", "wk", "wv", "wo", "w_gate", "w_up", "w_down")


def rope_tables(t):
    half = HEAD // 2
    angle = np.arange(t, dtype=np.float32)[:, None] * (np.float32(THETA) ** (-np.arange(half, dtype=np.float32) / half)).astype(np.float32)
    cos, sin = np.cos(angle.astype(np.float64)).astype(np.float32), np.sin(angle.astype(np.float64)).astype(np.float32)
    return jnp.asarray(np.concatenate([cos, cos], 1)), jnp.asarray(np.concatenate([-sin, sin], 1))


def solution(mesh):
    n = mesh.shape["dp"]

    def step(x, dy, *arrays):
        weights = dict(zip(NAMES, arrays[:7], strict=True))
        m, v = arrays[7:14], arrays[14:]
        layers = weights["wq"].shape[0]
        h = x[0]
        rope = rope_tables(h.shape[0])
        made = forward(n, h, weights, rope)
        hs = [h, *(one[6] for one in made[:-1])]
        own = {}
        by, upper, number = dy[0], None, 0
        for layer in reversed(range(layers)):
            if upper is None:
                got = mlp_back(n, number, layer, hs[layer], made[layer][3], by, weights, rope)
            else:
                got = mlp_back(n, number, layer, made[layer][5], made[layer][3], by, weights, rope, upper, made[layer][7:9])
                own[layer + 1].append(got[5 + n - BEHIND])
            by, datt, delta, left_ff, left_o = got[:5]
            dq, dk, dv, rest = attend_back(n, number + 1, *made[layer][:3], datt, made[layer][4], delta, left_ff, left_o)
            own[layer] = [*got[5 : 5 + n - BEHIND], rest]
            upper = hs[layer], dq, dk, dv
            number += 2
        pieces = [p for layer in range(layers) for p in own[layer]]
        last, factor, *whole = finish(n, number, *upper, rope, pieces, arrays[:7], m, v)
        own[0].append(last)
        return settle(n, factor, [p for layer in range(layers) for p in own[layer]], whole, m, v)

    states, all_of, cut = P(("rep", "dp"), None, None), P(None, None, None), P(None, "dp", None)
    return jax.shard_map(
        step,
        mesh=mesh,
        in_specs=(states, states) + (all_of,) * 7 + (cut,) * 14,
        out_specs=(P("rep", None, None),) * 7 + (P("rep", "dp", None),) * 14,
        check_vma=False,
    )
```

```python
import functools

import jax
import jax.numpy as jnp
import numpy as np
from jax import lax
from jax.experimental import pallas as pl
from jax.experimental.pallas import tpu as pltpu
from jax.sharding import PartitionSpec as P

F32, BF16 = jnp.float32, jnp.bfloat16
HEAD = 128
THETA = 10000
NEG = -1e30
HIDDEN = 2 * NEG
LOG2E = 1.4426950408889634
SCALE = HEAD**-0.5
VMEM = 67043328
REST = 30 * 2**20
BEHIND = 2


def _dot(a, b, ca=1, cb=0):
    return lax.dot_general(a, b, (((ca,), (cb,)), ((), ())), preferred_element_type=F32)


def _tile(size, most=512):
    return max(n for n in range(128, most + 1, 128) if size % n == 0)


def _call(kernel, grid, ins, outs, scratch, args, flops, moved, collective=None, vmem=VMEM):
    return pl.pallas_call(
        kernel,
        grid=grid,
        in_specs=[spec for spec in ins],
        out_specs=[spec for spec, _ in outs],
        out_shape=[shape for _, shape in outs],
        scratch_shapes=scratch,
        compiler_params=pltpu.CompilerParams(dimension_semantics=("arbitrary",) * len(grid), vmem_limit_bytes=vmem, collective_id=collective,
                                             has_side_effects=collective is not None),
        cost_estimate=pl.CostEstimate(flops=int(flops), transcendentals=0, bytes_accessed=int(moved)),
    )(*args)


def _norm_scale(x):
    return lax.rsqrt(jnp.mean(x * x, -1, keepdims=True) + 1e-6)


def _normed(x):
    return (x * _norm_scale(x)).astype(BF16)


def _norm_back(x, d_out):
    s = _norm_scale(x)
    inner = jnp.mean(x * d_out, -1, keepdims=True)
    return s * d_out - x * (s * s * s * inner)


def _turn(x, cos, sin):
    parts = [x[:, n : n + HEAD] for n in range(0, x.shape[1], HEAD)]
    return jnp.concatenate([p * cos + pltpu.roll(p, HEAD // 2, 1) * sin for p in parts], 1)


def _qkv(h, wq, wk, wv, cos, sin):
    a = _normed(h)
    q, k = (_turn(_dot(a, w).astype(BF16).astype(F32), cos, sin).astype(BF16) for w in (wq, wk))
    return a, q, k, _dot(a, wv).astype(BF16)


def _after_attention(h_ref, att_ref, wo):
    return (h_ref[...].astype(F32) + _dot(att_ref[...], wo).astype(BF16).astype(F32)).astype(BF16)


def _seen(keys, queries):
    return lax.broadcasted_iota(jnp.int32, (keys, queries), 1) >= lax.broadcasted_iota(jnp.int32, (keys, queries), 0)


def diagonal(block, first, size, part=256):
    part = min(part, size)
    for at in range(0, size, part):
        block(first + at, part, at, True)


def _attend(iq, q_ref, k_ref, v_ref, o_ref, lse_ref, top_s, mix_s, bk):
    bq = q_ref.shape[0]
    heads = q_ref.shape[1] // HEAD
    e = SCALE * LOG2E
    top_s[...] = jnp.full(top_s.shape, NEG, F32)
    mix_s[...] = jnp.zeros(mix_s.shape, F32)

    def block(first, keys, at, masked):
        here, ask = pl.ds(pl.multiple_of(first, keys), keys), slice(at, bq)
        cols = [slice(n * HEAD, (n + 1) * HEAD) for n in range(heads)]
        scores = [_dot(k_ref[here, c], q_ref[ask, c], 1, 1) for c in cols]
        weights, keeps = [], []
        seen = _seen(keys, bq - at) if masked else None
        for n, s in enumerate(scores):
            if masked:
                s = jnp.where(seen, s, HIDDEN)
            old = top_s[n : n + 1, ask]
            top = jnp.maximum(old, s.max(axis=0, keepdims=True))
            top_s[n : n + 1, ask] = top
            weights.append(jnp.exp2((s - top) * e).astype(BF16))
            keeps.append(jnp.exp2((old - top) * e))
        ones = jnp.ones((8, keys), BF16)
        for n, (c, p, keep) in enumerate(zip(cols, weights, keeps)):
            values = jnp.concatenate([v_ref[here, c].T, ones], axis=0)
            mix_s[n, :, ask] = mix_s[n, :, ask] * keep + _dot(values, p, 1, 0)

    lax.fori_loop(0, iq * (bq // bk), lambda j, _: block(j * bk, bk, 0, False), None)
    diagonal(block, iq * bq, bq)
    for n in range(heads):
        total = mix_s[n, HEAD : HEAD + 1, :]
        o_ref[:, n * HEAD : (n + 1) * HEAD] = (mix_s[n, :HEAD, :] * (1 / total)).T.astype(BF16)
        lse_ref[n : n + 1, :] = top_s[n : n + 1, :] * e + jnp.log2(total)


def _forward(h_ref, wq, wk, wv, wo, wg_ref, wu_ref, wd_ref, cos, sin, *refs, n, layers):
    outs, a_ref, scratch = refs[: 9 * layers - 4], refs[9 * layers - 4], refs[9 * layers - 3 :]
    k_s, v_s, wg, wu, wd, gate_s, up_s, top_s, mix_s, w_sem, out_sem = scratch
    step = pl.program_id(0)
    bt = h_ref.shape[0]
    rows = pl.ds(pl.multiple_of(step * bt, bt), bt)
    loads = [pltpu.make_async_copy(a.at[0], b.at[0], w_sem.at[i]) for i, (a, b) in enumerate(((wg_ref, wg), (wu_ref, wu), (wd_ref, wd)))]

    @pl.when(step == 0)
    def _():
        for load in loads:
            load.start()

    for layer in range(layers):
        q_ref, k_ref, v_ref, att_ref, lse_ref = outs[9 * layer : 9 * layer + 5]
        a, q_ref[...], k, v = _qkv(h_ref[...].astype(F32), wq[layer], wk[layer], wv[layer], cos[...], sin[...])
        if layer == 0:
            a_ref[...] = a
        k_ref[...] = k_s[layer, rows, :] = k
        v_ref[...] = v_s[layer, rows, :] = v
        _attend(step, q_ref, k_s.at[layer], v_s.at[layer], att_ref, lse_ref, top_s, mix_s, bt)
        if layer == layers - 1:
            break
        h1_ref, y_ref, gate_ref, up_ref = outs[9 * layer + 5 : 9 * layer + 9]
        stores = [
            pltpu.make_async_copy(a.at[j], b.at[j, rows], out_sem.at[layer, i, j])
            for i, (a, b) in enumerate(((gate_s, gate_ref), (up_s, up_ref)))
            for j in range(n)
        ]

        @pl.when(step == 0)
        def _(layer=layer):
            for load in loads:
                load.wait()

        @pl.when(step > 0)
        def _(stores=stores):
            for c in stores:
                c.wait()

        h1 = _after_attention(h_ref, att_ref, wo[layer])
        h1_ref[...] = h1
        h1 = h1.astype(F32)
        b = (h1 * _norm_scale(h1)).astype(BF16)
        total = jnp.zeros(h1.shape, F32)
        for j in range(n):
            gate, up = _dot(b, _strips(wg, j, n, n, 2)), _dot(b, _strips(wu, j, n, n, 2))
            gate_s[j] = gate
            up_s[j] = up
            total += _dot((gate * jax.nn.sigmoid(gate) * up).astype(BF16), _strips(wd, j, n, n, 1))
        for c in stores:
            c.start()
        y_ref[...] = (h1 + total.astype(BF16).astype(F32)).astype(BF16)
        h_ref = y_ref

        @pl.when(step == pl.num_programs(0) - 1)
        def _(stores=stores):
            for c in stores:
                c.wait()


def forward(n, h, weights, rope):
    t, d = h.shape
    layers, _, ff = weights["w_gate"].shape
    assert layers == 2
    heads = weights["wq"].shape[2] // HEAD
    bt = _tile(t)
    tile, table = (pl.BlockSpec((bt, w), lambda s: (s, 0)) for w in (d, HEAD))
    square = pl.BlockSpec((layers, d, d), lambda s: (0, 0, 0), pipeline_mode=pl.Buffered(1))
    anywhere = pl.BlockSpec(memory_space=pltpu.HBM)
    one = (tile, jax.ShapeDtypeStruct((t, d), BF16))
    two = (anywhere, jax.ShapeDtypeStruct((n, t, ff // n), F32))
    stats = (pl.BlockSpec((heads, bt), lambda s: (0, s)), jax.ShapeDtypeStruct((heads, t), F32))
    upper = [*[one] * 4, stats]
    got = _call(
        functools.partial(_forward, n=n, layers=layers),
        (t // bt,),
        [tile, *[square] * 4, *[anywhere] * 3, table, table],
        [*[*upper, one, one, two, two] * (layers - 1), *upper, one],
        [pltpu.VMEM((layers, t, d), BF16)] * 2
        + [pltpu.VMEM((1, d, ff), BF16)] * 2
        + [pltpu.VMEM((1, ff, d), BF16)]
        + [pltpu.VMEM((n, bt, ff // n), F32)] * 2
        + [pltpu.VMEM((heads, bt), F32), pltpu.VMEM((heads, HEAD + 8, bt), F32), pltpu.SemaphoreType.DMA((3,)),
           pltpu.SemaphoreType.DMA((layers, 2, n))],
        (h, *(weights[name] for name in ("wq", "wk", "wv", "wo")), *(weights[name] for name in ("w_gate", "w_up", "w_down")), *rope),
        2 * t * d * (8 * d + 3 * ff) + 4 * t * t * d,
        30 * t * d + 8 * t * ff,
    )
    return [got[9 * layer : 9 * layer + 9] for layer in range(layers - 1)] + [got[9 * layers - 9 : -1]], got[-1]


def _ring(n):
    me = lax.axis_index("dp")
    return me, lax.rem(me + 1, n), lax.rem(me + 2, n), lax.rem(me + n - 1, n)


def _greet(n):
    _, right, _, left = _ring(n)
    barrier = pltpu.get_barrier_semaphore()
    for other in (right, left):
        pl.semaphore_signal(barrier, inc=1, device_id={"dp": other}, device_id_type=pl.DeviceIdType.MESH)


def _met():
    pl.semaphore_wait(pltpu.get_barrier_semaphore(), 2)


def _rows_loop(rows, body, most=32):
    each = max(c for c in range(16, most + 1, 16) if rows % c == 0)
    lax.fori_loop(0, rows // each, lambda i, _: body(pl.ds(pl.multiple_of(i * each, each), each)), None)


class RingSum:
    def __init__(self, n, block, passing, arrived, sent, got):
        self.block, self.passing, self.arrived = block, passing, arrived
        self.me, right, far, left = _ring(n)
        self.near = right, left
        half = block.shape[1] // 2
        self.half = half
        a, b = pl.ds(0, half), pl.ds(half, half)
        moves = [
            (block.at[far, a], passing.at[0], right),
            (block.at[far, b], passing.at[1], left),
            (block.at[right, b], arrived.at[0, b], right),
            (block.at[left, a], arrived.at[1, a], left),
            (passing.at[0], arrived.at[0, a], right),
            (passing.at[1], arrived.at[1, b], left),
        ]
        self.copies = [
            pltpu.make_async_remote_copy(src_ref=s, dst_ref=d, send_sem=sent.at[i], recv_sem=got.at[i], device_id={"dp": to},
                                         device_id_type=pl.DeviceIdType.MESH)
            for i, (s, d, to) in enumerate(moves)
        ]

    @staticmethod
    def scratch(n, rows, columns):
        half = pltpu.VMEM((2, rows // 2, columns), BF16)
        return [half, pltpu.VMEM((2, rows, columns), BF16), pltpu.SemaphoreType.DMA((6,)), pltpu.SemaphoreType.DMA((6,))]

    def start(self):
        for c in self.copies[:4]:
            c.start()

    def add(self):
        for c in self.copies[:2]:
            c.wait_recv()
        for i, other in enumerate(self.near):

            def one(rows, i=i, other=other):
                mine = self.block[other, pl.ds(rows.start + i * self.half, rows.size), :]
                self.passing[i, rows, :] = (self.passing[i, rows, :].astype(F32) + mine.astype(F32)).astype(BF16)

            _rows_loop(self.half, one)

    def forward(self):
        for c in self.copies[4:]:
            c.start()

    def finish(self, out, squares=None):
        for c in self.copies[2:]:
            c.wait_recv()

        def one(rows):
            total = self.block[self.me, rows, :].astype(F32) + self.arrived[0, rows, :].astype(F32) + self.arrived[1, rows, :].astype(F32)
            total = total.astype(BF16)
            out[rows, :] = total
            if squares is not None:
                _add_squares(squares, total)

        _rows_loop(self.half * 2, one)
        for c in self.copies:
            c.wait_send()


def _add_squares(squares, value):
    value = value.astype(F32)
    value = value * value
    squares[...] += sum(value[i : i + 8] for i in range(0, value.shape[0], 8))


def _attend_back(q_ref, k_ref, v_ref, do_ref, lse_ref, delta_ref, cos, sin, part_ref, ff_ref, o_ref, dq_ref, dk_ref, dv_ref, own_ref, dq_s, dk_s, dv_s, block_s, load_sem,
                 *ring, bk, n):
    iq = pl.program_id(0)
    bq = q_ref.shape[0]
    heads = q_ref.shape[1] // HEAD
    e = SCALE * LOG2E
    steps = pl.num_programs(0)
    loads, at = [], 0
    for i, source in enumerate((part_ref, *(ff_ref.at[i] for i in range(ff_ref.shape[0])), o_ref)):
        loads.append(pltpu.make_async_copy(source, block_s.at[:, pl.ds(at, source.shape[1])], load_sem.at[i]))
        at += source.shape[1]
    job = RingSum(n, block_s, *ring)

    @pl.when(iq == 0)
    def _():
        _greet(n)
        for load in loads:
            load.start()
        dk_s[...] = jnp.zeros_like(dk_s)
        dv_s[...] = jnp.zeros_like(dv_s)

    @pl.when(iq == 1)
    def _():
        for load in loads:
            load.wait()
        _met()
        job.start()

    @pl.when(iq == steps - 1)
    def _():
        job.forward()

    dq_s[...] = jnp.zeros_like(dq_s)

    def block(first, keys, at, masked):
        here, ask = pl.ds(pl.multiple_of(first, keys), keys), slice(at, bq)
        cols = [slice(i * HEAD, (i + 1) * HEAD) for i in range(heads)]
        scores = [_dot(k_ref[here, c], q_ref[ask, c], 1, 1) for c in cols]
        dps = [_dot(v_ref[here, c], do_ref[ask, c], 1, 1) for c in cols]
        seen = _seen(keys, bq - at) if masked else None
        for i, c in enumerate(cols):
            p = jnp.exp2(scores[i] * e - lse_ref[i : i + 1, ask])
            if masked:
                p = jnp.where(seen, p, 0.0)
            ds = (p * (dps[i] - delta_ref[i : i + 1, ask])).astype(BF16)
            dv_s[here, c] += _dot(p.astype(BF16), do_ref[ask, c], 1, 0)
            dk_s[here, c] += _dot(ds, q_ref[ask, c], 1, 0)
            dq_s[i, :, ask] += _dot(k_ref[here, c].T, ds, 1, 0)

    lax.fori_loop(0, iq * (bq // bk), lambda j, _: block(j * bk, bk, 0, False), None)
    diagonal(block, iq * bq, bq)

    @pl.when(iq == steps - 2)
    def _():
        job.add()

    def back(d, rows):
        return _turn(d.astype(BF16).astype(F32), cos[rows, :], -sin[rows, :]).astype(BF16)

    mine = pl.ds(pl.multiple_of(iq * bq, bq), bq)
    for i in range(heads):
        dq_ref[:, i * HEAD : (i + 1) * HEAD] = back((dq_s[i] * SCALE).T, mine)

    @pl.when(iq == steps - 1)
    def _():
        def one(rows):
            dk_ref[rows, :] = back(dk_s[rows, :] * SCALE, rows)
            dv_ref[rows, :] = dv_s[rows, :].astype(BF16)

        _rows_loop(dk_ref.shape[0], one, 256)
        job.finish(own_ref)


def attend_back(n, number, q, k, v, d_out, lse, delta, rope, part, ff, o):
    t, width = q.shape
    heads = width // HEAD
    bq = bk = _tile(t)
    rows, whole = pl.BlockSpec((bq, width), lambda i: (i, 0)), pl.BlockSpec((t, width), lambda i: (0, 0))
    stats = pl.BlockSpec((heads, bq), lambda i: (0, i))
    table = pl.BlockSpec((t, HEAD), lambda i: (0, 0), pipeline_mode=pl.Buffered(1))
    one = jax.ShapeDtypeStruct((t, width), BF16)
    height, columns = part.shape[1] + ff.shape[0] * ff.shape[2] + o.shape[1], ff.shape[3]
    return _call(
        functools.partial(_attend_back, bk=bk, n=n),
        (t // bq,),
        [rows, whole, whole, rows, stats, stats, table, table, *[pl.BlockSpec(memory_space=pltpu.HBM)] * 3],
        [(rows, one), (whole, one), (whole, one),
         (pl.BlockSpec((height, columns), lambda i: (0, 0)), jax.ShapeDtypeStruct((height, columns), BF16))],
        [pltpu.VMEM((heads, HEAD, bq), F32), pltpu.VMEM((t, width), F32), pltpu.VMEM((t, width), F32),
         pltpu.VMEM((n, height, columns), BF16), pltpu.SemaphoreType.DMA((ff.shape[0] + 2,)),
         *RingSum.scratch(n, height, columns)],
        (q, k, v, d_out, lse, delta, *rope, part, ff, o),
        5 * t * t * width,
        14 * t * width,
        collective=number,
    )


def _strips(ref, block, n, blocks, axis):
    width = ref.shape[axis] // (n * blocks)
    at = [pl.ds(pl.multiple_of((d * blocks + block) * width, width), width) for d in range(n)]
    return jnp.concatenate([ref[0, :, a] if axis == 2 else ref[0, a, :] for a in at], axis - 1)


def _qkv_back(h, dq, dk, dv, wq, wk, wv, sums):
    a = (h * _norm_scale(h)).astype(BF16)
    for s, d in zip(sums, (dq, dk, dv), strict=True):
        s[...] += _dot(a, d, 0, 0)
    return _dot(jnp.concatenate([dq, dk, dv], 1), jnp.concatenate([wq, wk, wv], 1), 1, 1)


def _cut(ref, at, value):
    n = ref.shape[0]
    each = value.shape[0] // n
    for d in range(n):
        ref[d, at : at + each] = value[d * each : (d + 1) * each].astype(BF16)


def _mlp_back(*refs, n, layer, tiles, blocks, behind, last):
    take = iter(range(len(refs)))
    some = lambda count: [refs[next(take)] for _ in range(count)]
    h_ref, att_ref = some(2)
    if last:
        (dy_ref,) = some(1)
    else:
        hn_ref, dq_ref, dk_ref, dv_ref, dh_ref, wq, wk, wv, gate_ref, up_ref = some(10)
    wo, wg_ref, wu_ref, wd_ref = some(4)
    dh1_ref, datt_ref, delta_ref, left_part, left_ff, left_o = some(6)
    hosted = blocks - behind
    own = some(hosted + 1 + (not last))
    h1_s = some(1)[0] if last else None
    b_s, dy_s, p_s, dg_s, du_s, sum_b, g_s, go_s, out_sem = some(9)
    wg, wu, wd, w_sem = some(4)
    sums3 = some(1 if last else 3)
    sum_o = sums3[0]
    jobs = []
    for i in range(len(own)):
        if i < hosted:
            block = g_s.at[i]
        elif i == hosted:
            block = g_s.at[i, :, pl.ds(0, own[i].shape[0])]
        else:
            block = gqkv_s = g_s.at[blocks - 1]
        jobs.append(RingSum(n, block, *some(4)))
    step = pl.program_id(0)
    bt = h_ref.shape[0]
    middle = tiles * blocks
    r = jnp.where(step < tiles, step, lax.rem(step - tiles, tiles))
    j = lax.div(step - tiles, tiles)
    rows = pl.ds(pl.multiple_of(r * bt, bt), bt)
    @pl.when(step == 0)
    def _():
        _greet(n)
        for s in sums3:
            s[...] = jnp.zeros_like(s)

    loads = [pltpu.make_async_copy(a.at[layer], b.at[0], w_sem.at[i]) for i, (a, b) in enumerate(((wg_ref, wg), (wu_ref, wu), (wd_ref, wd)))]

    @pl.when(step == 0)
    def _():
        for load in loads:
            load.start()

    @pl.when(step == tiles)
    def _():
        for load in loads:
            load.wait()

    final = 2 * tiles + middle - 1
    times = [(at, min(at + tiles * 3 // 2, tiles + middle)) for at in (tiles * (2 + i) for i in range(hosted + 1))] + [(tiles, 2 * tiles)] * (not last)
    times = [(start, forward - 1, forward, min(forward + tiles * 3 // 2, final)) for start, forward in times]

    @pl.when(step == min(t[0] for t in times))
    def _():
        _met()

    for job, (_, _, at, _) in zip(jobs, times, strict=True):

        @pl.when(step == at)
        def _(job=job):
            job.forward()

    for job, (at, _, _, _) in zip(jobs, times, strict=True):

        @pl.when(step == at)
        def _(job=job):
            job.start()

    @pl.when(step < tiles)
    def _():
        if last:
            h1 = _after_attention(h_ref, att_ref, wo[0])
            h1_s[rows, :] = h1
            dy_s[rows, :] = dy_ref[...]
        else:
            h1 = h_ref[...]
            hn = hn_ref[...].astype(F32)
            da = _qkv_back(hn, dq_ref[...], dk_ref[...], dv_ref[...], wq[0], wk[0], wv[0], sums3)
            dy_s[rows, :] = (dh_ref[...].astype(F32) + _norm_back(hn, da.astype(BF16).astype(F32)).astype(BF16).astype(F32)).astype(BF16)

            @pl.when(step == tiles - 1)
            def _():
                for i, s in enumerate(sums3):
                    _cut(gqkv_s, i * (s.shape[0] // n), s[...])
                sum_o[...] = jnp.zeros_like(sum_o)

        h1 = h1.astype(F32)
        b_s[rows, :] = (h1 * _norm_scale(h1)).astype(BF16)
        sum_b[rows, :] = jnp.zeros((bt, sum_b.shape[1]), F32)

    @pl.when((step >= tiles) & (step < tiles + middle))
    def _():
        b, dy = b_s[rows, :], dy_s[rows, :]
        gate_w, up_w, down_w = _strips(wg, j, n, blocks, 2), _strips(wu, j, n, blocks, 2), _strips(wd, j, n, blocks, 1)
        terms = []
        for at in range(0, gate_w.shape[1], 256):
            c = slice(at, at + 256)
            gate, up = (_dot(b, gate_w[:, c]), _dot(b, up_w[:, c])) if last else (gate_ref[0, :, c], up_ref[0, :, c])
            dp = _dot(dy, down_w[c], 1, 1).astype(BF16).astype(F32)
            sg = jax.nn.sigmoid(gate)
            silu = gate * sg
            p_s[rows, c] = (silu * up).astype(BF16)
            du = (dp * silu).astype(BF16)
            dg = (dp * up * (sg + silu * (1 - sg))).astype(BF16)
            du_s[rows, c] = du
            dg_s[rows, c] = dg
            terms.append((dg, du))
        sum_b[rows, :] += _dot(jnp.concatenate([g for g, _ in terms] + [u for _, u in terms], 1), jnp.concatenate([gate_w, up_w], 1), 1, 1)

        @pl.when(r == tiles - 1)
        def _():
            each = b.shape[1] // n
            mine = g_s.at[j]
            _cut(mine, 0, _dot(p_s[...], dy_s[...], 0, 0))
            _cut(mine, mine.shape[1] - 2 * each, _dot(b_s[...], dg_s[...], 0, 0))
            _cut(mine, mine.shape[1] - each, _dot(b_s[...], du_s[...], 0, 0))

    part = own[hosted].shape[0]
    out_copies = [pltpu.make_async_copy(g_s.at[hosted, :, pl.ds(part, left_part.shape[1])], left_part, out_sem.at[0])]
    out_copies += [pltpu.make_async_copy(g_s.at[hosted + i], left_ff.at[i - 1], out_sem.at[i]) for i in range(1, behind)]
    out_copies.append(pltpu.make_async_copy(go_s, left_o, out_sem.at[behind]))

    @pl.when(step >= tiles + middle)
    def _():
        db = sum_b[rows, :]
        h1 = h1_s[rows, :] if last else h_ref[...]
        dh1 = dy_s[rows, :].astype(F32) + _norm_back(h1.astype(F32), db.astype(BF16).astype(F32)).astype(BF16).astype(F32)
        dh1 = dh1.astype(BF16)
        dh1_ref[...] = dh1
        datt = _dot(dh1, wo[0], 1, 1).astype(BF16)
        datt_ref[...] = datt
        att = att_ref[...]
        both = att.astype(F32) * datt.astype(F32)
        for i in range(both.shape[1] // HEAD):
            delta_ref[i : i + 1, :] = both[:, i * HEAD : (i + 1) * HEAD].T.sum(axis=0, keepdims=True)
        sum_o[...] += _dot(att, dh1, 0, 0)

        @pl.when(step == tiles + middle)
        def _():
            for c in out_copies[:-1]:
                c.start()

        @pl.when(step == 2 * tiles + middle - 1)
        def _():
            _cut(go_s, 0, sum_o[...])
            out_copies[-1].start()
            for c in out_copies:
                c.wait()

    for job, (_, at, _, _) in zip(jobs, times, strict=True):

        @pl.when(step == at)
        def _(job=job):
            job.add()

    for job, (_, _, _, at), out in zip(jobs, times, own, strict=True):

        @pl.when(step == at)
        def _(job=job, out=out):
            job.finish(out)


def mlp_back(n, number, layer, h, att, by, weights, upper=None, hidden=None):
    t, d = h.shape
    ff = weights["w_gate"].shape[2]
    bt = _tile(t)
    tiles, blocks = t // bt, n
    fb, each = ff // blocks, d // n
    down = fb // n
    height = down + 2 * each
    assert n == 4 and fb == d and height == 3 * each
    heads = att.shape[1] // HEAD
    middle = tiles * blocks
    r = lambda s: jnp.where(s < tiles, s, lax.rem(s - tiles, tiles))
    j = lambda s: jnp.clip(lax.div(s - tiles, tiles), 0, blocks - 1)
    edge = lambda s: jnp.where(s < tiles, s, jnp.where(s < tiles + middle, tiles - 1, s - tiles - middle))
    before = lambda s: jnp.minimum(s, tiles - 1)
    after = lambda s: jnp.maximum(s - tiles - middle, 0)
    tile = lambda f, w=d: pl.BlockSpec((bt, w), lambda s: (f(s), 0))
    fixed = lambda which, *shape: pl.BlockSpec((1, *shape), lambda s: (which, 0, 0), pipeline_mode=pl.Buffered(1))
    square, up_square = fixed(layer, d, d), fixed(layer + 1, d, d)
    anywhere = pl.BlockSpec(memory_space=pltpu.HBM)
    mlp = [square, anywhere, anywhere, anywhere]
    w4 = [weights[name] for name in ("wo", "w_gate", "w_up", "w_down")]
    last = upper is None
    if last:
        ins = [tile(before), tile(edge), tile(before), *mlp]
        args = [h, att, by, *w4]
    else:
        hn, dq, dk, dv = upper
        block = pl.BlockSpec((1, bt, fb), lambda s: (j(s), r(jnp.clip(s, tiles, tiles + middle - 1)), 0))
        ins = [tile(edge), tile(after), *[tile(before)] * 5, up_square, up_square, up_square, block, block, *mlp]
        args = [h, att, hn, dq, dk, dv, by, weights["wq"], weights["wk"], weights["wv"], *hidden, *w4]
    anywhere = pl.BlockSpec(memory_space=pltpu.HBM)
    outs = [
        (tile(after), jax.ShapeDtypeStruct((t, d), BF16)),
        (tile(after), jax.ShapeDtypeStruct((t, d), BF16)),
        (pl.BlockSpec((heads, bt), lambda s: (0, after(s))), jax.ShapeDtypeStruct((heads, t), F32)),
        (anywhere, jax.ShapeDtypeStruct((n, height - down, d), BF16)),
        (anywhere, jax.ShapeDtypeStruct((BEHIND - 1, n, height, d), BF16)),
        (anywhere, jax.ShapeDtypeStruct((n, each, d), BF16)),
        *[(pl.BlockSpec((height, d), lambda s: (0, 0)), jax.ShapeDtypeStruct((height, d), BF16))] * (blocks - BEHIND),
        (pl.BlockSpec((down, d), lambda s: (0, 0)), jax.ShapeDtypeStruct((down, d), BF16)),
    ]
    scratch = [pltpu.VMEM((t, d), BF16)] * (2 + last) + [pltpu.VMEM((t, fb), BF16)] * 3 + [pltpu.VMEM((t, d), F32)]
    scratch += [pltpu.VMEM((blocks, n, height, d), BF16), pltpu.VMEM((n, each, d), BF16), pltpu.SemaphoreType.DMA((BEHIND + 1,))]
    scratch += [pltpu.VMEM((1, d, ff), BF16)] * 2 + [pltpu.VMEM((1, ff, d), BF16), pltpu.SemaphoreType.DMA((3,))]
    scratch += [pltpu.VMEM((d, d), F32)] * (1 if last else 3)
    for _ in range(blocks - BEHIND):
        scratch += RingSum.scratch(n, height, d)
    scratch += RingSum.scratch(n, down, d)
    if not last:
        outs += [(pl.BlockSpec((3 * each, d), lambda s: (0, 0)), jax.ShapeDtypeStruct((3 * each, d), BF16))]
        scratch += RingSum.scratch(n, 3 * each, d)
    return _call(
        functools.partial(_mlp_back, n=n, layer=layer, tiles=tiles, blocks=blocks, behind=BEHIND, last=last),
        (2 * tiles + middle,),
        ins,
        outs,
        scratch,
        args,
        2 * t * d * (ff * 8 + d * 4),
        sum(a.size * a.dtype.itemsize for a in args),
        collective=number,
    )


class Parts:
    def __init__(self, n, each):
        self.hosted, self.per, self.each = n - BEHIND, n - BEHIND + 3, each

    def ff(self, layer, block, which):
        at = layer * self.per + self.hosted
        if block < self.hosted:
            return at - self.hosted + block, which * self.each
        entry = (block - self.hosted) * 3 + which
        return (at, 0) if entry == 0 else (at + 1, (entry - 1) * self.each)

    def square(self, layer, which):
        at = layer * self.per + self.hosted
        return (at + 1, (BEHIND * 3 - 1) * self.each) if which == 3 else (at + 2, which * self.each)


def _moments(m, v, g):
    return 0.9 * m + 0.1 * g, 0.95 * v + 0.05 * g * g


def _stepped(w, m, v):
    return (w - 0.02 * (m * lax.rsqrt(v + 1e-8) + 0.1 * w)).astype(BF16)


def _finish(*refs, n, layers, own_count, count):
    take = iter(range(len(refs)))
    some = lambda k: [refs[next(take)] for _ in range(k)]
    a_ref, dq_ref, dk_ref, dv_ref = some(4)
    own_in, w_ref, m_ref, v_ref = some(own_count), some(7), some(7), some(7)
    lands, m_s, v_s = some(7), some(7), some(7)
    a_s, dq_s, dk_s, dv_s, g_s, own_ref, squares, total_s, others_s = some(9)
    pieces_s = some(own_count)
    load_sem, w_sem, m_sem, v_sem, swap_out, swap_in, out_r, out_l, in_l, in_r, pass_r, pass_l, far_l, far_r = some(14)
    jobs = [RingSum(n, g_s.at[i], *some(4)) for i in range(3)]
    me, right, far, left = _ring(n)
    mesh = pl.DeviceIdType.MESH
    barrier = pltpu.get_barrier_semaphore()
    for other in (right, far, left):
        pl.semaphore_signal(barrier, inc=1, device_id={"dp": other}, device_id_type=mesh)
    pairs = [(a_ref, a_s), (dv_ref, dv_s), (dk_ref, dk_s), (dq_ref, dq_s), *zip(own_in, pieces_s, strict=True)]
    loads = [pltpu.make_async_copy(s, d, load_sem.at[i]) for i, (s, d) in enumerate(pairs)]
    for load in loads:
        load.start()
    state = []
    for i in range(7):
        state.append(pltpu.make_async_copy(w_ref[i].at[:, me], lands[i].at[:, me], w_sem.at[i]))
        state.append(pltpu.make_async_copy(m_ref[i], m_s[i], m_sem.at[i]))
        state.append(pltpu.make_async_copy(v_ref[i], v_s[i], v_sem.at[i]))
    each = g_s.shape[2]
    squares[...] = jnp.zeros_like(squares)
    for load in loads[:2]:
        load.wait()
    _cut(g_s.at[2], 0, _dot(a_s[...], dv_s[...], 0, 0))
    pl.semaphore_wait(barrier, 3)
    loads[2].wait()
    jobs[2].start()
    for c in state:
        c.start()
    _cut(g_s.at[1], 0, _dot(a_s[...], dk_s[...], 0, 0))
    loads[3].wait()
    jobs[1].start()
    jobs[2].add()
    _cut(g_s.at[0], 0, _dot(a_s[...], dq_s[...], 0, 0))
    jobs[2].forward()
    jobs[1].add()
    jobs[0].start()
    jobs[1].forward()
    for i, piece in enumerate(pieces_s):
        if i == len(pieces_s) // 2:
            jobs[0].add()
        loads[4 + i].wait()
        _rows_loop(piece.shape[0], lambda rows, piece=piece: _add_squares(squares, piece[rows, :]))
        if i == len(pieces_s) // 2:
            jobs[0].forward()
    jobs[2].finish(own_ref.at[pl.ds(2 * each, each)], squares)
    jobs[1].finish(own_ref.at[pl.ds(each, each)], squares)
    jobs[0].finish(own_ref.at[pl.ds(0, each)], squares)
    total_s[...] = sum(squares[:, i : i + 128] for i in range(0, squares.shape[1], 128))
    swaps = [
        pltpu.make_async_remote_copy(src_ref=total_s, dst_ref=others_s.at[i], send_sem=swap_out.at[i], recv_sem=swap_in.at[i], device_id={"dp": other},
                                     device_id_type=mesh)
        for i, other in enumerate((right, far, left))
    ]
    for c in state:
        c.wait()
    for s in swaps:
        s.start()
    for s in swaps:
        s.wait()
    everything = jnp.sum(total_s[...] + others_s[0] + others_s[1] + others_s[2], keepdims=True)
    factor = jnp.minimum(1.0, 0.5 * lax.rsqrt(everything / count + 1e-30))

    parts = Parts(n, each)
    grads = [*pieces_s[: parts.per - 1], own_ref, *pieces_s[parts.per - 1 :]]
    blocks = n

    def new_weights(i, layer):
        land, m_i, v_i = lands[i], m_s[i], v_s[i]

        def one(at, piece, row, rows, column, g_column, width):
            def body(some):
                here = pl.ds(at + some.start, some.size)
                g = grads[piece][pl.ds(row + some.start, some.size), g_column : g_column + width].astype(F32) * factor
                m, v = _moments(m_i[layer, here, column : column + width], v_i[layer, here, column : column + width], g)
                m_i[layer, here, column : column + width] = m
                v_i[layer, here, column : column + width] = v
                w = land[layer, me, here, column : column + width].astype(F32)
                land[layer, me, here, column : column + width] = _stepped(w, m, v)

            return body

        if i < 4:
            bodies, rows = [one(0, *parts.square(layer, i), each, 0, 0, land.shape[3])], each
        elif i == 6:
            rows = each
            bodies = [one(b * each, *parts.ff(layer, b, 0), each, 0, 0, land.shape[3]) for b in range(blocks)]
        else:
            width, rows = g_s.shape[3] // n, each
            bodies = [
                one(0, *parts.ff(layer, b, i - 3), each, (d * blocks + b) * width, d * width, width) for d in range(n) for b in range(blocks)
            ]

        def run(some):
            for body in bodies:
                body(some)

        _rows_loop(rows, run, 16)

    remote = lambda ref, to, sent, got: pltpu.make_async_remote_copy(
        src_ref=ref, dst_ref=ref, send_sem=sent, recv_sem=got, device_id={"dp": to}, device_id_type=mesh)
    units = [(i, layer) for i in (3, 0, 1, 2, 6, 4, 5) for layer in range(layers)]
    sends, passes = [], []
    for u, (i, layer) in enumerate(units):
        mine = lands[i].at[layer, me]
        sends.append((remote(mine, right, out_r.at[u], in_l.at[u]), remote(mine, left, out_l.at[u], in_r.at[u])))
    for u in range(len(units) + 1):
        if u < len(units):
            new_weights(*units[u])
        if u > 0:
            for c in sends[u - 1]:
                c.start()
    for u, (i, layer) in enumerate(units):
        half = lands[i].shape[2] // 2
        sends[u][0].wait_recv()
        one = remote(lands[i].at[layer, left, pl.ds(0, half)], right, pass_r.at[u], far_l.at[u])
        one.start()
        sends[u][1].wait_recv()
        two = remote(lands[i].at[layer, right, pl.ds(half, half)], left, pass_l.at[u], far_r.at[u])
        two.start()
        passes.append((one, two))
    for u in range(len(units)):
        for c in passes[u]:
            c.wait_recv()
        for c in (*sends[u], *passes[u]):
            c.wait_send()


def finish(n, number, a, dq, dk, dv, own, w, m, v):
    t, d = a.shape
    each, layers = d // n, w[0].shape[0]
    anywhere, here = pl.BlockSpec(memory_space=pltpu.HBM), pl.BlockSpec(memory_space=pltpu.VMEM)
    w = [one.reshape(layers, n, one.shape[1] // n, one.shape[2]) for one in w]
    scratch = [pltpu.VMEM((t, d), BF16)] * 4
    scratch += [pltpu.VMEM((3, n, each, d), BF16), pltpu.VMEM((3 * each, d), BF16), pltpu.VMEM((8, d), F32), pltpu.VMEM((8, 128), F32),
                pltpu.VMEM((3, 8, 128), F32)]
    scratch += [pltpu.VMEM(o.shape, BF16) for o in own]
    units = 7 * layers
    sem = lambda k: pltpu.SemaphoreType.DMA((k,))
    scratch += [sem(4 + len(own)), sem(7), sem(7), sem(7), sem(3), sem(3), *[sem(units)] * 8]
    for _ in range(3):
        scratch += RingSum.scratch(n, each, d)
    return _call(
        functools.partial(_finish, n=n, layers=layers, own_count=len(own), count=n * sum(one.size for one in m)),
        (),
        [anywhere] * (4 + len(own) + 21),
        [(here, pltpu.VMEM(one.shape, one.dtype)) for one in (*w, *m, *v)],
        scratch,
        (a, dq, dk, dv, *own, *w, *m, *v),
        6 * t * d * d,
        8 * t * d,
        collective=number,
        vmem=REST,
    )


def _settle(*refs):
    count = len(refs) // 2
    copies = [pltpu.make_async_copy(refs[i], refs[count + i], refs[-1].at[i]) for i in range(count)]
    for c in copies:
        c.start()
    for c in copies:
        c.wait()


def settle(arrays):
    there = pl.BlockSpec(memory_space=pltpu.HBM)
    return _call(
        _settle,
        (),
        [pl.BlockSpec(memory_space=pltpu.VMEM)] * len(arrays),
        [(there, jax.ShapeDtypeStruct(a.shape, a.dtype)) for a in arrays],
        [pltpu.SemaphoreType.DMA((len(arrays),))],
        [pltpu.with_memory_space_constraint(a, pltpu.VMEM) for a in arrays],
        0,
        2 * sum(a.size * a.dtype.itemsize for a in arrays),
        vmem=REST,
    )


NAMES = ("wq", "wk", "wv", "wo", "w_gate", "w_up", "w_down")


def rope_tables(t):
    half = HEAD // 2
    angle = np.arange(t, dtype=np.float32)[:, None] * (np.float32(THETA) ** (-np.arange(half, dtype=np.float32) / half)).astype(np.float32)
    cos, sin = np.cos(angle.astype(np.float64)).astype(np.float32), np.sin(angle.astype(np.float64)).astype(np.float32)
    return jnp.asarray(np.concatenate([cos, cos], 1)), jnp.asarray(np.concatenate([-sin, sin], 1))


def solution(mesh):
    n = mesh.shape["dp"]

    def step(x, dy, *arrays):
        weights = dict(zip(NAMES, arrays[:7], strict=True))
        m, v = arrays[7:14], arrays[14:]
        layers = weights["wq"].shape[0]
        h = x[0]
        rope = rope_tables(h.shape[0])
        made, a = forward(n, h, weights, rope)
        hs = [h, *(one[6] for one in made[:-1])]
        own = {}
        by, upper, number = dy[0], None, 0
        for layer in reversed(range(layers)):
            if upper is None:
                got = mlp_back(n, number, layer, hs[layer], made[layer][3], by, weights)
            else:
                got = mlp_back(n, number, layer, made[layer][5], made[layer][3], by, weights, upper, made[layer][7:9])
                own[layer + 1].append(got[-1])
            by, datt, delta, *left = got[:6]
            dq, dk, dv, rest = attend_back(n, number + 1, *made[layer][:3], datt, made[layer][4], delta, rope, *left)
            own[layer] = [*got[6 : 7 + n - BEHIND], rest]
            upper = hs[layer], dq, dk, dv
            number += 2
        pieces = [p for layer in range(layers) for p in own[layer]]
        out = settle(finish(n, number, a, *upper[1:], pieces, arrays[:7], m, v))
        return tuple(one.reshape(layers, -1, one.shape[-1]) for one in out)

    states, all_of, cut = P(("rep", "dp"), None, None), P(None, None, None), P(None, "dp", None)
    return jax.shard_map(
        step,
        mesh=mesh,
        in_specs=(states, states) + (all_of,) * 7 + (cut,) * 14,
        out_specs=(P("rep", None, None),) * 7 + (P("rep", "dp", None),) * 14,
        check_vma=False,
    )
```

```python
import functools

import jax
import jax.numpy as jnp
import numpy as np
from jax import lax
from jax.experimental import pallas as pl
from jax.experimental.pallas import tpu as pltpu
from jax.sharding import PartitionSpec as P

F32, BF16 = jnp.float32, jnp.bfloat16
HEAD = 128
THETA = 10000
NEG = -1e30
HIDDEN = 2 * NEG
LOG2E = 1.4426950408889634
SCALE = HEAD**-0.5
VMEM = 67043328
REST = 30 * 2**20
BEHIND = 2


def _dot(a, b, ca=1, cb=0):
    return lax.dot_general(a, b, (((ca,), (cb,)), ((), ())), preferred_element_type=F32)


def _tile(size, most=512):
    return max(n for n in range(128, most + 1, 128) if size % n == 0)


def _call(kernel, grid, ins, outs, scratch, args, flops, moved, collective=None, vmem=VMEM):
    return pl.pallas_call(
        kernel,
        grid=grid,
        in_specs=[spec for spec in ins],
        out_specs=[spec for spec, _ in outs],
        out_shape=[shape for _, shape in outs],
        scratch_shapes=scratch,
        compiler_params=pltpu.CompilerParams(dimension_semantics=("arbitrary",) * len(grid), vmem_limit_bytes=vmem, collective_id=collective,
                                             has_side_effects=collective is not None),
        cost_estimate=pl.CostEstimate(flops=int(flops), transcendentals=0, bytes_accessed=int(moved)),
    )(*args)


def _norm_scale(x):
    return lax.rsqrt(jnp.mean(x * x, -1, keepdims=True) + 1e-6)


def _normed(x):
    return (x * _norm_scale(x)).astype(BF16)


def _norm_back(x, d_out):
    s = _norm_scale(x)
    inner = jnp.mean(x * d_out, -1, keepdims=True)
    return s * d_out - x * (s * s * s * inner)


def _turn(x, cos, sin):
    parts = [x[:, n : n + HEAD] for n in range(0, x.shape[1], HEAD)]
    return jnp.concatenate([p * cos + pltpu.roll(p, HEAD // 2, 1) * sin for p in parts], 1)


def _qkv(h, wq, wk, wv, cos, sin):
    a = _normed(h)
    q, k = (_turn(_dot(a, w).astype(BF16).astype(F32), cos, sin).astype(BF16) for w in (wq, wk))
    return a, q, k, _dot(a, wv).astype(BF16)


def _after_attention(h_ref, att_ref, wo):
    return (h_ref[...].astype(F32) + _dot(att_ref[...], wo).astype(BF16).astype(F32)).astype(BF16)


def _ring(n):
    me = lax.axis_index("dp")
    return me, lax.rem(me + 1, n), lax.rem(me + 2, n), lax.rem(me + n - 1, n)


def _greet(n):
    _, right, _, left = _ring(n)
    barrier = pltpu.get_barrier_semaphore()
    for other in (right, left):
        pl.semaphore_signal(barrier, inc=1, device_id={"dp": other}, device_id_type=pl.DeviceIdType.MESH)


def _met():
    pl.semaphore_wait(pltpu.get_barrier_semaphore(), 2)


def _rows_loop(rows, body, most=32):
    each = max(c for c in range(16, most + 1, 16) if rows % c == 0)
    lax.fori_loop(0, rows // each, lambda i, _: body(pl.ds(pl.multiple_of(i * each, each), each)), None)


class RingSum:
    def __init__(self, n, block, passing, arrived, sent, got):
        self.block, self.passing, self.arrived = block, passing, arrived
        self.me, right, far, left = _ring(n)
        self.near = right, left
        half = block.shape[1] // 2
        self.half = half
        a, b = pl.ds(0, half), pl.ds(half, half)
        moves = [
            (block.at[far, a], passing.at[0], right),
            (block.at[far, b], passing.at[1], left),
            (block.at[right, b], arrived.at[0, b], right),
            (block.at[left, a], arrived.at[1, a], left),
            (passing.at[0], arrived.at[0, a], right),
            (passing.at[1], arrived.at[1, b], left),
        ]
        self.copies = [
            pltpu.make_async_remote_copy(src_ref=s, dst_ref=d, send_sem=sent.at[i], recv_sem=got.at[i], device_id={"dp": to},
                                         device_id_type=pl.DeviceIdType.MESH)
            for i, (s, d, to) in enumerate(moves)
        ]

    @staticmethod
    def scratch(n, rows, columns):
        half = pltpu.VMEM((2, rows // 2, columns), BF16)
        return [half, pltpu.VMEM((2, rows, columns), BF16), pltpu.SemaphoreType.DMA((6,)), pltpu.SemaphoreType.DMA((6,))]

    def start(self):
        for c in self.copies[:4]:
            c.start()

    def add(self):
        for c in self.copies[:2]:
            c.wait_recv()
        for i, other in enumerate(self.near):

            def one(rows, i=i, other=other):
                mine = self.block[other, pl.ds(rows.start + i * self.half, rows.size), :]
                self.passing[i, rows, :] = (self.passing[i, rows, :].astype(F32) + mine.astype(F32)).astype(BF16)

            _rows_loop(self.half, one)

    def forward(self):
        for c in self.copies[4:]:
            c.start()

    def finish(self, out, squares=None):
        for c in self.copies[2:]:
            c.wait_recv()

        def one(rows):
            total = self.block[self.me, rows, :].astype(F32) + self.arrived[0, rows, :].astype(F32) + self.arrived[1, rows, :].astype(F32)
            total = total.astype(BF16)
            out[rows, :] = total
            if squares is not None:
                _add_squares(squares, total)

        _rows_loop(self.half * 2, one)
        for c in self.copies:
            c.wait_send()


def _add_squares(squares, value):
    value = value.astype(F32)
    value = value * value
    squares[...] += sum(value[i : i + 8] for i in range(0, value.shape[0], 8))


class RingGather:
    def __init__(self, n, src, place, sent, got):
        me, right, _, left = _ring(n)
        rows = src.shape[0]
        half = rows // 2
        first, second = place(left, 0, half), place(right, half, half)
        moves = [(src, place(me, 0, rows), right), (src, place(me, 0, rows), left), (first, first, right), (second, second, left)]
        self.copies = [
            pltpu.make_async_remote_copy(src_ref=a, dst_ref=b, send_sem=sent.at[i], recv_sem=got.at[i], device_id={"dp": to},
                                         device_id_type=pl.DeviceIdType.MESH)
            for i, (a, b, to) in enumerate(moves)
        ]

    @staticmethod
    def scratch():
        return [pltpu.SemaphoreType.DMA((4,)), pltpu.SemaphoreType.DMA((4,))]

    def start(self):
        for c in self.copies[:2]:
            c.start()

    def forward(self):
        for here, there in zip(self.copies[:2], self.copies[2:], strict=True):
            here.wait_recv()
            there.start()

    def finish(self):
        for c in self.copies[2:]:
            c.wait_recv()
        for c in self.copies:
            c.wait_send()


def _seen(keys, queries):
    return lax.broadcasted_iota(jnp.int32, (keys, queries), 1) >= lax.broadcasted_iota(jnp.int32, (keys, queries), 0)


def diagonal(block, first, size, part=256):
    part = min(part, size)
    for at in range(0, size, part):
        block(first + at, part, at, True)


def _attend(iq, q_ref, k_ref, v_ref, o_ref, lse_ref, top_s, mix_s, bk):
    bq = q_ref.shape[0]
    heads = q_ref.shape[1] // HEAD
    e = SCALE * LOG2E
    top_s[...] = jnp.full(top_s.shape, NEG, F32)
    mix_s[...] = jnp.zeros(mix_s.shape, F32)

    def block(first, keys, at, masked):
        here, ask = pl.ds(pl.multiple_of(first, keys), keys), slice(at, bq)
        cols = [slice(n * HEAD, (n + 1) * HEAD) for n in range(heads)]
        scores = [_dot(k_ref[here, c], q_ref[ask, c], 1, 1) for c in cols]
        weights, keeps = [], []
        seen = _seen(keys, bq - at) if masked else None
        for n, s in enumerate(scores):
            if masked:
                s = jnp.where(seen, s, HIDDEN)
            old = top_s[n : n + 1, ask]
            top = jnp.maximum(old, s.max(axis=0, keepdims=True))
            top_s[n : n + 1, ask] = top
            weights.append(jnp.exp2((s - top) * e).astype(BF16))
            keeps.append(jnp.exp2((old - top) * e))
        ones = jnp.ones((8, keys), BF16)
        for n, (c, p, keep) in enumerate(zip(cols, weights, keeps)):
            values = jnp.concatenate([v_ref[here, c].T, ones], axis=0)
            mix_s[n, :, ask] = mix_s[n, :, ask] * keep + _dot(values, p, 1, 0)

    lax.fori_loop(0, iq * (bq // bk), lambda j, _: block(j * bk, bk, 0, False), None)
    diagonal(block, iq * bq, bq)
    for n in range(heads):
        total = mix_s[n, HEAD : HEAD + 1, :]
        o_ref[:, n * HEAD : (n + 1) * HEAD] = (mix_s[n, :HEAD, :] * (1 / total)).T.astype(BF16)
        lse_ref[n : n + 1, :] = top_s[n : n + 1, :] * e + jnp.log2(total)


def _forward(h_ref, wq, wk, wv, wo, wg_ref, wu_ref, wd_ref, cos, sin, m_ref, v_ref, *refs, n, layers):
    outs, (a_ref, m_all, v_all), scratch = refs[: 9 * layers - 4], refs[9 * layers - 4 : 9 * layers - 1], refs[9 * layers - 1 :]
    k_s, v_s, wg, wu, wd, gate_s, up_s, top_s, mix_s, w_sem, out_sem, *sems = scratch
    early = m_all.shape[1]
    gathers = [
        RingGather(n, a.at[layers - 1, pl.ds(0, early)], lambda d, at, rows, b=b: b.at[d, pl.ds(at, rows)], *sems[2 * i : 2 * i + 2])
        for i, (a, b) in enumerate(((m_ref, m_all), (v_ref, v_all)))
    ]
    step = pl.program_id(0)
    bt = h_ref.shape[0]
    rows = pl.ds(pl.multiple_of(step * bt, bt), bt)
    loads = [pltpu.make_async_copy(a.at[0], b.at[0], w_sem.at[i]) for i, (a, b) in enumerate(((wg_ref, wg), (wu_ref, wu), (wd_ref, wd)))]

    @pl.when(step == 0)
    def _():
        _greet(n)
        for load in loads:
            load.start()

    for layer in range(layers):
        q_ref, k_ref, v_ref, att_ref, lse_ref = outs[9 * layer : 9 * layer + 5]
        a, q_ref[...], k, v = _qkv(h_ref[...].astype(F32), wq[layer], wk[layer], wv[layer], cos[...], sin[...])
        if layer == 0:
            a_ref[...] = a
        k_ref[...] = k_s[layer, rows, :] = k
        v_ref[...] = v_s[layer, rows, :] = v
        _attend(step, q_ref, k_s.at[layer], v_s.at[layer], att_ref, lse_ref, top_s, mix_s, bt)
        if layer == layers - 1:
            break
        if layer == 0:

            @pl.when(step == 0)
            def _():
                _met()
                for g in gathers:
                    g.start()

            @pl.when(step == pl.num_programs(0) - 2)
            def _():
                gathers[0].forward()

        h1_ref, y_ref, gate_ref, up_ref = outs[9 * layer + 5 : 9 * layer + 9]
        stores = [
            pltpu.make_async_copy(a.at[j], b.at[j, rows], out_sem.at[layer, i, j])
            for i, (a, b) in enumerate(((gate_s, gate_ref), (up_s, up_ref)))
            for j in range(n)
        ]

        @pl.when(step == 0)
        def _(layer=layer):
            for load in loads:
                load.wait()

        @pl.when(step > 0)
        def _(stores=stores):
            for c in stores:
                c.wait()

        h1 = _after_attention(h_ref, att_ref, wo[layer])
        h1_ref[...] = h1
        h1 = h1.astype(F32)
        b = (h1 * _norm_scale(h1)).astype(BF16)
        total = jnp.zeros(h1.shape, F32)
        for j in range(n):
            gate, up = _dot(b, _strips(wg, j, n, n, 2)), _dot(b, _strips(wu, j, n, n, 2))
            gate_s[j] = gate
            up_s[j] = up
            total += _dot((gate * jax.nn.sigmoid(gate) * up).astype(BF16), _strips(wd, j, n, n, 1))
        for c in stores:
            c.start()
        y_ref[...] = (h1 + total.astype(BF16).astype(F32)).astype(BF16)
        h_ref = y_ref

        @pl.when(step == pl.num_programs(0) - 1)
        def _(stores=stores):
            for c in stores:
                c.wait()

    @pl.when(step == pl.num_programs(0) - 2)
    def _():
        gathers[1].forward()

    @pl.when(step == pl.num_programs(0) - 1)
    def _():
        for g in gathers:
            g.finish()


def anywhere_spec():
    return pl.BlockSpec(memory_space=pltpu.HBM)


def early_rows(n, d):
    return (n - BEHIND + 1) * (d // n)


def forward(n, number, h, weights, rope, m, v):
    t, d = h.shape
    layers, _, ff = weights["w_gate"].shape
    assert layers == 2
    many = (anywhere_spec(), jax.ShapeDtypeStruct((n, early_rows(n, d), d), F32))
    heads = weights["wq"].shape[2] // HEAD
    bt = _tile(t)
    tile, table = (pl.BlockSpec((bt, w), lambda s: (s, 0)) for w in (d, HEAD))
    square = pl.BlockSpec((layers, d, d), lambda s: (0, 0, 0), pipeline_mode=pl.Buffered(1))
    anywhere = pl.BlockSpec(memory_space=pltpu.HBM)
    one = (tile, jax.ShapeDtypeStruct((t, d), BF16))
    two = (anywhere, jax.ShapeDtypeStruct((n, t, ff // n), F32))
    stats = (pl.BlockSpec((heads, bt), lambda s: (0, s)), jax.ShapeDtypeStruct((heads, t), F32))
    upper = [*[one] * 4, stats]
    got = _call(
        functools.partial(_forward, n=n, layers=layers),
        (t // bt,),
        [tile, *[square] * 4, *[anywhere] * 3, table, table, anywhere, anywhere],
        [*[*upper, one, one, two, two] * (layers - 1), *upper, one, many, many],
        [pltpu.VMEM((layers, t, d), BF16)] * 2
        + [pltpu.VMEM((1, d, ff), BF16)] * 2
        + [pltpu.VMEM((1, ff, d), BF16)]
        + [pltpu.VMEM((n, bt, ff // n), F32)] * 2
        + [pltpu.VMEM((heads, bt), F32), pltpu.VMEM((heads, HEAD + 8, bt), F32), pltpu.SemaphoreType.DMA((3,)),
           pltpu.SemaphoreType.DMA((layers, 2, n)), *RingGather.scratch(), *RingGather.scratch()],
        (h, *(weights[name] for name in ("wq", "wk", "wv", "wo")), *(weights[name] for name in ("w_gate", "w_up", "w_down")), *rope, m, v),
        2 * t * d * (8 * d + 3 * ff) + 4 * t * t * d,
        30 * t * d + 8 * t * ff,
        collective=number,
    )
    return [got[9 * layer : 9 * layer + 9] for layer in range(layers - 1)] + [got[9 * layers - 9 : -3]], got[-3], got[-2:]


def _attend_back(q_ref, k_ref, v_ref, do_ref, lse_ref, delta_ref, cos, sin, part_ref, ff_ref, o_ref, dq_ref, dk_ref, dv_ref, own_ref, dq_s, dk_s, dv_s, block_s, load_sem,
                 *ring, bk, n):
    iq = pl.program_id(0)
    bq = q_ref.shape[0]
    heads = q_ref.shape[1] // HEAD
    e = SCALE * LOG2E
    steps = pl.num_programs(0)
    loads, at = [], 0
    for i, source in enumerate((part_ref, *(ff_ref.at[i] for i in range(ff_ref.shape[0])), o_ref)):
        loads.append(pltpu.make_async_copy(source, block_s.at[:, pl.ds(at, source.shape[1])], load_sem.at[i]))
        at += source.shape[1]
    job = RingSum(n, block_s, *ring)

    @pl.when(iq == 0)
    def _():
        _greet(n)
        for load in loads:
            load.start()
        dk_s[...] = jnp.zeros_like(dk_s)
        dv_s[...] = jnp.zeros_like(dv_s)

    @pl.when(iq == 1)
    def _():
        for load in loads:
            load.wait()
        _met()
        job.start()

    @pl.when(iq == steps - 1)
    def _():
        job.forward()

    dq_s[...] = jnp.zeros_like(dq_s)

    def block(first, keys, at, masked):
        here, ask = pl.ds(pl.multiple_of(first, keys), keys), slice(at, bq)
        cols = [slice(i * HEAD, (i + 1) * HEAD) for i in range(heads)]
        scores = [_dot(k_ref[here, c], q_ref[ask, c], 1, 1) for c in cols]
        dps = [_dot(v_ref[here, c], do_ref[ask, c], 1, 1) for c in cols]
        seen = _seen(keys, bq - at) if masked else None
        for i, c in enumerate(cols):
            p = jnp.exp2(scores[i] * e - lse_ref[i : i + 1, ask])
            if masked:
                p = jnp.where(seen, p, 0.0)
            ds = (p * (dps[i] - delta_ref[i : i + 1, ask])).astype(BF16)
            dv_s[here, c] += _dot(p.astype(BF16), do_ref[ask, c], 1, 0)
            dk_s[here, c] += _dot(ds, q_ref[ask, c], 1, 0)
            dq_s[i, :, ask] += _dot(k_ref[here, c].T, ds, 1, 0)

    lax.fori_loop(0, iq * (bq // bk), lambda j, _: block(j * bk, bk, 0, False), None)
    diagonal(block, iq * bq, bq)

    @pl.when(iq == steps - 2)
    def _():
        job.add()

    def back(d, rows):
        return _turn(d.astype(BF16).astype(F32), cos[rows, :], -sin[rows, :]).astype(BF16)

    mine = pl.ds(pl.multiple_of(iq * bq, bq), bq)
    for i in range(heads):
        dq_ref[:, i * HEAD : (i + 1) * HEAD] = back((dq_s[i] * SCALE).T, mine)

    @pl.when(iq == steps - 1)
    def _():
        def one(rows):
            dk_ref[rows, :] = back(dk_s[rows, :] * SCALE, rows)
            dv_ref[rows, :] = dv_s[rows, :].astype(BF16)

        _rows_loop(dk_ref.shape[0], one, 256)
        job.finish(own_ref)


def attend_back(n, number, q, k, v, d_out, lse, delta, rope, part, ff, o):
    t, width = q.shape
    heads = width // HEAD
    bq = bk = _tile(t)
    rows, whole = pl.BlockSpec((bq, width), lambda i: (i, 0)), pl.BlockSpec((t, width), lambda i: (0, 0))
    stats = pl.BlockSpec((heads, bq), lambda i: (0, i))
    table = pl.BlockSpec((t, HEAD), lambda i: (0, 0), pipeline_mode=pl.Buffered(1))
    one = jax.ShapeDtypeStruct((t, width), BF16)
    height, columns = part.shape[1] + ff.shape[0] * ff.shape[2] + o.shape[1], ff.shape[3]
    return _call(
        functools.partial(_attend_back, bk=bk, n=n),
        (t // bq,),
        [rows, whole, whole, rows, stats, stats, table, table, *[pl.BlockSpec(memory_space=pltpu.HBM)] * 3],
        [(rows, one), (whole, one), (whole, one),
         (pl.BlockSpec((height, columns), lambda i: (0, 0)), jax.ShapeDtypeStruct((height, columns), BF16))],
        [pltpu.VMEM((heads, HEAD, bq), F32), pltpu.VMEM((t, width), F32), pltpu.VMEM((t, width), F32),
         pltpu.VMEM((n, height, columns), BF16), pltpu.SemaphoreType.DMA((ff.shape[0] + 2,)),
         *RingSum.scratch(n, height, columns)],
        (q, k, v, d_out, lse, delta, *rope, part, ff, o),
        5 * t * t * width,
        14 * t * width,
        collective=number,
    )


def _strips(ref, block, n, blocks, axis):
    width = ref.shape[axis] // (n * blocks)
    at = [pl.ds(pl.multiple_of((d * blocks + block) * width, width), width) for d in range(n)]
    return jnp.concatenate([ref[0, :, a] if axis == 2 else ref[0, a, :] for a in at], axis - 1)


def _qkv_back(h, dq, dk, dv, wq, wk, wv, sums):
    a = (h * _norm_scale(h)).astype(BF16)
    for s, d in zip(sums, (dq, dk, dv), strict=True):
        s[...] += _dot(a, d, 0, 0)
    return _dot(jnp.concatenate([dq, dk, dv], 1), jnp.concatenate([wq, wk, wv], 1), 1, 1)


def _cut(ref, at, value):
    n = ref.shape[0]
    each = value.shape[0] // n
    for d in range(n):
        ref[d, at : at + each] = value[d * each : (d + 1) * each].astype(BF16)


def _mlp_back(*refs, n, layer, tiles, blocks, behind, last):
    take = iter(range(len(refs)))
    some = lambda count: [refs[next(take)] for _ in range(count)]
    h_ref, att_ref = some(2)
    if last:
        (dy_ref,) = some(1)
    else:
        hn_ref, dq_ref, dk_ref, dv_ref, dh_ref, wq, wk, wv, gate_ref, up_ref = some(10)
        sums_in = some(blocks - behind + 1)
    wo, wg_ref, wu_ref, wd_ref = some(4)
    dh1_ref, datt_ref, delta_ref, left_part, left_ff, left_o = some(6)
    hosted = blocks - behind
    own = some(hosted + 1 + (not last))
    g_all = None if last else some(1)[0]
    h1_s = some(1)[0] if last else None
    b_s, dy_s, p_s, dg_s, du_s, sum_b, g_s, go_s, out_sem = some(9)
    wg, wu, wd, w_sem = some(4)
    sums3 = some(1 if last else 3)
    sum_o = sums3[0]
    jobs = []
    for i in range(len(own)):
        if i < hosted:
            block = g_s.at[i]
        elif i == hosted:
            block = g_s.at[i, :, pl.ds(0, own[i].shape[0])]
        else:
            block = gqkv_s = g_s.at[blocks - 1]
        jobs.append(RingSum(n, block, *some(4)))
    gathers = []
    if not last:
        for i, source in enumerate(sums_in):
            each = own[hosted].shape[0]
            gathers.append(RingGather(n, source.at[pl.ds(0, each)], lambda d, at, rows, i=i: g_all.at[d, pl.ds(i * each + at, rows)], *some(2)))
    step = pl.program_id(0)
    bt = h_ref.shape[0]
    middle = tiles * blocks
    r = jnp.where(step < tiles, step, lax.rem(step - tiles, tiles))
    j = lax.div(step - tiles, tiles)
    rows = pl.ds(pl.multiple_of(r * bt, bt), bt)
    @pl.when(step == 0)
    def _():
        _greet(n)
        for s in sums3:
            s[...] = jnp.zeros_like(s)

    loads = [pltpu.make_async_copy(a.at[layer], b.at[0], w_sem.at[i]) for i, (a, b) in enumerate(((wg_ref, wg), (wu_ref, wu), (wd_ref, wd)))]

    @pl.when(step == 0)
    def _():
        for load in loads:
            load.start()

    @pl.when(step == tiles)
    def _():
        for load in loads:
            load.wait()

    final = 2 * tiles + middle - 1
    times = [(at, min(at + tiles * 3 // 2, tiles + middle)) for at in (tiles * (2 + i) for i in range(hosted + 1))] + [(tiles, 2 * tiles)] * (not last)
    times = [(start, forward - 1, forward, min(forward + tiles * 3 // 2, final)) for start, forward in times]

    @pl.when(step == (min(t[0] for t in times) if last else 1))
    def _():
        _met()
        for g in gathers:
            g.start()

    @pl.when(step == tiles)
    def _():
        for g in gathers:
            g.forward()

    for job, (_, _, at, _) in zip(jobs, times, strict=True):

        @pl.when(step == at)
        def _(job=job):
            job.forward()

    for job, (at, _, _, _) in zip(jobs, times, strict=True):

        @pl.when(step == at)
        def _(job=job):
            job.start()

    @pl.when(step < tiles)
    def _():
        if last:
            h1 = _after_attention(h_ref, att_ref, wo[0])
            h1_s[rows, :] = h1
            dy_s[rows, :] = dy_ref[...]
        else:
            h1 = h_ref[...]
            hn = hn_ref[...].astype(F32)
            da = _qkv_back(hn, dq_ref[...], dk_ref[...], dv_ref[...], wq[0], wk[0], wv[0], sums3)
            dy_s[rows, :] = (dh_ref[...].astype(F32) + _norm_back(hn, da.astype(BF16).astype(F32)).astype(BF16).astype(F32)).astype(BF16)

            @pl.when(step == tiles - 1)
            def _():
                for i, s in enumerate(sums3):
                    _cut(gqkv_s, i * (s.shape[0] // n), s[...])
                sum_o[...] = jnp.zeros_like(sum_o)

        h1 = h1.astype(F32)
        b_s[rows, :] = (h1 * _norm_scale(h1)).astype(BF16)
        sum_b[rows, :] = jnp.zeros((bt, sum_b.shape[1]), F32)

    @pl.when((step >= tiles) & (step < tiles + middle))
    def _():
        b, dy = b_s[rows, :], dy_s[rows, :]
        gate_w, up_w, down_w = _strips(wg, j, n, blocks, 2), _strips(wu, j, n, blocks, 2), _strips(wd, j, n, blocks, 1)
        terms = []
        for at in range(0, gate_w.shape[1], 256):
            c = slice(at, at + 256)
            gate, up = (_dot(b, gate_w[:, c]), _dot(b, up_w[:, c])) if last else (gate_ref[0, :, c], up_ref[0, :, c])
            dp = _dot(dy, down_w[c], 1, 1).astype(BF16).astype(F32)
            sg = jax.nn.sigmoid(gate)
            silu = gate * sg
            p_s[rows, c] = (silu * up).astype(BF16)
            du = (dp * silu).astype(BF16)
            dg = (dp * up * (sg + silu * (1 - sg))).astype(BF16)
            du_s[rows, c] = du
            dg_s[rows, c] = dg
            terms.append((dg, du))
        sum_b[rows, :] += _dot(jnp.concatenate([g for g, _ in terms] + [u for _, u in terms], 1), jnp.concatenate([gate_w, up_w], 1), 1, 1)

        @pl.when(r == tiles - 1)
        def _():
            each = b.shape[1] // n
            mine = g_s.at[j]
            _cut(mine, 0, _dot(p_s[...], dy_s[...], 0, 0))
            _cut(mine, mine.shape[1] - 2 * each, _dot(b_s[...], dg_s[...], 0, 0))
            _cut(mine, mine.shape[1] - each, _dot(b_s[...], du_s[...], 0, 0))

    part = own[hosted].shape[0]
    out_copies = [pltpu.make_async_copy(g_s.at[hosted, :, pl.ds(part, left_part.shape[1])], left_part, out_sem.at[0])]
    out_copies += [pltpu.make_async_copy(g_s.at[hosted + i], left_ff.at[i - 1], out_sem.at[i]) for i in range(1, behind)]
    out_copies.append(pltpu.make_async_copy(go_s, left_o, out_sem.at[behind]))

    @pl.when(step >= tiles + middle)
    def _():
        db = sum_b[rows, :]
        h1 = h1_s[rows, :] if last else h_ref[...]
        dh1 = dy_s[rows, :].astype(F32) + _norm_back(h1.astype(F32), db.astype(BF16).astype(F32)).astype(BF16).astype(F32)
        dh1 = dh1.astype(BF16)
        dh1_ref[...] = dh1
        datt = _dot(dh1, wo[0], 1, 1).astype(BF16)
        datt_ref[...] = datt
        att = att_ref[...]
        both = att.astype(F32) * datt.astype(F32)
        for i in range(both.shape[1] // HEAD):
            delta_ref[i : i + 1, :] = both[:, i * HEAD : (i + 1) * HEAD].T.sum(axis=0, keepdims=True)
        sum_o[...] += _dot(att, dh1, 0, 0)

        @pl.when(step == tiles + middle)
        def _():
            for c in out_copies[:-1]:
                c.start()

        @pl.when(step == 2 * tiles + middle - 1)
        def _():
            _cut(go_s, 0, sum_o[...])
            out_copies[-1].start()
            for c in out_copies:
                c.wait()

    for job, (_, at, _, _) in zip(jobs, times, strict=True):

        @pl.when(step == at)
        def _(job=job):
            job.add()

    @pl.when(step == final)
    def _():
        for g in gathers:
            g.finish()

    for job, (_, _, _, at), out in zip(jobs, times, own, strict=True):

        @pl.when(step == at)
        def _(job=job, out=out):
            job.finish(out)


def mlp_back(n, number, layer, h, att, by, weights, upper=None, hidden=None, sums=None):
    t, d = h.shape
    ff = weights["w_gate"].shape[2]
    bt = _tile(t)
    tiles, blocks = t // bt, n
    fb, each = ff // blocks, d // n
    down = fb // n
    height = down + 2 * each
    assert n == 4 and fb == d and height == 3 * each
    heads = att.shape[1] // HEAD
    middle = tiles * blocks
    r = lambda s: jnp.where(s < tiles, s, lax.rem(s - tiles, tiles))
    j = lambda s: jnp.clip(lax.div(s - tiles, tiles), 0, blocks - 1)
    edge = lambda s: jnp.where(s < tiles, s, jnp.where(s < tiles + middle, tiles - 1, s - tiles - middle))
    before = lambda s: jnp.minimum(s, tiles - 1)
    after = lambda s: jnp.maximum(s - tiles - middle, 0)
    tile = lambda f, w=d: pl.BlockSpec((bt, w), lambda s: (f(s), 0))
    fixed = lambda which, *shape: pl.BlockSpec((1, *shape), lambda s: (which, 0, 0), pipeline_mode=pl.Buffered(1))
    square, up_square = fixed(layer, d, d), fixed(layer + 1, d, d)
    anywhere = pl.BlockSpec(memory_space=pltpu.HBM)
    mlp = [square, anywhere, anywhere, anywhere]
    w4 = [weights[name] for name in ("wo", "w_gate", "w_up", "w_down")]
    last = upper is None
    if last:
        ins = [tile(before), tile(edge), tile(before), *mlp]
        args = [h, att, by, *w4]
    else:
        hn, dq, dk, dv = upper
        block = pl.BlockSpec((1, bt, fb), lambda s: (j(s), r(jnp.clip(s, tiles, tiles + middle - 1)), 0))
        ins = [tile(edge), tile(after), *[tile(before)] * 5, up_square, up_square, up_square, block, block, *[anywhere] * len(sums), *mlp]
        args = [h, att, hn, dq, dk, dv, by, weights["wq"], weights["wk"], weights["wv"], *hidden, *sums, *w4]
    anywhere = pl.BlockSpec(memory_space=pltpu.HBM)
    outs = [
        (tile(after), jax.ShapeDtypeStruct((t, d), BF16)),
        (tile(after), jax.ShapeDtypeStruct((t, d), BF16)),
        (pl.BlockSpec((heads, bt), lambda s: (0, after(s))), jax.ShapeDtypeStruct((heads, t), F32)),
        (anywhere, jax.ShapeDtypeStruct((n, height - down, d), BF16)),
        (anywhere, jax.ShapeDtypeStruct((BEHIND - 1, n, height, d), BF16)),
        (anywhere, jax.ShapeDtypeStruct((n, each, d), BF16)),
        *[(pl.BlockSpec((height, d), lambda s: (0, 0)), jax.ShapeDtypeStruct((height, d), BF16))] * (blocks - BEHIND),
        (pl.BlockSpec((down, d), lambda s: (0, 0)), jax.ShapeDtypeStruct((down, d), BF16)),
    ]
    scratch = [pltpu.VMEM((t, d), BF16)] * (2 + last) + [pltpu.VMEM((t, fb), BF16)] * 3 + [pltpu.VMEM((t, d), F32)]
    scratch += [pltpu.VMEM((blocks, n, height, d), BF16), pltpu.VMEM((n, each, d), BF16), pltpu.SemaphoreType.DMA((BEHIND + 1,))]
    scratch += [pltpu.VMEM((1, d, ff), BF16)] * 2 + [pltpu.VMEM((1, ff, d), BF16), pltpu.SemaphoreType.DMA((3,))]
    scratch += [pltpu.VMEM((d, d), F32)] * (1 if last else 3)
    for _ in range(blocks - BEHIND):
        scratch += RingSum.scratch(n, height, d)
    scratch += RingSum.scratch(n, down, d)
    if not last:
        outs += [(pl.BlockSpec((3 * each, d), lambda s: (0, 0)), jax.ShapeDtypeStruct((3 * each, d), BF16))]
        outs += [(anywhere, jax.ShapeDtypeStruct((n, early_rows(n, d), d), BF16))]
        scratch += RingSum.scratch(n, 3 * each, d)
        for _ in sums:
            scratch += RingGather.scratch()
    return _call(
        functools.partial(_mlp_back, n=n, layer=layer, tiles=tiles, blocks=blocks, behind=BEHIND, last=last),
        (2 * tiles + middle,),
        ins,
        outs,
        scratch,
        args,
        2 * t * d * (ff * 8 + d * 4),
        sum(a.size * a.dtype.itemsize for a in args),
        collective=number,
    )


class Parts:
    def __init__(self, n, each):
        self.hosted, self.per, self.each = n - BEHIND, n - BEHIND + 3, each

    def ff(self, layer, block, which):
        at = layer * self.per + self.hosted
        if block < self.hosted:
            return at - self.hosted + block, which * self.each
        entry = (block - self.hosted) * 3 + which
        return (at, 0) if entry == 0 else (at + 1, (entry - 1) * self.each)

    def square(self, layer, which):
        at = layer * self.per + self.hosted
        return (at + 1, (BEHIND * 3 - 1) * self.each) if which == 3 else (at + 2, which * self.each)


def _moments(m, v, g):
    return 0.9 * m + 0.1 * g, 0.95 * v + 0.05 * g * g


def _stepped(w, m, v):
    return (w - 0.02 * (m * lax.rsqrt(v + 1e-8) + 0.1 * w)).astype(BF16)


def _finish(*refs, n, layers, own_count, count):
    take = iter(range(len(refs)))
    some = lambda k: [refs[next(take)] for _ in range(k)]
    a_ref, dq_ref, dk_ref, dv_ref = some(4)
    own_in, w_ref, m_ref, v_ref, far_in = some(own_count), some(7), some(7), some(7), some(3)
    lands, m_s, v_s = some(7), some(7), some(7)
    a_s, dq_s, dk_s, dv_s, g_s, own_ref, squares, total_s, others_s = some(9)
    pieces_s, far_s, far_sem = some(own_count), some(3), some(1)[0]
    load_sem, w_sem, m_sem, v_sem, swap_out, swap_in, out_r, out_l, in_l, in_r, pass_r, pass_l, far_l, far_r = some(14)
    jobs = [RingSum(n, g_s.at[i], *some(4)) for i in range(3)]
    me, right, far, left = _ring(n)
    mesh = pl.DeviceIdType.MESH
    barrier = pltpu.get_barrier_semaphore()
    for other in (right, far, left):
        pl.semaphore_signal(barrier, inc=1, device_id={"dp": other}, device_id_type=mesh)
    pairs = [(a_ref, a_s), (dv_ref, dv_s), (dk_ref, dk_s), (dq_ref, dq_s), *zip(own_in, pieces_s, strict=True)]
    loads = [pltpu.make_async_copy(s, d, load_sem.at[i]) for i, (s, d) in enumerate(pairs)]
    for load in loads:
        load.start()
    top, early = layers - 1, far_s[0].shape[1]
    late = pl.ds(early, lands[6].shape[2] - early)
    pairs = [(w_ref[i].at[:, me], lands[i].at[:, me]) for i in range(6)] + [(w_ref[6].at[i, me], lands[6].at[i, me]) for i in range(top)]
    pairs += [(w_ref[6].at[top, me, late], lands[6].at[top, me, late])]
    pairs += [(w_ref[6].at[top, :, pl.ds(0, early)], lands[6].at[top, :, pl.ds(0, early)])]
    state = [pltpu.make_async_copy(a, b, w_sem.at[i]) for i, (a, b) in enumerate(pairs)]
    for i in range(7):
        state.append(pltpu.make_async_copy(m_ref[i], m_s[i], m_sem.at[i]))
        state.append(pltpu.make_async_copy(v_ref[i], v_s[i], v_sem.at[i]))
    state += [pltpu.make_async_copy(a, b, far_sem.at[i]) for i, (a, b) in enumerate(zip(far_in, far_s, strict=True))]
    each = g_s.shape[2]
    squares[...] = jnp.zeros_like(squares)
    for load in loads[:2]:
        load.wait()
    _cut(g_s.at[2], 0, _dot(a_s[...], dv_s[...], 0, 0))
    pl.semaphore_wait(barrier, 3)
    loads[2].wait()
    jobs[2].start()
    for c in state:
        c.start()
    _cut(g_s.at[1], 0, _dot(a_s[...], dk_s[...], 0, 0))
    loads[3].wait()
    jobs[1].start()
    jobs[2].add()
    _cut(g_s.at[0], 0, _dot(a_s[...], dq_s[...], 0, 0))
    jobs[2].forward()
    jobs[1].add()
    jobs[0].start()
    jobs[1].forward()
    for i, piece in enumerate(pieces_s):
        if i == len(pieces_s) // 2:
            jobs[0].add()
        loads[4 + i].wait()
        _rows_loop(piece.shape[0], lambda rows, piece=piece: _add_squares(squares, piece[rows, :]))
        if i == len(pieces_s) // 2:
            jobs[0].forward()
    jobs[2].finish(own_ref.at[pl.ds(2 * each, each)], squares)
    jobs[1].finish(own_ref.at[pl.ds(each, each)], squares)
    jobs[0].finish(own_ref.at[pl.ds(0, each)], squares)
    total_s[...] = sum(squares[:, i : i + 128] for i in range(0, squares.shape[1], 128))
    swaps = [
        pltpu.make_async_remote_copy(src_ref=total_s, dst_ref=others_s.at[i], send_sem=swap_out.at[i], recv_sem=swap_in.at[i], device_id={"dp": other},
                                     device_id_type=mesh)
        for i, other in enumerate((right, far, left))
    ]
    for c in state:
        c.wait()
    for s in swaps:
        s.start()
    for s in swaps:
        s.wait()
    everything = jnp.sum(total_s[...] + others_s[0] + others_s[1] + others_s[2], keepdims=True)
    factor = jnp.minimum(1.0, 0.5 * lax.rsqrt(everything / count + 1e-30))

    parts = Parts(n, each)
    grads = [*pieces_s[: parts.per - 1], own_ref, *pieces_s[parts.per - 1 :]]
    blocks = n

    def new_weights(i, layer):
        land, m_i, v_i = lands[i], m_s[i], v_s[i]

        def one(at, piece, row, rows, column, g_column, width):
            def body(some):
                here = pl.ds(at + some.start, some.size)
                g = grads[piece][pl.ds(row + some.start, some.size), g_column : g_column + width].astype(F32) * factor
                m, v = _moments(m_i[layer, here, column : column + width], v_i[layer, here, column : column + width], g)
                m_i[layer, here, column : column + width] = m
                v_i[layer, here, column : column + width] = v
                w = land[layer, me, here, column : column + width].astype(F32)
                land[layer, me, here, column : column + width] = _stepped(w, m, v)

            return body

        if i < 4:
            bodies, rows = [one(0, *parts.square(layer, i), each, 0, 0, land.shape[3])], each
        elif i == 6:
            rows = each
            bodies = [one(b * each, *parts.ff(layer, b, 0), each, 0, 0, land.shape[3]) for b in range(blocks)]
        else:
            width, rows = g_s.shape[3] // n, each
            bodies = [
                one(0, *parts.ff(layer, b, i - 3), each, (d * blocks + b) * width, d * width, width) for d in range(n) for b in range(blocks)
            ]

        def run(some):
            for body in bodies:
                body(some)

        _rows_loop(rows, run, 16)

    remote = lambda ref, to, sent, got: pltpu.make_async_remote_copy(
        src_ref=ref, dst_ref=ref, send_sem=sent, recv_sem=got, device_id={"dp": to}, device_id_type=mesh)
    units = [(i, layer) for i in (3, 0, 1, 2, 6, 4, 5) for layer in range(layers)]
    sends, passes = [], []

    def spread(i, layer):
        rows = lands[i].shape[2]
        return (early, rows - early) if (i, layer) == (6, top) else (0, rows)

    for u, (i, layer) in enumerate(units):
        mine = lands[i].at[layer, me, pl.ds(*spread(i, layer))]
        sends.append((remote(mine, right, out_r.at[u], in_l.at[u]), remote(mine, left, out_l.at[u], in_r.at[u])))
    for u in range(len(units) + 1):
        if u < len(units):
            new_weights(*units[u])
        if u > 0:
            for c in sends[u - 1]:
                c.start()
    for other in (right, far, left):

        def theirs(rows, other=other):
            m, v = _moments(far_s[0][other, rows, :], far_s[1][other, rows, :], far_s[2][other, rows, :].astype(F32) * factor)
            lands[6][top, other, rows, :] = _stepped(lands[6][top, other, rows, :].astype(F32), m, v)

        _rows_loop(early, theirs, 16)
    for u, (i, layer) in enumerate(units):
        at, half = spread(i, layer)[0], spread(i, layer)[1] // 2
        sends[u][0].wait_recv()
        one = remote(lands[i].at[layer, left, pl.ds(at, half)], right, pass_r.at[u], far_l.at[u])
        one.start()
        sends[u][1].wait_recv()
        two = remote(lands[i].at[layer, right, pl.ds(at + half, half)], left, pass_l.at[u], far_r.at[u])
        two.start()
        passes.append((one, two))
    for u in range(len(units)):
        for c in passes[u]:
            c.wait_recv()
        for c in (*sends[u], *passes[u]):
            c.wait_send()


def finish(n, number, a, dq, dk, dv, own, w, m, v, far):
    t, d = a.shape
    each, layers = d // n, w[0].shape[0]
    anywhere, here = pl.BlockSpec(memory_space=pltpu.HBM), pl.BlockSpec(memory_space=pltpu.VMEM)
    w = [one.reshape(layers, n, one.shape[1] // n, one.shape[2]) for one in w]
    scratch = [pltpu.VMEM((t, d), BF16)] * 4
    scratch += [pltpu.VMEM((3, n, each, d), BF16), pltpu.VMEM((3 * each, d), BF16), pltpu.VMEM((8, d), F32), pltpu.VMEM((8, 128), F32),
                pltpu.VMEM((3, 8, 128), F32)]
    scratch += [pltpu.VMEM(o.shape, o.dtype) for o in (*own, *far)] + [pltpu.SemaphoreType.DMA((3,))]
    units = 7 * layers
    sem = lambda k: pltpu.SemaphoreType.DMA((k,))
    scratch += [sem(4 + len(own)), sem(7 + layers), sem(7), sem(7), sem(3), sem(3), *[sem(units)] * 8]
    for _ in range(3):
        scratch += RingSum.scratch(n, each, d)
    return _call(
        functools.partial(_finish, n=n, layers=layers, own_count=len(own), count=n * sum(one.size for one in m)),
        (),
        [anywhere] * (4 + len(own) + 24),
        [(here, pltpu.VMEM(one.shape, one.dtype)) for one in (*w, *m, *v)],
        scratch,
        (a, dq, dk, dv, *own, *w, *m, *v, *far),
        6 * t * d * d,
        8 * t * d,
        collective=number,
        vmem=REST,
    )


def _settle(*refs):
    count = len(refs) // 2
    copies = [pltpu.make_async_copy(refs[i], refs[count + i], refs[-1].at[i]) for i in range(count)]
    for c in copies:
        c.start()
    for c in copies:
        c.wait()


def settle(arrays):
    there = pl.BlockSpec(memory_space=pltpu.HBM)
    return _call(
        _settle,
        (),
        [pl.BlockSpec(memory_space=pltpu.VMEM)] * len(arrays),
        [(there, jax.ShapeDtypeStruct(a.shape, a.dtype)) for a in arrays],
        [pltpu.SemaphoreType.DMA((len(arrays),))],
        [pltpu.with_memory_space_constraint(a, pltpu.VMEM) for a in arrays],
        0,
        2 * sum(a.size * a.dtype.itemsize for a in arrays),
        vmem=REST,
    )


NAMES = ("wq", "wk", "wv", "wo", "w_gate", "w_up", "w_down")


def rope_tables(t):
    half = HEAD // 2
    angle = np.arange(t, dtype=np.float32)[:, None] * (np.float32(THETA) ** (-np.arange(half, dtype=np.float32) / half)).astype(np.float32)
    cos, sin = np.cos(angle.astype(np.float64)).astype(np.float32), np.sin(angle.astype(np.float64)).astype(np.float32)
    return jnp.asarray(np.concatenate([cos, cos], 1)), jnp.asarray(np.concatenate([-sin, sin], 1))


def solution(mesh):
    n = mesh.shape["dp"]

    def step(x, dy, *arrays):
        weights = dict(zip(NAMES, arrays[:7], strict=True))
        m, v = arrays[7:14], arrays[14:]
        layers = weights["wq"].shape[0]
        h = x[0]
        rope = rope_tables(h.shape[0])
        made, a, far = forward(n, 0, h, weights, rope, m[6], v[6])
        hs = [h, *(one[6] for one in made[:-1])]
        own = {}
        by, upper, number = dy[0], None, 1
        for layer in reversed(range(layers)):
            if upper is None:
                got = mlp_back(n, number, layer, hs[layer], made[layer][3], by, weights)
            else:
                got = mlp_back(n, number, layer, made[layer][5], made[layer][3], by, weights, upper, made[layer][7:9],
                               own[layer + 1][: n - BEHIND + 1])
                own[layer + 1].append(got[-2])
                far = [*far, got[-1]]
            by, datt, delta, *left = got[:6]
            dq, dk, dv, rest = attend_back(n, number + 1, *made[layer][:3], datt, made[layer][4], delta, rope, *left)
            own[layer] = [*got[6 : 7 + n - BEHIND], rest]
            upper = hs[layer], dq, dk, dv
            number += 2
        pieces = [p for layer in range(layers) for p in own[layer]]
        out = settle(finish(n, number, a, *upper[1:], pieces, arrays[:7], m, v, far))
        return tuple(one.reshape(layers, -1, one.shape[-1]) for one in out)

    states, all_of, cut = P(("rep", "dp"), None, None), P(None, None, None), P(None, "dp", None)
    return jax.shard_map(
        step,
        mesh=mesh,
        in_specs=(states, states) + (all_of,) * 7 + (cut,) * 14,
        out_specs=(P("rep", None, None),) * 7 + (P("rep", "dp", None),) * 14,
        check_vma=False,
    )
```

```python
import functools

import jax
import jax.numpy as jnp
import numpy as np
from jax import lax
from jax.experimental import pallas as pl
from jax.experimental.pallas import tpu as pltpu
from jax.sharding import PartitionSpec as P

F32, BF16 = jnp.float32, jnp.bfloat16
HEAD = 128
THETA = 10000
NEG = -1e30
HIDDEN = 2 * NEG
LOG2E = 1.4426950408889634
SCALE = HEAD**-0.5
VMEM = 67043328
LESS = 55 * 2**20
REST = 30 * 2**20
BEHIND = 2


def _dot(a, b, ca=1, cb=0):
    return lax.dot_general(a, b, (((ca,), (cb,)), ((), ())), preferred_element_type=F32)


def _tile(size, most=512):
    return max(n for n in range(128, most + 1, 128) if size % n == 0)


def in_vmem(shape, dtype):
    return pltpu.VMEM(shape, dtype)


def from_vmem(a):
    return pltpu.with_memory_space_constraint(a, pltpu.VMEM)


HERE = pl.BlockSpec(memory_space=pltpu.VMEM)


def _call(kernel, grid, ins, outs, scratch, args, flops, moved, collective=None, vmem=VMEM):
    return pl.pallas_call(
        kernel,
        grid=grid,
        in_specs=[spec for spec in ins],
        out_specs=[spec for spec, _ in outs],
        out_shape=[shape for _, shape in outs],
        scratch_shapes=scratch,
        compiler_params=pltpu.CompilerParams(dimension_semantics=("arbitrary",) * len(grid), vmem_limit_bytes=vmem, collective_id=collective,
                                             has_side_effects=collective is not None),
        cost_estimate=pl.CostEstimate(flops=int(flops), transcendentals=0, bytes_accessed=int(moved)),
    )(*args)


def _norm_scale(x):
    return lax.rsqrt(jnp.mean(x * x, -1, keepdims=True) + 1e-6)


def _normed(x):
    return (x * _norm_scale(x)).astype(BF16)


def _norm_back(x, d_out):
    s = _norm_scale(x)
    inner = jnp.mean(x * d_out, -1, keepdims=True)
    return s * d_out - x * (s * s * s * inner)


def _turn(x, cos, sin):
    parts = [x[:, n : n + HEAD] for n in range(0, x.shape[1], HEAD)]
    return jnp.concatenate([p * cos + pltpu.roll(p, HEAD // 2, 1) * sin for p in parts], 1)


def _qkv(h, wq, wk, wv, cos, sin):
    a = _normed(h)
    q, k = (_turn(_dot(a, w).astype(BF16).astype(F32), cos, sin).astype(BF16) for w in (wq, wk))
    return a, q, k, _dot(a, wv).astype(BF16)


def _after_attention(h_ref, att_ref, wo):
    return (h_ref[...].astype(F32) + _dot(att_ref[...], wo).astype(BF16).astype(F32)).astype(BF16)


def _ring(n):
    me = lax.axis_index("dp")
    return me, lax.rem(me + 1, n), lax.rem(me + 2, n), lax.rem(me + n - 1, n)


def _greet(n):
    _, right, _, left = _ring(n)
    barrier = pltpu.get_barrier_semaphore()
    for other in (right, left):
        pl.semaphore_signal(barrier, inc=1, device_id={"dp": other}, device_id_type=pl.DeviceIdType.MESH)


def _met():
    pl.semaphore_wait(pltpu.get_barrier_semaphore(), 2)


def _rows_loop(rows, body, most=32):
    each = max(c for c in range(16, most + 1, 16) if rows % c == 0)
    lax.fori_loop(0, rows // each, lambda i, _: body(pl.ds(pl.multiple_of(i * each, each), each)), None)


class RingSum:
    def __init__(self, n, block, passing, arrived, sent, got):
        self.block, self.passing, self.arrived = block, passing, arrived
        self.me, right, far, left = _ring(n)
        self.near = right, left
        half = block.shape[1] // 2
        self.half = half
        a, b = pl.ds(0, half), pl.ds(half, half)
        moves = [
            (block.at[far, a], passing.at[0], right),
            (block.at[far, b], passing.at[1], left),
            (block.at[right, b], arrived.at[0, b], right),
            (block.at[left, a], arrived.at[1, a], left),
            (passing.at[0], arrived.at[0, a], right),
            (passing.at[1], arrived.at[1, b], left),
        ]
        self.copies = [
            pltpu.make_async_remote_copy(src_ref=s, dst_ref=d, send_sem=sent.at[i], recv_sem=got.at[i], device_id={"dp": to},
                                         device_id_type=pl.DeviceIdType.MESH)
            for i, (s, d, to) in enumerate(moves)
        ]

    @staticmethod
    def scratch(n, rows, columns):
        half = pltpu.VMEM((2, rows // 2, columns), BF16)
        return [half, pltpu.VMEM((2, rows, columns), BF16), pltpu.SemaphoreType.DMA((6,)), pltpu.SemaphoreType.DMA((6,))]

    def start(self):
        for c in self.copies[:4]:
            c.start()

    def add(self):
        for c in self.copies[:2]:
            c.wait_recv()
        for i, other in enumerate(self.near):

            def one(rows, i=i, other=other):
                mine = self.block[other, pl.ds(rows.start + i * self.half, rows.size), :]
                self.passing[i, rows, :] = (self.passing[i, rows, :].astype(F32) + mine.astype(F32)).astype(BF16)

            _rows_loop(self.half, one)

    def forward(self):
        for c in self.copies[4:]:
            c.start()

    def finish(self, out, squares=None):
        for c in self.copies[2:]:
            c.wait_recv()

        def one(rows):
            total = self.block[self.me, rows, :].astype(F32) + self.arrived[0, rows, :].astype(F32) + self.arrived[1, rows, :].astype(F32)
            total = total.astype(BF16)
            out[rows, :] = total
            if squares is not None:
                _add_squares(squares, total)

        _rows_loop(self.half * 2, one)
        for c in self.copies:
            c.wait_send()


def _add_squares(squares, value):
    value = value.astype(F32)
    value = value * value
    squares[...] += sum(value[i : i + 8] for i in range(0, value.shape[0], 8))


class RingGather:
    def __init__(self, n, src, place, sent, got):
        me, right, _, left = _ring(n)
        rows = src.shape[0]
        half = rows // 2
        first, second = place(left, 0, half), place(right, half, half)
        moves = [(src, place(me, 0, rows), right), (src, place(me, 0, rows), left), (first, first, right), (second, second, left)]
        self.copies = [
            pltpu.make_async_remote_copy(src_ref=a, dst_ref=b, send_sem=sent.at[i], recv_sem=got.at[i], device_id={"dp": to},
                                         device_id_type=pl.DeviceIdType.MESH)
            for i, (a, b, to) in enumerate(moves)
        ]

    @staticmethod
    def scratch():
        return [pltpu.SemaphoreType.DMA((4,)), pltpu.SemaphoreType.DMA((4,))]

    def start(self):
        for c in self.copies[:2]:
            c.start()

    def forward(self):
        for here, there in zip(self.copies[:2], self.copies[2:], strict=True):
            here.wait_recv()
            there.start()

    def finish(self):
        for c in self.copies[2:]:
            c.wait_recv()
        for c in self.copies:
            c.wait_send()


def _seen(keys, queries):
    return lax.broadcasted_iota(jnp.int32, (keys, queries), 1) >= lax.broadcasted_iota(jnp.int32, (keys, queries), 0)


def diagonal(block, first, size, part=256):
    part = min(part, size)
    for at in range(0, size, part):
        block(first + at, part, at, True)


def _attend(iq, q_ref, k_ref, v_ref, o_ref, lse_ref, top_s, mix_s, bk):
    bq = q_ref.shape[0]
    heads = q_ref.shape[1] // HEAD
    e = SCALE * LOG2E
    top_s[...] = jnp.full(top_s.shape, NEG, F32)
    mix_s[...] = jnp.zeros(mix_s.shape, F32)

    def block(first, keys, at, masked):
        here, ask = pl.ds(pl.multiple_of(first, keys), keys), slice(at, bq)
        cols = [slice(n * HEAD, (n + 1) * HEAD) for n in range(heads)]
        scores = [_dot(k_ref[here, c], q_ref[ask, c], 1, 1) for c in cols]
        weights, keeps = [], []
        seen = _seen(keys, bq - at) if masked else None
        for n, s in enumerate(scores):
            if masked:
                s = jnp.where(seen, s, HIDDEN)
            old = top_s[n : n + 1, ask]
            top = jnp.maximum(old, s.max(axis=0, keepdims=True))
            top_s[n : n + 1, ask] = top
            weights.append(jnp.exp2((s - top) * e).astype(BF16))
            keeps.append(jnp.exp2((old - top) * e))
        ones = jnp.ones((8, keys), BF16)
        for n, (c, p, keep) in enumerate(zip(cols, weights, keeps)):
            values = jnp.concatenate([v_ref[here, c].T, ones], axis=0)
            mix_s[n, :, ask] = mix_s[n, :, ask] * keep + _dot(values, p, 1, 0)

    lax.fori_loop(0, iq * (bq // bk), lambda j, _: block(j * bk, bk, 0, False), None)
    diagonal(block, iq * bq, bq)
    for n in range(heads):
        total = mix_s[n, HEAD : HEAD + 1, :]
        o_ref[:, n * HEAD : (n + 1) * HEAD] = (mix_s[n, :HEAD, :] * (1 / total)).T.astype(BF16)
        lse_ref[n : n + 1, :] = top_s[n : n + 1, :] * e + jnp.log2(total)


def _forward(h_ref, wq, wk, wv, wo, wg_ref, wu_ref, wd_ref, cos, sin, m_ref, v_ref, dy_ref, *refs, n, layers):
    at = 9 * layers - 4
    outs, (a_ref, m_all, v_all), handed, scratch = refs[:at], refs[at : at + 3], refs[at + 3 : at + 7], refs[at + 7 :]
    k_s, v_s, wg, wu, wd, gate_s, up_s, top_s, mix_s, w_sem, out_sem, hand_sem, *sems = scratch
    early = m_all.shape[1]
    gathers = [
        RingGather(n, a.at[layers - 1, pl.ds(0, early)], lambda d, at, rows, b=b: b.at[d, pl.ds(at, rows)], *sems[2 * i : 2 * i + 2])
        for i, (a, b) in enumerate(((m_ref, m_all), (v_ref, v_all)))
    ]
    step = pl.program_id(0)
    bt = h_ref.shape[0]
    rows = pl.ds(pl.multiple_of(step * bt, bt), bt)
    loads = [pltpu.make_async_copy(a.at[0], b.at[0], w_sem.at[i]) for i, (a, b) in enumerate(((wg_ref, wg), (wu_ref, wu), (wd_ref, wd)))]

    sources = (dy_ref, *(a.at[pl.ds(layers - 1, 1)] for a in (wg_ref, wu_ref, wd_ref)))
    hands = [pltpu.make_async_copy(a, b, hand_sem.at[i]) for i, (a, b) in enumerate(zip(sources, handed, strict=True))]

    @pl.when(step == 0)
    def _():
        _greet(n)
        for load in loads:
            load.start()

    @pl.when(step == pl.num_programs(0) - 1)
    def _():
        for c in hands:
            c.start()

    for layer in range(layers):
        q_ref, k_ref, v_ref, att_ref, lse_ref = outs[9 * layer : 9 * layer + 5]
        a, q_ref[...], k, v = _qkv(h_ref[...].astype(F32), wq[layer], wk[layer], wv[layer], cos[...], sin[...])
        if layer == 0:
            a_ref[...] = a
        k_ref[...] = k_s[layer, rows, :] = k
        v_ref[...] = v_s[layer, rows, :] = v
        _attend(step, q_ref, k_s.at[layer], v_s.at[layer], att_ref, lse_ref, top_s, mix_s, bt)
        if layer == layers - 1:
            break
        if layer == 0:

            @pl.when(step == 0)
            def _():
                _met()
                for g in gathers:
                    g.start()

            @pl.when(step == pl.num_programs(0) - 2)
            def _():
                gathers[0].forward()

        h1_ref, y_ref, gate_ref, up_ref = outs[9 * layer + 5 : 9 * layer + 9]
        stores = [
            pltpu.make_async_copy(a.at[j], b.at[j, rows], out_sem.at[layer, i, j])
            for i, (a, b) in enumerate(((gate_s, gate_ref), (up_s, up_ref)))
            for j in range(n)
        ]

        @pl.when(step == 0)
        def _(layer=layer):
            for load in loads:
                load.wait()

        @pl.when(step > 0)
        def _(stores=stores):
            for c in stores:
                c.wait()

        h1 = _after_attention(h_ref, att_ref, wo[layer])
        h1_ref[...] = h1
        h1 = h1.astype(F32)
        b = (h1 * _norm_scale(h1)).astype(BF16)
        total = jnp.zeros(h1.shape, F32)
        for j in range(n):
            gate, up = _dot(b, _strips(wg, j, n, n, 2)), _dot(b, _strips(wu, j, n, n, 2))
            gate_s[j] = gate
            up_s[j] = up
            total += _dot((gate * jax.nn.sigmoid(gate) * up).astype(BF16), _strips(wd, j, n, n, 1))
        for c in stores:
            c.start()
        y_ref[...] = (h1 + total.astype(BF16).astype(F32)).astype(BF16)
        h_ref = y_ref

        @pl.when(step == pl.num_programs(0) - 1)
        def _(stores=stores):
            for c in stores:
                c.wait()

    @pl.when(step == pl.num_programs(0) - 2)
    def _():
        gathers[1].forward()

    @pl.when(step == pl.num_programs(0) - 1)
    def _():
        for g in gathers:
            g.finish()
        for c in hands:
            c.wait()


def anywhere_spec():
    return pl.BlockSpec(memory_space=pltpu.HBM)


def early_rows(n, d):
    return (n - BEHIND + 1) * (d // n)


def forward(n, number, h, weights, rope, m, v, dy):
    t, d = h.shape
    layers, _, ff = weights["w_gate"].shape
    assert layers == 2
    many = (anywhere_spec(), jax.ShapeDtypeStruct((n, early_rows(n, d), d), F32))
    heads = weights["wq"].shape[2] // HEAD
    bt = _tile(t)
    tile, table = (pl.BlockSpec((bt, w), lambda s: (s, 0)) for w in (d, HEAD))
    square = pl.BlockSpec((layers, d, d), lambda s: (0, 0, 0), pipeline_mode=pl.Buffered(1))
    anywhere = pl.BlockSpec(memory_space=pltpu.HBM)
    one = (tile, jax.ShapeDtypeStruct((t, d), BF16))
    two = (anywhere, jax.ShapeDtypeStruct((n, t, ff // n), F32))
    stats = (pl.BlockSpec((heads, bt), lambda s: (0, s)), jax.ShapeDtypeStruct((heads, t), F32))
    upper = [*[one] * 4, stats]
    got = _call(
        functools.partial(_forward, n=n, layers=layers),
        (t // bt,),
        [tile, *[square] * 4, *[anywhere] * 3, table, table, *[anywhere] * 3],
        [*[*upper, one, one, two, two] * (layers - 1), *upper, one, many, many,
         *((HERE, in_vmem(s, BF16)) for s in ((t, d), (1, d, ff), (1, d, ff), (1, ff, d)))],
        [pltpu.VMEM((layers, t, d), BF16)] * 2
        + [pltpu.VMEM((1, d, ff), BF16)] * 2
        + [pltpu.VMEM((1, ff, d), BF16)]
        + [pltpu.VMEM((n, bt, ff // n), F32)] * 2
        + [pltpu.VMEM((heads, bt), F32), pltpu.VMEM((heads, HEAD + 8, bt), F32), pltpu.SemaphoreType.DMA((3,)),
           pltpu.SemaphoreType.DMA((layers, 2, n)), pltpu.SemaphoreType.DMA((4,)), *RingGather.scratch(), *RingGather.scratch()],
        (h, *(weights[name] for name in ("wq", "wk", "wv", "wo")), *(weights[name] for name in ("w_gate", "w_up", "w_down")), *rope, m, v, dy),
        2 * t * d * (8 * d + 3 * ff) + 4 * t * t * d,
        30 * t * d + 8 * t * ff,
        collective=number,
        vmem=LESS,
    )
    return [got[9 * layer : 9 * layer + 9] for layer in range(layers - 1)] + [got[9 * layers - 9 : -7]], got[-7], got[-6:-4], got[-4:]


def _attend_back(q_ref, k_ref, v_ref, do_ref, lse_ref, delta_ref, cos, sin, part_ref, ff_ref, o_ref, dq_ref, dk_ref, dv_ref, own_ref, dq_s, dk_s, dv_s, block_s, load_sem,
                 *ring, bk, n):
    iq = pl.program_id(0)
    bq = q_ref.shape[0]
    heads = q_ref.shape[1] // HEAD
    e = SCALE * LOG2E
    steps = pl.num_programs(0)
    loads, at = [], 0
    for i, source in enumerate((part_ref, *(ff_ref.at[i] for i in range(ff_ref.shape[0])), o_ref)):
        loads.append(pltpu.make_async_copy(source, block_s.at[:, pl.ds(at, source.shape[1])], load_sem.at[i]))
        at += source.shape[1]
    job = RingSum(n, block_s, *ring)

    @pl.when(iq == 0)
    def _():
        _greet(n)
        for load in loads:
            load.start()
        dk_s[...] = jnp.zeros_like(dk_s)
        dv_s[...] = jnp.zeros_like(dv_s)

    @pl.when(iq == 1)
    def _():
        for load in loads:
            load.wait()
        _met()
        job.start()

    @pl.when(iq == steps - 1)
    def _():
        job.forward()

    dq_s[...] = jnp.zeros_like(dq_s)

    def block(first, keys, at, masked):
        here, ask = pl.ds(pl.multiple_of(first, keys), keys), slice(at, bq)
        cols = [slice(i * HEAD, (i + 1) * HEAD) for i in range(heads)]
        scores = [_dot(k_ref[here, c], q_ref[ask, c], 1, 1) for c in cols]
        dps = [_dot(v_ref[here, c], do_ref[ask, c], 1, 1) for c in cols]
        seen = _seen(keys, bq - at) if masked else None
        for i, c in enumerate(cols):
            p = jnp.exp2(scores[i] * e - lse_ref[i : i + 1, ask])
            if masked:
                p = jnp.where(seen, p, 0.0)
            ds = (p * (dps[i] - delta_ref[i : i + 1, ask])).astype(BF16)
            dv_s[here, c] += _dot(p.astype(BF16), do_ref[ask, c], 1, 0)
            dk_s[here, c] += _dot(ds, q_ref[ask, c], 1, 0)
            dq_s[i, :, ask] += _dot(k_ref[here, c].T, ds, 1, 0)

    lax.fori_loop(0, iq * (bq // bk), lambda j, _: block(j * bk, bk, 0, False), None)
    diagonal(block, iq * bq, bq)

    @pl.when(iq == steps - 2)
    def _():
        job.add()

    def back(d, rows):
        return _turn(d.astype(BF16).astype(F32), cos[rows, :], -sin[rows, :]).astype(BF16)

    mine = pl.ds(pl.multiple_of(iq * bq, bq), bq)
    for i in range(heads):
        dq_ref[:, i * HEAD : (i + 1) * HEAD] = back((dq_s[i] * SCALE).T, mine)

    @pl.when(iq == steps - 1)
    def _():
        def one(rows):
            dk_ref[rows, :] = back(dk_s[rows, :] * SCALE, rows)
            dv_ref[rows, :] = dv_s[rows, :].astype(BF16)

        _rows_loop(dk_ref.shape[0], one, 256)
        job.finish(own_ref)


def attend_back(n, number, q, k, v, d_out, lse, delta, rope, part, ff, o):
    t, width = q.shape
    heads = width // HEAD
    bq = bk = _tile(t)
    rows, whole = pl.BlockSpec((bq, width), lambda i: (i, 0)), pl.BlockSpec((t, width), lambda i: (0, 0))
    stats = pl.BlockSpec((heads, bq), lambda i: (0, i))
    table = pl.BlockSpec((t, HEAD), lambda i: (0, 0), pipeline_mode=pl.Buffered(1))
    one = jax.ShapeDtypeStruct((t, width), BF16)
    height, columns = part.shape[1] + ff.shape[0] * ff.shape[2] + o.shape[1], ff.shape[3]
    return _call(
        functools.partial(_attend_back, bk=bk, n=n),
        (t // bq,),
        [rows, whole, whole, rows, stats, stats, table, table, *[pl.BlockSpec(memory_space=pltpu.HBM)] * 3],
        [(rows, one), (whole, one), (whole, one),
         (pl.BlockSpec((height, columns), lambda i: (0, 0)), jax.ShapeDtypeStruct((height, columns), BF16))],
        [pltpu.VMEM((heads, HEAD, bq), F32), pltpu.VMEM((t, width), F32), pltpu.VMEM((t, width), F32),
         pltpu.VMEM((n, height, columns), BF16), pltpu.SemaphoreType.DMA((ff.shape[0] + 2,)),
         *RingSum.scratch(n, height, columns)],
        (q, k, v, d_out, lse, delta, *rope, part, ff, o),
        5 * t * t * width,
        14 * t * width,
        collective=number,
    )


def _strips(ref, block, n, blocks, axis):
    width = ref.shape[axis] // (n * blocks)
    at = [pl.ds(pl.multiple_of((d * blocks + block) * width, width), width) for d in range(n)]
    return jnp.concatenate([ref[0, :, a] if axis == 2 else ref[0, a, :] for a in at], axis - 1)


def _qkv_back(h, dq, dk, dv, wq, wk, wv, sums):
    a = (h * _norm_scale(h)).astype(BF16)
    for s, d in zip(sums, (dq, dk, dv), strict=True):
        s[...] += _dot(a, d, 0, 0)
    return _dot(jnp.concatenate([dq, dk, dv], 1), jnp.concatenate([wq, wk, wv], 1), 1, 1)


def _cut(ref, at, value):
    n = ref.shape[0]
    each = value.shape[0] // n
    for d in range(n):
        ref[d, at : at + each] = value[d * each : (d + 1) * each].astype(BF16)


def _mlp_back(*refs, n, layer, tiles, blocks, behind, last):
    take = iter(range(len(refs)))
    some = lambda count: [refs[next(take)] for _ in range(count)]
    h_ref, att_ref = some(2)
    if not last:
        hn_ref, dq_ref, dk_ref, dv_ref, dh_ref, wq, wk, wv, gate_ref, up_ref = some(10)
        sums_in = some(blocks - behind + 1)
    wo, *from_refs = some(1 if last else 4)
    if last:
        dy_s, wg, wu, wd = some(4)
    dh1_ref, datt_ref, delta_ref, left_part, left_ff, left_o = some(6)
    hosted = blocks - behind
    own = some(hosted + 1 + (not last))
    g_all = None if last else some(1)[0]
    h1_s = some(1)[0] if last else None
    b_s, p_s, dg_s, du_s, sum_b, g_s, go_s, out_sem = some(8)
    if not last:
        dy_s, wg, wu, wd, w_sem = some(5)
    sums3 = some(1 if last else 3)
    sum_o = sums3[0]
    jobs = []
    for i in range(len(own)):
        if i < hosted:
            block = g_s.at[i]
        elif i == hosted:
            block = g_s.at[i, :, pl.ds(0, own[i].shape[0])]
        else:
            block = gqkv_s = g_s.at[blocks - 1]
        jobs.append(RingSum(n, block, *some(4)))
    gathers = []
    if not last:
        for i, source in enumerate(sums_in):
            each = own[hosted].shape[0]
            gathers.append(RingGather(n, source.at[pl.ds(0, each)], lambda d, at, rows, i=i: g_all.at[d, pl.ds(i * each + at, rows)], *some(2)))
    step = pl.program_id(0)
    bt = h_ref.shape[0]
    middle = tiles * blocks
    r = jnp.where(step < tiles, step, lax.rem(step - tiles, tiles))
    j = lax.div(step - tiles, tiles)
    rows = pl.ds(pl.multiple_of(r * bt, bt), bt)
    @pl.when(step == 0)
    def _():
        _greet(n)
        for s in sums3:
            s[...] = jnp.zeros_like(s)

    loads = [] if last else [pltpu.make_async_copy(a.at[layer], b.at[0], w_sem.at[i]) for i, (a, b) in enumerate(zip(from_refs, (wg, wu, wd)))]

    @pl.when(step == 0)
    def _():
        for load in loads:
            load.start()

    @pl.when(step == tiles)
    def _():
        for load in loads:
            load.wait()

    final = 2 * tiles + middle - 1
    times = [(at, min(at + tiles * 3 // 2, tiles + middle)) for at in (tiles * (2 + i) for i in range(hosted + 1))] + [(tiles, 2 * tiles)] * (not last)
    times = [(start, forward - 1, forward, min(forward + tiles * 3 // 2, final)) for start, forward in times]

    @pl.when(step == (min(t[0] for t in times) if last else 1))
    def _():
        _met()
        for g in gathers:
            g.start()

    @pl.when(step == tiles)
    def _():
        for g in gathers:
            g.forward()

    for job, (_, _, at, _) in zip(jobs, times, strict=True):

        @pl.when(step == at)
        def _(job=job):
            job.forward()

    for job, (at, _, _, _) in zip(jobs, times, strict=True):

        @pl.when(step == at)
        def _(job=job):
            job.start()

    @pl.when(step < tiles)
    def _():
        if last:
            h1 = _after_attention(h_ref, att_ref, wo[0])
            h1_s[rows, :] = h1
        else:
            h1 = h_ref[...]
            hn = hn_ref[...].astype(F32)
            da = _qkv_back(hn, dq_ref[...], dk_ref[...], dv_ref[...], wq[0], wk[0], wv[0], sums3)
            dy_s[rows, :] = (dh_ref[...].astype(F32) + _norm_back(hn, da.astype(BF16).astype(F32)).astype(BF16).astype(F32)).astype(BF16)

            @pl.when(step == tiles - 1)
            def _():
                for i, s in enumerate(sums3):
                    _cut(gqkv_s, i * (s.shape[0] // n), s[...])
                sum_o[...] = jnp.zeros_like(sum_o)

        h1 = h1.astype(F32)
        b_s[rows, :] = (h1 * _norm_scale(h1)).astype(BF16)
        sum_b[rows, :] = jnp.zeros((bt, sum_b.shape[1]), F32)

    @pl.when((step >= tiles) & (step < tiles + middle))
    def _():
        b, dy = b_s[rows, :], dy_s[rows, :]
        gate_w, up_w, down_w = _strips(wg, j, n, blocks, 2), _strips(wu, j, n, blocks, 2), _strips(wd, j, n, blocks, 1)
        terms = []
        for at in range(0, gate_w.shape[1], 256):
            c = slice(at, at + 256)
            gate, up = (_dot(b, gate_w[:, c]), _dot(b, up_w[:, c])) if last else (gate_ref[0, :, c], up_ref[0, :, c])
            dp = _dot(dy, down_w[c], 1, 1).astype(BF16).astype(F32)
            sg = jax.nn.sigmoid(gate)
            silu = gate * sg
            p_s[rows, c] = (silu * up).astype(BF16)
            du = (dp * silu).astype(BF16)
            dg = (dp * up * (sg + silu * (1 - sg))).astype(BF16)
            du_s[rows, c] = du
            dg_s[rows, c] = dg
            terms.append((dg, du))
        sum_b[rows, :] += _dot(jnp.concatenate([g for g, _ in terms] + [u for _, u in terms], 1), jnp.concatenate([gate_w, up_w], 1), 1, 1)

        @pl.when(r == tiles - 1)
        def _():
            each = b.shape[1] // n
            mine = g_s.at[j]
            _cut(mine, 0, _dot(p_s[...], dy_s[...], 0, 0))
            _cut(mine, mine.shape[1] - 2 * each, _dot(b_s[...], dg_s[...], 0, 0))
            _cut(mine, mine.shape[1] - each, _dot(b_s[...], du_s[...], 0, 0))

    part = own[hosted].shape[0]
    out_copies = [pltpu.make_async_copy(g_s.at[hosted, :, pl.ds(part, left_part.shape[1])], left_part, out_sem.at[0])]
    out_copies += [pltpu.make_async_copy(g_s.at[hosted + i], left_ff.at[i - 1], out_sem.at[i]) for i in range(1, behind)]
    out_copies.append(pltpu.make_async_copy(go_s, left_o, out_sem.at[behind]))

    @pl.when(step >= tiles + middle)
    def _():
        db = sum_b[rows, :]
        h1 = h1_s[rows, :] if last else h_ref[...]
        dh1 = dy_s[rows, :].astype(F32) + _norm_back(h1.astype(F32), db.astype(BF16).astype(F32)).astype(BF16).astype(F32)
        dh1 = dh1.astype(BF16)
        dh1_ref[...] = dh1
        datt = _dot(dh1, wo[0], 1, 1).astype(BF16)
        datt_ref[...] = datt
        att = att_ref[...]
        both = att.astype(F32) * datt.astype(F32)
        for i in range(both.shape[1] // HEAD):
            delta_ref[i : i + 1, :] = both[:, i * HEAD : (i + 1) * HEAD].T.sum(axis=0, keepdims=True)
        sum_o[...] += _dot(att, dh1, 0, 0)

        @pl.when(step == tiles + middle)
        def _():
            for c in out_copies[:-1]:
                c.start()

        @pl.when(step == 2 * tiles + middle - 1)
        def _():
            _cut(go_s, 0, sum_o[...])
            out_copies[-1].start()
            for c in out_copies:
                c.wait()

    for job, (_, at, _, _) in zip(jobs, times, strict=True):

        @pl.when(step == at)
        def _(job=job):
            job.add()

    @pl.when(step == final)
    def _():
        for g in gathers:
            g.finish()

    for job, (_, _, _, at), out in zip(jobs, times, own, strict=True):

        @pl.when(step == at)
        def _(job=job, out=out):
            job.finish(out)


def mlp_back(n, number, layer, h, att, by, weights, upper=None, hidden=None, sums=None):
    t, d = h.shape
    ff = weights["w_gate"].shape[2]
    bt = _tile(t)
    tiles, blocks = t // bt, n
    fb, each = ff // blocks, d // n
    down = fb // n
    height = down + 2 * each
    assert n == 4 and fb == d and height == 3 * each
    heads = att.shape[1] // HEAD
    middle = tiles * blocks
    r = lambda s: jnp.where(s < tiles, s, lax.rem(s - tiles, tiles))
    j = lambda s: jnp.clip(lax.div(s - tiles, tiles), 0, blocks - 1)
    edge = lambda s: jnp.where(s < tiles, s, jnp.where(s < tiles + middle, tiles - 1, s - tiles - middle))
    before = lambda s: jnp.minimum(s, tiles - 1)
    after = lambda s: jnp.maximum(s - tiles - middle, 0)
    tile = lambda f, w=d: pl.BlockSpec((bt, w), lambda s: (f(s), 0))
    fixed = lambda which, *shape: pl.BlockSpec((1, *shape), lambda s: (which, 0, 0), pipeline_mode=pl.Buffered(1))
    square, up_square = fixed(layer, d, d), fixed(layer + 1, d, d)
    anywhere = pl.BlockSpec(memory_space=pltpu.HBM)
    mlp = [square, anywhere, anywhere, anywhere]
    w4 = [weights[name] for name in ("wo", "w_gate", "w_up", "w_down")]
    last = upper is None
    if last:
        ins = [tile(before), tile(edge), square, *[HERE] * 4]
        args = [h, att, w4[0], *(from_vmem(a) for a in by)]
    else:
        hn, dq, dk, dv = upper
        block = pl.BlockSpec((1, bt, fb), lambda s: (j(s), r(jnp.clip(s, tiles, tiles + middle - 1)), 0))
        ins = [tile(edge), tile(after), *[tile(before)] * 5, up_square, up_square, up_square, block, block, *[anywhere] * len(sums), *mlp]
        args = [h, att, hn, dq, dk, dv, by, weights["wq"], weights["wk"], weights["wv"], *hidden, *sums, *w4]
    anywhere = pl.BlockSpec(memory_space=pltpu.HBM)
    outs = [
        (tile(after), jax.ShapeDtypeStruct((t, d), BF16)),
        (tile(after), jax.ShapeDtypeStruct((t, d), BF16)),
        (pl.BlockSpec((heads, bt), lambda s: (0, after(s))), jax.ShapeDtypeStruct((heads, t), F32)),
        (anywhere, jax.ShapeDtypeStruct((n, height - down, d), BF16)),
        (anywhere, jax.ShapeDtypeStruct((BEHIND - 1, n, height, d), BF16)),
        (anywhere, jax.ShapeDtypeStruct((n, each, d), BF16)),
        *[(pl.BlockSpec((height, d), lambda s: (0, 0)), jax.ShapeDtypeStruct((height, d), BF16))] * (blocks - BEHIND),
        (pl.BlockSpec((down, d), lambda s: (0, 0)), jax.ShapeDtypeStruct((down, d), BF16)),
    ]
    scratch = [pltpu.VMEM((t, d), BF16)] * (1 + last) + [pltpu.VMEM((t, fb), BF16)] * 3 + [pltpu.VMEM((t, d), F32)]
    scratch += [pltpu.VMEM((blocks, n, height, d), BF16), pltpu.VMEM((n, each, d), BF16), pltpu.SemaphoreType.DMA((BEHIND + 1,))]
    if not last:
        scratch += [pltpu.VMEM((t, d), BF16)] + [pltpu.VMEM((1, d, ff), BF16)] * 2 + [pltpu.VMEM((1, ff, d), BF16), pltpu.SemaphoreType.DMA((3,))]
    scratch += [pltpu.VMEM((d, d), F32)] * (1 if last else 3)
    for _ in range(blocks - BEHIND):
        scratch += RingSum.scratch(n, height, d)
    scratch += RingSum.scratch(n, down, d)
    if not last:
        outs += [(pl.BlockSpec((3 * each, d), lambda s: (0, 0)), jax.ShapeDtypeStruct((3 * each, d), BF16))]
        outs += [(anywhere, jax.ShapeDtypeStruct((n, early_rows(n, d), d), BF16))]
        scratch += RingSum.scratch(n, 3 * each, d)
        for _ in sums:
            scratch += RingGather.scratch()
    return _call(
        functools.partial(_mlp_back, n=n, layer=layer, tiles=tiles, blocks=blocks, behind=BEHIND, last=last),
        (2 * tiles + middle,),
        ins,
        outs,
        scratch,
        args,
        2 * t * d * (ff * 8 + d * 4),
        sum(a.size * a.dtype.itemsize for a in args),
        collective=number,
        vmem=LESS if last else VMEM,
    )


class Parts:
    def __init__(self, n, each):
        self.hosted, self.per, self.each = n - BEHIND, n - BEHIND + 3, each

    def ff(self, layer, block, which):
        at = layer * self.per + self.hosted
        if block < self.hosted:
            return at - self.hosted + block, which * self.each
        entry = (block - self.hosted) * 3 + which
        return (at, 0) if entry == 0 else (at + 1, (entry - 1) * self.each)

    def square(self, layer, which):
        at = layer * self.per + self.hosted
        return (at + 1, (BEHIND * 3 - 1) * self.each) if which == 3 else (at + 2, which * self.each)


def _moments(m, v, g):
    return 0.9 * m + 0.1 * g, 0.95 * v + 0.05 * g * g


def _stepped(w, m, v):
    return (w - 0.02 * (m * lax.rsqrt(v + 1e-8) + 0.1 * w)).astype(BF16)


def _finish(*refs, n, layers, own_count, count):
    take = iter(range(len(refs)))
    some = lambda k: [refs[next(take)] for _ in range(k)]
    a_ref, dq_ref, dk_ref, dv_ref = some(4)
    own_in, w_ref, m_ref, v_ref, far_in = some(own_count), some(7), some(7), some(7), some(3)
    lands, m_s, v_s = some(7), some(7), some(7)
    a_s, dq_s, dk_s, dv_s, g_s, own_ref, squares, total_s, others_s = some(9)
    pieces_s, far_s, far_sem = some(own_count), some(3), some(1)[0]
    load_sem, w_sem, m_sem, v_sem, swap_out, swap_in, out_r, out_l, in_l, in_r, pass_r, pass_l, far_l, far_r = some(14)
    jobs = [RingSum(n, g_s.at[i], *some(4)) for i in range(3)]
    me, right, far, left = _ring(n)
    mesh = pl.DeviceIdType.MESH
    barrier = pltpu.get_barrier_semaphore()
    for other in (right, far, left):
        pl.semaphore_signal(barrier, inc=1, device_id={"dp": other}, device_id_type=mesh)
    pairs = [(a_ref, a_s), (dv_ref, dv_s), (dk_ref, dk_s), (dq_ref, dq_s), *zip(own_in, pieces_s, strict=True)]
    loads = [pltpu.make_async_copy(s, d, load_sem.at[i]) for i, (s, d) in enumerate(pairs)]
    for load in loads:
        load.start()
    top, early = layers - 1, far_s[0].shape[1]
    late = pl.ds(early, lands[6].shape[2] - early)
    pairs = [(w_ref[i].at[:, me], lands[i].at[:, me]) for i in range(6)] + [(w_ref[6].at[i, me], lands[6].at[i, me]) for i in range(top)]
    pairs += [(w_ref[6].at[top, me, late], lands[6].at[top, me, late])]
    pairs += [(w_ref[6].at[top, :, pl.ds(0, early)], lands[6].at[top, :, pl.ds(0, early)])]
    state = [pltpu.make_async_copy(a, b, w_sem.at[i]) for i, (a, b) in enumerate(pairs)]
    for i in range(7):
        state.append(pltpu.make_async_copy(m_ref[i], m_s[i], m_sem.at[i]))
        state.append(pltpu.make_async_copy(v_ref[i], v_s[i], v_sem.at[i]))
    state += [pltpu.make_async_copy(a, b, far_sem.at[i]) for i, (a, b) in enumerate(zip(far_in, far_s, strict=True))]
    each = g_s.shape[2]
    squares[...] = jnp.zeros_like(squares)
    for load in loads[:2]:
        load.wait()
    _cut(g_s.at[2], 0, _dot(a_s[...], dv_s[...], 0, 0))
    pl.semaphore_wait(barrier, 3)
    loads[2].wait()
    jobs[2].start()
    for c in state:
        c.start()
    _cut(g_s.at[1], 0, _dot(a_s[...], dk_s[...], 0, 0))
    loads[3].wait()
    jobs[1].start()
    jobs[2].add()
    _cut(g_s.at[0], 0, _dot(a_s[...], dq_s[...], 0, 0))
    jobs[2].forward()
    jobs[1].add()
    jobs[0].start()
    jobs[1].forward()
    for i, piece in enumerate(pieces_s):
        if i == len(pieces_s) // 2:
            jobs[0].add()
        loads[4 + i].wait()
        _rows_loop(piece.shape[0], lambda rows, piece=piece: _add_squares(squares, piece[rows, :]))
        if i == len(pieces_s) // 2:
            jobs[0].forward()
    jobs[2].finish(own_ref.at[pl.ds(2 * each, each)], squares)
    jobs[1].finish(own_ref.at[pl.ds(each, each)], squares)
    jobs[0].finish(own_ref.at[pl.ds(0, each)], squares)
    total_s[...] = sum(squares[:, i : i + 128] for i in range(0, squares.shape[1], 128))
    swaps = [
        pltpu.make_async_remote_copy(src_ref=total_s, dst_ref=others_s.at[i], send_sem=swap_out.at[i], recv_sem=swap_in.at[i], device_id={"dp": other},
                                     device_id_type=mesh)
        for i, other in enumerate((right, far, left))
    ]
    for c in state:
        c.wait()
    for s in swaps:
        s.start()
    for s in swaps:
        s.wait()
    everything = jnp.sum(total_s[...] + others_s[0] + others_s[1] + others_s[2], keepdims=True)
    factor = jnp.minimum(1.0, 0.5 * lax.rsqrt(everything / count + 1e-30))

    parts = Parts(n, each)
    grads = [*pieces_s[: parts.per - 1], own_ref, *pieces_s[parts.per - 1 :]]
    blocks = n

    def new_weights(i, layer):
        land, m_i, v_i = lands[i], m_s[i], v_s[i]

        def one(at, piece, row, rows, column, g_column, width):
            def body(some):
                here = pl.ds(at + some.start, some.size)
                g = grads[piece][pl.ds(row + some.start, some.size), g_column : g_column + width].astype(F32) * factor
                m, v = _moments(m_i[layer, here, column : column + width], v_i[layer, here, column : column + width], g)
                m_i[layer, here, column : column + width] = m
                v_i[layer, here, column : column + width] = v
                w = land[layer, me, here, column : column + width].astype(F32)
                land[layer, me, here, column : column + width] = _stepped(w, m, v)

            return body

        if i < 4:
            bodies, rows = [one(0, *parts.square(layer, i), each, 0, 0, land.shape[3])], each
        elif i == 6:
            rows = each
            bodies = [one(b * each, *parts.ff(layer, b, 0), each, 0, 0, land.shape[3]) for b in range(blocks)]
        else:
            width, rows = g_s.shape[3] // n, each
            bodies = [
                one(0, *parts.ff(layer, b, i - 3), each, (d * blocks + b) * width, d * width, width) for d in range(n) for b in range(blocks)
            ]

        def run(some):
            for body in bodies:
                body(some)

        _rows_loop(rows, run, 16)

    remote = lambda ref, to, sent, got: pltpu.make_async_remote_copy(
        src_ref=ref, dst_ref=ref, send_sem=sent, recv_sem=got, device_id={"dp": to}, device_id_type=mesh)
    units = [(i, layer) for i in (3, 0, 1, 2, 6, 4, 5) for layer in range(layers)]
    sends, passes = [], []

    def spread(i, layer):
        rows = lands[i].shape[2]
        return (early, rows - early) if (i, layer) == (6, top) else (0, rows)

    for u, (i, layer) in enumerate(units):
        mine = lands[i].at[layer, me, pl.ds(*spread(i, layer))]
        sends.append((remote(mine, right, out_r.at[u], in_l.at[u]), remote(mine, left, out_l.at[u], in_r.at[u])))
    for u in range(len(units) + 1):
        if u < len(units):
            new_weights(*units[u])
        if u > 0:
            for c in sends[u - 1]:
                c.start()
    for other in (right, far, left):

        def theirs(rows, other=other):
            m, v = _moments(far_s[0][other, rows, :], far_s[1][other, rows, :], far_s[2][other, rows, :].astype(F32) * factor)
            lands[6][top, other, rows, :] = _stepped(lands[6][top, other, rows, :].astype(F32), m, v)

        _rows_loop(early, theirs, 16)
    for u, (i, layer) in enumerate(units):
        at, half = spread(i, layer)[0], spread(i, layer)[1] // 2
        sends[u][0].wait_recv()
        one = remote(lands[i].at[layer, left, pl.ds(at, half)], right, pass_r.at[u], far_l.at[u])
        one.start()
        sends[u][1].wait_recv()
        two = remote(lands[i].at[layer, right, pl.ds(at + half, half)], left, pass_l.at[u], far_r.at[u])
        two.start()
        passes.append((one, two))
    for u in range(len(units)):
        for c in passes[u]:
            c.wait_recv()
        for c in (*sends[u], *passes[u]):
            c.wait_send()


def finish(n, number, a, dq, dk, dv, own, w, m, v, far):
    t, d = a.shape
    each, layers = d // n, w[0].shape[0]
    anywhere = pl.BlockSpec(memory_space=pltpu.HBM)
    w = [one.reshape(layers, n, one.shape[1] // n, one.shape[2]) for one in w]
    scratch = [pltpu.VMEM((t, d), BF16)] * 4
    scratch += [pltpu.VMEM((3, n, each, d), BF16), pltpu.VMEM((3 * each, d), BF16), pltpu.VMEM((8, d), F32), pltpu.VMEM((8, 128), F32),
                pltpu.VMEM((3, 8, 128), F32)]
    scratch += [pltpu.VMEM(o.shape, o.dtype) for o in (*own, *far)] + [pltpu.SemaphoreType.DMA((3,))]
    units = 7 * layers
    sem = lambda k: pltpu.SemaphoreType.DMA((k,))
    scratch += [sem(4 + len(own)), sem(7 + layers), sem(7), sem(7), sem(3), sem(3), *[sem(units)] * 8]
    for _ in range(3):
        scratch += RingSum.scratch(n, each, d)
    return _call(
        functools.partial(_finish, n=n, layers=layers, own_count=len(own), count=n * sum(one.size for one in m)),
        (),
        [anywhere] * (4 + len(own) + 24),
        [(HERE, in_vmem(one.shape, one.dtype)) for one in (*w, *m, *v)],
        scratch,
        (a, dq, dk, dv, *own, *w, *m, *v, *far),
        6 * t * d * d,
        8 * t * d,
        collective=number,
        vmem=REST,
    )


def _settle(*refs):
    count = len(refs) // 2
    copies = [pltpu.make_async_copy(refs[i], refs[count + i], refs[-1].at[i]) for i in range(count)]
    for c in copies:
        c.start()
    for c in copies:
        c.wait()


def settle(arrays):
    there = pl.BlockSpec(memory_space=pltpu.HBM)
    return _call(
        _settle,
        (),
        [pl.BlockSpec(memory_space=pltpu.VMEM)] * len(arrays),
        [(there, jax.ShapeDtypeStruct(a.shape, a.dtype)) for a in arrays],
        [pltpu.SemaphoreType.DMA((len(arrays),))],
        [from_vmem(a) for a in arrays],
        0,
        2 * sum(a.size * a.dtype.itemsize for a in arrays),
        vmem=REST,
    )


NAMES = ("wq", "wk", "wv", "wo", "w_gate", "w_up", "w_down")


def rope_tables(t):
    half = HEAD // 2
    angle = np.arange(t, dtype=np.float32)[:, None] * (np.float32(THETA) ** (-np.arange(half, dtype=np.float32) / half)).astype(np.float32)
    cos, sin = np.cos(angle.astype(np.float64)).astype(np.float32), np.sin(angle.astype(np.float64)).astype(np.float32)
    return jnp.asarray(np.concatenate([cos, cos], 1)), jnp.asarray(np.concatenate([-sin, sin], 1))


def solution(mesh):
    n = mesh.shape["dp"]

    def step(x, dy, *arrays):
        weights = dict(zip(NAMES, arrays[:7], strict=True))
        m, v = arrays[7:14], arrays[14:]
        layers = weights["wq"].shape[0]
        h = x[0]
        rope = rope_tables(h.shape[0])
        made, a, far, by = forward(n, 0, h, weights, rope, m[6], v[6], dy[0])
        hs = [h, *(one[6] for one in made[:-1])]
        own = {}
        upper, number = None, 1
        for layer in reversed(range(layers)):
            if upper is None:
                got = mlp_back(n, number, layer, hs[layer], made[layer][3], by, weights)
            else:
                got = mlp_back(n, number, layer, made[layer][5], made[layer][3], by, weights, upper, made[layer][7:9],
                               own[layer + 1][: n - BEHIND + 1])
                own[layer + 1].append(got[-2])
                far = [*far, got[-1]]
            by, datt, delta, *left = got[:6]
            dq, dk, dv, rest = attend_back(n, number + 1, *made[layer][:3], datt, made[layer][4], delta, rope, *left)
            own[layer] = [*got[6 : 7 + n - BEHIND], rest]
            upper = hs[layer], dq, dk, dv
            number += 2
        pieces = [p for layer in range(layers) for p in own[layer]]
        out = settle(finish(n, number, a, *upper[1:], pieces, arrays[:7], m, v, far))
        return tuple(one.reshape(layers, -1, one.shape[-1]) for one in out)

    states, all_of, cut = P(("rep", "dp"), None, None), P(None, None, None), P(None, "dp", None)
    return jax.shard_map(
        step,
        mesh=mesh,
        in_specs=(states, states) + (all_of,) * 7 + (cut,) * 14,
        out_specs=(P("rep", None, None),) * 7 + (P("rep", "dp", None),) * 14,
        check_vma=False,
    )
```

```python
import functools

import jax
import jax.numpy as jnp
import numpy as np
from jax import lax
from jax.experimental import pallas as pl
from jax.experimental.pallas import tpu as pltpu
from jax.sharding import PartitionSpec as P

F32, BF16 = jnp.float32, jnp.bfloat16
HEAD = 128
THETA = 10000
NEG = -1e30
HIDDEN = 2 * NEG
LOG2E = 1.4426950408889634
SCALE = HEAD**-0.5
VMEM = 67043328
LESS = 55 * 2**20
REST = 30 * 2**20
BEHIND = 2


def _dot(a, b, ca=1, cb=0):
    return lax.dot_general(a, b, (((ca,), (cb,)), ((), ())), preferred_element_type=F32)


def _tile(size, most=512):
    return max(n for n in range(128, most + 1, 128) if size % n == 0)


def in_vmem(shape, dtype):
    return pltpu.VMEM(shape, dtype)


def from_vmem(a):
    return pltpu.with_memory_space_constraint(a, pltpu.VMEM)


HERE = pl.BlockSpec(memory_space=pltpu.VMEM)


def _call(kernel, grid, ins, outs, scratch, args, flops, moved, collective=None, vmem=VMEM):
    return pl.pallas_call(
        kernel,
        grid=grid,
        in_specs=[spec for spec in ins],
        out_specs=[spec for spec, _ in outs],
        out_shape=[shape for _, shape in outs],
        scratch_shapes=scratch,
        compiler_params=pltpu.CompilerParams(dimension_semantics=("arbitrary",) * len(grid), vmem_limit_bytes=vmem, collective_id=collective,
                                             has_side_effects=collective is not None),
        cost_estimate=pl.CostEstimate(flops=int(flops), transcendentals=0, bytes_accessed=int(moved)),
    )(*args)


def _norm_scale(x):
    return lax.rsqrt(jnp.mean(x * x, -1, keepdims=True) + 1e-6)


def _normed(x):
    return (x * _norm_scale(x)).astype(BF16)


def _norm_back(x, d_out):
    s = _norm_scale(x)
    inner = jnp.mean(x * d_out, -1, keepdims=True)
    return s * d_out - x * (s * s * s * inner)


def _turn(x, table, back=False):
    first = lax.broadcasted_iota(jnp.int32, table.shape, 1) < HEAD // 2
    other = pltpu.roll(table, HEAD // 2, 1)
    cos, sin = jnp.where(first, table, other), jnp.where(first, -other, table)
    sin = -sin if back else sin
    parts = [x[:, n : n + HEAD] for n in range(0, x.shape[1], HEAD)]
    return jnp.concatenate([p * cos + pltpu.roll(p, HEAD // 2, 1) * sin for p in parts], 1)


def _qkv(h, wq, wk, wv, table):
    a = _normed(h)
    q, k = (_turn(_dot(a, w).astype(BF16).astype(F32), table).astype(BF16) for w in (wq, wk))
    return a, q, k, _dot(a, wv).astype(BF16)


def _after_attention(h_ref, att_ref, wo):
    return (h_ref[...].astype(F32) + _dot(att_ref[...], wo).astype(BF16).astype(F32)).astype(BF16)


def _ring(n):
    me = lax.axis_index("dp")
    return me, lax.rem(me + 1, n), lax.rem(me + 2, n), lax.rem(me + n - 1, n)


def _greet(n):
    _, right, _, left = _ring(n)
    barrier = pltpu.get_barrier_semaphore()
    for other in (right, left):
        pl.semaphore_signal(barrier, inc=1, device_id={"dp": other}, device_id_type=pl.DeviceIdType.MESH)


def _met():
    pl.semaphore_wait(pltpu.get_barrier_semaphore(), 2)


def _rows_loop(rows, body, most=32):
    each = max(c for c in range(16, most + 1, 16) if rows % c == 0)
    lax.fori_loop(0, rows // each, lambda i, _: body(pl.ds(pl.multiple_of(i * each, each), each)), None)


def _zero(ref):
    def one(rows):
        ref[rows, :] = jnp.zeros((rows.size, ref.shape[1]), ref.dtype)

    _rows_loop(ref.shape[0], one, 64)


class RingSum:
    def __init__(self, n, block, passing, arrived, sent, got):
        self.block, self.passing, self.arrived = block, passing, arrived
        self.me, right, far, left = _ring(n)
        self.near = right, left
        half = block.shape[1] // 2
        self.half = half
        a, b = pl.ds(0, half), pl.ds(half, half)
        moves = [
            (block.at[far, a], passing.at[0], right),
            (block.at[far, b], passing.at[1], left),
            (block.at[right, b], arrived.at[0, b], right),
            (block.at[left, a], arrived.at[1, a], left),
            (passing.at[0], arrived.at[0, a], right),
            (passing.at[1], arrived.at[1, b], left),
        ]
        self.copies = [
            pltpu.make_async_remote_copy(src_ref=s, dst_ref=d, send_sem=sent.at[i], recv_sem=got.at[i], device_id={"dp": to},
                                         device_id_type=pl.DeviceIdType.MESH)
            for i, (s, d, to) in enumerate(moves)
        ]

    @staticmethod
    def scratch(n, rows, columns):
        half = pltpu.VMEM((2, rows // 2, columns), BF16)
        return [half, pltpu.VMEM((2, rows, columns), BF16), pltpu.SemaphoreType.DMA((6,)), pltpu.SemaphoreType.DMA((6,))]

    def start(self):
        for c in self.copies[:4]:
            c.start()

    def add(self):
        for c in self.copies[:2]:
            c.wait_recv()
        for i, other in enumerate(self.near):

            def one(rows, i=i, other=other):
                mine = self.block[other, pl.ds(rows.start + i * self.half, rows.size), :]
                self.passing[i, rows, :] = (self.passing[i, rows, :].astype(F32) + mine.astype(F32)).astype(BF16)

            _rows_loop(self.half, one)

    def forward(self):
        for c in self.copies[4:]:
            c.start()

    def finish(self, out, squares=None):
        for c in self.copies[2:]:
            c.wait_recv()

        def one(rows):
            total = self.block[self.me, rows, :].astype(F32) + self.arrived[0, rows, :].astype(F32) + self.arrived[1, rows, :].astype(F32)
            total = total.astype(BF16)
            out[rows, :] = total
            if squares is not None:
                _add_squares(squares, total)

        _rows_loop(self.half * 2, one)
        for c in self.copies:
            c.wait_send()


def _add_squares(squares, value):
    value = value.astype(F32)
    value = value * value
    squares[...] += sum(value[i : i + 8] for i in range(0, value.shape[0], 8))


class RingGather:
    def __init__(self, n, src, place, sent, got):
        me, right, _, left = _ring(n)
        rows = src.shape[0]
        half = rows // 2
        first, second = place(left, 0, half), place(right, half, half)
        moves = [(src, place(me, 0, rows), right), (src, place(me, 0, rows), left), (first, first, right), (second, second, left)]
        self.copies = [
            pltpu.make_async_remote_copy(src_ref=a, dst_ref=b, send_sem=sent.at[i], recv_sem=got.at[i], device_id={"dp": to},
                                         device_id_type=pl.DeviceIdType.MESH)
            for i, (a, b, to) in enumerate(moves)
        ]

    @staticmethod
    def scratch():
        return [pltpu.SemaphoreType.DMA((4,)), pltpu.SemaphoreType.DMA((4,))]

    def start(self):
        for c in self.copies[:2]:
            c.start()

    def forward(self):
        for here, there in zip(self.copies[:2], self.copies[2:], strict=True):
            here.wait_recv()
            there.start()

    def finish(self):
        for c in self.copies[2:]:
            c.wait_recv()
        for c in self.copies:
            c.wait_send()


def _seen(keys, queries):
    return lax.broadcasted_iota(jnp.int32, (keys, queries), 1) >= lax.broadcasted_iota(jnp.int32, (keys, queries), 0)


def diagonal(block, first, size, part=256):
    part = min(part, size)
    for at in range(0, size, part):
        block(first + at, part, at, True)


def _attend(iq, q_ref, k_ref, v_ref, o_ref, lse_ref, top_s, mix_s, bk):
    bq = q_ref.shape[0]
    heads = q_ref.shape[1] // HEAD
    e = SCALE * LOG2E
    top_s[...] = jnp.full(top_s.shape, NEG, F32)
    mix_s[...] = jnp.zeros(mix_s.shape, F32)

    def block(first, keys, at, masked):
        here, ask = pl.ds(pl.multiple_of(first, keys), keys), slice(at, bq)
        cols = [slice(n * HEAD, (n + 1) * HEAD) for n in range(heads)]
        scores = [_dot(k_ref[here, c], q_ref[ask, c], 1, 1) for c in cols]
        weights, keeps = [], []
        seen = _seen(keys, bq - at) if masked else None
        for n, s in enumerate(scores):
            if masked:
                s = jnp.where(seen, s, HIDDEN)
            old = top_s[n : n + 1, ask]
            top = jnp.maximum(old, s.max(axis=0, keepdims=True))
            top_s[n : n + 1, ask] = top
            weights.append(jnp.exp2((s - top) * e).astype(BF16))
            keeps.append(jnp.exp2((old - top) * e))
        ones = jnp.ones((8, keys), BF16)
        for n, (c, p, keep) in enumerate(zip(cols, weights, keeps)):
            values = jnp.concatenate([v_ref[here, c].T, ones], axis=0)
            mix_s[n, :, ask] = mix_s[n, :, ask] * keep + _dot(values, p, 1, 0)

    lax.fori_loop(0, iq * (bq // bk), lambda j, _: block(j * bk, bk, 0, False), None)
    diagonal(block, iq * bq, bq)
    for n in range(heads):
        total = mix_s[n, HEAD : HEAD + 1, :]
        o_ref[:, n * HEAD : (n + 1) * HEAD] = (mix_s[n, :HEAD, :] * (1 / total)).T.astype(BF16)
        lse_ref[n : n + 1, :] = top_s[n : n + 1, :] * e + jnp.log2(total)


def _forward(h_ref, wq, wk, wv, wo, wg_ref, wu_ref, wd_ref, table, m_ref, v_ref, dy_ref, *refs, n, layers):
    at = 9 * layers - 4
    outs, (a_ref, m_all, v_all), handed, scratch = refs[:at], refs[at : at + 3], refs[at + 3 : at + 7], refs[at + 7 :]
    k_s, v_s, wg, wu, wd, gate_s, up_s, top_s, mix_s, w_sem, out_sem, hand_sem, *sems = scratch
    early = m_all.shape[1]
    gathers = [
        RingGather(n, a.at[layers - 1, pl.ds(0, early)], lambda d, at, rows, b=b: b.at[d, pl.ds(at, rows)], *sems[2 * i : 2 * i + 2])
        for i, (a, b) in enumerate(((m_ref, m_all), (v_ref, v_all)))
    ]
    step = pl.program_id(0)
    bt = h_ref.shape[0]
    rows = pl.ds(pl.multiple_of(step * bt, bt), bt)
    loads = [pltpu.make_async_copy(a.at[0], b.at[0], w_sem.at[i]) for i, (a, b) in enumerate(((wg_ref, wg), (wu_ref, wu), (wd_ref, wd)))]

    sources = (dy_ref, *(a.at[pl.ds(layers - 1, 1)] for a in (wg_ref, wu_ref, wd_ref)))
    hands = [pltpu.make_async_copy(a, b, hand_sem.at[i]) for i, (a, b) in enumerate(zip(sources, handed, strict=True))]

    @pl.when(step == 0)
    def _():
        _greet(n)
        for load in loads:
            load.start()

    @pl.when(step == pl.num_programs(0) - 1)
    def _():
        for c in hands:
            c.start()

    for layer in range(layers):
        q_ref, k_ref, v_ref, att_ref, lse_ref = outs[9 * layer : 9 * layer + 5]
        a, q_ref[...], k, v = _qkv(h_ref[...].astype(F32), wq[layer], wk[layer], wv[layer], table[...])
        if layer == 0:
            a_ref[...] = a
        k_ref[...] = k_s[layer, rows, :] = k
        v_ref[...] = v_s[layer, rows, :] = v
        _attend(step, q_ref, k_s.at[layer], v_s.at[layer], att_ref, lse_ref, top_s, mix_s, bt)
        if layer == layers - 1:
            break
        if layer == 0:

            @pl.when(step == 0)
            def _():
                _met()
                for g in gathers:
                    g.start()

            @pl.when(step == pl.num_programs(0) - 2)
            def _():
                gathers[0].forward()

        h1_ref, y_ref, gate_ref, up_ref = outs[9 * layer + 5 : 9 * layer + 9]
        stores = [
            pltpu.make_async_copy(a.at[j], b.at[j, rows], out_sem.at[layer, i, j])
            for i, (a, b) in enumerate(((gate_s, gate_ref), (up_s, up_ref)))
            for j in range(n)
        ]

        @pl.when(step == 0)
        def _(layer=layer):
            for load in loads:
                load.wait()

        @pl.when(step > 0)
        def _(stores=stores):
            for c in stores:
                c.wait()

        h1 = _after_attention(h_ref, att_ref, wo[layer])
        h1_ref[...] = h1
        h1 = h1.astype(F32)
        b = (h1 * _norm_scale(h1)).astype(BF16)
        total = jnp.zeros(h1.shape, F32)
        for j in range(n):
            gate, up = _dot(b, _strips(wg, j, n, n, 2)), _dot(b, _strips(wu, j, n, n, 2))
            gate_s[j] = gate
            up_s[j] = up
            total += _dot((gate * jax.nn.sigmoid(gate) * up).astype(BF16), _strips(wd, j, n, n, 1))
        for c in stores:
            c.start()
        y_ref[...] = (h1 + total.astype(BF16).astype(F32)).astype(BF16)
        h_ref = y_ref

        @pl.when(step == pl.num_programs(0) - 1)
        def _(stores=stores):
            for c in stores:
                c.wait()

    @pl.when(step == pl.num_programs(0) - 2)
    def _():
        gathers[1].forward()

    @pl.when(step == pl.num_programs(0) - 1)
    def _():
        for g in gathers:
            g.finish()
        for c in hands:
            c.wait()


def anywhere_spec():
    return pl.BlockSpec(memory_space=pltpu.HBM)


def early_rows(n, d):
    return (n - BEHIND + 1) * (d // n)


def forward(n, number, h, weights, rope, m, v, dy):
    t, d = h.shape
    layers, _, ff = weights["w_gate"].shape
    assert layers == 2
    many = (anywhere_spec(), jax.ShapeDtypeStruct((n, early_rows(n, d), d), F32))
    heads = weights["wq"].shape[2] // HEAD
    bt = _tile(t)
    tile, table = (pl.BlockSpec((bt, w), lambda s: (s, 0)) for w in (d, HEAD))
    square = pl.BlockSpec((layers, d, d), lambda s: (0, 0, 0), pipeline_mode=pl.Buffered(1))
    anywhere = pl.BlockSpec(memory_space=pltpu.HBM)
    one = (tile, jax.ShapeDtypeStruct((t, d), BF16))
    two = (anywhere, jax.ShapeDtypeStruct((n, t, ff // n), F32))
    stats = (pl.BlockSpec((heads, bt), lambda s: (0, s)), jax.ShapeDtypeStruct((heads, t), F32))
    upper = [*[one] * 4, stats]
    got = _call(
        functools.partial(_forward, n=n, layers=layers),
        (t // bt,),
        [tile, *[square] * 4, *[anywhere] * 3, table, *[anywhere] * 3],
        [*[*upper, one, one, two, two] * (layers - 1), *upper, one, many, many,
         *((HERE, in_vmem(s, BF16)) for s in ((t, d), (1, d, ff), (1, d, ff), (1, ff, d)))],
        [pltpu.VMEM((layers, t, d), BF16)] * 2
        + [pltpu.VMEM((1, d, ff), BF16)] * 2
        + [pltpu.VMEM((1, ff, d), BF16)]
        + [pltpu.VMEM((n, bt, ff // n), F32)] * 2
        + [pltpu.VMEM((heads, bt), F32), pltpu.VMEM((heads, HEAD + 8, bt), F32), pltpu.SemaphoreType.DMA((3,)),
           pltpu.SemaphoreType.DMA((layers, 2, n)), pltpu.SemaphoreType.DMA((4,)), *RingGather.scratch(), *RingGather.scratch()],
        (h, *(weights[name] for name in ("wq", "wk", "wv", "wo")), *(weights[name] for name in ("w_gate", "w_up", "w_down")), rope, m, v, dy),
        2 * t * d * (8 * d + 3 * ff) + 4 * t * t * d,
        30 * t * d + 8 * t * ff,
        collective=number,
        vmem=LESS,
    )
    return [got[9 * layer : 9 * layer + 9] for layer in range(layers - 1)] + [got[9 * layers - 9 : -7]], got[-7], got[-6:-4], got[-4:]


def _attend_back(q_ref, k_ref, v_ref, do_ref, lse_ref, delta_ref, table, part_ref, ff_ref, o_ref, dq_ref, dk_ref, dv_ref, own_ref, dq_s, dk_s, dv_s, block_s, load_sem,
                 *ring, bk, n):
    iq = pl.program_id(0)
    bq = q_ref.shape[0]
    heads = q_ref.shape[1] // HEAD
    e = SCALE * LOG2E
    steps = pl.num_programs(0)
    loads, at = [], 0
    for i, source in enumerate((part_ref, *(ff_ref.at[i] for i in range(ff_ref.shape[0])), o_ref)):
        loads.append(pltpu.make_async_copy(source, block_s.at[:, pl.ds(at, source.shape[1])], load_sem.at[i]))
        at += source.shape[1]
    job = RingSum(n, block_s, *ring)

    @pl.when(iq == 0)
    def _():
        _greet(n)
        for load in loads:
            load.start()
        _zero(dk_s)
        _zero(dv_s)

    @pl.when(iq == 1)
    def _():
        for load in loads:
            load.wait()
        _met()
        job.start()

    @pl.when(iq == steps - 1)
    def _():
        job.forward()

    dq_s[...] = jnp.zeros_like(dq_s)

    def block(first, keys, at, masked):
        here, ask = pl.ds(pl.multiple_of(first, keys), keys), slice(at, bq)
        cols = [slice(i * HEAD, (i + 1) * HEAD) for i in range(heads)]
        scores = [_dot(k_ref[here, c], q_ref[ask, c], 1, 1) for c in cols]
        dps = [_dot(v_ref[here, c], do_ref[ask, c], 1, 1) for c in cols]
        seen = _seen(keys, bq - at) if masked else None
        for i, c in enumerate(cols):
            p = jnp.exp2(scores[i] * e - lse_ref[i : i + 1, ask])
            if masked:
                p = jnp.where(seen, p, 0.0)
            ds = (p * (dps[i] - delta_ref[i : i + 1, ask])).astype(BF16)
            dv_s[here, c] += _dot(p.astype(BF16), do_ref[ask, c], 1, 0)
            dk_s[here, c] += _dot(ds, q_ref[ask, c], 1, 0)
            dq_s[i, :, ask] += _dot(k_ref[here, c].T, ds, 1, 0)

    lax.fori_loop(0, iq * (bq // bk), lambda j, _: block(j * bk, bk, 0, False), None)
    diagonal(block, iq * bq, bq)

    @pl.when(iq == steps - 2)
    def _():
        job.add()

    def back(d, rows):
        return _turn(d.astype(BF16).astype(F32), table[rows, :], back=True).astype(BF16)

    mine = pl.ds(pl.multiple_of(iq * bq, bq), bq)
    for i in range(heads):
        dq_ref[:, i * HEAD : (i + 1) * HEAD] = back((dq_s[i] * SCALE).T, mine)

    @pl.when(iq == steps - 1)
    def _():
        def one(rows):
            dk_ref[rows, :] = back(dk_s[rows, :] * SCALE, rows)
            dv_ref[rows, :] = dv_s[rows, :].astype(BF16)

        _rows_loop(dk_ref.shape[0], one, 256)
        job.finish(own_ref)


def attend_back(n, number, q, k, v, d_out, lse, delta, rope, part, ff, o):
    t, width = q.shape
    heads = width // HEAD
    bq = bk = _tile(t)
    rows, whole = pl.BlockSpec((bq, width), lambda i: (i, 0)), pl.BlockSpec((t, width), lambda i: (0, 0))
    stats = pl.BlockSpec((heads, bq), lambda i: (0, i))
    table = pl.BlockSpec((t, HEAD), lambda i: (0, 0), pipeline_mode=pl.Buffered(1))
    one = jax.ShapeDtypeStruct((t, width), BF16)
    height, columns = part.shape[1] + ff.shape[0] * ff.shape[2] + o.shape[1], ff.shape[3]
    return _call(
        functools.partial(_attend_back, bk=bk, n=n),
        (t // bq,),
        [rows, whole, whole, rows, stats, stats, table, *[pl.BlockSpec(memory_space=pltpu.HBM)] * 3],
        [(rows, one), (whole, one), (whole, one),
         (pl.BlockSpec((height, columns), lambda i: (0, 0)), jax.ShapeDtypeStruct((height, columns), BF16))],
        [pltpu.VMEM((heads, HEAD, bq), F32), pltpu.VMEM((t, width), F32), pltpu.VMEM((t, width), F32),
         pltpu.VMEM((n, height, columns), BF16), pltpu.SemaphoreType.DMA((ff.shape[0] + 2,)),
         *RingSum.scratch(n, height, columns)],
        (q, k, v, d_out, lse, delta, rope, part, ff, o),
        5 * t * t * width,
        14 * t * width,
        collective=number,
    )


def _strips(ref, block, n, blocks, axis):
    width = ref.shape[axis] // (n * blocks)
    at = [pl.ds(pl.multiple_of((d * blocks + block) * width, width), width) for d in range(n)]
    return jnp.concatenate([ref[0, :, a] if axis == 2 else ref[0, a, :] for a in at], axis - 1)


def _qkv_back(h, dq, dk, dv, wq, wk, wv, sums):
    a = (h * _norm_scale(h)).astype(BF16)
    for s, d in zip(sums, (dq, dk, dv), strict=True):
        s[...] += _dot(a, d, 0, 0)
    return _dot(jnp.concatenate([dq, dk, dv], 1), jnp.concatenate([wq, wk, wv], 1), 1, 1)


def _cut(ref, at, value):
    n = ref.shape[0]
    each = value.shape[0] // n
    for d in range(n):
        ref[d, at : at + each] = value[d * each : (d + 1) * each].astype(BF16)


def _mlp_back(*refs, n, layer, tiles, blocks, behind, last):
    take = iter(range(len(refs)))
    some = lambda count: [refs[next(take)] for _ in range(count)]
    h_ref, att_ref = some(2)
    if not last:
        hn_ref, dq_ref, dk_ref, dv_ref, dh_ref, wq, wk, wv, gate_ref, up_ref = some(10)
        sums_in = some(blocks - behind + 1)
    wo, *from_refs = some(1 if last else 4)
    if last:
        dy_s, wg, wu, wd = some(4)
    dh1_ref, datt_ref, delta_ref, left_part, left_ff, left_o = some(6)
    hosted = blocks - behind
    own = some(hosted + 1 + (not last))
    g_all = None if last else some(1)[0]
    h1_s = some(1)[0] if last else None
    b_s, p_s, dg_s, du_s, sum_b, g_s, go_s, out_sem = some(8)
    if not last:
        dy_s, wg, wu, wd, w_sem = some(5)
    sums3 = some(1 if last else 3)
    sum_o = sums3[0]
    jobs = []
    for i in range(len(own)):
        if i < hosted:
            block = g_s.at[i]
        elif i == hosted:
            block = g_s.at[i, :, pl.ds(0, own[i].shape[0])]
        else:
            block = gqkv_s = g_s.at[blocks - 1]
        jobs.append(RingSum(n, block, *some(4)))
    gathers = []
    if not last:
        for i, source in enumerate(sums_in):
            each = own[hosted].shape[0]
            gathers.append(RingGather(n, source.at[pl.ds(0, each)], lambda d, at, rows, i=i: g_all.at[d, pl.ds(i * each + at, rows)], *some(2)))
    step = pl.program_id(0)
    bt = h_ref.shape[0]
    middle = tiles * blocks
    r = jnp.where(step < tiles, step, lax.rem(step - tiles, tiles))
    j = lax.div(step - tiles, tiles)
    rows = pl.ds(pl.multiple_of(r * bt, bt), bt)
    @pl.when(step == 0)
    def _():
        _greet(n)
        for s in sums3:
            _zero(s)

    loads = [] if last else [pltpu.make_async_copy(a.at[layer], b.at[0], w_sem.at[i]) for i, (a, b) in enumerate(zip(from_refs, (wg, wu, wd)))]

    @pl.when(step == 0)
    def _():
        for load in loads:
            load.start()

    @pl.when(step == tiles)
    def _():
        for load in loads:
            load.wait()

    final = 2 * tiles + middle - 1
    times = [(at, min(at + tiles * 3 // 2, tiles + middle)) for at in (tiles * (2 + i) for i in range(hosted + 1))] + [(tiles, 2 * tiles)] * (not last)
    times = [(start, forward - 1, forward, min(forward + tiles * 3 // 2, final)) for start, forward in times]

    @pl.when(step == (min(t[0] for t in times) if last else 1))
    def _():
        _met()
        for g in gathers:
            g.start()

    @pl.when(step == tiles)
    def _():
        for g in gathers:
            g.forward()

    for job, (_, _, at, _) in zip(jobs, times, strict=True):

        @pl.when(step == at)
        def _(job=job):
            job.forward()

    for job, (at, _, _, _) in zip(jobs, times, strict=True):

        @pl.when(step == at)
        def _(job=job):
            job.start()

    @pl.when(step < tiles)
    def _():
        if last:
            h1 = _after_attention(h_ref, att_ref, wo[0])
            h1_s[rows, :] = h1
        else:
            h1 = h_ref[...]
            hn = hn_ref[...].astype(F32)
            da = _qkv_back(hn, dq_ref[...], dk_ref[...], dv_ref[...], wq[0], wk[0], wv[0], sums3)
            dy_s[rows, :] = (dh_ref[...].astype(F32) + _norm_back(hn, da.astype(BF16).astype(F32)).astype(BF16).astype(F32)).astype(BF16)

            @pl.when(step == tiles - 1)
            def _():
                for i, s in enumerate(sums3):
                    _cut(gqkv_s, i * (s.shape[0] // n), s[...])
                _zero(sum_o)

        h1 = h1.astype(F32)
        b_s[rows, :] = (h1 * _norm_scale(h1)).astype(BF16)
        sum_b[rows, :] = jnp.zeros((bt, sum_b.shape[1]), F32)

    @pl.when((step >= tiles) & (step < tiles + middle))
    def _():
        b, dy = b_s[rows, :], dy_s[rows, :]
        gate_w, up_w, down_w = _strips(wg, j, n, blocks, 2), _strips(wu, j, n, blocks, 2), _strips(wd, j, n, blocks, 1)
        terms = []
        for at in range(0, gate_w.shape[1], 256):
            c = slice(at, at + 256)
            gate, up = (_dot(b, gate_w[:, c]), _dot(b, up_w[:, c])) if last else (gate_ref[0, :, c], up_ref[0, :, c])
            dp = _dot(dy, down_w[c], 1, 1).astype(BF16).astype(F32)
            sg = jax.nn.sigmoid(gate)
            silu = gate * sg
            p_s[rows, c] = (silu * up).astype(BF16)
            du = (dp * silu).astype(BF16)
            dg = (dp * up * (sg + silu * (1 - sg))).astype(BF16)
            du_s[rows, c] = du
            dg_s[rows, c] = dg
            terms.append((dg, du))
        sum_b[rows, :] += _dot(jnp.concatenate([g for g, _ in terms] + [u for _, u in terms], 1), jnp.concatenate([gate_w, up_w], 1), 1, 1)

        @pl.when(r == tiles - 1)
        def _():
            each = b.shape[1] // n
            mine = g_s.at[j]
            _cut(mine, 0, _dot(p_s[...], dy_s[...], 0, 0))
            _cut(mine, mine.shape[1] - 2 * each, _dot(b_s[...], dg_s[...], 0, 0))
            _cut(mine, mine.shape[1] - each, _dot(b_s[...], du_s[...], 0, 0))

    part = own[hosted].shape[0]
    out_copies = [pltpu.make_async_copy(g_s.at[hosted, :, pl.ds(part, left_part.shape[1])], left_part, out_sem.at[0])]
    out_copies += [pltpu.make_async_copy(g_s.at[hosted + i], left_ff.at[i - 1], out_sem.at[i]) for i in range(1, behind)]
    out_copies.append(pltpu.make_async_copy(go_s, left_o, out_sem.at[behind]))

    @pl.when(step >= tiles + middle)
    def _():
        db = sum_b[rows, :]
        h1 = h1_s[rows, :] if last else h_ref[...]
        dh1 = dy_s[rows, :].astype(F32) + _norm_back(h1.astype(F32), db.astype(BF16).astype(F32)).astype(BF16).astype(F32)
        dh1 = dh1.astype(BF16)
        dh1_ref[...] = dh1
        datt = _dot(dh1, wo[0], 1, 1).astype(BF16)
        datt_ref[...] = datt
        att = att_ref[...]
        both = att.astype(F32) * datt.astype(F32)
        for i in range(both.shape[1] // HEAD):
            delta_ref[i : i + 1, :] = both[:, i * HEAD : (i + 1) * HEAD].T.sum(axis=0, keepdims=True)
        sum_o[...] += _dot(att, dh1, 0, 0)

        @pl.when(step == tiles + middle)
        def _():
            for c in out_copies[:-1]:
                c.start()

        @pl.when(step == 2 * tiles + middle - 1)
        def _():
            _cut(go_s, 0, sum_o[...])
            out_copies[-1].start()
            for c in out_copies:
                c.wait()

    for job, (_, at, _, _) in zip(jobs, times, strict=True):

        @pl.when(step == at)
        def _(job=job):
            job.add()

    @pl.when(step == final)
    def _():
        for g in gathers:
            g.finish()

    for job, (_, _, _, at), out in zip(jobs, times, own, strict=True):

        @pl.when(step == at)
        def _(job=job, out=out):
            job.finish(out)


def mlp_back(n, number, layer, h, att, by, weights, upper=None, hidden=None, sums=None):
    t, d = h.shape
    ff = weights["w_gate"].shape[2]
    bt = _tile(t)
    tiles, blocks = t // bt, n
    fb, each = ff // blocks, d // n
    down = fb // n
    height = down + 2 * each
    assert n == 4 and fb == d and height == 3 * each
    heads = att.shape[1] // HEAD
    middle = tiles * blocks
    r = lambda s: jnp.where(s < tiles, s, lax.rem(s - tiles, tiles))
    j = lambda s: jnp.clip(lax.div(s - tiles, tiles), 0, blocks - 1)
    edge = lambda s: jnp.where(s < tiles, s, jnp.where(s < tiles + middle, tiles - 1, s - tiles - middle))
    before = lambda s: jnp.minimum(s, tiles - 1)
    after = lambda s: jnp.maximum(s - tiles - middle, 0)
    tile = lambda f, w=d: pl.BlockSpec((bt, w), lambda s: (f(s), 0))
    fixed = lambda which, *shape: pl.BlockSpec((1, *shape), lambda s: (which, 0, 0), pipeline_mode=pl.Buffered(1))
    square, up_square = fixed(layer, d, d), fixed(layer + 1, d, d)
    anywhere = pl.BlockSpec(memory_space=pltpu.HBM)
    mlp = [square, anywhere, anywhere, anywhere]
    w4 = [weights[name] for name in ("wo", "w_gate", "w_up", "w_down")]
    last = upper is None
    if last:
        ins = [tile(before), tile(edge), square, *[HERE] * 4]
        args = [h, att, w4[0], *(from_vmem(a) for a in by)]
    else:
        hn, dq, dk, dv = upper
        block = pl.BlockSpec((1, bt, fb), lambda s: (j(s), r(jnp.clip(s, tiles, tiles + middle - 1)), 0))
        ins = [tile(edge), tile(after), *[tile(before)] * 5, up_square, up_square, up_square, block, block, *[anywhere] * len(sums), *mlp]
        args = [h, att, hn, dq, dk, dv, by, weights["wq"], weights["wk"], weights["wv"], *hidden, *sums, *w4]
    anywhere = pl.BlockSpec(memory_space=pltpu.HBM)
    outs = [
        (tile(after), jax.ShapeDtypeStruct((t, d), BF16)),
        (tile(after), jax.ShapeDtypeStruct((t, d), BF16)),
        (pl.BlockSpec((heads, bt), lambda s: (0, after(s))), jax.ShapeDtypeStruct((heads, t), F32)),
        (anywhere, jax.ShapeDtypeStruct((n, height - down, d), BF16)),
        (anywhere, jax.ShapeDtypeStruct((BEHIND - 1, n, height, d), BF16)),
        (anywhere, jax.ShapeDtypeStruct((n, each, d), BF16)),
        *[(pl.BlockSpec((height, d), lambda s: (0, 0)), jax.ShapeDtypeStruct((height, d), BF16))] * (blocks - BEHIND),
        (pl.BlockSpec((down, d), lambda s: (0, 0)), jax.ShapeDtypeStruct((down, d), BF16)),
    ]
    scratch = [pltpu.VMEM((t, d), BF16)] * (1 + last) + [pltpu.VMEM((t, fb), BF16)] * 3 + [pltpu.VMEM((t, d), F32)]
    scratch += [pltpu.VMEM((blocks, n, height, d), BF16), pltpu.VMEM((n, each, d), BF16), pltpu.SemaphoreType.DMA((BEHIND + 1,))]
    if not last:
        scratch += [pltpu.VMEM((t, d), BF16)] + [pltpu.VMEM((1, d, ff), BF16)] * 2 + [pltpu.VMEM((1, ff, d), BF16), pltpu.SemaphoreType.DMA((3,))]
    scratch += [pltpu.VMEM((d, d), F32)] * (1 if last else 3)
    for _ in range(blocks - BEHIND):
        scratch += RingSum.scratch(n, height, d)
    scratch += RingSum.scratch(n, down, d)
    if not last:
        outs += [(pl.BlockSpec((3 * each, d), lambda s: (0, 0)), jax.ShapeDtypeStruct((3 * each, d), BF16))]
        outs += [(anywhere, jax.ShapeDtypeStruct((n, early_rows(n, d), d), BF16))]
        scratch += RingSum.scratch(n, 3 * each, d)
        for _ in sums:
            scratch += RingGather.scratch()
    return _call(
        functools.partial(_mlp_back, n=n, layer=layer, tiles=tiles, blocks=blocks, behind=BEHIND, last=last),
        (2 * tiles + middle,),
        ins,
        outs,
        scratch,
        args,
        2 * t * d * (ff * 8 + d * 4),
        sum(a.size * a.dtype.itemsize for a in args),
        collective=number,
        vmem=LESS if last else VMEM,
    )


class Parts:
    def __init__(self, n, each):
        self.hosted, self.per, self.each = n - BEHIND, n - BEHIND + 3, each

    def ff(self, layer, block, which):
        at = layer * self.per + self.hosted
        if block < self.hosted:
            return at - self.hosted + block, which * self.each
        entry = (block - self.hosted) * 3 + which
        return (at, 0) if entry == 0 else (at + 1, (entry - 1) * self.each)

    def square(self, layer, which):
        at = layer * self.per + self.hosted
        return (at + 1, (BEHIND * 3 - 1) * self.each) if which == 3 else (at + 2, which * self.each)


def _moments(m, v, g):
    return 0.9 * m + 0.1 * g, 0.95 * v + 0.05 * g * g


def _stepped(w, m, v):
    return (w - 0.02 * (m * lax.rsqrt(v + 1e-8) + 0.1 * w)).astype(BF16)


def _finish(*refs, n, layers, own_count, count):
    take = iter(range(len(refs)))
    some = lambda k: [refs[next(take)] for _ in range(k)]
    a_ref, dq_ref, dk_ref, dv_ref = some(4)
    own_in, w_ref, m_ref, v_ref, far_in = some(own_count), some(7), some(7), some(7), some(3)
    lands, m_s, v_s = some(7), some(7), some(7)
    a_s, dq_s, dk_s, dv_s, g_s, own_ref, squares, total_s, others_s = some(9)
    pieces_s, far_s, far_sem = some(own_count), some(3), some(1)[0]
    load_sem, w_sem, m_sem, v_sem, swap_out, swap_in, out_r, out_l, in_l, in_r, pass_r, pass_l, far_l, far_r = some(14)
    jobs = [RingSum(n, g_s.at[i], *some(4)) for i in range(3)]
    me, right, far, left = _ring(n)
    mesh = pl.DeviceIdType.MESH
    barrier = pltpu.get_barrier_semaphore()
    for other in (right, far, left):
        pl.semaphore_signal(barrier, inc=1, device_id={"dp": other}, device_id_type=mesh)
    pairs = [(a_ref, a_s), (dv_ref, dv_s), (dk_ref, dk_s), (dq_ref, dq_s), *zip(own_in, pieces_s, strict=True)]
    loads = [pltpu.make_async_copy(s, d, load_sem.at[i]) for i, (s, d) in enumerate(pairs)]
    for load in loads:
        load.start()
    top, early = layers - 1, far_s[0].shape[1]
    late = pl.ds(early, lands[6].shape[2] - early)
    pairs = [(w_ref[i].at[:, me], lands[i].at[:, me]) for i in range(6)] + [(w_ref[6].at[i, me], lands[6].at[i, me]) for i in range(top)]
    pairs += [(w_ref[6].at[top, me, late], lands[6].at[top, me, late])]
    pairs += [(w_ref[6].at[top, :, pl.ds(0, early)], lands[6].at[top, :, pl.ds(0, early)])]
    state = [pltpu.make_async_copy(a, b, w_sem.at[i]) for i, (a, b) in enumerate(pairs)]
    for i in range(7):
        state.append(pltpu.make_async_copy(m_ref[i], m_s[i], m_sem.at[i]))
        state.append(pltpu.make_async_copy(v_ref[i], v_s[i], v_sem.at[i]))
    state += [pltpu.make_async_copy(a, b, far_sem.at[i]) for i, (a, b) in enumerate(zip(far_in, far_s, strict=True))]
    each = g_s.shape[2]
    squares[...] = jnp.zeros_like(squares)
    for load in loads[:2]:
        load.wait()
    _cut(g_s.at[2], 0, _dot(a_s[...], dv_s[...], 0, 0))
    pl.semaphore_wait(barrier, 3)
    loads[2].wait()
    jobs[2].start()
    for c in state:
        c.start()
    _cut(g_s.at[1], 0, _dot(a_s[...], dk_s[...], 0, 0))
    loads[3].wait()
    jobs[1].start()
    jobs[2].add()
    _cut(g_s.at[0], 0, _dot(a_s[...], dq_s[...], 0, 0))
    jobs[2].forward()
    jobs[1].add()
    jobs[0].start()
    jobs[1].forward()
    for i, piece in enumerate(pieces_s):
        if i == len(pieces_s) // 2:
            jobs[0].add()
        loads[4 + i].wait()
        _rows_loop(piece.shape[0], lambda rows, piece=piece: _add_squares(squares, piece[rows, :]))
        if i == len(pieces_s) // 2:
            jobs[0].forward()
    jobs[2].finish(own_ref.at[pl.ds(2 * each, each)], squares)
    jobs[1].finish(own_ref.at[pl.ds(each, each)], squares)
    jobs[0].finish(own_ref.at[pl.ds(0, each)], squares)
    total_s[...] = sum(squares[:, i : i + 128] for i in range(0, squares.shape[1], 128))
    swaps = [
        pltpu.make_async_remote_copy(src_ref=total_s, dst_ref=others_s.at[i], send_sem=swap_out.at[i], recv_sem=swap_in.at[i], device_id={"dp": other},
                                     device_id_type=mesh)
        for i, other in enumerate((right, far, left))
    ]
    for c in state:
        c.wait()
    for s in swaps:
        s.start()
    for s in swaps:
        s.wait()
    everything = jnp.sum(total_s[...] + others_s[0] + others_s[1] + others_s[2], keepdims=True)
    factor = jnp.minimum(1.0, 0.5 * lax.rsqrt(everything / count + 1e-30))

    parts = Parts(n, each)
    grads = [*pieces_s[: parts.per - 1], own_ref, *pieces_s[parts.per - 1 :]]
    blocks = n

    def new_weights(i, layer):
        land, m_i, v_i = lands[i], m_s[i], v_s[i]

        def one(at, piece, row, rows, column, g_column, width):
            def body(some):
                here = pl.ds(at + some.start, some.size)
                g = grads[piece][pl.ds(row + some.start, some.size), g_column : g_column + width].astype(F32) * factor
                m, v = _moments(m_i[layer, here, column : column + width], v_i[layer, here, column : column + width], g)
                m_i[layer, here, column : column + width] = m
                v_i[layer, here, column : column + width] = v
                w = land[layer, me, here, column : column + width].astype(F32)
                land[layer, me, here, column : column + width] = _stepped(w, m, v)

            return body

        if i < 4:
            bodies, rows = [one(0, *parts.square(layer, i), each, 0, 0, land.shape[3])], each
        elif i == 6:
            rows = each
            bodies = [one(b * each, *parts.ff(layer, b, 0), each, 0, 0, land.shape[3]) for b in range(blocks)]
        else:
            width, rows = g_s.shape[3] // n, each
            bodies = [
                one(0, *parts.ff(layer, b, i - 3), each, (d * blocks + b) * width, d * width, width) for d in range(n) for b in range(blocks)
            ]

        def run(some):
            for body in bodies:
                body(some)

        _rows_loop(rows, run, 16)

    remote = lambda ref, to, sent, got: pltpu.make_async_remote_copy(
        src_ref=ref, dst_ref=ref, send_sem=sent, recv_sem=got, device_id={"dp": to}, device_id_type=mesh)
    units = [(i, layer) for i in (3, 0, 1, 2, 6, 4, 5) for layer in range(layers)]
    sends, passes = [], []

    def spread(i, layer):
        rows = lands[i].shape[2]
        return (early, rows - early) if (i, layer) == (6, top) else (0, rows)

    for u, (i, layer) in enumerate(units):
        mine = lands[i].at[layer, me, pl.ds(*spread(i, layer))]
        sends.append((remote(mine, right, out_r.at[u], in_l.at[u]), remote(mine, left, out_l.at[u], in_r.at[u])))
    for u in range(len(units) + 1):
        if u < len(units):
            new_weights(*units[u])
        if u > 0:
            for c in sends[u - 1]:
                c.start()
    for other in (right, far, left):

        def theirs(rows, other=other):
            m, v = _moments(far_s[0][other, rows, :], far_s[1][other, rows, :], far_s[2][other, rows, :].astype(F32) * factor)
            lands[6][top, other, rows, :] = _stepped(lands[6][top, other, rows, :].astype(F32), m, v)

        _rows_loop(early, theirs, 16)
    for u, (i, layer) in enumerate(units):
        at, half = spread(i, layer)[0], spread(i, layer)[1] // 2
        sends[u][0].wait_recv()
        one = remote(lands[i].at[layer, left, pl.ds(at, half)], right, pass_r.at[u], far_l.at[u])
        one.start()
        sends[u][1].wait_recv()
        two = remote(lands[i].at[layer, right, pl.ds(at + half, half)], left, pass_l.at[u], far_r.at[u])
        two.start()
        passes.append((one, two))
    for u in range(len(units)):
        for c in passes[u]:
            c.wait_recv()
        for c in (*sends[u], *passes[u]):
            c.wait_send()


def finish(n, number, a, dq, dk, dv, own, w, m, v, far):
    t, d = a.shape
    each, layers = d // n, w[0].shape[0]
    anywhere = pl.BlockSpec(memory_space=pltpu.HBM)
    w = [one.reshape(layers, n, one.shape[1] // n, one.shape[2]) for one in w]
    scratch = [pltpu.VMEM((t, d), BF16)] * 4
    scratch += [pltpu.VMEM((3, n, each, d), BF16), pltpu.VMEM((3 * each, d), BF16), pltpu.VMEM((8, d), F32), pltpu.VMEM((8, 128), F32),
                pltpu.VMEM((3, 8, 128), F32)]
    scratch += [pltpu.VMEM(o.shape, o.dtype) for o in (*own, *far)] + [pltpu.SemaphoreType.DMA((3,))]
    units = 7 * layers
    sem = lambda k: pltpu.SemaphoreType.DMA((k,))
    scratch += [sem(4 + len(own)), sem(7 + layers), sem(7), sem(7), sem(3), sem(3), *[sem(units)] * 8]
    for _ in range(3):
        scratch += RingSum.scratch(n, each, d)
    return _call(
        functools.partial(_finish, n=n, layers=layers, own_count=len(own), count=n * sum(one.size for one in m)),
        (),
        [anywhere] * (4 + len(own) + 24),
        [(HERE, in_vmem(one.shape, one.dtype)) for one in (*w, *m, *v)],
        scratch,
        (a, dq, dk, dv, *own, *w, *m, *v, *far),
        6 * t * d * d,
        8 * t * d,
        collective=number,
        vmem=REST,
    )


def _settle(*refs):
    count = len(refs) // 2
    copies = [pltpu.make_async_copy(refs[i], refs[count + i], refs[-1].at[i]) for i in range(count)]
    for c in copies:
        c.start()
    for c in copies:
        c.wait()


def settle(arrays):
    there = pl.BlockSpec(memory_space=pltpu.HBM)
    return _call(
        _settle,
        (),
        [pl.BlockSpec(memory_space=pltpu.VMEM)] * len(arrays),
        [(there, jax.ShapeDtypeStruct(a.shape, a.dtype)) for a in arrays],
        [pltpu.SemaphoreType.DMA((len(arrays),))],
        [from_vmem(a) for a in arrays],
        0,
        2 * sum(a.size * a.dtype.itemsize for a in arrays),
        vmem=REST,
    )


NAMES = ("wq", "wk", "wv", "wo", "w_gate", "w_up", "w_down")


def rope_table(t):
    half = HEAD // 2
    angle = np.arange(t, dtype=np.float32)[:, None] * (np.float32(THETA) ** (-np.arange(half, dtype=np.float32) / half)).astype(np.float32)
    cos, sin = np.cos(angle.astype(np.float64)).astype(np.float32), np.sin(angle.astype(np.float64)).astype(np.float32)
    return jnp.asarray(np.concatenate([cos, sin], 1))


def solution(mesh):
    n = mesh.shape["dp"]

    def step(x, dy, *arrays):
        weights = dict(zip(NAMES, arrays[:7], strict=True))
        m, v = arrays[7:14], arrays[14:]
        layers = weights["wq"].shape[0]
        h = x[0]
        rope = rope_table(h.shape[0])
        made, a, far, by = forward(n, 0, h, weights, rope, m[6], v[6], dy[0])
        hs = [h, *(one[6] for one in made[:-1])]
        own = {}
        upper, number = None, 1
        for layer in reversed(range(layers)):
            if upper is None:
                got = mlp_back(n, number, layer, hs[layer], made[layer][3], by, weights)
            else:
                got = mlp_back(n, number, layer, made[layer][5], made[layer][3], by, weights, upper, made[layer][7:9],
                               own[layer + 1][: n - BEHIND + 1])
                own[layer + 1].append(got[-2])
                far = [*far, got[-1]]
            by, datt, delta, *left = got[:6]
            dq, dk, dv, rest = attend_back(n, number + 1, *made[layer][:3], datt, made[layer][4], delta, rope, *left)
            own[layer] = [*got[6 : 7 + n - BEHIND], rest]
            upper = hs[layer], dq, dk, dv
            number += 2
        pieces = [p for layer in range(layers) for p in own[layer]]
        out = settle(finish(n, number, a, *upper[1:], pieces, arrays[:7], m, v, far))
        return tuple(one.reshape(layers, -1, one.shape[-1]) for one in out)

    states, all_of, cut = P(("rep", "dp"), None, None), P(None, None, None), P(None, "dp", None)
    return jax.shard_map(
        step,
        mesh=mesh,
        in_specs=(states, states) + (all_of,) * 7 + (cut,) * 14,
        out_specs=(P("rep", None, None),) * 7 + (P("rep", "dp", None),) * 14,
        check_vma=False,
    )
```

```python
import functools

import jax
import jax.numpy as jnp
import numpy as np
from jax import lax
from jax.experimental import pallas as pl
from jax.experimental.pallas import tpu as pltpu
from jax.sharding import PartitionSpec as P

F32, BF16 = jnp.float32, jnp.bfloat16
HEAD = 128
THETA = 10000
NEG = -1e30
HIDDEN = 2 * NEG
LOG2E = 1.4426950408889634
SCALE = HEAD**-0.5
VMEM = 67043328
LESS = 55 * 2**20
REST = 30 * 2**20
PART = 2
BEHIND = 2


def _dot(a, b, ca=1, cb=0):
    return lax.dot_general(a, b, (((ca,), (cb,)), ((), ())), preferred_element_type=F32)


def _tile(size, most=512):
    return max(n for n in range(128, most + 1, 128) if size % n == 0)


def in_vmem(shape, dtype):
    return pltpu.VMEM(shape, dtype)


def from_vmem(a):
    return pltpu.with_memory_space_constraint(a, pltpu.VMEM)


HERE = pl.BlockSpec(memory_space=pltpu.VMEM)


def _call(kernel, grid, ins, outs, scratch, args, flops, moved, collective=None, vmem=VMEM):
    return pl.pallas_call(
        kernel,
        grid=grid,
        in_specs=[spec for spec in ins],
        out_specs=[spec for spec, _ in outs],
        out_shape=[shape for _, shape in outs],
        scratch_shapes=scratch,
        compiler_params=pltpu.CompilerParams(dimension_semantics=("arbitrary",) * len(grid), vmem_limit_bytes=vmem, collective_id=collective,
                                             has_side_effects=collective is not None),
        cost_estimate=pl.CostEstimate(flops=int(flops), transcendentals=0, bytes_accessed=int(moved)),
    )(*args)


def _norm_scale(x):
    return lax.rsqrt(jnp.mean(x * x, -1, keepdims=True) + 1e-6)


def _normed(x):
    return (x * _norm_scale(x)).astype(BF16)


def _norm_back(x, d_out):
    s = _norm_scale(x)
    inner = jnp.mean(x * d_out, -1, keepdims=True)
    return s * d_out - x * (s * s * s * inner)


def _turn(x, table, back=False):
    first = lax.broadcasted_iota(jnp.int32, table.shape, 1) < HEAD // 2
    other = pltpu.roll(table, HEAD // 2, 1)
    cos, sin = jnp.where(first, table, other), jnp.where(first, -other, table)
    sin = -sin if back else sin
    parts = [x[:, n : n + HEAD] for n in range(0, x.shape[1], HEAD)]
    return jnp.concatenate([p * cos + pltpu.roll(p, HEAD // 2, 1) * sin for p in parts], 1)


def _qkv(h, wq, wk, wv, table):
    a = _normed(h)
    q, k = (_turn(_dot(a, w).astype(BF16).astype(F32), table).astype(BF16) for w in (wq, wk))
    return a, q, k, _dot(a, wv).astype(BF16)


def _after_attention(h_ref, att_ref, wo):
    return (h_ref[...].astype(F32) + _dot(att_ref[...], wo).astype(BF16).astype(F32)).astype(BF16)


def _ring(n):
    me = lax.axis_index("dp")
    return me, lax.rem(me + 1, n), lax.rem(me + 2, n), lax.rem(me + n - 1, n)


def _greet(n):
    _, right, _, left = _ring(n)
    barrier = pltpu.get_barrier_semaphore()
    for other in (right, left):
        pl.semaphore_signal(barrier, inc=1, device_id={"dp": other}, device_id_type=pl.DeviceIdType.MESH)


def _met():
    pl.semaphore_wait(pltpu.get_barrier_semaphore(), 2)


def _rows_loop(rows, body, most=32):
    each = max(c for c in range(16, most + 1, 16) if rows % c == 0)
    lax.fori_loop(0, rows // each, lambda i, _: body(pl.ds(pl.multiple_of(i * each, each), each)), None)


def _zero(ref):
    def one(rows):
        ref[rows, :] = jnp.zeros((rows.size, ref.shape[1]), ref.dtype)

    _rows_loop(ref.shape[0], one, 64)


class RingSum:
    def __init__(self, n, block, passing, arrived, sent, got):
        self.block, self.passing, self.arrived = block, passing, arrived
        self.me, right, far, left = _ring(n)
        self.near = right, left
        half = block.shape[1] // 2
        self.half = half
        a, b = pl.ds(0, half), pl.ds(half, half)
        moves = [
            (block.at[far, a], passing.at[0], right),
            (block.at[far, b], passing.at[1], left),
            (block.at[right, b], arrived.at[0, b], right),
            (block.at[left, a], arrived.at[1, a], left),
            (passing.at[0], arrived.at[0, a], right),
            (passing.at[1], arrived.at[1, b], left),
        ]
        self.copies = [
            pltpu.make_async_remote_copy(src_ref=s, dst_ref=d, send_sem=sent.at[i], recv_sem=got.at[i], device_id={"dp": to},
                                         device_id_type=pl.DeviceIdType.MESH)
            for i, (s, d, to) in enumerate(moves)
        ]

    @staticmethod
    def scratch(n, rows, columns):
        half = pltpu.VMEM((2, rows // 2, columns), BF16)
        return [half, pltpu.VMEM((2, rows, columns), BF16), pltpu.SemaphoreType.DMA((6,)), pltpu.SemaphoreType.DMA((6,))]

    def start(self):
        for c in self.copies[:4]:
            c.start()

    def add(self):
        for c in self.copies[:2]:
            c.wait_recv()
        for i, other in enumerate(self.near):

            def one(rows, i=i, other=other):
                mine = self.block[other, pl.ds(rows.start + i * self.half, rows.size), :]
                self.passing[i, rows, :] = (self.passing[i, rows, :].astype(F32) + mine.astype(F32)).astype(BF16)

            _rows_loop(self.half, one)

    def forward(self):
        for c in self.copies[4:]:
            c.start()

    def finish(self, out, squares=None):
        for c in self.copies[2:]:
            c.wait_recv()

        def one(rows):
            total = self.block[self.me, rows, :].astype(F32) + self.arrived[0, rows, :].astype(F32) + self.arrived[1, rows, :].astype(F32)
            total = total.astype(BF16)
            out[rows, :] = total
            if squares is not None:
                _add_squares(squares, total)

        _rows_loop(self.half * 2, one)
        for c in self.copies:
            c.wait_send()


def _add_squares(squares, value):
    value = value.astype(F32)
    value = value * value
    squares[...] += sum(value[i : i + 8] for i in range(0, value.shape[0], 8))


class RingGather:
    def __init__(self, n, src, place, sent, got):
        me, right, _, left = _ring(n)
        rows = src.shape[0]
        half = rows // 2
        first, second = place(left, 0, half), place(right, half, half)
        moves = [(src, place(me, 0, rows), right), (src, place(me, 0, rows), left), (first, first, right), (second, second, left)]
        self.copies = [
            pltpu.make_async_remote_copy(src_ref=a, dst_ref=b, send_sem=sent.at[i], recv_sem=got.at[i], device_id={"dp": to},
                                         device_id_type=pl.DeviceIdType.MESH)
            for i, (a, b, to) in enumerate(moves)
        ]

    @staticmethod
    def scratch():
        return [pltpu.SemaphoreType.DMA((4,)), pltpu.SemaphoreType.DMA((4,))]

    def start(self):
        for c in self.copies[:2]:
            c.start()

    def forward(self):
        for here, there in zip(self.copies[:2], self.copies[2:], strict=True):
            here.wait_recv()
            there.start()

    def finish(self):
        for c in self.copies[2:]:
            c.wait_recv()
        for c in self.copies:
            c.wait_send()


def _seen(keys, queries):
    return lax.broadcasted_iota(jnp.int32, (keys, queries), 1) >= lax.broadcasted_iota(jnp.int32, (keys, queries), 0)


def diagonal(block, first, size, part=256):
    part = min(part, size)
    for at in range(0, size, part):
        block(first + at, part, at, True)


def _attend(iq, q_ref, k_ref, v_ref, o_ref, lse_ref, top_s, mix_s, bk):
    bq = q_ref.shape[0]
    heads = q_ref.shape[1] // HEAD
    e = SCALE * LOG2E
    top_s[...] = jnp.full(top_s.shape, NEG, F32)
    mix_s[...] = jnp.zeros(mix_s.shape, F32)

    def block(first, keys, at, masked):
        here, ask = pl.ds(pl.multiple_of(first, keys), keys), slice(at, bq)
        cols = [slice(n * HEAD, (n + 1) * HEAD) for n in range(heads)]
        scores = [_dot(k_ref[here, c], q_ref[ask, c], 1, 1) for c in cols]
        weights, keeps = [], []
        seen = _seen(keys, bq - at) if masked else None
        for n, s in enumerate(scores):
            if masked:
                s = jnp.where(seen, s, HIDDEN)
            old = top_s[n : n + 1, ask]
            top = jnp.maximum(old, s.max(axis=0, keepdims=True))
            top_s[n : n + 1, ask] = top
            weights.append(jnp.exp2((s - top) * e).astype(BF16))
            keeps.append(jnp.exp2((old - top) * e))
        ones = jnp.ones((8, keys), BF16)
        for n, (c, p, keep) in enumerate(zip(cols, weights, keeps)):
            values = jnp.concatenate([v_ref[here, c].T, ones], axis=0)
            mix_s[n, :, ask] = mix_s[n, :, ask] * keep + _dot(values, p, 1, 0)

    lax.fori_loop(0, iq * (bq // bk), lambda j, _: block(j * bk, bk, 0, False), None)
    diagonal(block, iq * bq, bq)
    for n in range(heads):
        total = mix_s[n, HEAD : HEAD + 1, :]
        o_ref[:, n * HEAD : (n + 1) * HEAD] = (mix_s[n, :HEAD, :] * (1 / total)).T.astype(BF16)
        lse_ref[n : n + 1, :] = top_s[n : n + 1, :] * e + jnp.log2(total)


def _forward(h_ref, wq, wk, wv, wo, wg_ref, wu_ref, wd_ref, table, m_ref, v_ref, dy_ref, *refs, n, layers):
    at = 9 * layers - 4
    outs, (a_ref, m_all, v_all), handed, scratch = refs[:at], refs[at : at + 3], refs[at + 3 : at + 7], refs[at + 7 :]
    k_s, v_s, wg, wu, wd, gate_s, up_s, top_s, mix_s, w_sem, out_sem, hand_sem, *sems = scratch
    early = m_all.shape[1]
    gathers = [
        RingGather(n, a.at[layers - 1, pl.ds(0, early)], lambda d, at, rows, b=b: b.at[d, pl.ds(at, rows)], *sems[2 * i : 2 * i + 2])
        for i, (a, b) in enumerate(((m_ref, m_all), (v_ref, v_all)))
    ]
    step = pl.program_id(0)
    bt = h_ref.shape[0]
    rows = pl.ds(pl.multiple_of(step * bt, bt), bt)
    loads = [pltpu.make_async_copy(a.at[0], b.at[0], w_sem.at[i]) for i, (a, b) in enumerate(((wg_ref, wg), (wu_ref, wu), (wd_ref, wd)))]

    sources = (dy_ref, *(a.at[pl.ds(layers - 1, 1)] for a in (wg_ref, wu_ref, wd_ref)))
    hands = [pltpu.make_async_copy(a, b, hand_sem.at[i]) for i, (a, b) in enumerate(zip(sources, handed, strict=True))]

    @pl.when(step == 0)
    def _():
        _greet(n)
        for load in loads:
            load.start()

    @pl.when(step == pl.num_programs(0) - 1)
    def _():
        for c in hands:
            c.start()

    for layer in range(layers):
        q_ref, k_ref, v_ref, att_ref, lse_ref = outs[9 * layer : 9 * layer + 5]
        a, q_ref[...], k, v = _qkv(h_ref[...].astype(F32), wq[layer], wk[layer], wv[layer], table[...])
        if layer == 0:
            a_ref[...] = a
        k_ref[...] = k_s[layer, rows, :] = k
        v_ref[...] = v_s[layer, rows, :] = v
        _attend(step, q_ref, k_s.at[layer], v_s.at[layer], att_ref, lse_ref, top_s, mix_s, bt)
        if layer == layers - 1:
            break
        if layer == 0:

            @pl.when(step == 0)
            def _():
                _met()
                for g in gathers:
                    g.start()

            @pl.when(step == pl.num_programs(0) - 2)
            def _():
                gathers[0].forward()

        h1_ref, y_ref, gate_ref, up_ref = outs[9 * layer + 5 : 9 * layer + 9]
        stores = [
            pltpu.make_async_copy(a.at[j], b.at[j, rows], out_sem.at[layer, i, j])
            for i, (a, b) in enumerate(((gate_s, gate_ref), (up_s, up_ref)))
            for j in range(n)
        ]

        @pl.when(step == 0)
        def _(layer=layer):
            for load in loads:
                load.wait()

        @pl.when(step > 0)
        def _(stores=stores):
            for c in stores:
                c.wait()

        h1 = _after_attention(h_ref, att_ref, wo[layer])
        h1_ref[...] = h1
        h1 = h1.astype(F32)
        b = (h1 * _norm_scale(h1)).astype(BF16)
        total = jnp.zeros(h1.shape, F32)
        for j in range(n):
            gate, up = _dot(b, _strips(wg, j, n, n, 2)), _dot(b, _strips(wu, j, n, n, 2))
            gate_s[j] = gate
            up_s[j] = up
            total += _dot((gate * jax.nn.sigmoid(gate) * up).astype(BF16), _strips(wd, j, n, n, 1))
        for c in stores:
            c.start()
        y_ref[...] = (h1 + total.astype(BF16).astype(F32)).astype(BF16)
        h_ref = y_ref

        @pl.when(step == pl.num_programs(0) - 1)
        def _(stores=stores):
            for c in stores:
                c.wait()

    @pl.when(step == pl.num_programs(0) - 2)
    def _():
        gathers[1].forward()

    @pl.when(step == pl.num_programs(0) - 1)
    def _():
        for g in gathers:
            g.finish()
        for c in hands:
            c.wait()


def anywhere_spec():
    return pl.BlockSpec(memory_space=pltpu.HBM)


def early_rows(n, d):
    return (n - BEHIND + 1) * (d // n)


def forward(n, number, h, weights, rope, m, v, dy):
    t, d = h.shape
    layers, _, ff = weights["w_gate"].shape
    assert layers == 2
    many = (anywhere_spec(), jax.ShapeDtypeStruct((n, early_rows(n, d), d), F32))
    heads = weights["wq"].shape[2] // HEAD
    bt = _tile(t)
    tile, table = (pl.BlockSpec((bt, w), lambda s: (s, 0)) for w in (d, HEAD))
    square = pl.BlockSpec((layers, d, d), lambda s: (0, 0, 0), pipeline_mode=pl.Buffered(1))
    anywhere = pl.BlockSpec(memory_space=pltpu.HBM)
    one = (tile, jax.ShapeDtypeStruct((t, d), BF16))
    two = (anywhere, jax.ShapeDtypeStruct((n, t, ff // n), F32))
    stats = (pl.BlockSpec((heads, bt), lambda s: (0, s)), jax.ShapeDtypeStruct((heads, t), F32))
    upper = [*[one] * 4, stats]
    got = _call(
        functools.partial(_forward, n=n, layers=layers),
        (t // bt,),
        [tile, *[square] * 4, *[anywhere] * 3, table, *[anywhere] * 3],
        [*[*upper, one, one, two, two] * (layers - 1), *upper, one, many, many,
         *((HERE, in_vmem(s, BF16)) for s in ((t, d), (1, d, ff), (1, d, ff), (1, ff, d)))],
        [pltpu.VMEM((layers, t, d), BF16)] * 2
        + [pltpu.VMEM((1, d, ff), BF16)] * 2
        + [pltpu.VMEM((1, ff, d), BF16)]
        + [pltpu.VMEM((n, bt, ff // n), F32)] * 2
        + [pltpu.VMEM((heads, bt), F32), pltpu.VMEM((heads, HEAD + 8, bt), F32), pltpu.SemaphoreType.DMA((3,)),
           pltpu.SemaphoreType.DMA((layers, 2, n)), pltpu.SemaphoreType.DMA((4,)), *RingGather.scratch(), *RingGather.scratch()],
        (h, *(weights[name] for name in ("wq", "wk", "wv", "wo")), *(weights[name] for name in ("w_gate", "w_up", "w_down")), rope, m, v, dy),
        2 * t * d * (8 * d + 3 * ff) + 4 * t * t * d,
        30 * t * d + 8 * t * ff,
        collective=number,
        vmem=LESS,
    )
    return [got[9 * layer : 9 * layer + 9] for layer in range(layers - 1)] + [got[9 * layers - 9 : -7]], got[-7], got[-6:-4], got[-4:]


def _attend_back(q_ref, k_ref, v_ref, do_ref, lse_ref, delta_ref, table, part_ref, ff_ref, o_ref, dq_ref, dk_ref, dv_ref, own_ref, dq_s, dk_s, dv_s, block_s, load_sem,
                 *ring, bk, n):
    iq = pl.program_id(0)
    bq = q_ref.shape[0]
    heads = q_ref.shape[1] // HEAD
    e = SCALE * LOG2E
    steps = pl.num_programs(0)
    loads, at = [], 0
    for i, source in enumerate((part_ref, *(ff_ref.at[i] for i in range(ff_ref.shape[0])), o_ref)):
        loads.append(pltpu.make_async_copy(source, block_s.at[:, pl.ds(at, source.shape[1])], load_sem.at[i]))
        at += source.shape[1]
    job = RingSum(n, block_s, *ring)

    @pl.when(iq == 0)
    def _():
        _greet(n)
        for load in loads:
            load.start()
        _zero(dk_s)
        _zero(dv_s)

    @pl.when(iq == 1)
    def _():
        for load in loads:
            load.wait()
        _met()
        job.start()

    @pl.when(iq == steps - 1)
    def _():
        job.forward()

    dq_s[...] = jnp.zeros_like(dq_s)

    def block(first, keys, at, masked):
        here, ask = pl.ds(pl.multiple_of(first, keys), keys), slice(at, bq)
        cols = [slice(i * HEAD, (i + 1) * HEAD) for i in range(heads)]
        scores = [_dot(k_ref[here, c], q_ref[ask, c], 1, 1) for c in cols]
        dps = [_dot(v_ref[here, c], do_ref[ask, c], 1, 1) for c in cols]
        seen = _seen(keys, bq - at) if masked else None
        for i, c in enumerate(cols):
            p = jnp.exp2(scores[i] * e - lse_ref[i : i + 1, ask])
            if masked:
                p = jnp.where(seen, p, 0.0)
            ds = (p * (dps[i] - delta_ref[i : i + 1, ask])).astype(BF16)
            dv_s[here, c] += _dot(p.astype(BF16), do_ref[ask, c], 1, 0)
            dk_s[here, c] += _dot(ds, q_ref[ask, c], 1, 0)
            dq_s[i, :, ask] += _dot(k_ref[here, c].T, ds, 1, 0)

    lax.fori_loop(0, iq * (bq // bk), lambda j, _: block(j * bk, bk, 0, False), None)
    diagonal(block, iq * bq, bq)

    @pl.when(iq == steps - 2)
    def _():
        job.add()

    def back(d, rows):
        return _turn(d.astype(BF16).astype(F32), table[rows, :], back=True).astype(BF16)

    mine = pl.ds(pl.multiple_of(iq * bq, bq), bq)
    dq_ref[...] = back(jnp.concatenate([(dq_s[i] * SCALE).T for i in range(heads)], 1), mine)

    @pl.when(iq == steps - 1)
    def _():
        def one(rows):
            dk_ref[rows, :] = back(dk_s[rows, :] * SCALE, rows)
            dv_ref[rows, :] = dv_s[rows, :].astype(BF16)

        _rows_loop(dk_ref.shape[0], one, 256)
        job.finish(own_ref)


def attend_back(n, number, q, k, v, d_out, lse, delta, rope, part, ff, o):
    t, width = q.shape
    heads = width // HEAD
    bq = bk = _tile(t)
    rows, whole = pl.BlockSpec((bq, width), lambda i: (i, 0)), pl.BlockSpec((t, width), lambda i: (0, 0))
    stats = pl.BlockSpec((heads, bq), lambda i: (0, i))
    table = pl.BlockSpec((t, HEAD), lambda i: (0, 0), pipeline_mode=pl.Buffered(1))
    one = jax.ShapeDtypeStruct((t, width), BF16)
    height, columns = part.shape[1] + ff.shape[0] * ff.shape[2] + o.shape[1], ff.shape[3]
    return _call(
        functools.partial(_attend_back, bk=bk, n=n),
        (t // bq,),
        [rows, whole, whole, rows, stats, stats, table, *[pl.BlockSpec(memory_space=pltpu.HBM)] * 3],
        [(rows, one), (whole, one), (whole, one),
         (pl.BlockSpec((height, columns), lambda i: (0, 0)), jax.ShapeDtypeStruct((height, columns), BF16))],
        [pltpu.VMEM((heads, HEAD, bq), F32), pltpu.VMEM((t, width), F32), pltpu.VMEM((t, width), F32),
         pltpu.VMEM((n, height, columns), BF16), pltpu.SemaphoreType.DMA((ff.shape[0] + 2,)),
         *RingSum.scratch(n, height, columns)],
        (q, k, v, d_out, lse, delta, rope, part, ff, o),
        5 * t * t * width,
        14 * t * width,
        collective=number,
    )


def _strips(ref, block, n, blocks, axis):
    width = ref.shape[axis] // (n * blocks)
    at = [pl.ds(pl.multiple_of((d * blocks + block) * width, width), width) for d in range(n)]
    return jnp.concatenate([ref[0, :, a] if axis == 2 else ref[0, a, :] for a in at], axis - 1)


def _qkv_back(h, dq, dk, dv, wq, wk, wv, sums):
    a = (h * _norm_scale(h)).astype(BF16)
    for s, d in zip(sums, (dq, dk, dv), strict=True):
        s[...] += _dot(a, d, 0, 0)
    return _dot(jnp.concatenate([dq, dk, dv], 1), jnp.concatenate([wq, wk, wv], 1), 1, 1)


def _cut(ref, at, value):
    n = ref.shape[0]
    each = value.shape[0] // n
    for d in range(n):
        ref[d, at : at + each] = value[d * each : (d + 1) * each].astype(BF16)


def _mlp_back(*refs, n, layer, tiles, blocks, behind, last):
    take = iter(range(len(refs)))
    some = lambda count: [refs[next(take)] for _ in range(count)]
    h_ref, att_ref = some(2)
    if not last:
        hn_ref, dq_ref, dk_ref, dv_ref, dh_ref, wq, wk, wv, gate_ref, up_ref = some(10)
        sums_in = some(blocks - behind + 1)
    wo, *from_refs = some(1 if last else 4)
    if last:
        dy_s, wg, wu, wd = some(4)
    dh1_ref, datt_ref, delta_ref, left_part, left_ff, left_o = some(6)
    hosted = blocks - behind
    own = some(hosted + 1 + (not last))
    g_all = None if last else some(1)[0]
    h1_s = some(1)[0] if last else None
    b_s, p_s, dg_s, du_s, sum_b, g_s, go_s, out_sem = some(8)
    if not last:
        dy_s, wg, wu, wd, w_sem = some(5)
    sums3 = some(1 if last else 3)
    sum_o = sums3[0]
    jobs = []
    for i in range(len(own)):
        if i < hosted:
            block = g_s.at[i]
        elif i == hosted:
            block = g_s.at[i, :, pl.ds(0, own[i].shape[0])]
        else:
            block = gqkv_s = g_s.at[blocks - 1]
        jobs.append(RingSum(n, block, *some(4)))
    gathers = []
    if not last:
        for i, source in enumerate(sums_in):
            each = own[hosted].shape[0] // PART
            gathers.append(RingGather(n, source.at[pl.ds(0, each)], lambda d, at, rows, i=i: g_all.at[d, pl.ds(i * each + at, rows)], *some(2)))
    step = pl.program_id(0)
    bt = h_ref.shape[0]
    middle = tiles * blocks
    r = jnp.where(step < tiles, step, lax.rem(step - tiles, tiles))
    j = lax.div(step - tiles, tiles)
    rows = pl.ds(pl.multiple_of(r * bt, bt), bt)
    @pl.when(step == 0)
    def _():
        _greet(n)
        for s in sums3:
            _zero(s)

    loads = [] if last else [pltpu.make_async_copy(a.at[layer], b.at[0], w_sem.at[i]) for i, (a, b) in enumerate(zip(from_refs, (wg, wu, wd)))]

    @pl.when(step == 0)
    def _():
        for load in loads:
            load.start()

    @pl.when(step == tiles)
    def _():
        for load in loads:
            load.wait()

    final = 2 * tiles + middle - 1
    times = [(at, min(at + tiles * 3 // 2, tiles + middle)) for at in (tiles * (2 + i) for i in range(hosted + 1))] + [(tiles, 2 * tiles)] * (not last)
    times = [(start, forward - 1, forward, min(forward + tiles * 3 // 2, final)) for start, forward in times]

    @pl.when(step == (min(t[0] for t in times) if last else 1))
    def _():
        _met()
        for g in gathers:
            g.start()

    @pl.when(step == tiles)
    def _():
        for g in gathers:
            g.forward()

    for job, (_, _, at, _) in zip(jobs, times, strict=True):

        @pl.when(step == at)
        def _(job=job):
            job.forward()

    for job, (at, _, _, _) in zip(jobs, times, strict=True):

        @pl.when(step == at)
        def _(job=job):
            job.start()

    @pl.when(step < tiles)
    def _():
        if last:
            h1 = _after_attention(h_ref, att_ref, wo[0])
            h1_s[rows, :] = h1
        else:
            h1 = h_ref[...]
            hn = hn_ref[...].astype(F32)
            da = _qkv_back(hn, dq_ref[...], dk_ref[...], dv_ref[...], wq[0], wk[0], wv[0], sums3)
            dy_s[rows, :] = (dh_ref[...].astype(F32) + _norm_back(hn, da.astype(BF16).astype(F32)).astype(BF16).astype(F32)).astype(BF16)

            @pl.when(step == tiles - 1)
            def _():
                for i, s in enumerate(sums3):
                    _cut(gqkv_s, i * (s.shape[0] // n), s[...])
                _zero(sum_o)

        h1 = h1.astype(F32)
        b_s[rows, :] = (h1 * _norm_scale(h1)).astype(BF16)
        sum_b[rows, :] = jnp.zeros((bt, sum_b.shape[1]), F32)

    @pl.when((step >= tiles) & (step < tiles + middle))
    def _():
        b, dy = b_s[rows, :], dy_s[rows, :]
        gate_w, up_w, down_w = _strips(wg, j, n, blocks, 2), _strips(wu, j, n, blocks, 2), _strips(wd, j, n, blocks, 1)
        terms = []
        for at in range(0, gate_w.shape[1], 256):
            c = slice(at, at + 256)
            gate, up = (_dot(b, gate_w[:, c]), _dot(b, up_w[:, c])) if last else (gate_ref[0, :, c], up_ref[0, :, c])
            dp = _dot(dy, down_w[c], 1, 1).astype(BF16).astype(F32)
            sg = jax.nn.sigmoid(gate)
            silu = gate * sg
            p_s[rows, c] = (silu * up).astype(BF16)
            du = (dp * silu).astype(BF16)
            dg = (dp * up * (sg + silu * (1 - sg))).astype(BF16)
            du_s[rows, c] = du
            dg_s[rows, c] = dg
            terms.append((dg, du))
        sum_b[rows, :] += _dot(jnp.concatenate([g for g, _ in terms] + [u for _, u in terms], 1), jnp.concatenate([gate_w, up_w], 1), 1, 1)

        @pl.when(r == tiles - 1)
        def _():
            each = b.shape[1] // n
            mine = g_s.at[j]
            _cut(mine, 0, _dot(p_s[...], dy_s[...], 0, 0))
            _cut(mine, mine.shape[1] - 2 * each, _dot(b_s[...], dg_s[...], 0, 0))
            _cut(mine, mine.shape[1] - each, _dot(b_s[...], du_s[...], 0, 0))

    part = own[hosted].shape[0]
    out_copies = [pltpu.make_async_copy(g_s.at[hosted, :, pl.ds(part, left_part.shape[1])], left_part, out_sem.at[0])]
    out_copies += [pltpu.make_async_copy(g_s.at[hosted + i], left_ff.at[i - 1], out_sem.at[i]) for i in range(1, behind)]
    out_copies.append(pltpu.make_async_copy(go_s, left_o, out_sem.at[behind]))

    @pl.when(step >= tiles + middle)
    def _():
        db = sum_b[rows, :]
        h1 = h1_s[rows, :] if last else h_ref[...]
        dh1 = dy_s[rows, :].astype(F32) + _norm_back(h1.astype(F32), db.astype(BF16).astype(F32)).astype(BF16).astype(F32)
        dh1 = dh1.astype(BF16)
        dh1_ref[...] = dh1
        datt = _dot(dh1, wo[0], 1, 1).astype(BF16)
        datt_ref[...] = datt
        att = att_ref[...]
        both = att.astype(F32) * datt.astype(F32)
        for i in range(both.shape[1] // HEAD):
            delta_ref[i : i + 1, :] = both[:, i * HEAD : (i + 1) * HEAD].T.sum(axis=0, keepdims=True)
        sum_o[...] += _dot(att, dh1, 0, 0)

        @pl.when(step == tiles + middle)
        def _():
            for c in out_copies[:-1]:
                c.start()

        @pl.when(step == 2 * tiles + middle - 1)
        def _():
            _cut(go_s, 0, sum_o[...])
            out_copies[-1].start()
            for c in out_copies:
                c.wait()

    for job, (_, at, _, _) in zip(jobs, times, strict=True):

        @pl.when(step == at)
        def _(job=job):
            job.add()

    @pl.when(step == final)
    def _():
        for g in gathers:
            g.finish()

    for job, (_, _, _, at), out in zip(jobs, times, own, strict=True):

        @pl.when(step == at)
        def _(job=job, out=out):
            job.finish(out)


def mlp_back(n, number, layer, h, att, by, weights, upper=None, hidden=None, sums=None):
    t, d = h.shape
    ff = weights["w_gate"].shape[2]
    bt = _tile(t)
    tiles, blocks = t // bt, n
    fb, each = ff // blocks, d // n
    down = fb // n
    height = down + 2 * each
    assert n == 4 and fb == d and height == 3 * each
    heads = att.shape[1] // HEAD
    middle = tiles * blocks
    r = lambda s: jnp.where(s < tiles, s, lax.rem(s - tiles, tiles))
    j = lambda s: jnp.clip(lax.div(s - tiles, tiles), 0, blocks - 1)
    edge = lambda s: jnp.where(s < tiles, s, jnp.where(s < tiles + middle, tiles - 1, s - tiles - middle))
    before = lambda s: jnp.minimum(s, tiles - 1)
    after = lambda s: jnp.maximum(s - tiles - middle, 0)
    tile = lambda f, w=d: pl.BlockSpec((bt, w), lambda s: (f(s), 0))
    fixed = lambda which, *shape: pl.BlockSpec((1, *shape), lambda s: (which, 0, 0), pipeline_mode=pl.Buffered(1))
    square, up_square = fixed(layer, d, d), fixed(layer + 1, d, d)
    anywhere = pl.BlockSpec(memory_space=pltpu.HBM)
    mlp = [square, anywhere, anywhere, anywhere]
    w4 = [weights[name] for name in ("wo", "w_gate", "w_up", "w_down")]
    last = upper is None
    if last:
        ins = [tile(before), tile(edge), square, *[HERE] * 4]
        args = [h, att, w4[0], *(from_vmem(a) for a in by)]
    else:
        hn, dq, dk, dv = upper
        block = pl.BlockSpec((1, bt, fb), lambda s: (j(s), r(jnp.clip(s, tiles, tiles + middle - 1)), 0))
        ins = [tile(edge), tile(after), *[tile(before)] * 5, up_square, up_square, up_square, block, block, *[anywhere] * len(sums), *mlp]
        args = [h, att, hn, dq, dk, dv, by, weights["wq"], weights["wk"], weights["wv"], *hidden, *sums, *w4]
    anywhere = pl.BlockSpec(memory_space=pltpu.HBM)
    outs = [
        (tile(after), jax.ShapeDtypeStruct((t, d), BF16)),
        (tile(after), jax.ShapeDtypeStruct((t, d), BF16)),
        (pl.BlockSpec((heads, bt), lambda s: (0, after(s))), jax.ShapeDtypeStruct((heads, t), F32)),
        (anywhere, jax.ShapeDtypeStruct((n, height - PART * each, d), BF16)),
        (anywhere, jax.ShapeDtypeStruct((BEHIND - 1, n, height, d), BF16)),
        (anywhere, jax.ShapeDtypeStruct((n, each, d), BF16)),
        *[(pl.BlockSpec((height, d), lambda s: (0, 0)), jax.ShapeDtypeStruct((height, d), BF16))] * (blocks - BEHIND),
        (pl.BlockSpec((PART * each, d), lambda s: (0, 0)), jax.ShapeDtypeStruct((PART * each, d), BF16)),
    ]
    scratch = [pltpu.VMEM((t, d), BF16)] * (1 + last) + [pltpu.VMEM((t, fb), BF16)] * 3 + [pltpu.VMEM((t, d), F32)]
    scratch += [pltpu.VMEM((blocks, n, height, d), BF16), pltpu.VMEM((n, each, d), BF16), pltpu.SemaphoreType.DMA((BEHIND + 1,))]
    if not last:
        scratch += [pltpu.VMEM((t, d), BF16)] + [pltpu.VMEM((1, d, ff), BF16)] * 2 + [pltpu.VMEM((1, ff, d), BF16), pltpu.SemaphoreType.DMA((3,))]
    scratch += [pltpu.VMEM((d, d), F32)] * (1 if last else 3)
    for _ in range(blocks - BEHIND):
        scratch += RingSum.scratch(n, height, d)
    scratch += RingSum.scratch(n, PART * each, d)
    if not last:
        outs += [(pl.BlockSpec((3 * each, d), lambda s: (0, 0)), jax.ShapeDtypeStruct((3 * each, d), BF16))]
        outs += [(anywhere, jax.ShapeDtypeStruct((n, early_rows(n, d), d), BF16))]
        scratch += RingSum.scratch(n, 3 * each, d)
        for _ in sums:
            scratch += RingGather.scratch()
    return _call(
        functools.partial(_mlp_back, n=n, layer=layer, tiles=tiles, blocks=blocks, behind=BEHIND, last=last),
        (2 * tiles + middle,),
        ins,
        outs,
        scratch,
        args,
        2 * t * d * (ff * 8 + d * 4),
        sum(a.size * a.dtype.itemsize for a in args),
        collective=number,
        vmem=LESS if last else VMEM,
    )


class Parts:
    def __init__(self, n, each):
        self.hosted, self.per, self.each = n - BEHIND, n - BEHIND + 3, each

    def ff(self, layer, block, which):
        at = layer * self.per + self.hosted
        if block < self.hosted:
            return at - self.hosted + block, which * self.each
        entry = (block - self.hosted) * 3 + which
        return (at, entry * self.each) if entry < PART else (at + 1, (entry - PART) * self.each)

    def square(self, layer, which):
        at = layer * self.per + self.hosted
        return (at + 1, (BEHIND * 3 - PART) * self.each) if which == 3 else (at + 2, which * self.each)


def _moments(m, v, g):
    return 0.9 * m + 0.1 * g, 0.95 * v + 0.05 * g * g


def _stepped(w, m, v):
    return (w - 0.02 * (m * lax.rsqrt(v + 1e-8) + 0.1 * w)).astype(BF16)


def _finish(*refs, n, layers, own_count, count):
    take = iter(range(len(refs)))
    some = lambda k: [refs[next(take)] for _ in range(k)]
    a_ref, dq_ref, dk_ref, dv_ref = some(4)
    own_in, w_ref, m_ref, v_ref, far_in = some(own_count), some(7), some(7), some(7), some(3)
    lands, m_s, v_s = some(7), some(7), some(7)
    a_s, dq_s, dk_s, dv_s, g_s, own_ref, squares, total_s, others_s = some(9)
    pieces_s, far_s, far_sem = some(own_count), some(3), some(1)[0]
    load_sem, w_sem, m_sem, v_sem, swap_out, swap_in, out_r, out_l, in_l, in_r, pass_r, pass_l, far_l, far_r = some(14)
    jobs = [RingSum(n, g_s.at[i], *some(4)) for i in range(3)]
    me, right, far, left = _ring(n)
    mesh = pl.DeviceIdType.MESH
    barrier = pltpu.get_barrier_semaphore()
    for other in (right, far, left):
        pl.semaphore_signal(barrier, inc=1, device_id={"dp": other}, device_id_type=mesh)
    pairs = [(a_ref, a_s), (dv_ref, dv_s), (dk_ref, dk_s), (dq_ref, dq_s), *zip(own_in, pieces_s, strict=True)]
    loads = [pltpu.make_async_copy(s, d, load_sem.at[i]) for i, (s, d) in enumerate(pairs)]
    for load in loads:
        load.start()
    top, early = layers - 1, far_s[0].shape[1]
    late = pl.ds(early, lands[6].shape[2] - early)
    pairs = [(w_ref[i].at[:, me], lands[i].at[:, me]) for i in range(6)] + [(w_ref[6].at[i, me], lands[6].at[i, me]) for i in range(top)]
    pairs += [(w_ref[6].at[top, me, late], lands[6].at[top, me, late])]
    pairs += [(w_ref[6].at[top, :, pl.ds(0, early)], lands[6].at[top, :, pl.ds(0, early)])]
    state = [pltpu.make_async_copy(a, b, w_sem.at[i]) for i, (a, b) in enumerate(pairs)]
    for i in range(7):
        state.append(pltpu.make_async_copy(m_ref[i], m_s[i], m_sem.at[i]))
        state.append(pltpu.make_async_copy(v_ref[i], v_s[i], v_sem.at[i]))
    state += [pltpu.make_async_copy(a, b, far_sem.at[i]) for i, (a, b) in enumerate(zip(far_in, far_s, strict=True))]
    each = g_s.shape[2]
    squares[...] = jnp.zeros_like(squares)
    for load in loads[:2]:
        load.wait()
    _cut(g_s.at[2], 0, _dot(a_s[...], dv_s[...], 0, 0))
    pl.semaphore_wait(barrier, 3)
    loads[2].wait()
    jobs[2].start()
    for c in state:
        c.start()
    _cut(g_s.at[1], 0, _dot(a_s[...], dk_s[...], 0, 0))
    loads[3].wait()
    jobs[1].start()
    jobs[2].add()
    _cut(g_s.at[0], 0, _dot(a_s[...], dq_s[...], 0, 0))
    jobs[2].forward()
    jobs[1].add()
    jobs[0].start()
    jobs[1].forward()
    for i, piece in enumerate(pieces_s):
        if i == len(pieces_s) // 2:
            jobs[0].add()
        loads[4 + i].wait()
        _rows_loop(piece.shape[0], lambda rows, piece=piece: _add_squares(squares, piece[rows, :]))
        if i == len(pieces_s) // 2:
            jobs[0].forward()
    jobs[2].finish(own_ref.at[pl.ds(2 * each, each)], squares)
    jobs[1].finish(own_ref.at[pl.ds(each, each)], squares)
    jobs[0].finish(own_ref.at[pl.ds(0, each)], squares)
    total_s[...] = sum(squares[:, i : i + 128] for i in range(0, squares.shape[1], 128))
    swaps = [
        pltpu.make_async_remote_copy(src_ref=total_s, dst_ref=others_s.at[i], send_sem=swap_out.at[i], recv_sem=swap_in.at[i], device_id={"dp": other},
                                     device_id_type=mesh)
        for i, other in enumerate((right, far, left))
    ]
    for c in state:
        c.wait()
    for s in swaps:
        s.start()
    for s in swaps:
        s.wait()
    everything = jnp.sum(total_s[...] + others_s[0] + others_s[1] + others_s[2], keepdims=True)
    factor = jnp.minimum(1.0, 0.5 * lax.rsqrt(everything / count + 1e-30))

    parts = Parts(n, each)
    grads = [*pieces_s[: parts.per - 1], own_ref, *pieces_s[parts.per - 1 :]]
    blocks = n

    def new_weights(i, layer):
        land, m_i, v_i = lands[i], m_s[i], v_s[i]

        def one(at, piece, row, rows, column, g_column, width):
            def body(some):
                here = pl.ds(at + some.start, some.size)
                g = grads[piece][pl.ds(row + some.start, some.size), g_column : g_column + width].astype(F32) * factor
                m, v = _moments(m_i[layer, here, column : column + width], v_i[layer, here, column : column + width], g)
                m_i[layer, here, column : column + width] = m
                v_i[layer, here, column : column + width] = v
                w = land[layer, me, here, column : column + width].astype(F32)
                land[layer, me, here, column : column + width] = _stepped(w, m, v)

            return body

        if i < 4:
            bodies, rows = [one(0, *parts.square(layer, i), each, 0, 0, land.shape[3])], each
        elif i == 6:
            rows = each
            bodies = [one(b * each, *parts.ff(layer, b, 0), each, 0, 0, land.shape[3]) for b in range(blocks)]
        else:
            width, rows = g_s.shape[3] // n, each
            bodies = [
                one(0, *parts.ff(layer, b, i - 3), each, (d * blocks + b) * width, d * width, width) for d in range(n) for b in range(blocks)
            ]

        def run(some):
            for body in bodies:
                body(some)

        _rows_loop(rows, run, 16)

    remote = lambda ref, to, sent, got: pltpu.make_async_remote_copy(
        src_ref=ref, dst_ref=ref, send_sem=sent, recv_sem=got, device_id={"dp": to}, device_id_type=mesh)
    units = [(i, layer) for i in (3, 0, 1, 2, 6, 4, 5) for layer in range(layers)]
    sends, passes = [], []

    def spread(i, layer):
        rows = lands[i].shape[2]
        return (early, rows - early) if (i, layer) == (6, top) else (0, rows)

    for u, (i, layer) in enumerate(units):
        mine = lands[i].at[layer, me, pl.ds(*spread(i, layer))]
        sends.append((remote(mine, right, out_r.at[u], in_l.at[u]), remote(mine, left, out_l.at[u], in_r.at[u])))
    for u in range(len(units) + 1):
        if u < len(units):
            new_weights(*units[u])
        if u > 0:
            for c in sends[u - 1]:
                c.start()
    for other in (right, far, left):

        def theirs(rows, other=other):
            m, v = _moments(far_s[0][other, rows, :], far_s[1][other, rows, :], far_s[2][other, rows, :].astype(F32) * factor)
            lands[6][top, other, rows, :] = _stepped(lands[6][top, other, rows, :].astype(F32), m, v)

        _rows_loop(early, theirs, 16)
    for u, (i, layer) in enumerate(units):
        at, half = spread(i, layer)[0], spread(i, layer)[1] // 2
        sends[u][0].wait_recv()
        one = remote(lands[i].at[layer, left, pl.ds(at, half)], right, pass_r.at[u], far_l.at[u])
        one.start()
        sends[u][1].wait_recv()
        two = remote(lands[i].at[layer, right, pl.ds(at + half, half)], left, pass_l.at[u], far_r.at[u])
        two.start()
        passes.append((one, two))
    for u in range(len(units)):
        for c in passes[u]:
            c.wait_recv()
        for c in (*sends[u], *passes[u]):
            c.wait_send()


def finish(n, number, a, dq, dk, dv, own, w, m, v, far):
    t, d = a.shape
    each, layers = d // n, w[0].shape[0]
    anywhere = pl.BlockSpec(memory_space=pltpu.HBM)
    w = [one.reshape(layers, n, one.shape[1] // n, one.shape[2]) for one in w]
    scratch = [pltpu.VMEM((t, d), BF16)] * 4
    scratch += [pltpu.VMEM((3, n, each, d), BF16), pltpu.VMEM((3 * each, d), BF16), pltpu.VMEM((8, d), F32), pltpu.VMEM((8, 128), F32),
                pltpu.VMEM((3, 8, 128), F32)]
    scratch += [pltpu.VMEM(o.shape, o.dtype) for o in (*own, *far)] + [pltpu.SemaphoreType.DMA((3,))]
    units = 7 * layers
    sem = lambda k: pltpu.SemaphoreType.DMA((k,))
    scratch += [sem(4 + len(own)), sem(7 + layers), sem(7), sem(7), sem(3), sem(3), *[sem(units)] * 8]
    for _ in range(3):
        scratch += RingSum.scratch(n, each, d)
    return _call(
        functools.partial(_finish, n=n, layers=layers, own_count=len(own), count=n * sum(one.size for one in m)),
        (),
        [anywhere] * (4 + len(own) + 24),
        [(HERE, in_vmem(one.shape, one.dtype)) for one in (*w, *m, *v)],
        scratch,
        (a, dq, dk, dv, *own, *w, *m, *v, *far),
        6 * t * d * d,
        8 * t * d,
        collective=number,
        vmem=REST,
    )


def _settle(*refs):
    count = len(refs) // 2
    copies = [pltpu.make_async_copy(refs[i], refs[count + i], refs[-1].at[i]) for i in range(count)]
    for c in copies:
        c.start()
    for c in copies:
        c.wait()


def settle(arrays):
    there = pl.BlockSpec(memory_space=pltpu.HBM)
    return _call(
        _settle,
        (),
        [pl.BlockSpec(memory_space=pltpu.VMEM)] * len(arrays),
        [(there, jax.ShapeDtypeStruct(a.shape, a.dtype)) for a in arrays],
        [pltpu.SemaphoreType.DMA((len(arrays),))],
        [from_vmem(a) for a in arrays],
        0,
        2 * sum(a.size * a.dtype.itemsize for a in arrays),
        vmem=REST,
    )


NAMES = ("wq", "wk", "wv", "wo", "w_gate", "w_up", "w_down")


def rope_table(t):
    half = HEAD // 2
    angle = np.arange(t, dtype=np.float32)[:, None] * (np.float32(THETA) ** (-np.arange(half, dtype=np.float32) / half)).astype(np.float32)
    cos, sin = np.cos(angle.astype(np.float64)).astype(np.float32), np.sin(angle.astype(np.float64)).astype(np.float32)
    return jnp.asarray(np.concatenate([cos, sin], 1))


def solution(mesh):
    n = mesh.shape["dp"]

    def step(x, dy, *arrays):
        weights = dict(zip(NAMES, arrays[:7], strict=True))
        m, v = arrays[7:14], arrays[14:]
        layers = weights["wq"].shape[0]
        h = x[0]
        rope = rope_table(h.shape[0])
        made, a, far, by = forward(n, 0, h, weights, rope, m[6], v[6], dy[0])
        hs = [h, *(one[6] for one in made[:-1])]
        own = {}
        upper, number = None, 1
        for layer in reversed(range(layers)):
            if upper is None:
                got = mlp_back(n, number, layer, hs[layer], made[layer][3], by, weights)
            else:
                got = mlp_back(n, number, layer, made[layer][5], made[layer][3], by, weights, upper, made[layer][7:9],
                               own[layer + 1][: n - BEHIND + 1])
                own[layer + 1].append(got[-2])
                far = [*far, got[-1]]
            by, datt, delta, *left = got[:6]
            dq, dk, dv, rest = attend_back(n, number + 1, *made[layer][:3], datt, made[layer][4], delta, rope, *left)
            own[layer] = [*got[6 : 7 + n - BEHIND], rest]
            upper = hs[layer], dq, dk, dv
            number += 2
        pieces = [p for layer in range(layers) for p in own[layer]]
        out = settle(finish(n, number, a, *upper[1:], pieces, arrays[:7], m, v, far))
        return tuple(one.reshape(layers, -1, one.shape[-1]) for one in out)

    states, all_of, cut = P(("rep", "dp"), None, None), P(None, None, None), P(None, "dp", None)
    return jax.shard_map(
        step,
        mesh=mesh,
        in_specs=(states, states) + (all_of,) * 7 + (cut,) * 14,
        out_specs=(P("rep", None, None),) * 7 + (P("rep", "dp", None),) * 14,
        check_vma=False,
    )
```
